8 devices in a mesh: dp: 1 (over z), cp: 2 (over y), tp: 4 (over x, core).
Axes of the slice: x: 2, y: 2, z: 1, core: 2. Of those that a mesh axis runs over, the one named last changes fastest.
Arguments:
- x: bfloat16 [1, 8192, 4096], P('dp', ('cp', 'tp'))
- g_attn: bfloat16 [4096], replicated
- w_q: bfloat16 [4096, 32, 128], P(None, 'tp')
- w_k: bfloat16 [4096, 8, 128], P(None, 'tp')
- w_v: bfloat16 [4096, 8, 128], P(None, 'tp')
- w_o: bfloat16 [32, 128, 4096], P('tp')
- g_mlp: bfloat16 [4096], replicated
- w_gate: bfloat16 [4096, 12288], P(None, 'tp')
- w_up: bfloat16 [4096, 12288], P(None, 'tp')
- w_down: bfloat16 [12288, 4096], P('tp')
Outputs:
- output: bfloat16 [1, 8192, 4096], P('dp', ('cp', 'tp'))
All inputs are finite; a program needn't handle non-finite values.
Results may differ from the reference program's by a relative error of at most 0.02.
Values are sent between devices in bfloat16 or wider.
A program may use at most 1 GiB of HBM per device.

```python
import math
import jax
import jax.numpy as jnp
from jax import lax

SEQ_LEN = 8192
MODEL_DIM = 4096
N_HEADS = 32
N_KV_HEADS = 8
HEAD_DIM = 128
FFN_DIM = 12288
CP_SIZE = 2
Q_BLOCK = 128
NORM_EPS = 1e-5
ROPE_THETA = 500000.0


def stored_positions(row_ids):
    piece_len = SEQ_LEN // (2 * CP_SIZE)
    owner_cp = row_ids // (2 * piece_len)
    within = row_ids % (2 * piece_len)
    return jnp.where(within < piece_len, owner_cp * piece_len + within,
                     (2 * CP_SIZE - 1 - owner_cp) * piece_len + within - piece_len)


def rms_norm(rows_in, gain_vec):
    rows_f32 = rows_in.astype(jnp.float32)
    mean_sq = jnp.mean(rows_f32 * rows_f32, axis=-1, keepdims=True)
    return (rows_f32 * lax.rsqrt(mean_sq + NORM_EPS) * gain_vec.astype(jnp.float32)).astype(jnp.bfloat16)


def apply_rope(heads_in, positions):
    half_dim = HEAD_DIM // 2
    inv_freq = ROPE_THETA ** (-2.0 * jnp.arange(half_dim, dtype=jnp.float32) / HEAD_DIM)
    angles = positions.astype(jnp.float32)[:, None] * inv_freq[None, :]
    angles = jnp.concatenate([angles, angles], axis=-1)[:, None, :]
    heads_f32 = heads_in.astype(jnp.float32)
    rotated = jnp.concatenate([-heads_f32[..., half_dim:], heads_f32[..., :half_dim]], axis=-1)
    return (heads_f32 * jnp.cos(angles) + rotated * jnp.sin(angles)).astype(jnp.bfloat16)


def draw_weight(key_in, weight_shape, std_dev):
    return (std_dev * jax.random.normal(key_in, weight_shape, jnp.float32)).astype(jnp.bfloat16)


def setup_inputs(seed: int = 0, part: int = 0) -> dict:
    key_list = jax.random.split(jax.random.key(seed), 10)
    qk_std = math.log(SEQ_LEN / 32.0) ** 0.25 / math.sqrt(MODEL_DIM)
    x = 0.5 * jax.random.normal(jax.random.fold_in(key_list[0], part), (1, SEQ_LEN, MODEL_DIM), jnp.float32)
    return {
        'x': x.astype(jnp.bfloat16),
        'g_attn': (0.5 + jax.random.uniform(key_list[1], (MODEL_DIM,), jnp.float32)).astype(jnp.bfloat16),
        'w_q': draw_weight(key_list[2], (MODEL_DIM, N_HEADS, HEAD_DIM), qk_std),
        'w_k': draw_weight(key_list[3], (MODEL_DIM, N_KV_HEADS, HEAD_DIM), qk_std),
        'w_v': draw_weight(key_list[4], (MODEL_DIM, N_KV_HEADS, HEAD_DIM), MODEL_DIM ** -0.5),
        'w_o': draw_weight(key_list[5], (N_HEADS, HEAD_DIM, MODEL_DIM), 2.0 * (N_HEADS * HEAD_DIM) ** -0.5),
        'g_mlp': (0.5 + jax.random.uniform(key_list[6], (MODEL_DIM,), jnp.float32)).astype(jnp.bfloat16),
        'w_gate': draw_weight(key_list[7], (MODEL_DIM, FFN_DIM), MODEL_DIM ** -0.5),
        'w_up': draw_weight(key_list[8], (MODEL_DIM, FFN_DIM), MODEL_DIM ** -0.5),
        'w_down': draw_weight(key_list[9], (FFN_DIM, MODEL_DIM), FFN_DIM ** -0.5),
    }


def reference(x, g_attn, w_q, w_k, w_v, w_o, g_mlp, w_gate, w_up, w_down):
    group_size = N_HEADS // N_KV_HEADS
    n_blocks = SEQ_LEN // Q_BLOCK
    positions = stored_positions(jnp.arange(SEQ_LEN, dtype=jnp.int32))
    x_rows = x[0]
    normed = rms_norm(x_rows, g_attn)
    q_all = jnp.dot(normed, w_q.reshape(MODEL_DIM, N_HEADS * HEAD_DIM), preferred_element_type=jnp.float32).astype(jnp.bfloat16)
    k_all = jnp.dot(normed, w_k.reshape(MODEL_DIM, N_KV_HEADS * HEAD_DIM), preferred_element_type=jnp.float32).astype(jnp.bfloat16)
    v_all = jnp.dot(normed, w_v.reshape(MODEL_DIM, N_KV_HEADS * HEAD_DIM), preferred_element_type=jnp.float32).astype(jnp.bfloat16)
    q_all = apply_rope(q_all.reshape(SEQ_LEN, N_HEADS, HEAD_DIM), positions)
    k_all = apply_rope(k_all.reshape(SEQ_LEN, N_KV_HEADS, HEAD_DIM), positions).astype(jnp.float32)
    v_all = v_all.reshape(SEQ_LEN, N_KV_HEADS, HEAD_DIM).astype(jnp.float32)
    w_o_flat = w_o.reshape(N_HEADS * HEAD_DIM, MODEL_DIM)
    score_scale = HEAD_DIM ** -0.5

    def one_block(block_in):
        q_blk, pos_blk, x_blk = block_in
        q_grp = q_blk.reshape(Q_BLOCK, N_KV_HEADS, group_size, HEAD_DIM).astype(jnp.float32)
        scores = jnp.einsum('qgrd,kgd->gqrk', q_grp, k_all) * score_scale
        visible = pos_blk[None, :, None, None] >= positions[None, None, None, :]
        scores = jnp.where(visible, scores, -1e30)
        weights = jnp.exp(scores - jnp.max(scores, axis=-1, keepdims=True))
        row_sum = jnp.sum(weights, axis=-1, keepdims=True)
        mixed_vals = jnp.einsum('gqrk,kgd->gqrd', weights.astype(jnp.bfloat16).astype(jnp.float32), v_all) / row_sum
        attn_rows = jnp.transpose(mixed_vals, (1, 0, 2, 3)).astype(jnp.bfloat16).reshape(Q_BLOCK, N_HEADS * HEAD_DIM)
        attn_proj = jnp.dot(attn_rows, w_o_flat, preferred_element_type=jnp.float32).astype(jnp.bfloat16)
        resid_rows = (x_blk.astype(jnp.float32) + attn_proj.astype(jnp.float32)).astype(jnp.bfloat16)
        normed_mlp = rms_norm(resid_rows, g_mlp)
        gate_proj = jnp.dot(normed_mlp, w_gate, preferred_element_type=jnp.float32)
        up_proj = jnp.dot(normed_mlp, w_up, preferred_element_type=jnp.float32)
        hidden = (jax.nn.silu(gate_proj) * up_proj).astype(jnp.bfloat16)
        down_proj = jnp.dot(hidden, w_down, preferred_element_type=jnp.float32).astype(jnp.bfloat16)
        return (resid_rows.astype(jnp.float32) + down_proj.astype(jnp.float32)).astype(jnp.bfloat16)

    blocks = lax.map(one_block, (q_all.reshape(n_blocks, Q_BLOCK, N_HEADS, HEAD_DIM),
                                 positions.reshape(n_blocks, Q_BLOCK),
                                 x_rows.reshape(n_blocks, Q_BLOCK, MODEL_DIM)))
    return blocks.reshape(1, SEQ_LEN, MODEL_DIM)
```

```python
import functools
import math
import jax
import jax.numpy as jnp
from jax import lax
from jax.experimental import pallas as pl
from jax.experimental.pallas import tpu as pltpu
from jax.sharding import PartitionSpec as P

NORM_EPS = 1e-5
ROPE_THETA = 500000.0
HD = 128
NEG = -1e30
LOG2E = math.log2(math.e)
DN = (((1,), (0,)), ((), ()))
MIB = 1 << 20


def rms_norm(rows_in, gain_vec):
    rows_f32 = rows_in.astype(jnp.float32)
    mean_sq = jnp.mean(rows_f32 * rows_f32, axis=-1, keepdims=True)
    return (rows_f32 * lax.rsqrt(mean_sq + NORM_EPS) * gain_vec.astype(jnp.float32)).astype(jnp.bfloat16)


def rope_tables(positions):
    half = HD // 2
    inv_freq = ROPE_THETA ** (-2.0 * jnp.arange(half, dtype=jnp.float32) / HD)
    angles = positions.astype(jnp.float32)[:, None] * inv_freq[None, :]
    cos, sin = jnp.cos(angles), jnp.sin(angles)
    return jnp.concatenate([cos, cos], axis=-1), jnp.concatenate([-sin, sin], axis=-1)


def stored_positions(row_ids, piece_len, cp_size):
    owner_cp = row_ids // (2 * piece_len)
    within = row_ids % (2 * piece_len)
    return jnp.where(within < piece_len, owner_cp * piece_len + within,
                     (2 * cp_size - 1 - owner_cp) * piece_len + within - piece_len)


def qkv_kernel(a_ref, wq_ref, wk_ref, wv_ref, cos_ref, sin_ref, q_ref, k_ref, vt_ref):
    a = a_ref[...]
    cos, sin = cos_ref[...], sin_ref[...]

    def rope(val):
        f = val.astype(jnp.bfloat16).astype(jnp.float32)
        return (f * cos + pltpu.roll(f, HD // 2, 1) * sin).astype(jnp.bfloat16)

    nq = wq_ref.shape[1]
    for n in range(0, nq, 256):
        r = jnp.dot(a, wq_ref[:, n:n + 256], preferred_element_type=jnp.float32)
        q_ref[:, n:n + HD] = rope(r[:, :HD])
        q_ref[:, n + HD:n + 256] = rope(r[:, HD:])
    r = jnp.dot(a, wk_ref[...], preferred_element_type=jnp.float32)
    for n in range(0, wk_ref.shape[1], HD):
        k_ref[:, n:n + HD] = rope(r[:, n:n + HD])
    r = jnp.dot(a, wv_ref[...], preferred_element_type=jnp.float32)
    for n in range(0, wv_ref.shape[1], HD):
        vt_ref[n:n + HD, :] = r[:, n:n + HD].T.astype(jnp.bfloat16)


def qkv(a, wq, wk, wv, cos, sin, tile=256):
    rows, dim = a.shape
    nq, nk = wq.shape[1], wk.shape[1]
    whole = lambda shape: pl.BlockSpec(shape, lambda i: (0, 0), pipeline_mode=pl.Buffered(1))
    return pl.pallas_call(
        qkv_kernel,
        grid=(rows // tile,),
        in_specs=[pl.BlockSpec((tile, dim), lambda i: (i, 0)), whole((dim, nq)), whole((dim, nk)), whole((dim, nk)),
                  pl.BlockSpec((tile, HD), lambda i: (i, 0)), pl.BlockSpec((tile, HD), lambda i: (i, 0))],
        out_specs=[pl.BlockSpec((tile, nq), lambda i: (i, 0)), pl.BlockSpec((tile, nk), lambda i: (i, 0)),
                   pl.BlockSpec((nk, tile), lambda i: (0, i))],
        out_shape=[jax.ShapeDtypeStruct((rows, nq), jnp.bfloat16), jax.ShapeDtypeStruct((rows, nk), jnp.bfloat16),
                   jax.ShapeDtypeStruct((nk, rows), jnp.bfloat16)],
        name="qkv",
        cost_estimate=pl.CostEstimate(flops=2 * rows * dim * (nq + 2 * nk), transcendentals=0,
                                      bytes_accessed=2 * (rows * dim + dim * (nq + 2 * nk) + rows * (nq + 2 * nk))),
        compiler_params=pltpu.CompilerParams(dimension_semantics=("arbitrary",), vmem_limit_bytes=56 * MIB),
    )(a, wq, wk, wv, cos, sin)


def flash_kernel(qpos_ref, order_ref, q_ref, k_ref, vt_ref, o_ref,
                 qt_scr, s_scr, mb_scr, acc_scr, m_scr, l_scr, *, T, B, G, D, piece):
    p0 = qpos_ref[pl.program_id(1)]
    c = (HD ** -0.5) * LOG2E
    ppb = piece // B

    for h in range(G):
        qt_scr[h] = q_ref[:, h * HD:(h + 1) * HD].astype(jnp.float32).T.astype(jnp.bfloat16)
    m_scr[...] = jnp.full_like(m_scr, NEG)
    l_scr[...] = jnp.zeros_like(l_scr)
    acc_scr[...] = jnp.zeros_like(acc_scr)

    def off(b):
        st = order_ref[lax.div(b, ppb)]
        return lax.div(st, 2), pl.multiple_of(lax.rem(st, 2) * piece + lax.rem(b, ppb) * B, B)

    def put(s, slot, mask):
        if mask is not None:
            s = jnp.where(mask, s, NEG)
        s_scr[slot] = s
        mb = jnp.max(s.reshape(B // 8, 8, T), axis=0)
        for r in (4, 2, 1):
            mb = jnp.maximum(mb, pltpu.roll(mb, r, 0))
        mb_scr[slot] = mb

    def stage_a(at, h, mask=None):
        kb = k_ref[at[0], pl.ds(at[1], B), :]
        put(lax.dot_general(kb, qt_scr[h], DN, preferred_element_type=jnp.float32), h, mask)

    def stage_b(at, h):
        m_prev = m_scr[h]
        m_new = jnp.maximum(m_prev, mb_scr[h])
        m_scr[h] = m_new
        m_c = m_new * c
        p = jnp.exp2(s_scr[h].reshape(B // 8, 8, T) * c - m_c[None])
        alpha = jnp.exp2(m_prev * c - m_c)
        l_scr[h] = l_scr[h] * alpha + jnp.sum(p, axis=0)
        vb = vt_ref[at[0], :, pl.ds(at[1], B)]
        pv = lax.dot_general(vb, p.reshape(B, T).astype(jnp.bfloat16), DN, preferred_element_type=jnp.float32)
        acc_scr[h] = (acc_scr[h].reshape(HD // 8, 8, T) * alpha[None]).reshape(HD, T) + pv

    nfull = lax.div(p0, B)
    for h in range(D):
        stage_a(off(0), h)

    def body(j, carry):
        cur, nxt = off(j), off(j + 1)
        for h in range(G):
            a = h + D
            stage_a(cur if a < G else nxt, a % G)
            stage_b(cur, h)
        return carry

    lax.fori_loop(0, nfull, body, 0)

    cur = off(nfull)
    kp = nfull * B + lax.broadcasted_iota(jnp.int32, (B, T), 0)
    qp = p0 + lax.broadcasted_iota(jnp.int32, (B, T), 1)
    mask = kp <= qp
    for h in range(D):
        put(s_scr[h], h, mask)
    for h in range(G):
        if h + D < G:
            stage_a(cur, h + D, mask)
        stage_b(cur, h)
    for h in range(G):
        l = jnp.sum(l_scr[h], axis=0, keepdims=True)
        o_ref[:, h * HD:(h + 1) * HD] = (acc_scr[h] / l).T.astype(jnp.bfloat16)


def flash(qpos, order, q, k, vt, *, piece, T=256, B=512, D=3):
    rows, nq = q.shape
    cps, seq, nk = k.shape
    n_kv = nk // HD
    G = nq // nk
    keys = cps * seq
    return pl.pallas_call(
        functools.partial(flash_kernel, T=T, B=B, G=G, D=D, piece=piece),
        grid_spec=pltpu.PrefetchScalarGridSpec(
            num_scalar_prefetch=2, grid=(n_kv, rows // T),
            in_specs=[pl.BlockSpec((T, G * HD), lambda g, i, *_: (i, g)),
                      pl.BlockSpec((cps, seq, HD), lambda g, i, *_: (0, 0, g)),
                      pl.BlockSpec((cps, HD, seq), lambda g, i, *_: (0, g, 0))],
            out_specs=pl.BlockSpec((T, G * HD), lambda g, i, *_: (i, g)),
            scratch_shapes=[pltpu.VMEM((G, HD, T), jnp.bfloat16),
                            pltpu.VMEM((G, B, T), jnp.float32),
                            pltpu.VMEM((G, 8, T), jnp.float32),
                            pltpu.VMEM((G, HD, T), jnp.float32),
                            pltpu.VMEM((G, 8, T), jnp.float32),
                            pltpu.VMEM((G, 8, T), jnp.float32)]),
        out_shape=jax.ShapeDtypeStruct((rows, nq), jnp.bfloat16),
        name="flash",
        cost_estimate=pl.CostEstimate(flops=2 * rows * keys * nq, transcendentals=rows * keys * nq // HD // 2,
                                      bytes_accessed=4 * rows * nq + 4 * keys * nk),
        compiler_params=pltpu.CompilerParams(dimension_semantics=("arbitrary", "arbitrary"), vmem_limit_bytes=56 * MIB),
    )(qpos, order, q, k, vt)


def solution(mesh):
    cp_size = mesh.shape['cp']
    row_spec = P('dp', ('cp', 'tp'), None)
    head_cols = P(None, 'tp', None)

    def local_layer(x, g_attn, w_q, w_k, w_v, w_o, g_mlp, w_gate, w_up, w_down):
        x_rows = x[0]
        dim = w_q.shape[0]
        cp_index = lax.axis_index('cp')
        normed = lax.all_gather(rms_norm(x_rows, g_attn), 'tp', axis=0, tiled=True)
        seq_local = normed.shape[0]
        piece_len = seq_local // 2
        positions = stored_positions(cp_index * seq_local + jnp.arange(seq_local, dtype=jnp.int32), piece_len, cp_size)
        cos, sin = rope_tables(positions)
        q, k, vt = qkv(normed, w_q.reshape(dim, -1), w_k.reshape(dim, -1), w_v.reshape(dim, -1), cos, sin)
        k_seq = lax.all_gather(k, 'cp', axis=0, tiled=False)
        vt_seq = lax.all_gather(vt, 'cp', axis=0, tiled=False)
        order = jnp.array([2 * p if p < cp_size else 2 * (2 * cp_size - 1 - p) + 1 for p in range(2 * cp_size)], jnp.int32)
        attn_out = flash(positions[::256], order, q, k_seq, vt_seq, piece=piece_len)
        attn_part = jnp.dot(attn_out, w_o.reshape(-1, dim), preferred_element_type=jnp.float32).astype(jnp.bfloat16)
        attn_rows = lax.psum_scatter(attn_part, 'tp', scatter_dimension=0, tiled=True)
        resid_rows = (x_rows.astype(jnp.float32) + attn_rows.astype(jnp.float32)).astype(jnp.bfloat16)
        normed_mlp = lax.all_gather(rms_norm(resid_rows, g_mlp), 'tp', axis=0, tiled=True)
        gate_proj = jnp.dot(normed_mlp, w_gate, preferred_element_type=jnp.float32)
        up_proj = jnp.dot(normed_mlp, w_up, preferred_element_type=jnp.float32)
        hidden = (jax.nn.silu(gate_proj) * up_proj).astype(jnp.bfloat16)
        down_part = jnp.dot(hidden, w_down, preferred_element_type=jnp.float32).astype(jnp.bfloat16)
        down_rows = lax.psum_scatter(down_part, 'tp', scatter_dimension=0, tiled=True)
        z_rows = (resid_rows.astype(jnp.float32) + down_rows.astype(jnp.float32)).astype(jnp.bfloat16)
        return z_rows[None]

    return jax.shard_map(local_layer, mesh=mesh,
                         in_specs=(row_spec, P(), head_cols, head_cols, head_cols, P('tp', None, None),
                                   P(), P(None, 'tp'), P(None, 'tp'), P('tp', None)),
                         out_specs=row_spec, check_vma=False)
```

```python
import functools
import math
import jax
import jax.numpy as jnp
import numpy as np
from jax import lax
from jax.experimental import pallas as pl
from jax.experimental.pallas import tpu as pltpu
from jax.sharding import PartitionSpec as P

NORM_EPS = 1e-5
ROPE_THETA = 500000.0
HD = 128
RUN = 256
NEG = -1e30
FAR = 1 << 29
LOG2E = math.log2(math.e)
DN = (((1,), (0,)), ((), ()))
MIB = 1 << 20
BF = jnp.bfloat16
F32 = jnp.float32
ANY = pl.BlockSpec(memory_space=pl.ANY)


def params(n, mib):
    return pltpu.CompilerParams(dimension_semantics=("arbitrary",) * n, vmem_limit_bytes=mib * MIB)


def rope_tables(positions):
    half = HD // 2
    inv_freq = ROPE_THETA ** (-2.0 * jnp.arange(half, dtype=F32) / HD)
    angles = positions.astype(F32)[..., None] * inv_freq
    cos, sin = jnp.cos(angles), jnp.sin(angles)
    return jnp.concatenate([cos, cos], axis=-1), jnp.concatenate([-sin, sin], axis=-1)


def norm_rows(rows, gain):
    f = rows.astype(F32)
    mean_sq = jnp.mean(f * f, axis=-1, keepdims=True)
    return (f * lax.rsqrt(mean_sq + NORM_EPS) * gain.astype(F32)).astype(BF)


def ordered(kernel, n_in, after):
    n = len(after)
    return lambda *refs: kernel(*refs[:n_in], *refs[n_in + n:])


def load_all(pairs, sem):
    copies = [pltpu.make_async_copy(src, dst, sem.at[i]) for i, (src, dst) in enumerate(pairs)]
    for cp in copies:
        cp.start()
    for cp in copies:
        cp.wait()


def norm_kernel(x_ref, g_ref, o_ref):
    o_ref[...] = norm_rows(x_ref[...], g_ref[...])


def norm_run(x_rows, gain, j, after=(), tile=128):
    dim = x_rows.shape[1]
    per = RUN // tile
    return pl.pallas_call(
        ordered(norm_kernel, 2, after), grid=(per,),
        in_specs=[pl.BlockSpec((tile, dim), lambda i: (j * per + i, 0)), pl.BlockSpec((1, dim), lambda i: (0, 0))]
        + [ANY] * len(after),
        out_specs=pl.BlockSpec((tile, dim), lambda i: (i, 0)),
        out_shape=jax.ShapeDtypeStruct((RUN, dim), BF),
        name="norm", compiler_params=params(1, 60),
        cost_estimate=pl.CostEstimate(flops=8 * RUN * dim, transcendentals=0, bytes_accessed=4 * RUN * dim),
    )(x_rows, gain, *after)


def qkv_kernel(*refs, n_in, nq):
    a_refs = refs[:n_in]
    w_ref, cos_ref, sin_ref, q_ref, kv_ref, a_scr, sem = refs[n_in:]
    n = pl.program_id(0)

    @pl.when(n == 0)
    def _():
        load_all([(r, a_scr.at[pl.ds(i * RUN, RUN), :]) for i, r in enumerate(a_refs)], sem)

    r = jnp.dot(a_scr[...], w_ref[...], preferred_element_type=F32)

    def rope(h):
        f = r[:, h * HD:(h + 1) * HD].astype(BF).astype(F32)
        cos, sin = cos_ref[...].reshape(n_in * RUN, HD), sin_ref[...].reshape(n_in * RUN, HD)
        return (f * cos + pltpu.roll(f, HD // 2, 1) * sin).astype(BF).reshape(n_in, RUN, HD)

    @pl.when(n < nq)
    def _():
        for h in range(2):
            q_ref[:, :, h * HD:(h + 1) * HD] = rope(h)

    @pl.when(n == nq)
    def _():
        for h in range(2):
            kv_ref[:, 0, :, h * HD:(h + 1) * HD] = rope(h)

    @pl.when(n == nq + 1)
    def _():
        for i in range(n_in):
            for h in range(2):
                kv_ref[i, 0, h * HD:(h + 1) * HD, :] = r[i * RUN:(i + 1) * RUN, h * HD:(h + 1) * HD].T.astype(BF)


def qkv(rows, w_all, cos, sin, first_run, after=()):
    n_in = len(rows)
    dim, cols = w_all.shape
    nq = cols // 256 - 2
    at = first_run // n_in
    tab = pl.BlockSpec((n_in, RUN, HD), lambda n: (at, 0, 0))
    return pl.pallas_call(
        ordered(functools.partial(qkv_kernel, n_in=n_in, nq=nq), n_in + 3, after),
        grid=(nq + 2,),
        in_specs=[ANY] * n_in + [pl.BlockSpec((dim, 256), lambda n: (0, n)), tab, tab] + [ANY] * len(after),
        out_specs=[pl.BlockSpec((n_in, RUN, 256), lambda n: (0, 0, jnp.minimum(n, nq - 1))),
                   pl.BlockSpec((n_in, 1, 256, 256), lambda n: (0, jnp.maximum(n - nq, 0), 0, 0))],
        out_shape=[jax.ShapeDtypeStruct((n_in, RUN, nq * 256), BF), jax.ShapeDtypeStruct((n_in, 2, 256, 256), BF)],
        scratch_shapes=[pltpu.VMEM((n_in * RUN, dim), BF), pltpu.SemaphoreType.DMA((n_in,))],
        name="qkv", compiler_params=params(1, 60),
        cost_estimate=pl.CostEstimate(flops=2 * n_in * RUN * dim * cols, transcendentals=0,
                                      bytes_accessed=2 * (n_in * RUN * dim + dim * cols + n_in * RUN * cols)),
    )(*rows, w_all, cos, sin, *after)


def flash_kernel(tab_ref, *refs, q_src, kv_src, n_q, n_kv, base, stride, G, D, n_out):
    qs, kvs = refs[:n_q], refs[n_q:n_q + n_kv]
    outs = refs[n_q + n_kv:n_q + n_kv + n_out]
    q_scr, kv_scr, qt_scr, s_scr, mb_scr, acc_scr, m_scr, l_scr, sem = refs[n_q + n_kv + n_out:]
    tile, g = pl.program_id(0), pl.program_id(1)
    T = RUN
    c = (HD ** -0.5) * LOG2E

    @pl.when((tile == 0) & (g == 0))
    def _():
        load_all([(qs[a].at[pl.ds(i, n)], q_scr.at[pl.ds(dst, n)]) for dst, (a, i, n) in q_src]
                 + [(kvs[a], kv_scr.at[pl.ds(dst, n)]) for a, (dst, n) in enumerate(kv_src)], sem)

    row = base + tile * stride
    npairs = tab_ref[row]
    qpos = tab_ref[row + 1]
    gcol = pl.multiple_of(g * HD, HD)

    for h in range(G):
        qh = q_scr[tile, :, pl.ds(pl.multiple_of((g * G + h) * HD, HD), HD)]
        qt_scr[h] = qh.astype(F32).T.astype(BF)
    m_scr[...] = jnp.full_like(m_scr, NEG)
    l_scr[...] = jnp.zeros_like(l_scr)
    acc_scr[...] = jnp.zeros_like(acc_scr)

    def pair(p):
        return tab_ref[row + 4 + 2 * p], tab_ref[row + 5 + 2 * p]

    def put(s, h):
        s_scr[h] = s
        mb = jnp.max(s.reshape(2 * RUN // 8, 8, T), axis=0)
        for r in (4, 2, 1):
            mb = jnp.maximum(mb, pltpu.roll(mb, r, 0))
        mb_scr[h] = mb

    def stage_a(pr, h, mask=None):
        s = jnp.concatenate([lax.dot_general(kv_scr[r, 0, :, pl.ds(gcol, HD)], qt_scr[h], DN, preferred_element_type=F32)
                             for r in pr], axis=0)
        put(s if mask is None else jnp.where(mask, s, NEG), h)

    def stage_b(pr, h):
        m_prev = m_scr[h]
        m_new = jnp.maximum(m_prev, mb_scr[h])
        m_scr[h] = m_new
        m_c = m_new * c
        p = jnp.exp2(s_scr[h].reshape(2 * RUN // 8, 8, T) * c - m_c[None])
        alpha = jnp.exp2(m_prev * c - m_c)
        l_scr[h] = l_scr[h] * alpha + jnp.sum(p, axis=0)
        pb = p.reshape(2 * RUN, T).astype(BF)
        pv = sum(lax.dot_general(kv_scr[r, 1, pl.ds(gcol, HD), :], pb[i * RUN:(i + 1) * RUN], DN, preferred_element_type=F32)
                 for i, r in enumerate(pr))
        acc_scr[h] = (acc_scr[h].reshape(HD // 8, 8, T) * alpha[None]).reshape(HD, T) + pv

    first = pair(0)
    for h in range(D):
        stage_a(first, h)

    def body(j, carry):
        cur, nxt = pair(j), pair(j + 1)
        for h in range(G):
            a = h + D
            stage_a(cur if a < G else nxt, a % G)
            stage_b(cur, h)
        return carry

    lax.fori_loop(0, npairs - 1, body, 0)

    last = pair(npairs - 1)
    key = lax.broadcasted_iota(jnp.int32, (RUN, T), 0)
    qry = lax.broadcasted_iota(jnp.int32, (RUN, T), 1) + qpos
    mask = jnp.concatenate([key + tab_ref[row + 2] <= qry, key + tab_ref[row + 3] <= qry], axis=0)
    for h in range(D):
        put(jnp.where(mask, s_scr[h], NEG), h)
    for h in range(G):
        if h + D < G:
            stage_a(last, h + D, mask)
        stage_b(last, h)
    for h in range(G):
        l = jnp.sum(l_scr[h], axis=0, keepdims=True)
        q_scr[tile, :, pl.ds(pl.multiple_of((g * G + h) * HD, HD), HD)] = (acc_scr[h] / l).T.astype(BF)
    for k in range(n_out):
        @pl.when(tile == k)
        def _():
            outs[k][...] = q_scr[k, :, pl.ds(pl.multiple_of(g * G * HD, G * HD), G * HD)]


def flash(tab, qs, q_src, kvs, kv_src, *, base, stride, work, after=(), D=3):
    nq = qs[0].shape[2]
    n_kv_heads = 2
    G = nq // HD // n_kv_heads
    n_tiles = 4
    n_runs = max(d + n for d, n in kv_src)

    def out_spec(k):
        return pl.BlockSpec((RUN, G * HD), lambda i, g, *_: (0, jnp.where(i < k, 0, jnp.where(i == k, g, n_kv_heads - 1))))

    return pl.pallas_call(
        ordered(functools.partial(flash_kernel, q_src=q_src, kv_src=kv_src, n_q=len(qs), n_kv=len(kvs), base=base,
                                  stride=stride, G=G, D=D, n_out=n_tiles), 1 + len(qs) + len(kvs), after),
        grid_spec=pltpu.PrefetchScalarGridSpec(
            num_scalar_prefetch=1, grid=(n_tiles, n_kv_heads),
            in_specs=[ANY] * (len(qs) + len(kvs) + len(after)),
            out_specs=[out_spec(k) for k in range(n_tiles)],
            scratch_shapes=[pltpu.VMEM((n_tiles, RUN, nq), BF),
                            pltpu.VMEM((n_runs, 2, 256, 256), BF),
                            pltpu.VMEM((G, HD, RUN), BF),
                            pltpu.VMEM((G, 2 * RUN, RUN), F32),
                            pltpu.VMEM((G, 8, RUN), F32),
                            pltpu.VMEM((G, HD, RUN), F32),
                            pltpu.VMEM((G, 8, RUN), F32),
                            pltpu.VMEM((G, 8, RUN), F32),
                            pltpu.SemaphoreType.DMA((len(q_src) + len(kv_src),))]),
        out_shape=[jax.ShapeDtypeStruct((RUN, nq), BF)] * n_tiles,
        name="flash", compiler_params=params(2, 60),
        cost_estimate=pl.CostEstimate(flops=8 * work * RUN * RUN * nq, transcendentals=work * RUN * RUN * nq // HD,
                                      bytes_accessed=n_runs * 2 * 256 * 256 * 2 + 4 * n_tiles * RUN * nq),
    )(tab, *qs, *kvs, *after)


def out_kernel(*refs, n_w):
    o_refs, w_refs = refs[:4], refs[4:4 + n_w]
    x_ref, g_ref, y_ref, b_ref, o_scr, sem = refs[4 + n_w:]
    n = pl.program_id(0)
    tn = w_refs[0].shape[1]
    width = o_refs[0].shape[1]
    half = width // 2

    @pl.when(n == 0)
    def _():
        mine = lax.axis_index('cp')
        pairs = [(o_refs[0], o_scr.at[:, pl.ds(0, width)]), (o_refs[1], o_scr.at[:, pl.ds(width, width)])]
        for k in range(2, 4):
            for i, part in enumerate((mine, 1 - mine)):
                pairs.append((o_refs[k].at[:, pl.ds(pl.multiple_of(part * half, half), half)],
                              o_scr.at[:, pl.ds(k * width + i * half, half)]))
        load_all(pairs, sem)

    acc, k0 = None, 0
    for w in w_refs:
        d = jnp.dot(o_scr[:, k0:k0 + w.shape[0]], w[...], preferred_element_type=F32)
        acc = d if acc is None else acc + d
        k0 += w.shape[0]
    cols = pl.ds(pl.multiple_of(n * tn, tn), tn)
    y_ref[:, cols] = (x_ref[:, cols].astype(F32) + acc.astype(BF).astype(F32)).astype(BF)

    @pl.when(n == pl.num_programs(0) - 1)
    def _():
        for i in range(0, RUN, 64):
            b_ref[i:i + 64, :] = norm_rows(y_ref[i:i + 64, :], g_ref[...])


def out_proj(os, ws, x_rows, gain, j, after=(), tn=512):
    dim = x_rows.shape[1]
    width = os[0].shape[1]
    whole = lambda s: pl.BlockSpec((RUN, dim), lambda n: (s, 0))
    return pl.pallas_call(
        ordered(functools.partial(out_kernel, n_w=len(ws)), 6 + len(ws), after),
        grid=(dim // tn,),
        in_specs=[ANY] * 4 + [pl.BlockSpec((w.shape[0], tn), lambda n: (0, n)) for w in ws]
        + [whole(j), pl.BlockSpec((1, dim), lambda n: (0, 0))] + [ANY] * len(after),
        out_specs=[whole(0), whole(0)],
        out_shape=[jax.ShapeDtypeStruct((RUN, dim), BF)] * 2,
        scratch_shapes=[pltpu.VMEM((RUN, 4 * width), BF), pltpu.SemaphoreType.DMA((6,))],
        name="outp", compiler_params=params(1, 60),
        cost_estimate=pl.CostEstimate(flops=8 * RUN * width * dim, transcendentals=0,
                                      bytes_accessed=8 * width * dim + 8 * RUN * dim),
    )(*os, *ws, x_rows, gain, *after)


def hidden_kernel(*refs, n_in):
    b_refs = refs[:n_in]
    wg_ref, wu_ref, u_ref, b_scr, sem = refs[n_in:]

    @pl.when(pl.program_id(0) == 0)
    def _():
        load_all([(r, b_scr.at[pl.ds(k * RUN, RUN), :]) for k, r in enumerate(b_refs)], sem)

    b = b_scr[...]
    gate = jnp.dot(b, wg_ref[...], preferred_element_type=F32)
    up = jnp.dot(b, wu_ref[...], preferred_element_type=F32)
    u_ref[...] = (jax.nn.silu(gate) * up).astype(BF)


def hidden(bs, wg, wu, after=(), tn=512):
    rows, dim = RUN * len(bs), bs[0].shape[1]
    ffn = wg.shape[1]
    cols = lambda i: (0, i)
    return pl.pallas_call(
        ordered(functools.partial(hidden_kernel, n_in=len(bs)), len(bs) + 2, after),
        grid=(ffn // tn,),
        in_specs=[ANY] * len(bs) + [pl.BlockSpec((dim, tn), cols)] * 2 + [ANY] * len(after),
        out_specs=pl.BlockSpec((rows, tn), cols),
        out_shape=jax.ShapeDtypeStruct((rows, ffn), BF),
        scratch_shapes=[pltpu.VMEM((rows, dim), BF), pltpu.SemaphoreType.DMA((len(bs),))],
        name="hidden", compiler_params=params(1, 60),
        cost_estimate=pl.CostEstimate(flops=4 * rows * dim * ffn, transcendentals=rows * ffn,
                                      bytes_accessed=4 * dim * ffn + 2 * rows * (dim + ffn)),
    )(*bs, wg, wu, *after)


def down_kernel(u_ref, w_ref, o_ref):
    o_ref[...] = jnp.dot(u_ref[...], w_ref[...], preferred_element_type=F32).astype(BF)


def down(u, wd, part, after=(), td=512):
    rows, ffn = u.shape[0] // 2, u.shape[1]
    dim = wd.shape[1]
    return pl.pallas_call(
        ordered(down_kernel, 2, after),
        grid=(dim // td,),
        in_specs=[pl.BlockSpec((rows, ffn), lambda i: (part, 0)), pl.BlockSpec((ffn, td), lambda i: (0, i))]
        + [ANY] * len(after),
        out_specs=pl.BlockSpec((rows, td), lambda i: (0, i)),
        out_shape=jax.ShapeDtypeStruct((rows, dim), BF),
        name="down", compiler_params=params(1, 60),
        cost_estimate=pl.CostEstimate(flops=2 * rows * dim * ffn, transcendentals=0,
                                      bytes_accessed=2 * dim * ffn + 2 * rows * (dim + ffn)),
    )(u, wd, *after)


def sum_kernel(*refs):
    p_ref, r_ref, t_ref, y_ref, z_ref = refs[-5:]
    total = p_ref[...].astype(F32) + r_ref[...].astype(F32) + t_ref[...].astype(F32)
    z_ref[...] = (y_ref[...].astype(F32) + total.astype(BF).astype(F32)).astype(BF)


def sum_run(z, keep, recv, far, y, j, n_runs, after=(), tile=64):
    dim = y.shape[1]
    per = RUN // tile
    spec = pl.BlockSpec((tile, dim), lambda i: (i, 0))
    prev = () if z is None else (z,)
    return pl.pallas_call(
        ordered(sum_kernel, len(prev) + 4, after), grid=(per,),
        in_specs=[ANY] * len(prev) + [spec] * 4 + [ANY] * len(after),
        out_specs=pl.BlockSpec((tile, dim), lambda i: (j * per + i, 0)),
        out_shape=jax.ShapeDtypeStruct((n_runs * RUN, dim), BF),
        input_output_aliases={0: 0} if prev else {},
        name="zsum", compiler_params=params(1, 60),
        cost_estimate=pl.CostEstimate(flops=6 * RUN * dim, transcendentals=0, bytes_accessed=10 * RUN * dim),
    )(*prev, keep, recv, far, y, *after)


def run_positions(xi, ci, y, cps, piece):
    def start(x, c):
        return (y if x == 0 else 2 * cps - 1 - y) * piece + c * (piece // 2)

    per = piece // 2 // RUN
    out = [start(xi, ci) + RUN * j for j in range(per)] + [start(xi, 1 - ci) + RUN * j for j in range(per)]
    for j in range(per):
        out += [start(1 - xi, ci) + RUN * j, start(1 - xi, 1 - ci) + RUN * j]
    return out


def work_tables(cps, piece):
    per = piece // 2 // RUN
    tabs, runs, work = [], [], []
    stride = 4 + 2 * (2 * per * 2 * cps // 2 + 1)
    for y in range(cps):
        for xi in range(2):
            for ci in range(2):
                mine = run_positions(xi, ci, y, cps, piece)
                pos = mine + run_positions(xi, ci, 1 - y, cps, piece)
                runs.append(mine)
                rows, amount = [], []
                for j in range(per):
                    for tile in (j, per + j, 2 * per + 2 * j, 2 * per + 2 * j + 1):
                        q = pos[tile]
                        ids = [r for r in range(len(pos)) if pos[r] < q] + [tile]
                        where = [pos[r] for r in ids]
                        if len(ids) % 2:
                            ids.append(tile)
                            where.append(FAR)
                        row = [len(ids) // 2, q, where[-2], where[-1]] + ids
                        rows.append(row + [0] * (stride - len(row)))
                        amount.append(len(ids))
                tabs.append(np.array(rows, np.int32).reshape(-1))
                work.append(amount)
    return np.stack(tabs), np.array(runs, np.int32), stride, np.array(work).reshape(len(tabs), per, 4).sum(-1).max(0)


def solution(mesh):
    cps = mesh.shape['cp']
    row_spec = P('dp', ('cp', 'tp'), None)
    head_cols = P(None, 'tp', None)
    n_tp = mesh.shape['tp']

    over_core, over_x, over_both = (('tp', [(t, t ^ k) for t in range(n_tp)]) for k in (1, 2, 3))
    over_y = ('cp', [(i, i ^ 1) for i in range(cps)])

    def layer(x, g_attn, w_q, w_k, w_v, w_o, g_mlp, w_gate, w_up, w_down):
        x_rows = x[0]
        dim = x_rows.shape[1]
        n_run = x_rows.shape[0] // RUN
        piece = 2 * x_rows.shape[0]
        t_id, y_id = lax.axis_index('tp'), lax.axis_index('cp')
        np_tab, np_runs, stride, work = work_tables(cps, piece)
        dev = y_id * n_tp + t_id
        tab = lax.dynamic_index_in_dim(jnp.asarray(np_tab), dev, 0, keepdims=False)
        run_pos = lax.dynamic_index_in_dim(jnp.asarray(np_runs), dev, 0, keepdims=False)

        def tied(v, *others):
            return lax.optimization_barrier((v, *others))[0]

        def send(axis_pairs, v):
            return lax.ppermute(v, *axis_pairs)

        ga, gm = g_attn.reshape(1, dim), g_mlp.reshape(1, dim)
        own = []
        for j in range(n_run):
            own.append(norm_run(x_rows, ga, j, after=own[-1:]))
        far = [send(over_x, own[j]) for j in range(n_run)]
        mate = [send(over_core, own[j]) for j in range(n_run)]

        w_all = jnp.concatenate([tied(w, own[-1]).reshape(dim, -1) for w in (w_q, w_k, w_v)], axis=1)
        cos, sin = rope_tables(tied(run_pos, own[-1])[:, None] + jnp.arange(RUN, dtype=jnp.int32)[None, :])

        q_own, kv_own = qkv(own, w_all, cos, sin, 0)
        q_mate, kv_mate = qkv(mate, w_all, cos, sin, n_run, after=(kv_own,))
        kvs = [kv_own, kv_mate]
        q_far = []
        for j in range(n_run):
            here = tied(far[j], kvs[-1])
            q, kv = qkv([here, send(over_core, here)], w_all, cos, sin, 2 * n_run + 2 * j,
                         after=(kvs[-1],))
            q_far.append(q)
            kvs.append(kv)
        gate, last = kvs[3], kvs[-1]
        kvs = kvs + [send(over_y, kv) for kv in kvs]
        kv_src, at = [], 0
        for kv in kvs:
            kv_src.append((at, kv.shape[0]))
            at += kv.shape[0]

        wo = w_o.reshape(-1, dim)
        half = wo.shape[0] // 2
        wo_gated = tied(wo, gate)
        wo_xa = send(over_x, lax.dynamic_slice_in_dim(wo_gated, y_id * half, half, axis=0))
        ws = [wo, send(over_core, wo_gated)]

        os, outs = [], []
        prev = last

        def attend(j):
            o_own, o_mate, o_far, o_fm = flash(
                tab, [q_own, q_mate, q_far[j]], [(0, (0, j, 1)), (1, (1, j, 1)), (2, (2, 0, 2))],
                kvs, kv_src, base=j * 4 * stride, stride=stride, work=int(work[j]), after=(prev,))
            os.append([o_own, send(over_core, o_mate), send(over_x, o_far), send(over_both, o_fm)])
            return o_own

        def project(j):
            y, b = out_proj(os[j], ws, x_rows, gm, j, after=(prev,))
            outs.append((y, b, send(over_x, b), send(over_core, b)))
            return b

        prev = attend(0)
        wo_a = tied(wo_xa, prev)
        wo_xb = send(over_y, wo_a)
        ws += [wo_a, None, send(over_core, wo_a), None]
        prev = attend(1)
        prev = attend(2)
        wo_b = tied(wo_xb, prev)
        ws[3], ws[5] = wo_b, send(over_core, wo_b)
        prev = project(0)
        prev = attend(3)

        z, pending, relay = None, None, {}

        def relay_b(j):
            here = tied(outs[j][2], prev)
            relay[j] = (here, send(over_core, here))

        relay_b(0)
        prev = project(1)
        for j in range(n_run):
            y, b, _, b_mate = outs[j]
            u = hidden([b, relay[j][0], b_mate, relay[j][1]], w_gate, w_up, after=(prev,))
            out = down(u, w_down, 1)
            recv = send(over_core, out)
            prev = out
            if j + 1 < n_run:
                relay_b(j + 1)
            keep = down(u, w_down, 0, after=(out,))
            prev = s_far = (keep[RUN:].astype(F32) + recv[RUN:].astype(F32)).astype(BF)
            got = send(over_x, s_far)
            if j + 2 < n_run:
                prev = project(j + 2)
            if pending is not None:
                prev = z = sum_run(z, *pending, j - 1, n_run, after=(prev,))
            pending = (keep, recv, got, y)
        z = sum_run(z, *pending, n_run - 1, n_run)
        return z[None]

    return jax.shard_map(layer, mesh=mesh,
                         in_specs=(row_spec, P(), head_cols, head_cols, head_cols, P('tp', None, None),
                                   P(), P(None, 'tp'), P(None, 'tp'), P('tp', None)),
                         out_specs=row_spec, check_vma=False)
```

```python
import functools
import math
import jax
import jax.numpy as jnp
import numpy as np
from jax import lax
from jax.experimental import pallas as pl
from jax.experimental.pallas import tpu as pltpu
from jax.sharding import PartitionSpec as P

NORM_EPS = 1e-5
ROPE_THETA = 500000.0
HD = 128
RUN = 256
NEG = -1e30
FAR = 1 << 29
LOG2E = math.log2(math.e)
DN = (((1,), (0,)), ((), ()))
VMEM = 67043328
BF = jnp.bfloat16
F32 = jnp.float32
ANY = pl.BlockSpec(memory_space=pltpu.HBM)


def params(n):
    return pltpu.CompilerParams(dimension_semantics=("arbitrary",) * n, vmem_limit_bytes=VMEM)


def rope_tables(positions):
    half = HD // 2
    inv_freq = ROPE_THETA ** (-2.0 * jnp.arange(half, dtype=F32) / HD)
    angles = inv_freq[:, None] * positions.astype(F32)[..., None, :]
    return jnp.cos(angles), jnp.sin(angles)


def norm_rows(rows, gain):
    f = rows.astype(F32)
    mean_sq = jnp.mean(f * f, axis=-1, keepdims=True)
    return (f * lax.rsqrt(mean_sq + NORM_EPS) * gain.astype(F32)).astype(BF)


def ordered(kernel, n_in, after):
    n = len(after)
    return lambda *refs: kernel(*refs[:n_in], *refs[n_in + n:])


def load_all(pairs, sem):
    copies = [pltpu.make_async_copy(src, dst, sem.at[i]) for i, (src, dst) in enumerate(pairs)]
    for cp in copies:
        cp.start()
    for cp in copies:
        cp.wait()


def norm_kernel(x_ref, g_ref, o_ref):
    o_ref[...] = norm_rows(x_ref[...], g_ref[...])


def norm_run(x_rows, gain, j, after=(), tile=128):
    dim = x_rows.shape[1]
    per = RUN // tile
    return pl.pallas_call(
        ordered(norm_kernel, 2, after), grid=(per,),
        in_specs=[pl.BlockSpec((tile, dim), lambda i: (j * per + i, 0)), pl.BlockSpec((1, dim), lambda i: (0, 0))]
        + [ANY] * len(after),
        out_specs=pl.BlockSpec((tile, dim), lambda i: (i, 0)),
        out_shape=jax.ShapeDtypeStruct((RUN, dim), BF),
        name="norm", compiler_params=params(1),
        cost_estimate=pl.CostEstimate(flops=8 * RUN * dim, transcendentals=0, bytes_accessed=4 * RUN * dim),
    )(x_rows, gain, *after)


def qkv_kernel(*refs, n_in, nq):
    a_refs = refs[:n_in]
    w_ref, cos_ref, sin_ref, q_ref, kv_ref, a_scr, sem = refs[n_in:]
    n = pl.program_id(0)

    @pl.when(n == 0)
    def _():
        load_all([(r, a_scr.at[pl.ds(i * RUN, RUN), :]) for i, r in enumerate(a_refs)], sem)

    r = jnp.dot(a_scr[...], w_ref[...], preferred_element_type=F32)

    def piece(i, h):
        return r[i * RUN:(i + 1) * RUN, h * HD:(h + 1) * HD].T

    def rope(i, h):
        f = piece(i, h).astype(BF).astype(F32)
        lo, hi, cos, sin = f[:HD // 2], f[HD // 2:], cos_ref[i], sin_ref[i]
        return jnp.concatenate([lo * cos - hi * sin, hi * cos + lo * sin], axis=0)

    parts = [(i, h) for i in range(n_in) for h in range(2)]

    @pl.when(n < nq)
    def _():
        for i, h in parts:
            q_ref[i, h * HD:(h + 1) * HD, :] = rope(i, h).astype(BF)

    @pl.when(n == nq)
    def _():
        for i, h in parts:
            kv_ref[i, 0, :, h * HD:(h + 1) * HD] = rope(i, h).T.astype(BF)

    @pl.when(n == nq + 1)
    def _():
        for i, h in parts:
            kv_ref[i, 0, h * HD:(h + 1) * HD, :] = piece(i, h).astype(BF)


def qkv(rows, w_all, cos, sin, first_run, after=()):
    n_in = len(rows)
    dim, cols = w_all.shape
    nq = cols // 256 - 2
    at = first_run // n_in
    tab = pl.BlockSpec((n_in, HD // 2, RUN), lambda n: (at, 0, 0))
    return pl.pallas_call(
        ordered(functools.partial(qkv_kernel, n_in=n_in, nq=nq), n_in + 3, after),
        grid=(nq + 2,),
        in_specs=[ANY] * n_in + [pl.BlockSpec((dim, 256), lambda n: (0, n)), tab, tab] + [ANY] * len(after),
        out_specs=[pl.BlockSpec((n_in, 256, RUN), lambda n: (0, jnp.minimum(n, nq - 1), 0)),
                   pl.BlockSpec((n_in, 1, 256, 256), lambda n: (0, jnp.maximum(n - nq, 0), 0, 0))],
        out_shape=[jax.ShapeDtypeStruct((n_in, nq * 256, RUN), BF), jax.ShapeDtypeStruct((n_in, 2, 256, 256), BF)],
        scratch_shapes=[pltpu.VMEM((n_in * RUN, dim), BF), pltpu.SemaphoreType.DMA((n_in,))],
        name="qkv", compiler_params=params(1),
        cost_estimate=pl.CostEstimate(flops=2 * n_in * RUN * dim * cols, transcendentals=0,
                                      bytes_accessed=2 * (n_in * RUN * dim + dim * cols + n_in * RUN * cols)),
    )(*rows, w_all, cos, sin, *after)


BLK = 12
MASK0, MASK1, LAST = 1, 2, 4


def flash_kernel(tab_ref, *refs, q_src, kv_src, n_q, n_kv, base, G, n_tiles, n_heads):
    qs, kvs, outs = refs[:n_q], refs[n_q:n_q + n_kv], refs[n_q + n_kv:n_q + n_kv + n_tiles]
    q_scr, kv_scr, o_scr, s_scr, mb_scr, acc_scr, m_scr, l_scr, q_sem, kv_sem, o_sem = refs[n_q + n_kv + n_tiles:]
    T = RUN
    c = (HD ** -0.5) * LOG2E
    n_blocks = tab_ref[base]
    row0 = base + 1 + n_tiles

    q_copies = [pltpu.make_async_copy(qs[a].at[i], q_scr.at[t], q_sem.at[t]) for t, (a, i) in enumerate(q_src)]
    kv_copies = [pltpu.make_async_copy(kvs[a].at[i], kv_scr.at[r], kv_sem.at[r]) for r, (a, i) in enumerate(kv_src)]
    for cp in q_copies + kv_copies:
        cp.start()
    for cp in q_copies:
        cp.wait()

    def clear():
        acc_scr[...] = jnp.zeros_like(acc_scr)
        l_scr[...] = jnp.zeros_like(l_scr)
        m_scr[...] = jnp.full_like(m_scr, NEG)

    def block(i):
        g = lax.div(i, n_blocks)
        return row0 + BLK * (i - g * n_blocks), g

    def arrived(have, need):
        def one(r, carry):
            pltpu.make_async_copy(kv_scr.at[r], kv_scr.at[r], kv_sem.at[r]).wait()
            return carry

        lax.fori_loop(have, need, one, 0)
        return jnp.maximum(have, need)

    def put(s, slot):
        s_scr[slot] = s
        mb = jnp.max(s.reshape(2 * RUN // 8, 8, T), axis=0)
        for r in (4, 2, 1):
            mb = jnp.maximum(mb, pltpu.roll(mb, r, 0))
        mb_scr[slot] = mb

    def stage_a(row, g, it, h):
        col = pl.multiple_of(g * HD, HD)
        qt = q_scr[tab_ref[row], pl.ds(pl.multiple_of((g * G + h) * HD, HD), HD), :]
        put(jnp.concatenate([lax.dot_general(kv_scr[tab_ref[row + 3 + 2 * it + k], 0, :, pl.ds(col, HD)], qt, DN,
                                             preferred_element_type=F32) for k in range(2)], axis=0), it * G + h)

    def stage_b(row, g, it, h):
        slot = it * G + h
        col = pl.multiple_of(g * HD, HD)
        m_prev = m_scr[h]
        m_new = jnp.maximum(m_prev, mb_scr[slot])
        m_scr[h] = m_new
        m_c = m_new * c
        p = jnp.exp2(s_scr[slot].reshape(2 * RUN // 8, 8, T) * c - m_c[None])
        alpha = jnp.exp2(m_prev * c - m_c)
        l_scr[h] = l_scr[h] * alpha + jnp.sum(p, axis=0)
        pb = p.reshape(2 * RUN, T).astype(BF)
        pv = sum(lax.dot_general(kv_scr[tab_ref[row + 3 + 2 * it + k], 1, pl.ds(col, HD), :], pb[k * RUN:(k + 1) * RUN], DN,
                                 preferred_element_type=F32) for k in range(2))
        acc_scr[h] = (acc_scr[h].reshape(HD // 8, 8, T) * alpha[None]).reshape(HD, T) + pv

    def mask_item(row, it):
        key = lax.broadcasted_iota(jnp.int32, (RUN, T), 0)
        qry = lax.broadcasted_iota(jnp.int32, (RUN, T), 1) + tab_ref[base + 1 + tab_ref[row]]
        mask = jnp.concatenate([key + tab_ref[row + 7 + 2 * it + k] <= qry for k in range(2)], axis=0)
        for h in range(G):
            put(jnp.where(mask, s_scr[it * G + h], NEG), it * G + h)

    row, g = block(0)
    have = arrived(0, tab_ref[row + 2])
    clear()
    for it in range(2):
        for h in range(G):
            stage_a(row, g, it, h)

    def body(i, have):
        row, g = block(i)
        nrow, ng = block(jnp.minimum(i + 1, n_heads * n_blocks - 1))
        have = arrived(have, tab_ref[nrow + 2])
        flags = tab_ref[row + 1]

        @pl.when((flags & MASK0) != 0)
        def _():
            mask_item(row, 0)

        @pl.when((flags & MASK1) != 0)
        def _():
            mask_item(row, 1)

        for it in range(2):
            for h in range(G):
                stage_b(row, g, it, h)
                stage_a(nrow, ng, it, h)

        @pl.when((flags & LAST) != 0)
        def _():
            tile = tab_ref[row]
            for h in range(G):
                l = jnp.sum(l_scr[h], axis=0, keepdims=True)
                o_scr[tile, :, pl.ds(pl.multiple_of((g * G + h) * HD, HD), HD)] = (acc_scr[h] / l).T.astype(BF)
            clear()
            for k in range(n_tiles):
                @pl.when((tile == k) & (g == n_heads - 1))
                def _():
                    pltpu.make_async_copy(o_scr.at[k], outs[k], o_sem.at[k]).start()

        return have

    have = lax.fori_loop(0, n_heads * n_blocks, body, have)
    arrived(have, len(kv_src))
    for k in range(n_tiles):
        pltpu.make_async_copy(o_scr.at[k], outs[k], o_sem.at[k]).wait()


def flash(tab, qs, q_src, kvs, *, base, work, after=()):
    nq = qs[0].shape[1]
    n_heads = 2
    G = nq // HD // n_heads
    n_tiles = len(q_src)
    kv_src = [(a, i) for a, kv in enumerate(kvs) for i in range(kv.shape[0])]
    n_runs = len(kv_src)
    slots = 2 * G
    return pl.pallas_call(
        ordered(functools.partial(flash_kernel, q_src=q_src, kv_src=kv_src, n_q=len(qs), n_kv=len(kvs), base=base, G=G,
                                  n_tiles=n_tiles, n_heads=n_heads), 1 + len(qs) + len(kvs), after),
        grid_spec=pltpu.PrefetchScalarGridSpec(
            num_scalar_prefetch=1, grid=(),
            in_specs=[ANY] * (len(qs) + len(kvs) + len(after)),
            out_specs=[ANY] * n_tiles,
            scratch_shapes=[pltpu.VMEM((n_tiles, nq, RUN), BF),
                            pltpu.VMEM((n_runs, 2, 256, 256), BF),
                            pltpu.VMEM((n_tiles, RUN, nq), BF),
                            pltpu.VMEM((slots, 2 * RUN, RUN), F32),
                            pltpu.VMEM((slots, 8, RUN), F32),
                            pltpu.VMEM((G, HD, RUN), F32),
                            pltpu.VMEM((G, 8, RUN), F32),
                            pltpu.VMEM((G, 8, RUN), F32),
                            pltpu.SemaphoreType.DMA((n_tiles,)),
                            pltpu.SemaphoreType.DMA((n_runs,)),
                            pltpu.SemaphoreType.DMA((n_tiles,))]),
        out_shape=[jax.ShapeDtypeStruct((RUN, nq), BF)] * n_tiles,
        name="flash", compiler_params=pltpu.CompilerParams(vmem_limit_bytes=VMEM),
        cost_estimate=pl.CostEstimate(flops=8 * work * RUN * RUN * nq, transcendentals=work * RUN * RUN * nq // HD,
                                      bytes_accessed=n_runs * 2 * 256 * 256 * 2 + 4 * n_tiles * RUN * nq),
    )(tab, *qs, *kvs, *after)


def out_kernel(*refs, n_w, n_run):
    o_refs, w_refs = refs[:4 * n_run], refs[4 * n_run:4 * n_run + n_w]
    x_ref, g_ref, y_ref = refs[4 * n_run + n_w:4 * n_run + n_w + 3]
    b_refs, (o_scr, sem) = refs[4 * n_run + n_w + 3:-2], refs[-2:]
    n = pl.program_id(0)
    tn = w_refs[0].shape[1]
    width = o_refs[0].shape[1]
    half = width // 2

    @pl.when(n == 0)
    def _():
        mine = lax.axis_index('cp')
        pairs = []
        for i in range(n_run):
            rows = pl.ds(i * RUN, RUN)
            os = o_refs[4 * i:4 * i + 4]
            pairs += [(os[0], o_scr.at[rows, pl.ds(0, width)]), (os[1], o_scr.at[rows, pl.ds(width, width)])]
            for k in range(2, 4):
                for p, part in enumerate((mine, 1 - mine)):
                    pairs.append((os[k].at[:, pl.ds(pl.multiple_of(part * half, half), half)],
                                  o_scr.at[rows, pl.ds(k * width + p * half, half)]))
        load_all(pairs, sem)

    acc, k0 = None, 0
    for w in w_refs:
        d = jnp.dot(o_scr[:, k0:k0 + w.shape[0]], w[...], preferred_element_type=F32)
        acc = d if acc is None else acc + d
        k0 += w.shape[0]
    cols = pl.ds(pl.multiple_of(n * tn, tn), tn)
    y_ref[:, cols] = (x_ref[:, cols].astype(F32) + acc.astype(BF).astype(F32)).astype(BF)

    @pl.when(n == pl.num_programs(0) - 1)
    def _():
        for k in range(n_run):
            def rows64(i, carry):
                at = pl.multiple_of(i * 64, 64)
                b_refs[k][pl.ds(at, 64), :] = norm_rows(y_ref[pl.ds(k * RUN + at, 64), :], g_ref[...])
                return carry

            lax.fori_loop(0, RUN // 64, rows64, 0)


def out_proj(os, ws, x_rows, gain, at, after=(), tn=256):
    dim = x_rows.shape[1]
    n_run = len(os) // 4
    width = os[0].shape[1]
    rows = n_run * RUN
    whole = lambda m, s: pl.BlockSpec((m, dim), lambda n: (s, 0))
    return pl.pallas_call(
        ordered(functools.partial(out_kernel, n_w=len(ws), n_run=n_run), len(os) + len(ws) + 2, after),
        grid=(dim // tn,),
        in_specs=[ANY] * len(os) + [pl.BlockSpec((w.shape[0], tn), lambda n: (0, n)) for w in ws]
        + [whole(rows, at), pl.BlockSpec((1, dim), lambda n: (0, 0))] + [ANY] * len(after),
        out_specs=[whole(rows, 0)] + [whole(RUN, 0)] * n_run,
        out_shape=[jax.ShapeDtypeStruct((rows, dim), BF)] + [jax.ShapeDtypeStruct((RUN, dim), BF)] * n_run,
        scratch_shapes=[pltpu.VMEM((rows, 4 * width), BF), pltpu.SemaphoreType.DMA((6 * n_run,))],
        name="outp", compiler_params=params(1),
        cost_estimate=pl.CostEstimate(flops=8 * rows * width * dim, transcendentals=0,
                                      bytes_accessed=8 * width * dim + 8 * rows * dim),
    )(*os, *ws, x_rows, gain, *after)


def mlp_kernel(*refs, n_in, tn, nk):
    b_refs = refs[:n_in]
    wg_ref, wu_ref, wd_ref, keep_ref, send_ref, b_scr, u_scr, sem = refs[n_in:]
    i = pl.program_id(0)

    def gated(rows, cols):
        b = b_scr[rows, :]
        gate = jnp.dot(b, wg_ref[...], preferred_element_type=F32)
        up = jnp.dot(b, wu_ref[...], preferred_element_type=F32)
        u_scr[rows, cols] = (jax.nn.silu(gate) * up).astype(BF)

    @pl.when(i == 0)
    def _():
        copies = [pltpu.make_async_copy(r, b_scr.at[pl.ds(k * RUN, RUN), :], sem.at[k]) for k, r in enumerate(b_refs)]
        for cp in copies:
            cp.start()

        def one(k, carry):
            rows = pl.ds(pl.multiple_of(k * RUN, RUN), RUN)
            pltpu.make_async_copy(b_scr.at[rows, :], b_scr.at[rows, :], sem.at[k]).wait()
            gated(rows, pl.ds(0, tn))
            return carry

        lax.fori_loop(0, n_in, one, 0)

    @pl.when((i > 0) & (i < nk))
    def _():
        gated(slice(None), pl.ds(pl.multiple_of(i * tn, tn), tn))

    @pl.when(i >= nk)
    def _():
        d = jnp.dot(u_scr[...], wd_ref[...], preferred_element_type=F32).astype(BF)
        half = d.shape[0] // 2
        keep_ref[...] = d[:half]
        send_ref[...] = d[half:]


def mlp(bs, wg, wu, wd, after=(), tn=256, td=256):
    rows, dim = RUN * len(bs), bs[0].shape[1]
    ffn = wg.shape[1]
    nk, nd = ffn // tn, dim // td
    up = lambda i: (0, jnp.minimum(i, nk - 1))
    dn = lambda i: (0, jnp.maximum(i - nk, 0))
    return pl.pallas_call(
        ordered(functools.partial(mlp_kernel, n_in=len(bs), tn=tn, nk=nk), len(bs) + 3, after),
        grid=(nk + nd,),
        in_specs=[ANY] * len(bs) + [pl.BlockSpec((dim, tn), up), pl.BlockSpec((dim, tn), up), pl.BlockSpec((ffn, td), dn)]
        + [ANY] * len(after),
        out_specs=[pl.BlockSpec((rows // 2, td), dn)] * 2,
        out_shape=[jax.ShapeDtypeStruct((rows // 2, dim), BF)] * 2,
        scratch_shapes=[pltpu.VMEM((rows, dim), BF), pltpu.VMEM((rows, ffn), BF), pltpu.SemaphoreType.DMA((len(bs),))],
        name="mlp", compiler_params=params(1),
        cost_estimate=pl.CostEstimate(flops=6 * rows * dim * ffn, transcendentals=rows * ffn,
                                      bytes_accessed=6 * dim * ffn + 4 * rows * dim),
    )(*bs, wg, wu, wd, *after)


def sum_kernel(*refs):
    p_ref, r_ref, t_ref, y_ref, z_ref = refs[-5:]
    total = p_ref[...].astype(F32) + r_ref[...].astype(F32) + t_ref[...].astype(F32)
    z_ref[...] = (y_ref[...].astype(F32) + total.astype(BF).astype(F32)).astype(BF)


def sum_run(z, keep, recv, far, y, y_at, j, n_runs, after=(), tile=64):
    dim = y.shape[1]
    per = RUN // tile
    spec = pl.BlockSpec((tile, dim), lambda i: (i, 0))
    prev = () if z is None else (z,)
    return pl.pallas_call(
        ordered(sum_kernel, len(prev) + 4, after), grid=(per,),
        in_specs=[ANY] * len(prev) + [spec] * 3 + [pl.BlockSpec((tile, dim), lambda i: (y_at * per + i, 0))] + [ANY] * len(after),
        out_specs=pl.BlockSpec((tile, dim), lambda i: (j * per + i, 0)),
        out_shape=jax.ShapeDtypeStruct((n_runs * RUN, dim), BF),
        input_output_aliases={0: 0} if prev else {},
        name="zsum", compiler_params=params(1),
        cost_estimate=pl.CostEstimate(flops=6 * RUN * dim, transcendentals=0, bytes_accessed=10 * RUN * dim),
    )(*prev, keep, recv, far, y, *after)


def run_positions(xi, ci, y, cps, piece):
    def start(x, c):
        return (y if x == 0 else 2 * cps - 1 - y) * piece + c * (piece // 2)

    per = piece // 2 // RUN
    out = [start(xi, ci) + RUN * j for j in range(per)] + [start(xi, 1 - ci) + RUN * j for j in range(per)]
    for j in range(per):
        out += [start(1 - xi, ci) + RUN * j, start(1 - xi, 1 - ci) + RUN * j]
    return out


def block_list(tile, ids, pos, diag):
    runs = [(r, pos[r]) for r in ids]
    if diag is not None:
        n_tail = (len(runs) % 4) + 1
        tail = [(diag, pos[diag])] + runs[len(runs) - (n_tail - 1):]
        runs = runs[:len(runs) - (n_tail - 1)]
    else:
        n_tail = len(runs) % 4
        tail = runs[len(runs) - n_tail:]
        runs = runs[:len(runs) - n_tail]
    blocks = [[0, runs[i:i + 4]] for i in range(0, len(runs), 4)]
    if tail:
        full = tail + [(tail[0][0], FAR)] * (4 - len(tail))
        flags = (MASK0 if diag is not None or len(tail) < 2 else 0) | (MASK1 if len(tail) < 4 else 0)
        blocks.append([flags, full])
    blocks[-1][0] |= LAST
    return [[tile, flags, 0] + [r for r, _ in four] + [p for _, p in four] + [0] for flags, four in blocks]


def call_table(tiles, pos, pairs):
    rows, most = [], 0
    for t, tile in enumerate(tiles):
        ids, own = pairs[t]
        rows += block_list(t, ids, pos, tile if own else None)
    for row in rows:
        most = max(most, max(row[3:7]) + 1)
        row[2] = most
    return [len(rows)] + [pos[t] for t in tiles] + [v for row in rows for v in row], len(rows)


def work_tables(cps, piece):
    per = piece // 2 // RUN
    calls = [[j, per + j, 2 * per + 2 * j, 2 * per + 2 * j + 1] for j in range(per)]
    tabs, all_runs, sizes = [], [], []
    for y in range(cps):
        for xi in range(2):
            for ci in range(2):
                mine = run_positions(xi, ci, y, cps, piece)
                pos = mine + run_positions(xi, ci, 1 - y, cps, piece)
                all_runs.append(mine)
                tabs.append([])
                sizes.append([])
                for tiles in calls:
                    pairs = [([r for r in range(len(pos)) if pos[r] < pos[t]], True) for t in tiles]
                    tab, n = call_table(tiles, pos, pairs)
                    tabs[-1].append(tab)
                    sizes[-1].append(n)
    widths = [max(len(t[k]) for t in tabs) for k in range(len(calls))]
    flat = [[v for k, t in enumerate(tab) for v in t + [0] * (widths[k] - len(t))] for tab in tabs]
    bases = [sum(widths[:k]) for k in range(len(calls))]
    return np.array(flat, np.int32), np.array(all_runs, np.int32), bases, np.array(sizes).max(0) * 4


def solution(mesh):
    cps = mesh.shape['cp']
    row_spec = P('dp', ('cp', 'tp'), None)
    head_cols = P(None, 'tp', None)
    n_tp = mesh.shape['tp']

    over_core, over_x, over_both = (('tp', [(t, t ^ k) for t in range(n_tp)]) for k in (1, 2, 3))
    over_y = ('cp', [(i, i ^ 1) for i in range(cps)])

    def layer(x, g_attn, w_q, w_k, w_v, w_o, g_mlp, w_gate, w_up, w_down):
        x_rows = x[0]
        dim = x_rows.shape[1]
        n_run = x_rows.shape[0] // RUN
        piece = 2 * x_rows.shape[0]
        t_id, y_id = lax.axis_index('tp'), lax.axis_index('cp')
        np_tab, np_runs, bases, work = work_tables(cps, piece)
        dev = y_id * n_tp + t_id
        tab = lax.dynamic_index_in_dim(jnp.asarray(np_tab), dev, 0, keepdims=False)
        run_pos = lax.dynamic_index_in_dim(jnp.asarray(np_runs), dev, 0, keepdims=False)

        def tied(v, *others):
            return lax.optimization_barrier((v, *others))[0]

        def send(axis_pairs, v):
            return lax.ppermute(v, *axis_pairs)

        ga, gm = g_attn.reshape(1, dim), g_mlp.reshape(1, dim)
        own = []
        for j in range(n_run):
            own.append(norm_run(x_rows, ga, j, after=own[-1:]))
        far = [send(over_x, own[j]) for j in range(n_run)]
        mate = [send(over_core, own[j]) for j in range(n_run)]

        w_all = jnp.concatenate([tied(w, own[-1]).reshape(dim, -1) for w in (w_q, w_k, w_v)], axis=1)
        cos, sin = rope_tables(tied(run_pos, own[-1])[:, None] + jnp.arange(RUN, dtype=jnp.int32)[None, :])

        q_own, kv_own = qkv(own, w_all, cos, sin, 0)
        q_mate, kv_mate = qkv(mate, w_all, cos, sin, n_run, after=(kv_own,))
        kvs = [kv_own, kv_mate]
        q_far = []
        for j in range(n_run):
            here = tied(far[j], kvs[-1])
            q, kv = qkv([here, send(over_core, here)], w_all, cos, sin, 2 * n_run + 2 * j,
                         after=(kvs[-1],))
            q_far.append(q)
            kvs.append(kv)
        gate, last = kvs[3], kvs[-1]
        kvs = kvs + [send(over_y, kv) for kv in kvs]

        wo = w_o.reshape(-1, dim)
        half = wo.shape[0] // 2
        wo_gated = tied(wo, gate)
        wo_xa = send(over_x, lax.dynamic_slice_in_dim(wo_gated, y_id * half, half, axis=0))
        ws = [wo, send(over_core, wo_gated)]

        os, outs = [], []
        prev = last

        def attend(j):
            o_own, o_mate, o_far, o_fm = flash(
                tab, [q_own, q_mate, q_far[j]], [(0, j), (1, j), (2, 0), (2, 1)], kvs,
                base=bases[j], work=int(work[j]), after=(prev,))
            os.append([o_own, send(over_core, o_mate), send(over_x, o_far), send(over_both, o_fm)])
            return o_own

        def project(i):
            y, b0, b1 = out_proj(os[2 * i] + os[2 * i + 1], ws, x_rows, gm, i, after=(prev,))
            for k, b in enumerate((b0, b1)):
                outs.append((y, k, b, send(over_x, b), send(over_core, b)))
            return y

        prev = attend(0)
        wo_a = tied(wo_xa, prev)
        wo_xb = send(over_y, wo_a)
        ws += [wo_a, None, send(over_core, wo_a), None]
        prev = attend(1)
        prev = attend(2)
        wo_b = tied(wo_xb, prev)
        ws[3], ws[5] = wo_b, send(over_core, wo_b)
        prev = project(0)
        prev = attend(3)

        z, pending, relay = None, None, {}

        def relay_b(j):
            here = tied(outs[j][3], prev)
            relay[j] = (here, send(over_core, here))

        relay_b(0)
        for j in range(n_run):
            y, k, b, _, b_mate = outs[j]
            keep, out = mlp([b, relay[j][0], b_mate, relay[j][1]], w_gate, w_up, w_down, after=(prev,))
            recv = send(over_core, out)
            prev = keep
            if j + 1 < n_run:
                relay_b(j + 1)
            if j == 0:
                prev = project(1)
            if pending is not None:
                prev = z = sum_run(z, *pending, j - 1, n_run, after=(prev,))
            kept = tied(keep, prev)
            prev = s_far = (kept[RUN:].astype(F32) + recv[RUN:].astype(F32)).astype(BF)
            pending = (keep, recv, send(over_x, s_far), y, k)
        z = sum_run(z, *pending, n_run - 1, n_run)
        return z[None]

    return jax.shard_map(layer, mesh=mesh,
                         in_specs=(row_spec, P(), head_cols, head_cols, head_cols, P('tp', None, None),
                                   P(), P(None, 'tp'), P(None, 'tp'), P('tp', None)),
                         out_specs=row_spec, check_vma=False)
```

```python
import functools
import math
import jax
import jax.numpy as jnp
import numpy as np
from jax import lax
from jax.experimental import pallas as pl
from jax.experimental.pallas import tpu as pltpu
from jax.sharding import PartitionSpec as P

NORM_EPS = 1e-5
ROPE_THETA = 500000.0
HD = 128
RUN = 256
NEG = -1e30
FAR = 1 << 29
LOG2E = math.log2(math.e)
DN = (((1,), (0,)), ((), ()))
VMEM = 67043328
BF = jnp.bfloat16
F32 = jnp.float32
ANY = pl.BlockSpec(memory_space=pltpu.HBM)


def params(n):
    return pltpu.CompilerParams(dimension_semantics=("arbitrary",) * n, vmem_limit_bytes=VMEM)


def rope_tables(positions):
    half = HD // 2
    inv_freq = ROPE_THETA ** (-2.0 * jnp.arange(half, dtype=F32) / HD)
    angles = inv_freq[:, None] * positions.astype(F32)[..., None, :]
    return jnp.cos(angles), jnp.sin(angles)


def norm_rows(rows, gain):
    f = rows.astype(F32)
    mean_sq = jnp.mean(f * f, axis=-1, keepdims=True)
    return (f * lax.rsqrt(mean_sq + NORM_EPS) * gain.astype(F32)).astype(BF)


def ordered(kernel, n_in, after):
    n = len(after)
    return lambda *refs: kernel(*refs[:n_in], *refs[n_in + n:])


def load_all(pairs, sem):
    copies = [pltpu.make_async_copy(src, dst, sem.at[i]) for i, (src, dst) in enumerate(pairs)]
    for cp in copies:
        cp.start()
    for cp in copies:
        cp.wait()


def norm_kernel(x_ref, g_ref, o_ref):
    o_ref[...] = norm_rows(x_ref[...], g_ref[...])


def norm_run(x_rows, gain, j, after=(), tile=128):
    dim = x_rows.shape[1]
    per = RUN // tile
    return pl.pallas_call(
        ordered(norm_kernel, 2, after), grid=(per,),
        in_specs=[pl.BlockSpec((tile, dim), lambda i: (j * per + i, 0)), pl.BlockSpec((1, dim), lambda i: (0, 0))]
        + [ANY] * len(after),
        out_specs=pl.BlockSpec((tile, dim), lambda i: (i, 0)),
        out_shape=jax.ShapeDtypeStruct((RUN, dim), BF),
        name="norm", compiler_params=params(1),
        cost_estimate=pl.CostEstimate(flops=8 * RUN * dim, transcendentals=0, bytes_accessed=4 * RUN * dim),
    )(x_rows, gain, *after)


def qkv_kernel(*refs, n_in, n_q, group):
    a_refs = refs[:n_in]
    w_ref, cos_ref, sin_ref, q_ref, kv_ref, a_scr, sem = refs[n_in:]
    n = pl.program_id(0)
    heads = w_ref.shape[1] // HD

    @pl.when(n == 0)
    def _():
        for k, r in enumerate(a_refs):
            pltpu.make_async_copy(r, a_scr.at[pl.ds(k * RUN, RUN), :], sem.at[k]).start()

    def rope(f, i):
        f = f.astype(BF).astype(F32)
        lo, hi, cos, sin = f[:HD // 2], f[HD // 2:], cos_ref[i], sin_ref[i]
        return jnp.concatenate([lo * cos - hi * sin, hi * cos + lo * sin], axis=0)

    def one(k, carry):
        @pl.when(n == 0)
        def _():
            for i in range(group):
                rows = pl.ds(pl.multiple_of((k * group + i) * RUN, RUN), RUN)
                pltpu.make_async_copy(a_scr.at[rows, :], a_scr.at[rows, :], sem.at[k * group + i]).wait()

        rows = pl.ds(pl.multiple_of(k * group * RUN, group * RUN), group * RUN)
        r = jnp.dot(a_scr[rows, :], w_ref[...], preferred_element_type=F32)

        def piece(i, h):
            return r[i * RUN:(i + 1) * RUN, h * HD:(h + 1) * HD].T

        @pl.when(n < n_q)
        def _():
            for i in range(group):
                for h in range(heads):
                    q_ref[k * group + i, h * HD:(h + 1) * HD, :] = rope(piece(i, h), k * group + i).astype(BF)

        @pl.when(n == n_q)
        def _():
            for i in range(group):
                for h in range(heads // 2):
                    kv_ref[k * group + i, 0, :, h * HD:(h + 1) * HD] = rope(piece(i, h), k * group + i).T.astype(BF)
                    kv_ref[k * group + i, 1, h * HD:(h + 1) * HD, :] = piece(i, h + heads // 2).astype(BF)

        return carry

    lax.fori_loop(0, n_in // group, one, 0)


def qkv(rows, w_all, tables, after=(), group=2):
    n_in = len(rows)
    dim = w_all.shape[0]
    tn = 512
    n_q = w_all.shape[1] // tn - 1
    (cos, sin), first_run = tables
    at = first_run // n_in
    tab = pl.BlockSpec((n_in, HD // 2, RUN), lambda n: (at, 0, 0))
    return pl.pallas_call(
        ordered(functools.partial(qkv_kernel, n_in=n_in, n_q=n_q, group=group), n_in + 3, after),
        grid=(n_q + 1,),
        in_specs=[ANY] * n_in + [pl.BlockSpec((dim, tn), lambda n: (0, n)), tab, tab] + [ANY] * len(after),
        out_specs=[pl.BlockSpec((n_in, tn, RUN), lambda n: (0, jnp.minimum(n, n_q - 1), 0)),
                   pl.BlockSpec((n_in, 2, 256, 256), lambda n: (0, 0, 0, 0))],
        out_shape=[jax.ShapeDtypeStruct((n_in, n_q * tn, RUN), BF), jax.ShapeDtypeStruct((n_in, 2, 256, 256), BF)],
        scratch_shapes=[pltpu.VMEM((n_in * RUN, dim), BF), pltpu.SemaphoreType.DMA((n_in,))],
        name="qkv", compiler_params=params(1),
        cost_estimate=pl.CostEstimate(flops=2 * n_in * RUN * w_all.size, transcendentals=0,
                                      bytes_accessed=2 * (n_in * RUN * dim + w_all.size)),
    )(*rows, w_all, cos, sin, *after)


BLK = 12
MASK0, MASK1, LAST, FIRST, CARRY = 1, 2, 4, 8, 16
ST = HD + 16


def flash_kernel(tab_ref, *refs, q_src, kv_src, n_q, n_kv, st_src, n_st, base, G, n_tiles, n_heads, final):
    qs, kvs, sts = refs[:n_q], refs[n_q:n_q + n_kv], refs[n_q + n_kv:n_q + n_kv + n_st]
    n_out = n_tiles if final else 1
    at = n_q + n_kv + n_st
    outs = refs[at:at + n_out]
    q_scr, kv_scr, o_scr, st_scr, s_scr, mb_scr, acc_scr, m_scr, l_scr, q_sem, kv_sem, o_sem, st_sem = refs[at + n_out:]
    T = RUN
    c = (HD ** -0.5) * LOG2E
    n_blocks = tab_ref[base]
    carried = base + 1 + n_tiles
    row0 = base + 1 + 2 * n_tiles

    q_copies = [pltpu.make_async_copy(qs[a].at[i], q_scr.at[t], q_sem.at[t]) for t, (a, i) in enumerate(q_src)]
    kv_copies = [pltpu.make_async_copy(kvs[a].at[i], kv_scr.at[r], kv_sem.at[r]) for r, (a, i) in enumerate(kv_src)]
    for cp in q_copies:
        cp.start()
    for t, i in enumerate(st_src):
        if i is not None:
            @pl.when(tab_ref[carried + t] != 0)
            def _():
                pltpu.make_async_copy(sts[0].at[i], st_scr.at[t], st_sem.at[t]).start()
    for cp in kv_copies:
        cp.start()
    for cp in q_copies:
        cp.wait()

    def block(i):
        g = lax.div(i, n_blocks)
        return row0 + BLK * (i - g * n_blocks), g

    def arrived(have, need):
        def one(r, carry):
            pltpu.make_async_copy(kv_scr.at[r], kv_scr.at[r], kv_sem.at[r]).wait()
            return carry

        lax.fori_loop(have, need, one, 0)
        return jnp.maximum(have, need)

    def put(s, slot):
        s_scr[slot] = s
        mb = jnp.max(s.reshape(2 * RUN // 8, 8, T), axis=0)
        for r in (4, 2, 1):
            mb = jnp.maximum(mb, pltpu.roll(mb, r, 0))
        mb_scr[slot] = mb

    def stage_a(row, g, it, h):
        col = pl.multiple_of(g * HD, HD)
        qt = q_scr[tab_ref[row], pl.ds(pl.multiple_of((g * G + h) * HD, HD), HD), :]
        put(jnp.concatenate([lax.dot_general(kv_scr[tab_ref[row + 3 + 2 * it + k], 0, :, pl.ds(col, HD)], qt, DN,
                                             preferred_element_type=F32) for k in range(2)], axis=0), it * G + h)

    def stage_b(row, g, it, h):
        slot = it * G + h
        col = pl.multiple_of(g * HD, HD)
        m_prev = m_scr[h]
        m_new = jnp.maximum(m_prev, mb_scr[slot])
        m_scr[h] = m_new
        m_c = m_new * c
        p = jnp.exp2(s_scr[slot].reshape(2 * RUN // 8, 8, T) * c - m_c[None])
        alpha = jnp.exp2(m_prev * c - m_c)
        l_scr[h] = l_scr[h] * alpha + jnp.sum(p, axis=0)
        pb = p.reshape(2 * RUN, T).astype(BF)
        pv = sum(lax.dot_general(kv_scr[tab_ref[row + 3 + 2 * it + k], 1, pl.ds(col, HD), :], pb[k * RUN:(k + 1) * RUN], DN,
                                 preferred_element_type=F32) for k in range(2))
        acc_scr[h] = (acc_scr[h].reshape(HD // 8, 8, T) * alpha[None]).reshape(HD, T) + pv

    def mask_item(row, it):
        key = lax.broadcasted_iota(jnp.int32, (RUN, T), 0)
        qry = lax.broadcasted_iota(jnp.int32, (RUN, T), 1) + tab_ref[base + 1 + tab_ref[row]]
        mask = jnp.concatenate([key + tab_ref[row + 7 + 2 * it + k] <= qry for k in range(2)], axis=0)
        for h in range(G):
            put(jnp.where(mask, s_scr[it * G + h], NEG), it * G + h)

    def finish(tile, g, get):
        for h in range(G):
            acc, l = get(h)
            o_scr[tile, :, pl.ds(pl.multiple_of((g * G + h) * HD, HD), HD)] = (acc / jnp.sum(l, axis=0, keepdims=True)).T.astype(BF)

        @pl.when(g == n_heads - 1)
        def _():
            for k in range(n_tiles):
                @pl.when(tile == k)
                def _():
                    pltpu.make_async_copy(o_scr.at[k], outs[k], o_sem.at[k]).start()

    if final and n_st:
        def idle(i, carry):
            tile, g = lax.div(i, n_heads), lax.rem(i, n_heads)

            @pl.when(tab_ref[carried + tile] == 2)
            def _():
                @pl.when(g == 0)
                def _():
                    pltpu.make_async_copy(st_scr.at[tile], st_scr.at[tile], st_sem.at[tile]).wait()

                finish(tile, g, lambda h: (st_scr[tile, g, h, :HD, :], st_scr[tile, g, h, HD + 8:, :]))

            return carry

        lax.fori_loop(0, n_tiles * n_heads, idle, 0)

    row, g = block(0)
    have = arrived(0, tab_ref[row + 2])
    for it in range(2):
        for h in range(G):
            stage_a(row, g, it, h)

    def body(i, have):
        row, g = block(i)
        nrow, ng = block(jnp.minimum(i + 1, n_heads * n_blocks - 1))
        have = arrived(have, tab_ref[nrow + 2])
        flags = tab_ref[row + 1]
        tile = tab_ref[row]

        @pl.when((flags & (FIRST | CARRY)) == FIRST)
        def _():
            acc_scr[...] = jnp.zeros_like(acc_scr)
            l_scr[...] = jnp.zeros_like(l_scr)
            m_scr[...] = jnp.full_like(m_scr, NEG)

        if n_st:
            @pl.when((flags & (FIRST | CARRY)) == (FIRST | CARRY))
            def _():
                @pl.when(g == 0)
                def _():
                    pltpu.make_async_copy(st_scr.at[tile], st_scr.at[tile], st_sem.at[tile]).wait()

                for h in range(G):
                    acc_scr[h] = st_scr[tile, g, h, :HD, :]
                    m_scr[h] = st_scr[tile, g, h, HD:HD + 8, :]
                    l_scr[h] = st_scr[tile, g, h, HD + 8:, :]

        @pl.when((flags & MASK0) != 0)
        def _():
            mask_item(row, 0)

        @pl.when((flags & MASK1) != 0)
        def _():
            mask_item(row, 1)

        for it in range(2):
            for h in range(G):
                stage_b(row, g, it, h)
                stage_a(nrow, ng, it, h)

        @pl.when((flags & LAST) != 0)
        def _():
            if final:
                finish(tile, g, lambda h: (acc_scr[h], l_scr[h]))
            else:
                for h in range(G):
                    st_scr[tile, g, h, :HD, :] = acc_scr[h]
                    st_scr[tile, g, h, HD:HD + 8, :] = m_scr[h]
                    st_scr[tile, g, h, HD + 8:, :] = l_scr[h]

                @pl.when(g == n_heads - 1)
                def _():
                    pltpu.make_async_copy(st_scr.at[tile], outs[0].at[tile], o_sem.at[tile]).start()

        return have

    have = lax.fori_loop(0, n_heads * n_blocks, body, have)
    arrived(have, len(kv_src))
    if final:
        for k in range(n_tiles):
            pltpu.make_async_copy(o_scr.at[k], outs[k], o_sem.at[k]).wait()
    else:
        def wait_out(i, carry):
            row = row0 + BLK * i

            @pl.when((tab_ref[row + 1] & LAST) != 0)
            def _():
                t = tab_ref[row]
                pltpu.make_async_copy(st_scr.at[t], st_scr.at[t], o_sem.at[t]).wait()

            return carry

        lax.fori_loop(0, n_blocks, wait_out, 0)


def flash(tab, qs, q_src, kvs, *, base, work, st=None, st_src=None, st_tiles=None, after=()):
    nq = qs[0].shape[1]
    n_heads = 2
    G = nq // HD // n_heads
    n_tiles = len(q_src)
    final = st_tiles is None
    kv_src = [(a, i) for a, kv in enumerate(kvs) for i in range(kv.shape[0])]
    n_runs = len(kv_src)
    slots = 2 * G
    sts = () if st is None else (st,)
    n_in = 1 + len(qs) + len(kvs) + len(sts)
    state = (n_heads, G, ST, RUN)
    has_st = not final or sts
    return pl.pallas_call(
        ordered(functools.partial(flash_kernel, q_src=q_src, kv_src=kv_src, n_q=len(qs), n_kv=len(kvs),
                                  st_src=st_src or [None] * n_tiles, n_st=len(sts), base=base, G=G, n_tiles=n_tiles,
                                  n_heads=n_heads, final=final), n_in, after),
        grid_spec=pltpu.PrefetchScalarGridSpec(
            num_scalar_prefetch=1, grid=(),
            in_specs=[ANY] * (n_in - 1 + len(after)),
            out_specs=[ANY] * n_tiles if final else [ANY],
            scratch_shapes=[pltpu.VMEM((n_tiles, nq, RUN), BF),
                            pltpu.VMEM((n_runs, 2, 256, 256), BF),
                            pltpu.VMEM((n_tiles if final else 1, RUN, nq), BF),
                            pltpu.VMEM((n_tiles if has_st else 1, *state), F32),
                            pltpu.VMEM((slots, 2 * RUN, RUN), F32),
                            pltpu.VMEM((slots, 8, RUN), F32),
                            pltpu.VMEM((G, HD, RUN), F32),
                            pltpu.VMEM((G, 8, RUN), F32),
                            pltpu.VMEM((G, 8, RUN), F32),
                            pltpu.SemaphoreType.DMA((n_tiles,)),
                            pltpu.SemaphoreType.DMA((n_runs,)),
                            pltpu.SemaphoreType.DMA((n_tiles,)),
                            pltpu.SemaphoreType.DMA((n_tiles,))]),
        out_shape=[jax.ShapeDtypeStruct((RUN, nq), BF)] * n_tiles if final
        else [jax.ShapeDtypeStruct((st_tiles, *state), F32)],
        input_output_aliases={n_in - 1: 0} if sts and not final else {},
        name="flash" if final else "flash_part", compiler_params=pltpu.CompilerParams(vmem_limit_bytes=VMEM),
        cost_estimate=pl.CostEstimate(flops=8 * work * RUN * RUN * nq, transcendentals=work * RUN * RUN * nq // HD,
                                      bytes_accessed=n_runs * 2 * 256 * 256 * 2 + 4 * n_tiles * RUN * nq),
    )(tab, *qs, *kvs, *sts, *after)


def out_kernel(*refs, blocks, n_w):
    o_refs, w_refs = refs[:4], refs[4:4 + n_w]
    x_ref, g_ref, y_ref, b_ref, o_scr, w_scr, acc_scr, o_sem, w_sem = refs[4 + n_w:]
    width = o_refs[0].shape[1]
    half = width // 2
    n_slots = w_scr.shape[0]

    def fetch(k):
        for i, parts in enumerate(blocks):
            @pl.when(k == i)
            def _():
                at = 0
                for a, r0, n in parts:
                    pltpu.make_async_copy(w_refs[a].at[pl.ds(r0, n), :], w_scr.at[i % n_slots, pl.ds(at, n), :],
                                          w_sem.at[i % n_slots]).start()
                    at += n

    for i in range(n_slots - 1):
        fetch(jnp.int32(i))
    mine = lax.axis_index('cp')
    pairs = [(o_refs[0], o_scr.at[:, pl.ds(0, width)]), (o_refs[1], o_scr.at[:, pl.ds(width, width)])]
    for k in range(2, 4):
        for p, part in enumerate((mine, 1 - mine)):
            pairs.append((o_refs[k].at[:, pl.ds(pl.multiple_of(part * half, half), half)],
                          o_scr.at[:, pl.ds(k * width + p * half, half)]))
    load_all(pairs, o_sem)
    acc_scr[...] = jnp.zeros_like(acc_scr)

    def one(k, carry):
        fetch(k + n_slots - 1)
        slot = lax.rem(k, n_slots)
        pltpu.make_async_copy(w_scr.at[slot], w_scr.at[slot], w_sem.at[slot]).wait()
        acc_scr[...] += jnp.dot(o_scr[:, pl.ds(pl.multiple_of(k * half, half), half)], w_scr[slot], preferred_element_type=F32)
        return carry

    lax.fori_loop(0, len(blocks), one, 0)

    def rows32(i, carry):
        rows = pl.ds(pl.multiple_of(i * 32, 32), 32)
        y = (x_ref[rows, :].astype(F32) + acc_scr[rows, :].astype(BF).astype(F32)).astype(BF)
        y_ref[rows, :] = y
        b_ref[rows, :] = norm_rows(y, g_ref[...])
        return carry

    lax.fori_loop(0, RUN // 32, rows32, 0)


def out_proj(os, ws, blocks, x_rows, gain, j, after=()):
    dim = x_rows.shape[1]
    width = os[0].shape[1]
    one = lambda s: pl.BlockSpec((RUN, dim), lambda i: (s, 0))
    n_after = len(after)
    return pl.pallas_call(
        ordered(functools.partial(out_kernel, blocks=blocks, n_w=len(ws)), 6 + len(ws), after),
        grid=(1,),
        in_specs=[ANY] * (4 + len(ws)) + [one(j), pl.BlockSpec((1, dim), lambda i: (0, 0))] + [ANY] * n_after,
        out_specs=[one(0)] * 2,
        out_shape=[jax.ShapeDtypeStruct((RUN, dim), BF)] * 2,
        scratch_shapes=[pltpu.VMEM((RUN, 4 * width), BF), pltpu.VMEM((3, width // 2, dim), BF), pltpu.VMEM((RUN, dim), F32),
                        pltpu.SemaphoreType.DMA((6,)), pltpu.SemaphoreType.DMA((3,))],
        name="outp", compiler_params=params(1),
        cost_estimate=pl.CostEstimate(flops=8 * RUN * width * dim, transcendentals=0,
                                      bytes_accessed=8 * width * dim + 8 * RUN * dim),
    )(*os, *ws, x_rows, gain, *after)


def mlp_kernel(*refs, n_in, tn, nk):
    b_refs = refs[:n_in]
    wg_ref, wu_ref, wd_ref, keep_ref, send_ref, b_scr, u_scr, sem = refs[n_in:]
    i = pl.program_id(0)

    def gated(rows, cols):
        b = b_scr[rows, :]
        gate = jnp.dot(b, wg_ref[...], preferred_element_type=F32)
        up = jnp.dot(b, wu_ref[...], preferred_element_type=F32)
        u_scr[rows, cols] = (jax.nn.silu(gate) * up).astype(BF)

    @pl.when(i == 0)
    def _():
        copies = [pltpu.make_async_copy(r, b_scr.at[pl.ds(k * RUN, RUN), :], sem.at[k]) for k, r in enumerate(b_refs)]
        for cp in copies:
            cp.start()

        def one(k, carry):
            rows = pl.ds(pl.multiple_of(k * RUN, RUN), RUN)
            pltpu.make_async_copy(b_scr.at[rows, :], b_scr.at[rows, :], sem.at[k]).wait()
            gated(rows, pl.ds(0, tn))
            return carry

        lax.fori_loop(0, n_in, one, 0)

    @pl.when((i > 0) & (i < nk))
    def _():
        gated(slice(None), pl.ds(pl.multiple_of(i * tn, tn), tn))

    @pl.when(i >= nk)
    def _():
        d = jnp.dot(u_scr[...], wd_ref[...], preferred_element_type=F32).astype(BF)
        half = d.shape[0] // 2
        keep_ref[...] = d[:half]
        send_ref[...] = d[half:]


def mlp(bs, wg, wu, wd, after=(), tn=256, td=256):
    rows, dim = RUN * len(bs), bs[0].shape[1]
    ffn = wg.shape[1]
    nk, nd = ffn // tn, dim // td
    up = lambda i: (0, jnp.minimum(i, nk - 1))
    dn = lambda i: (0, jnp.maximum(i - nk, 0))
    return pl.pallas_call(
        ordered(functools.partial(mlp_kernel, n_in=len(bs), tn=tn, nk=nk), len(bs) + 3, after),
        grid=(nk + nd,),
        in_specs=[ANY] * len(bs) + [pl.BlockSpec((dim, tn), up), pl.BlockSpec((dim, tn), up), pl.BlockSpec((ffn, td), dn)]
        + [ANY] * len(after),
        out_specs=[pl.BlockSpec((rows // 2, td), dn)] * 2,
        out_shape=[jax.ShapeDtypeStruct((rows // 2, dim), BF)] * 2,
        scratch_shapes=[pltpu.VMEM((rows, dim), BF), pltpu.VMEM((rows, ffn), BF), pltpu.SemaphoreType.DMA((len(bs),))],
        name="mlp", compiler_params=params(1),
        cost_estimate=pl.CostEstimate(flops=6 * rows * dim * ffn, transcendentals=rows * ffn,
                                      bytes_accessed=6 * dim * ffn + 4 * rows * dim),
    )(*bs, wg, wu, wd, *after)


def sum_kernel(*refs):
    p_ref, r_ref, t_ref, y_ref, z_ref = refs[-5:]
    total = p_ref[...].astype(F32) + r_ref[...].astype(F32) + t_ref[...].astype(F32)
    z_ref[...] = (y_ref[...].astype(F32) + total.astype(BF).astype(F32)).astype(BF)


def sum_run(z, keep, recv, far, y, j, n_runs, after=(), tile=64):
    dim = y.shape[1]
    per = RUN // tile
    spec = pl.BlockSpec((tile, dim), lambda i: (i, 0))
    prev = () if z is None else (z,)
    return pl.pallas_call(
        ordered(sum_kernel, len(prev) + 4, after), grid=(per,),
        in_specs=[ANY] * len(prev) + [spec] * 4 + [ANY] * len(after),
        out_specs=pl.BlockSpec((tile, dim), lambda i: (j * per + i, 0)),
        out_shape=jax.ShapeDtypeStruct((n_runs * RUN, dim), BF),
        input_output_aliases={0: 0} if prev else {},
        name="zsum", compiler_params=params(1),
        cost_estimate=pl.CostEstimate(flops=6 * RUN * dim, transcendentals=0, bytes_accessed=10 * RUN * dim),
    )(*prev, keep, recv, far, y, *after)


def run_positions(xi, ci, y, cps, piece):
    def start(x, c):
        return (y if x == 0 else 2 * cps - 1 - y) * piece + c * (piece // 2)

    per = piece // 2 // RUN
    out = [start(xi, ci) + RUN * j for j in range(per)] + [start(xi, 1 - ci) + RUN * j for j in range(per)]
    for j in range(per):
        out += [start(1 - xi, ci) + RUN * j, start(1 - xi, 1 - ci) + RUN * j]
    return out


def block_list(tile, ids, pos, diag):
    runs = [(r, pos[r]) for r in ids]
    if diag is not None:
        n_tail = (len(runs) % 4) + 1
        tail = [(diag, pos[diag])] + runs[len(runs) - (n_tail - 1):]
        runs = runs[:len(runs) - (n_tail - 1)]
    else:
        n_tail = len(runs) % 4
        tail = runs[len(runs) - n_tail:]
        runs = runs[:len(runs) - n_tail]
    blocks = [[0, runs[i:i + 4]] for i in range(0, len(runs), 4)]
    if tail:
        full = tail + [(tail[0][0], FAR)] * (4 - len(tail))
        flags = (MASK0 if diag is not None or len(tail) < 2 else 0) | (MASK1 if len(tail) < 4 else 0)
        blocks.append([flags, full])
    blocks[-1][0] |= LAST
    blocks[0][0] |= FIRST
    return [[tile, flags, 0] + [r for r, _ in four] + [p for _, p in four] + [0] for flags, four in blocks]


def call_table(tiles, pos, pairs, carry, idle):
    rows, most = [], 0
    carry = [c if pairs[t][0] or pairs[t][1] else idle for t, c in enumerate(carry)]
    for t, tile in enumerate(tiles):
        ids, own = pairs[t]
        if ids or own:
            mine = block_list(t, ids, pos, tile if own else None)
            mine[0][1] |= CARRY if carry[t] else 0
            rows += mine
    for row in rows:
        most = max(most, max(row[3:7]) + 1)
        row[2] = most
    return [len(rows)] + [pos[t] for t in tiles] + carry + [v for row in rows for v in row], len(rows)


def work_tables(cps, piece):
    per = piece // 2 // RUN
    early = 2 * per + 2
    later = early + 4
    stage = lambda r: 0 if r < early else 1 if r < later else 2
    calls = [(0, list(range(early))), (1, list(range(later)))]
    calls += [(2, [j, per + j, 2 * per + 2 * j, 2 * per + 2 * j + 1]) for j in range(per)]
    tabs, all_runs, sizes = [], [], []
    for y in range(cps):
        for xi in range(2):
            for ci in range(2):
                mine = run_positions(xi, ci, y, cps, piece)
                pos = mine + run_positions(xi, ci, 1 - y, cps, piece)
                all_runs.append(mine)
                tabs.append([])
                sizes.append([])
                for now, tiles in calls:
                    pairs, carry = [], []
                    for t in tiles:
                        seen = [r for r in range(len(pos)) if pos[r] < pos[t]]
                        pairs.append(([r for r in seen if max(stage(r), stage(t)) == now], stage(t) == now))
                        carry.append(int(stage(t) < now))
                    tab, n = call_table(tiles, pos, pairs, carry, 2 if now == 2 else 0)
                    tabs[-1].append(tab)
                    sizes[-1].append(n)
    widths = [max(len(t[k]) for t in tabs) for k in range(len(calls))]
    flat = [[v for k, t in enumerate(tab) for v in t + [0] * (widths[k] - len(t))] for tab in tabs]
    bases = [sum(widths[:k]) for k in range(len(calls))]
    return np.array(flat, np.int32), np.array(all_runs, np.int32), bases, np.array(sizes).max(0) * 4


def solution(mesh):
    cps = mesh.shape['cp']
    row_spec = P('dp', ('cp', 'tp'), None)
    head_cols = P(None, 'tp', None)
    n_tp = mesh.shape['tp']

    over_core, over_x, over_both = (('tp', [(t, t ^ k) for t in range(n_tp)]) for k in (1, 2, 3))
    over_y = ('cp', [(i, i ^ 1) for i in range(cps)])

    def layer(x, g_attn, w_q, w_k, w_v, w_o, g_mlp, w_gate, w_up, w_down):
        x_rows = x[0]
        dim = x_rows.shape[1]
        n_run = x_rows.shape[0] // RUN
        piece = 2 * x_rows.shape[0]
        t_id, y_id = lax.axis_index('tp'), lax.axis_index('cp')
        np_tab, np_runs, bases, work = work_tables(cps, piece)
        dev = y_id * n_tp + t_id
        tab = lax.dynamic_index_in_dim(jnp.asarray(np_tab), dev, 0, keepdims=False)
        order = list(range(2 * n_run)) + [2 * n_run + i for i in (2, 3, 4, 5, 0, 1, 6, 7)]
        run_pos = lax.dynamic_index_in_dim(jnp.asarray(np_runs[:, order]), dev, 0, keepdims=False)

        def tied(v, *others):
            return lax.optimization_barrier((v, *others))[0]

        def send(axis_pairs, v):
            return lax.ppermute(v, *axis_pairs)

        ga, gm = g_attn.reshape(1, dim), g_mlp.reshape(1, dim)
        own = []
        for j in range(n_run):
            own.append(norm_run(x_rows, ga, j, after=own[-1:]))
        far = [send(over_x, own[j]) for j in range(n_run)]
        mate = [send(over_core, own[j]) for j in range(n_run)]

        w_all = jnp.concatenate([tied(w, own[-1]).reshape(dim, -1) for w in (w_q, w_k, w_v)], axis=1)
        tables = rope_tables(tied(run_pos, own[-1])[:, None] + jnp.arange(RUN, dtype=jnp.int32)[None, :])

        def relayed(j, after):
            here = tied(far[j], after)
            return [here, send(over_core, here)]

        q_own, kv_own = qkv(own, w_all, (tables, 0))
        q_mate, kv_mate = qkv(mate, w_all, (tables, n_run), after=(kv_own,))
        q_a, kv_a = qkv(relayed(0, kv_mate), w_all, (tables, 2 * n_run + 4), after=(kv_mate,))

        wo = w_o.reshape(-1, dim)
        half = wo.shape[0] // 2
        n_piece = 4
        rows = half // n_piece
        wo_gated = tied(wo, kv_a)
        wo_x = [send(over_x, lax.dynamic_slice_in_dim(wo_gated, y_id * half + p * rows, rows, axis=0))
                for p in range(n_piece)]
        wo_c = send(over_core, wo_gated)
        early = relayed(1, kv_a)

        tile = lambda a, n: [(a, i) for i in range(n)]
        tiles = tile(0, n_run) + tile(1, n_run) + tile(2, 2)
        st, = flash(tab, [q_own, q_mate, q_a], tiles, [kv_own, kv_mate, kv_a], base=bases[0],
                   work=int(work[0]), st_tiles=len(tiles) + 4)
        q_b, kv_b = qkv(early + relayed(2, st), w_all, (tables, 2 * n_run), after=(st,))
        st, = flash(tab, [q_own, q_mate, q_a, q_b], tiles + tile(3, 4), [kv_own, kv_mate, kv_a, kv_b],
                   base=bases[1], work=int(work[1]), st=st, st_src=list(range(len(tiles))) + [None] * 4,
                   st_tiles=len(tiles) + 4)
        q_c, kv_c = qkv(relayed(3, st), w_all, (tables, 2 * n_run + 6), after=(st,))
        kvs = [kv_own, kv_mate, kv_a, kv_b, kv_c]
        kvs = kvs + [send(over_y, kv) for kv in kvs]
        q_far = [(q_a, 0), (q_b, 0), (q_b, 2), (q_c, 0)]

        os, outs, prev = [], [], kv_c
        wo_a, wo_ya, wo_yb = {}, {}, {}

        def forward_w(p):
            here = tied(wo_x[p], prev)
            wo_ya[p] = (here, send(over_core, here))
            wo_a[p] = send(over_y, here)

        def relay_w(p):
            here = tied(wo_a[p], prev)
            wo_yb[p] = (here, send(over_core, here))

        def attend(j):
            q, at = q_far[j]
            held = 2 * n_run + 2 * j
            carried = [j, n_run + j] + ([held, held + 1] if j + 1 < n_run else [None, None])
            o_own, o_mate, o_far, o_fm = flash(
                tab, [q_own, q_mate, q], [(0, j), (1, j), (2, at), (2, at + 1)], kvs,
                base=bases[2 + j], work=int(work[2 + j]), st=st, st_src=carried, after=(prev,))
            os.append([o_own, send(over_core, o_mate), send(over_x, o_far), send(over_both, o_fm)])
            return o_own

        def project(j):
            ws = [wo, wo_c]
            blocks = [[(0, 0, half)], [(0, half, half)], [(1, 0, half)], [(1, half, half)]]
            for k in range(2):
                for held in (wo_ya, wo_yb):
                    blocks.append([(len(ws) + p, 0, rows) for p in range(n_piece)])
                    ws += [held[p][k] for p in range(n_piece)]
            y, b = out_proj(os[j], ws, blocks, x_rows, gm, j, after=(prev,))
            outs.append((y, b, send(over_x, b), send(over_core, b)))
            return y

        forward_w(0)
        prev = attend(0)
        forward_w(1)
        relay_w(0)
        prev = attend(1)
        forward_w(2)
        forward_w(3)
        relay_w(1)
        prev = attend(2)
        relay_w(2)
        relay_w(3)
        prev = project(0)
        prev = attend(3)
        prev = project(1)

        z, sums, relay = None, [], {}

        def relay_b(j):
            here = tied(outs[j][2], prev)
            relay[j] = (here, send(over_core, here))

        def finish(j):
            return sum_run(z, *sums[j], j, n_run, after=() if prev is z else (prev,))

        relay_b(0)
        for j in range(n_run):
            y, b, _, b_mate = outs[j]
            keep, out = mlp([b, relay[j][0], b_mate, relay[j][1]], w_gate, w_up, w_down, after=(prev,))
            recv = send(over_core, out)
            prev = keep
            if j + 1 < n_run:
                relay_b(j + 1)
            if j + 2 < n_run:
                prev = project(j + 2)
            else:
                prev = z = finish(j - 2)
            kept = tied(keep, prev)
            prev = s_far = (kept[RUN:].astype(F32) + recv[RUN:].astype(F32)).astype(BF)
            sums.append((keep, recv, send(over_x, s_far), y))
        for j in range(n_run - 2, n_run):
            prev = z = finish(j)
        return z[None]

    return jax.shard_map(layer, mesh=mesh,
                         in_specs=(row_spec, P(), head_cols, head_cols, head_cols, P('tp', None, None),
                                   P(), P(None, 'tp'), P(None, 'tp'), P('tp', None)),
                         out_specs=row_spec, check_vma=False)
```

```python
import functools
import math
import jax
import jax.numpy as jnp
import numpy as np
from jax import lax
from jax.experimental import pallas as pl
from jax.experimental.pallas import tpu as pltpu
from jax.sharding import PartitionSpec as P

NORM_EPS = 1e-5
ROPE_THETA = 500000.0
HD = 128
RUN = 256
NEG = -1e30
FAR = 1 << 29
LOG2E = math.log2(math.e)
DN = (((1,), (0,)), ((), ()))
VMEM = 67043328
BF = jnp.bfloat16
F32 = jnp.float32
ANY = pl.BlockSpec(memory_space=pltpu.HBM)


def params(n):
    return pltpu.CompilerParams(dimension_semantics=("arbitrary",) * n, vmem_limit_bytes=VMEM)


def rope_tables(positions):
    half = HD // 2
    inv_freq = ROPE_THETA ** (-2.0 * jnp.arange(half, dtype=F32) / HD)
    angles = inv_freq[:, None] * positions.astype(F32)[..., None, :]
    return jnp.cos(angles), jnp.sin(angles)


def norm_rows(rows, gain):
    f = rows.astype(F32)
    mean_sq = jnp.mean(f * f, axis=-1, keepdims=True)
    return (f * lax.rsqrt(mean_sq + NORM_EPS) * gain.astype(F32)).astype(BF)


def ordered(kernel, n_in, after):
    n = len(after)
    return lambda *refs: kernel(*refs[:n_in], *refs[n_in + n:])


def norm_kernel(x_ref, g_ref, o_ref):
    o_ref[...] = norm_rows(x_ref[...], g_ref[...])


def norm_run(x_rows, gain, j, after=(), tile=128):
    dim = x_rows.shape[1]
    per = RUN // tile
    return pl.pallas_call(
        ordered(norm_kernel, 2, after), grid=(per,),
        in_specs=[pl.BlockSpec((tile, dim), lambda i: (j * per + i, 0)), pl.BlockSpec((1, dim), lambda i: (0, 0))]
        + [ANY] * len(after),
        out_specs=pl.BlockSpec((tile, dim), lambda i: (i, 0)),
        out_shape=jax.ShapeDtypeStruct((RUN, dim), BF),
        name="norm", compiler_params=params(1),
        cost_estimate=pl.CostEstimate(flops=8 * RUN * dim, transcendentals=0, bytes_accessed=4 * RUN * dim),
    )(x_rows, gain, *after)


def qkv_kernel(*refs, n_in, n_q, group):
    a_refs = refs[:n_in]
    w_ref, cos_ref, sin_ref, q_ref, kv_ref, a_scr, sem = refs[n_in:]
    n = pl.program_id(0)
    heads = w_ref.shape[1] // HD

    @pl.when(n == 0)
    def _():
        for k, r in enumerate(a_refs):
            pltpu.make_async_copy(r, a_scr.at[pl.ds(k * RUN, RUN), :], sem.at[k]).start()

    def rope(f, i):
        f = f.astype(BF).astype(F32)
        lo, hi, cos, sin = f[:HD // 2], f[HD // 2:], cos_ref[i], sin_ref[i]
        return jnp.concatenate([lo * cos - hi * sin, hi * cos + lo * sin], axis=0)

    def one(k, carry):
        @pl.when(n == 0)
        def _():
            for i in range(group):
                rows = pl.ds(pl.multiple_of((k * group + i) * RUN, RUN), RUN)
                pltpu.make_async_copy(a_scr.at[rows, :], a_scr.at[rows, :], sem.at[k * group + i]).wait()

        rows = pl.ds(pl.multiple_of(k * group * RUN, group * RUN), group * RUN)
        r = jnp.dot(a_scr[rows, :], w_ref[...], preferred_element_type=F32)

        def piece(i, h):
            return r[i * RUN:(i + 1) * RUN, h * HD:(h + 1) * HD].T

        @pl.when(n < n_q)
        def _():
            for i in range(group):
                for h in range(heads):
                    q_ref[k * group + i, h * HD:(h + 1) * HD, :] = rope(piece(i, h), k * group + i).astype(BF)

        @pl.when(n == n_q)
        def _():
            for i in range(group):
                for h in range(heads // 2):
                    kv_ref[k * group + i, 0, :, h * HD:(h + 1) * HD] = rope(piece(i, h), k * group + i).T.astype(BF)
                    kv_ref[k * group + i, 1, h * HD:(h + 1) * HD, :] = piece(i, h + heads // 2).astype(BF)

        return carry

    lax.fori_loop(0, n_in // group, one, 0)


def qkv(rows, w_all, tables, after=(), group=2):
    n_in = len(rows)
    dim = w_all.shape[0]
    tn = 512
    n_q = w_all.shape[1] // tn - 1
    (cos, sin), first_run = tables
    at = first_run // n_in
    tab = pl.BlockSpec((n_in, HD // 2, RUN), lambda n: (at, 0, 0))
    return pl.pallas_call(
        ordered(functools.partial(qkv_kernel, n_in=n_in, n_q=n_q, group=group), n_in + 3, after),
        grid=(n_q + 1,),
        in_specs=[ANY] * n_in + [pl.BlockSpec((dim, tn), lambda n: (0, n)), tab, tab] + [ANY] * len(after),
        out_specs=[pl.BlockSpec((n_in, tn, RUN), lambda n: (0, jnp.minimum(n, n_q - 1), 0)),
                   pl.BlockSpec((n_in, 2, 256, 256), lambda n: (0, 0, 0, 0))],
        out_shape=[jax.ShapeDtypeStruct((n_in, n_q * tn, RUN), BF), jax.ShapeDtypeStruct((n_in, 2, 256, 256), BF)],
        scratch_shapes=[pltpu.VMEM((n_in * RUN, dim), BF), pltpu.SemaphoreType.DMA((n_in,))],
        name="qkv", compiler_params=params(1),
        cost_estimate=pl.CostEstimate(flops=2 * n_in * RUN * w_all.size, transcendentals=0,
                                      bytes_accessed=2 * (n_in * RUN * dim + w_all.size)),
    )(*rows, w_all, cos, sin, *after)


BLK = 12
LAST, FIRST, CARRY = 16, 32, 64
ST = HD + 16


def flash_kernel(tab_ref, *refs, q_src, kv_src, n_q, n_kv, st_src, n_st, base, G, n_tiles, n_heads, final):
    qs, kvs, sts = refs[:n_q], refs[n_q:n_q + n_kv], refs[n_q + n_kv:n_q + n_kv + n_st]
    n_out = n_tiles if final else 1
    at = n_q + n_kv + n_st
    outs = refs[at:at + n_out]
    q_scr, kv_scr, o_scr, st_scr, s_scr, mb_scr, acc_scr, m_scr, l_scr, q_sem, kv_sem, o_sem, st_sem = refs[at + n_out:]
    T = RUN
    c = (HD ** -0.5) * LOG2E
    n_blocks = tab_ref[base]
    carried = base + 1 + n_tiles
    row0 = base + 1 + 2 * n_tiles

    q_copies = [pltpu.make_async_copy(qs[a].at[i], q_scr.at[t], q_sem.at[t]) for t, (a, i) in enumerate(q_src)]
    kv_copies = [pltpu.make_async_copy(kvs[a].at[i], kv_scr.at[r], kv_sem.at[r]) for r, (a, i) in enumerate(kv_src)]
    for cp in q_copies:
        cp.start()
    for t, i in enumerate(st_src):
        if i is not None:
            @pl.when(tab_ref[carried + t] != 0)
            def _():
                pltpu.make_async_copy(sts[0].at[i], st_scr.at[t], st_sem.at[t]).start()
    for cp in kv_copies:
        cp.start()
    for cp in q_copies:
        cp.wait()

    def block(i):
        g = lax.div(i, n_blocks)
        return row0 + BLK * (i - g * n_blocks), g

    def arrived(have, need):
        def one(r, carry):
            pltpu.make_async_copy(kv_scr.at[r], kv_scr.at[r], kv_sem.at[r]).wait()
            return carry

        lax.fori_loop(have, need, one, 0)
        return jnp.maximum(have, need)

    def put(s, h, k):
        s_scr[h, pl.ds(k * RUN, RUN), :] = s
        mb_scr[h, k] = jnp.max(s.reshape(RUN // 8, 8, T), axis=0)

    def stage_a(row, g, h):
        col = pl.multiple_of(g * HD, HD)
        qt = q_scr[tab_ref[row], pl.ds(pl.multiple_of((g * G + h) * HD, HD), HD), :]
        for k in range(4):
            put(lax.dot_general(kv_scr[tab_ref[row + 3 + k], 0, :, pl.ds(col, HD)], qt, DN, preferred_element_type=F32), h, k)

    def stage_b(row, g, h):
        col = pl.multiple_of(g * HD, HD)
        m_prev = m_scr[h]
        mb = jnp.maximum(jnp.maximum(mb_scr[h, 0], mb_scr[h, 1]), jnp.maximum(mb_scr[h, 2], mb_scr[h, 3]))
        for r in (4, 2, 1):
            mb = jnp.maximum(mb, pltpu.roll(mb, r, 0))
        m_new = jnp.maximum(m_prev, mb)
        m_scr[h] = m_new
        m_c = m_new * c
        alpha = jnp.exp2(m_prev * c - m_c)
        l, pv = l_scr[h] * alpha, None
        for k in range(4):
            p = jnp.exp2(s_scr[h, k * RUN:(k + 1) * RUN].reshape(RUN // 8, 8, T) * c - m_c[None])
            l = l + jnp.sum(p, axis=0)
            d = lax.dot_general(kv_scr[tab_ref[row + 3 + k], 1, pl.ds(col, HD), :], p.reshape(RUN, T).astype(BF), DN,
                                preferred_element_type=F32)
            pv = d if pv is None else pv + d
        l_scr[h] = l
        acc_scr[h] = (acc_scr[h].reshape(HD // 8, 8, T) * alpha[None]).reshape(HD, T) + pv

    def mask_runs(row, flags):
        qry = lax.broadcasted_iota(jnp.int32, (RUN, T), 1) + tab_ref[base + 1 + tab_ref[row]]
        key = lax.broadcasted_iota(jnp.int32, (RUN, T), 0)

        def one(k, carry):
            @pl.when((lax.shift_right_logical(flags, k) & 1) != 0)
            def _():
                mask = key + tab_ref[row + 7 + k] <= qry
                rows = pl.multiple_of(k * RUN, RUN)
                for h in range(G):
                    put(jnp.where(mask, s_scr[h, pl.ds(rows, RUN), :], NEG), h, k)

            return carry

        lax.fori_loop(0, 4, one, 0)

    def finish(tile, g, get):
        for h in range(G):
            acc, l = get(h)
            o_scr[tile, :, pl.ds(pl.multiple_of((g * G + h) * HD, HD), HD)] = (acc / jnp.sum(l, axis=0, keepdims=True)).T.astype(BF)

        @pl.when(g == n_heads - 1)
        def _():
            for k in range(n_tiles):
                @pl.when(tile == k)
                def _():
                    pltpu.make_async_copy(o_scr.at[k], outs[k], o_sem.at[k]).start()

    if final and n_st:
        def idle(i, carry):
            tile, g = lax.div(i, n_heads), lax.rem(i, n_heads)

            @pl.when(tab_ref[carried + tile] == 2)
            def _():
                @pl.when(g == 0)
                def _():
                    pltpu.make_async_copy(st_scr.at[tile], st_scr.at[tile], st_sem.at[tile]).wait()

                finish(tile, g, lambda h: (st_scr[tile, g, h, :HD, :], st_scr[tile, g, h, HD + 8:, :]))

            return carry

        lax.fori_loop(0, n_tiles * n_heads, idle, 0)

    row, g = block(0)
    have = arrived(0, tab_ref[row + 2])
    for h in range(G):
        stage_a(row, g, h)

    def body(i, have):
        row, g = block(i)
        nrow, ng = block(jnp.minimum(i + 1, n_heads * n_blocks - 1))
        have = arrived(have, tab_ref[nrow + 2])
        flags = tab_ref[row + 1]
        tile = tab_ref[row]

        @pl.when((flags & (FIRST | CARRY)) == FIRST)
        def _():
            acc_scr[...] = jnp.zeros_like(acc_scr)
            l_scr[...] = jnp.zeros_like(l_scr)
            m_scr[...] = jnp.full_like(m_scr, NEG)

        if n_st:
            @pl.when((flags & (FIRST | CARRY)) == (FIRST | CARRY))
            def _():
                @pl.when(g == 0)
                def _():
                    pltpu.make_async_copy(st_scr.at[tile], st_scr.at[tile], st_sem.at[tile]).wait()

                for h in range(G):
                    acc_scr[h] = st_scr[tile, g, h, :HD, :]
                    m_scr[h] = st_scr[tile, g, h, HD:HD + 8, :]
                    l_scr[h] = st_scr[tile, g, h, HD + 8:, :]

        @pl.when((flags & 15) != 0)
        def _():
            mask_runs(row, flags)

        for h in range(G):
            stage_b(row, g, h)
            stage_a(nrow, ng, h)

        @pl.when((flags & LAST) != 0)
        def _():
            if final:
                finish(tile, g, lambda h: (acc_scr[h], l_scr[h]))
            else:
                for h in range(G):
                    st_scr[tile, g, h, :HD, :] = acc_scr[h]
                    st_scr[tile, g, h, HD:HD + 8, :] = m_scr[h]
                    st_scr[tile, g, h, HD + 8:, :] = l_scr[h]

                @pl.when(g == n_heads - 1)
                def _():
                    pltpu.make_async_copy(st_scr.at[tile], outs[0].at[tile], o_sem.at[tile]).start()

        return have

    have = lax.fori_loop(0, n_heads * n_blocks, body, have)
    arrived(have, len(kv_src))
    if final:
        for k in range(n_tiles):
            pltpu.make_async_copy(o_scr.at[k], outs[k], o_sem.at[k]).wait()
    else:
        def wait_out(i, carry):
            row = row0 + BLK * i

            @pl.when((tab_ref[row + 1] & LAST) != 0)
            def _():
                t = tab_ref[row]
                pltpu.make_async_copy(st_scr.at[t], st_scr.at[t], o_sem.at[t]).wait()

            return carry

        lax.fori_loop(0, n_blocks, wait_out, 0)


def flash(tab, qs, q_src, kvs, *, base, work, st=None, st_src=None, st_tiles=None, after=()):
    nq = qs[0].shape[1]
    n_heads = 2
    G = nq // HD // n_heads
    n_tiles = len(q_src)
    final = st_tiles is None
    kv_src = [(a, i) for a, kv in enumerate(kvs) for i in range(kv.shape[0])]
    n_runs = len(kv_src)
    sts = () if st is None else (st,)
    n_in = 1 + len(qs) + len(kvs) + len(sts)
    state = (n_heads, G, ST, RUN)
    has_st = not final or sts
    return pl.pallas_call(
        ordered(functools.partial(flash_kernel, q_src=q_src, kv_src=kv_src, n_q=len(qs), n_kv=len(kvs),
                                  st_src=st_src or [None] * n_tiles, n_st=len(sts), base=base, G=G, n_tiles=n_tiles,
                                  n_heads=n_heads, final=final), n_in, after),
        grid_spec=pltpu.PrefetchScalarGridSpec(
            num_scalar_prefetch=1, grid=(),
            in_specs=[ANY] * (n_in - 1 + len(after)),
            out_specs=[ANY] * n_tiles if final else [ANY],
            scratch_shapes=[pltpu.VMEM((n_tiles, nq, RUN), BF),
                            pltpu.VMEM((n_runs, 2, 256, 256), BF),
                            pltpu.VMEM((n_tiles if final else 1, RUN, nq), BF),
                            pltpu.VMEM((n_tiles if has_st else 1, *state), F32),
                            pltpu.VMEM((G, 4 * RUN, RUN), F32),
                            pltpu.VMEM((G, 4, 8, RUN), F32),
                            pltpu.VMEM((G, HD, RUN), F32),
                            pltpu.VMEM((G, 8, RUN), F32),
                            pltpu.VMEM((G, 8, RUN), F32),
                            pltpu.SemaphoreType.DMA((n_tiles,)),
                            pltpu.SemaphoreType.DMA((n_runs,)),
                            pltpu.SemaphoreType.DMA((n_tiles,)),
                            pltpu.SemaphoreType.DMA((n_tiles,))]),
        out_shape=[jax.ShapeDtypeStruct((RUN, nq), BF)] * n_tiles if final
        else [jax.ShapeDtypeStruct((st_tiles, *state), F32)],
        input_output_aliases={n_in - 1: 0} if sts and not final else {},
        name="flash" if final else "flash_part", compiler_params=pltpu.CompilerParams(vmem_limit_bytes=VMEM),
        cost_estimate=pl.CostEstimate(flops=8 * work * RUN * RUN * nq, transcendentals=work * RUN * RUN * nq // HD,
                                      bytes_accessed=n_runs * 2 * 256 * 256 * 2 + 4 * n_tiles * RUN * nq),
    )(tab, *qs, *kvs, *sts, *after)


def out_kernel(*refs, blocks, n_w, n_run):
    n_o = 4 * n_run
    o_refs, w_refs, x_ref, g_ref = refs[:n_o], refs[n_o:n_o + n_w], refs[n_o + n_w], refs[n_o + n_w + 1]
    outs = refs[n_o + n_w + 2:n_o + n_w + 2 + 2 * n_run]
    o_scr, w_scr, acc_scr, o_sem, w_sem = refs[n_o + n_w + 2 + 2 * n_run:]
    width = o_refs[0].shape[1]
    half = width // 2
    n_slots = w_scr.shape[0]

    def fetch(k):
        for i, parts in enumerate(blocks):
            @pl.when(k == i)
            def _():
                at = 0
                for a, r0, n in parts:
                    pltpu.make_async_copy(w_refs[a].at[pl.ds(r0, n), :], w_scr.at[i % n_slots, pl.ds(at, n), :],
                                          w_sem.at[i % n_slots]).start()
                    at += n

    mine = lax.axis_index('cp')
    pairs = []
    for i in range(n_run):
        os, rows = o_refs[4 * i:4 * i + 4], pl.ds(i * RUN, RUN)
        pairs += [(os[0], o_scr.at[rows, pl.ds(0, width)]), (os[1], o_scr.at[rows, pl.ds(width, width)])]
        for k in range(2, 4):
            for p, part in enumerate((mine, 1 - mine)):
                pairs.append((os[k].at[:, pl.ds(pl.multiple_of(part * half, half), half)],
                              o_scr.at[rows, pl.ds(k * width + p * half, half)]))
    copies = [pltpu.make_async_copy(src, dst, o_sem.at[i]) for i, (src, dst) in enumerate(pairs)]
    for cp in copies:
        cp.start()
    for i in range(n_slots - 1):
        fetch(jnp.int32(i))
    acc_scr[...] = jnp.zeros_like(acc_scr)
    for cp in copies:
        cp.wait()

    def one(k, carry):
        fetch(k + n_slots - 1)
        slot = lax.rem(k, n_slots)
        pltpu.make_async_copy(w_scr.at[slot], w_scr.at[slot], w_sem.at[slot]).wait()
        acc_scr[...] += jnp.dot(o_scr[:, pl.ds(pl.multiple_of(k * half, half), half)], w_scr[slot], preferred_element_type=F32)
        return carry

    lax.fori_loop(0, len(blocks), one, 0)

    for i in range(n_run):
        def rows32(r, carry):
            at = pl.multiple_of(r * 32, 32)
            rows, mine = pl.ds(at, 32), pl.ds(i * RUN + at, 32)
            y = (x_ref[mine, :].astype(F32) + acc_scr[mine, :].astype(BF).astype(F32)).astype(BF)
            outs[2 * i][rows, :] = y
            outs[2 * i + 1][rows, :] = norm_rows(y, g_ref[...])
            return carry

        lax.fori_loop(0, RUN // 32, rows32, 0)


def out_proj(os, ws, blocks, x_rows, gain, at, after=()):
    dim = x_rows.shape[1]
    width = os[0].shape[1]
    n_run = len(os) // 4
    rows = n_run * RUN
    one = lambda m, s: pl.BlockSpec((m, dim), lambda i: (s, 0))
    return pl.pallas_call(
        ordered(functools.partial(out_kernel, blocks=blocks, n_w=len(ws), n_run=n_run), len(os) + len(ws) + 2, after),
        grid=(1,),
        in_specs=[ANY] * (len(os) + len(ws)) + [one(rows, at), pl.BlockSpec((1, dim), lambda i: (0, 0))] + [ANY] * len(after),
        out_specs=[one(RUN, 0)] * (2 * n_run),
        out_shape=[jax.ShapeDtypeStruct((RUN, dim), BF)] * (2 * n_run),
        scratch_shapes=[pltpu.VMEM((rows, 4 * width), BF), pltpu.VMEM((3, width // 2, dim), BF), pltpu.VMEM((rows, dim), F32),
                        pltpu.SemaphoreType.DMA((6 * n_run,)), pltpu.SemaphoreType.DMA((3,))],
        name="outp", compiler_params=params(1),
        cost_estimate=pl.CostEstimate(flops=8 * rows * width * dim, transcendentals=0,
                                      bytes_accessed=8 * width * dim + 8 * rows * dim),
    )(*os, *ws, x_rows, gain, *after)


def mlp_kernel(*refs, n_in, tn, nk):
    b_refs = refs[:n_in]
    wg_ref, wu_ref, wd_ref, keep_ref, send_ref, b_scr, u_scr, sem = refs[n_in:]
    i = pl.program_id(0)

    def gated(rows, cols):
        b = b_scr[rows, :]
        gate = jnp.dot(b, wg_ref[...], preferred_element_type=F32)
        up = jnp.dot(b, wu_ref[...], preferred_element_type=F32)
        u_scr[rows, cols] = (jax.nn.silu(gate) * up).astype(BF)

    @pl.when(i == 0)
    def _():
        copies = [pltpu.make_async_copy(r, b_scr.at[pl.ds(k * RUN, RUN), :], sem.at[k]) for k, r in enumerate(b_refs)]
        for cp in copies:
            cp.start()

        def one(k, carry):
            rows = pl.ds(pl.multiple_of(k * RUN, RUN), RUN)
            pltpu.make_async_copy(b_scr.at[rows, :], b_scr.at[rows, :], sem.at[k]).wait()
            gated(rows, pl.ds(0, tn))
            return carry

        lax.fori_loop(0, n_in, one, 0)

    @pl.when((i > 0) & (i < nk))
    def _():
        gated(slice(None), pl.ds(pl.multiple_of(i * tn, tn), tn))

    @pl.when(i >= nk)
    def _():
        d = jnp.dot(u_scr[...], wd_ref[...], preferred_element_type=F32).astype(BF)
        half = d.shape[0] // 2
        keep_ref[...] = d[:half]
        send_ref[...] = d[half:]


def mlp(bs, wg, wu, wd, after=(), tn=256, td=256):
    rows, dim = RUN * len(bs), bs[0].shape[1]
    ffn = wg.shape[1]
    nk, nd = ffn // tn, dim // td
    up = lambda i: (0, jnp.minimum(i, nk - 1))
    dn = lambda i: (0, jnp.maximum(i - nk, 0))
    return pl.pallas_call(
        ordered(functools.partial(mlp_kernel, n_in=len(bs), tn=tn, nk=nk), len(bs) + 3, after),
        grid=(nk + nd,),
        in_specs=[ANY] * len(bs) + [pl.BlockSpec((dim, tn), up), pl.BlockSpec((dim, tn), up), pl.BlockSpec((ffn, td), dn)]
        + [ANY] * len(after),
        out_specs=[pl.BlockSpec((rows // 2, td), dn)] * 2,
        out_shape=[jax.ShapeDtypeStruct((rows // 2, dim), BF)] * 2,
        scratch_shapes=[pltpu.VMEM((rows, dim), BF), pltpu.VMEM((rows, ffn), BF), pltpu.SemaphoreType.DMA((len(bs),))],
        name="mlp", compiler_params=params(1),
        cost_estimate=pl.CostEstimate(flops=6 * rows * dim * ffn, transcendentals=rows * ffn,
                                      bytes_accessed=6 * dim * ffn + 4 * rows * dim),
    )(*bs, wg, wu, wd, *after)


def sum_kernel(*refs):
    p_ref, r_ref, t_ref, y_ref, z_ref = refs[-5:]
    total = p_ref[...].astype(F32) + r_ref[...].astype(F32) + t_ref[...].astype(F32)
    z_ref[...] = (y_ref[...].astype(F32) + total.astype(BF).astype(F32)).astype(BF)


def sum_run(z, keep, recv, far, y, j, n_runs, after=(), tile=64):
    dim = y.shape[1]
    per = RUN // tile
    spec = pl.BlockSpec((tile, dim), lambda i: (i, 0))
    prev = () if z is None else (z,)
    return pl.pallas_call(
        ordered(sum_kernel, len(prev) + 4, after), grid=(per,),
        in_specs=[ANY] * len(prev) + [spec] * 4 + [ANY] * len(after),
        out_specs=pl.BlockSpec((tile, dim), lambda i: (j * per + i, 0)),
        out_shape=jax.ShapeDtypeStruct((n_runs * RUN, dim), BF),
        input_output_aliases={0: 0} if prev else {},
        name="zsum", compiler_params=params(1),
        cost_estimate=pl.CostEstimate(flops=6 * RUN * dim, transcendentals=0, bytes_accessed=10 * RUN * dim),
    )(*prev, keep, recv, far, y, *after)


def run_positions(xi, ci, y, cps, piece):
    def start(x, c):
        return (y if x == 0 else 2 * cps - 1 - y) * piece + c * (piece // 2)

    per = piece // 2 // RUN
    out = [start(xi, ci) + RUN * j for j in range(per)] + [start(xi, 1 - ci) + RUN * j for j in range(per)]
    for j in range(per):
        out += [start(1 - xi, ci) + RUN * j, start(1 - xi, 1 - ci) + RUN * j]
    return out


def block_list(tile, ids, pos, diag):
    runs = [(r, pos[r]) for r in ids]
    if diag is not None:
        n_tail = (len(runs) % 4) + 1
        tail = [(diag, pos[diag])] + runs[len(runs) - (n_tail - 1):]
        runs = runs[:len(runs) - (n_tail - 1)]
    else:
        n_tail = len(runs) % 4
        tail = runs[len(runs) - n_tail:]
        runs = runs[:len(runs) - n_tail]
    blocks = [[0, runs[i:i + 4]] for i in range(0, len(runs), 4)]
    if tail:
        full = tail + [(tail[0][0], FAR)] * (4 - len(tail))
        flags = sum(1 << k for k, (r, p) in enumerate(full) if p == FAR or r == diag)
        blocks.append([flags, full])
    blocks[-1][0] |= LAST
    blocks[0][0] |= FIRST
    return [[tile, flags, 0] + [r for r, _ in four] + [p for _, p in four] + [0] for flags, four in blocks]


def call_table(tiles, pos, pairs, carry, idle):
    rows, most = [], 0
    carry = [c if pairs[t][0] or pairs[t][1] else idle for t, c in enumerate(carry)]
    for t, tile in enumerate(tiles):
        ids, own = pairs[t]
        if ids or own:
            mine = block_list(t, ids, pos, tile if own else None)
            mine[0][1] |= CARRY if carry[t] else 0
            rows += mine
    for row in rows:
        most = max(most, max(row[3:7]) + 1)
        row[2] = most
    return [len(rows)] + [pos[t] for t in tiles] + carry + [v for row in rows for v in row], len(rows)


def work_tables(cps, piece):
    per = piece // 2 // RUN
    early = 2 * per + 2
    stage = lambda r: 0 if r < early else 1
    calls = [(0, list(range(early)))]
    calls += [(1, [j, per + j, 2 * per + 2 * j, 2 * per + 2 * j + 1]) for j in range(per)]
    tabs, all_runs, sizes = [], [], []
    for y in range(cps):
        for xi in range(2):
            for ci in range(2):
                mine = run_positions(xi, ci, y, cps, piece)
                pos = mine + run_positions(xi, ci, 1 - y, cps, piece)
                all_runs.append(mine)
                tabs.append([])
                sizes.append([])
                for now, tiles in calls:
                    pairs, carry = [], []
                    for t in tiles:
                        seen = [r for r in range(len(pos)) if pos[r] < pos[t]]
                        pairs.append(([r for r in seen if max(stage(r), stage(t)) == now], stage(t) == now))
                        carry.append(int(stage(t) < now))
                    tab, n = call_table(tiles, pos, pairs, carry, 2 if now == 1 else 0)
                    tabs[-1].append(tab)
                    sizes[-1].append(n)
    widths = [max(len(t[k]) for t in tabs) for k in range(len(calls))]
    flat = [[v for k, t in enumerate(tab) for v in t + [0] * (widths[k] - len(t))] for tab in tabs]
    bases = [sum(widths[:k]) for k in range(len(calls))]
    return np.array(flat, np.int32), np.array(all_runs, np.int32), bases, np.array(sizes).max(0) * 4


def solution(mesh):
    cps = mesh.shape['cp']
    row_spec = P('dp', ('cp', 'tp'), None)
    head_cols = P(None, 'tp', None)
    n_tp = mesh.shape['tp']

    over_core, over_x, over_both = (('tp', [(t, t ^ k) for t in range(n_tp)]) for k in (1, 2, 3))
    over_y = ('cp', [(i, i ^ 1) for i in range(cps)])

    def layer(x, g_attn, w_q, w_k, w_v, w_o, g_mlp, w_gate, w_up, w_down):
        x_rows = x[0]
        dim = x_rows.shape[1]
        n_run = x_rows.shape[0] // RUN
        piece = 2 * x_rows.shape[0]
        t_id, y_id = lax.axis_index('tp'), lax.axis_index('cp')
        np_tab, np_runs, bases, work = work_tables(cps, piece)
        dev = y_id * n_tp + t_id
        tab = lax.dynamic_index_in_dim(jnp.asarray(np_tab), dev, 0, keepdims=False)
        order = list(range(2 * n_run)) + [2 * n_run + i for i in (2, 3, 4, 5, 0, 1, 6, 7)]
        run_pos = lax.dynamic_index_in_dim(jnp.asarray(np_runs[:, order]), dev, 0, keepdims=False)

        def tied(v, *others):
            return lax.optimization_barrier((v, *others))[0]

        def send(axis_pairs, v):
            return lax.ppermute(v, *axis_pairs)

        ga, gm = g_attn.reshape(1, dim), g_mlp.reshape(1, dim)
        own = []
        for j in range(n_run):
            own.append(norm_run(x_rows, ga, j, after=own[-1:]))
        far = [send(over_x, own[j]) for j in range(n_run)]
        mate = [send(over_core, own[j]) for j in range(n_run)]

        w_all = jnp.concatenate([tied(w, own[-1]).reshape(dim, -1) for w in (w_q, w_k, w_v)], axis=1)
        tables = rope_tables(tied(run_pos, own[-1])[:, None] + jnp.arange(RUN, dtype=jnp.int32)[None, :])

        def relayed(j, after):
            here = tied(far[j], after)
            return [here, send(over_core, here)]

        q_own, kv_own = qkv(own, w_all, (tables, 0))
        q_mate, kv_mate = qkv(mate, w_all, (tables, n_run), after=(kv_own,))
        q_a, kv_a = qkv(relayed(0, kv_mate), w_all, (tables, 2 * n_run + 4), after=(kv_mate,))

        wo = w_o.reshape(-1, dim)
        half = wo.shape[0] // 2
        n_piece = 4
        rows = half // n_piece
        wo_gated = tied(wo, kv_a)
        wo_x = [send(over_x, lax.dynamic_slice_in_dim(wo_gated, y_id * half + p * rows, rows, axis=0))
                for p in range(n_piece)]
        wo_c = send(over_core, wo_gated)
        early = relayed(1, kv_a)

        tile = lambda a, n: [(a, i) for i in range(n)]
        tiles = tile(0, n_run) + tile(1, n_run) + tile(2, 2)
        st, = flash(tab, [q_own, q_mate, q_a], tiles, [kv_own, kv_mate, kv_a], base=bases[0],
                   work=int(work[0]), st_tiles=len(tiles))
        q_b, kv_b = qkv(early + relayed(2, st), w_all, (tables, 2 * n_run), after=(st,))
        q_c, kv_c = qkv(relayed(3, kv_b), w_all, (tables, 2 * n_run + 6), after=(kv_b,))
        kvs = [kv_own, kv_mate, kv_a, kv_b, kv_c]
        kvs = kvs + [send(over_y, kv) for kv in kvs]
        q_far = [(q_a, 0), (q_b, 0), (q_b, 2), (q_c, 0)]

        os, outs, prev = [], [], kv_c
        wo_a, wo_ya, wo_yb = {}, {}, {}

        def forward_w(p):
            here = tied(wo_x[p], prev)
            wo_ya[p] = (here, send(over_core, here))
            wo_a[p] = send(over_y, here)

        def relay_w(p):
            here = tied(wo_a[p], prev)
            wo_yb[p] = (here, send(over_core, here))

        def attend(j):
            q, at = q_far[j]
            held = 2 * n_run + 2 * j
            carried = [j, n_run + j] + ([held, held + 1] if j == 0 else [None, None])
            o_own, o_mate, o_far, o_fm = flash(
                tab, [q_own, q_mate, q], [(0, j), (1, j), (2, at), (2, at + 1)], kvs,
                base=bases[1 + j], work=int(work[1 + j]), st=st, st_src=carried, after=(prev,))
            os.append([o_own, send(over_core, o_mate), send(over_x, o_far), send(over_both, o_fm)])
            return o_own

        def project(i):
            ws = [wo, wo_c]
            blocks = [[(0, 0, half)], [(0, half, half)], [(1, 0, half)], [(1, half, half)]]
            for k in range(2):
                for held in (wo_ya, wo_yb):
                    blocks.append([(len(ws) + p, 0, rows) for p in range(n_piece)])
                    ws += [held[p][k] for p in range(n_piece)]
            got = out_proj(os[2 * i] + os[2 * i + 1], ws, blocks, x_rows, gm, i, after=(prev,))
            for k in range(2):
                y, b = got[2 * k:2 * k + 2]
                outs.append((y, b, send(over_x, b), send(over_core, b)))
            return got[0]

        forward_w(0)
        prev = attend(0)
        forward_w(1)
        relay_w(0)
        prev = attend(1)
        forward_w(2)
        forward_w(3)
        relay_w(1)
        prev = attend(2)
        relay_w(2)
        relay_w(3)
        prev = project(0)
        prev = attend(3)

        z, sums, relay = None, [], {}

        def relay_b(j):
            here = tied(outs[j][2], prev)
            relay[j] = (here, send(over_core, here))

        def finish(j):
            return sum_run(z, *sums[j], j, n_run, after=() if prev is z else (prev,))

        relay_b(0)
        for j in range(n_run):
            y, b, _, b_mate = outs[j]
            keep, out = mlp([b, relay[j][0], b_mate, relay[j][1]], w_gate, w_up, w_down, after=(prev,))
            recv = send(over_core, out)
            prev = keep
            if j + 1 < n_run:
                relay_b(j + 1)
            if j == 0:
                prev = project(1)
            elif j > 1:
                prev = z = finish(j - 2)
            kept = keep if prev is keep else tied(keep, prev)
            prev = s_far = (kept[RUN:].astype(F32) + recv[RUN:].astype(F32)).astype(BF)
            sums.append((keep, recv, send(over_x, s_far), y))
        for j in range(n_run - 2, n_run):
            prev = z = finish(j)
        return z[None]

    return jax.shard_map(layer, mesh=mesh,
                         in_specs=(row_spec, P(), head_cols, head_cols, head_cols, P('tp', None, None),
                                   P(), P(None, 'tp'), P(None, 'tp'), P('tp', None)),
                         out_specs=row_spec, check_vma=False)
```

```python
import functools
import math
import jax
import jax.numpy as jnp
import numpy as np
from jax import lax
from jax.experimental import pallas as pl
from jax.experimental.pallas import tpu as pltpu
from jax.sharding import PartitionSpec as P

NORM_EPS = 1e-5
ROPE_THETA = 500000.0
HD = 128
RUN = 256
NEG = -1e30
FAR = 1 << 29
LOG2E = math.log2(math.e)
DN = (((1,), (0,)), ((), ()))
VMEM = 67043328
BF = jnp.bfloat16
F32 = jnp.float32
ANY = pl.BlockSpec(memory_space=pltpu.HBM)


def params(n):
    return pltpu.CompilerParams(dimension_semantics=("arbitrary",) * n, vmem_limit_bytes=VMEM)


def rope_tables(positions):
    half = HD // 2
    inv_freq = ROPE_THETA ** (-2.0 * jnp.arange(half, dtype=F32) / HD)
    angles = inv_freq[:, None] * positions.astype(F32)[..., None, :]
    return jnp.cos(angles), jnp.sin(angles)


def norm_rows(rows, gain):
    f = rows.astype(F32)
    mean_sq = jnp.mean(f * f, axis=-1, keepdims=True)
    return (f * lax.rsqrt(mean_sq + NORM_EPS) * gain.astype(F32)).astype(BF)


def cost(flops, moved):
    return pl.CostEstimate(flops=flops, transcendentals=0, bytes_accessed=moved)


def ordered(kernel, n_in, after):
    n = len(after)
    return lambda *refs: kernel(*refs[:n_in], *refs[n_in + n:])


def norm_kernel(x_ref, g_ref, o_ref):
    o_ref[...] = norm_rows(x_ref[...], g_ref[...])


def norm_run(x_rows, gain, j, after=(), tile=128):
    dim = x_rows.shape[1]
    per = RUN // tile
    return pl.pallas_call(
        ordered(norm_kernel, 2, after), grid=(per,),
        in_specs=[pl.BlockSpec((tile, dim), lambda i: (j * per + i, 0)), pl.BlockSpec((1, dim), lambda i: (0, 0))]
        + [ANY] * len(after),
        out_specs=pl.BlockSpec((tile, dim), lambda i: (i, 0)),
        out_shape=jax.ShapeDtypeStruct((RUN, dim), BF),
        name="norm", compiler_params=params(1),
        cost_estimate=cost(RUN * dim, RUN * dim),
    )(x_rows, gain, *after)


def qkv_kernel(*refs, n_in, n_q, group):
    a_refs = refs[:n_in]
    w_ref, cos_ref, sin_ref, q_ref, kv_ref, a_scr, sem = refs[n_in:]
    n = pl.program_id(0)
    heads = w_ref.shape[1] // HD

    @pl.when(n == 0)
    def _():
        for k, r in enumerate(a_refs):
            pltpu.make_async_copy(r, a_scr.at[pl.ds(k * RUN, RUN), :], sem.at[k]).start()

    def rope(f, i):
        f = f.astype(BF).astype(F32)
        lo, hi, cos, sin = f[:HD // 2], f[HD // 2:], cos_ref[i], sin_ref[i]
        return jnp.concatenate([lo * cos - hi * sin, hi * cos + lo * sin], axis=0)

    def one(k, carry):
        @pl.when(n == 0)
        def _():
            for i in range(group):
                rows = pl.ds(pl.multiple_of((k * group + i) * RUN, RUN), RUN)
                pltpu.make_async_copy(a_scr.at[rows, :], a_scr.at[rows, :], sem.at[k * group + i]).wait()

        rows = pl.ds(pl.multiple_of(k * group * RUN, group * RUN), group * RUN)
        r = jnp.dot(a_scr[rows, :], w_ref[...], preferred_element_type=F32)

        def piece(i, h):
            return r[i * RUN:(i + 1) * RUN, h * HD:(h + 1) * HD].T

        @pl.when(n < n_q)
        def _():
            for i in range(group):
                for h in range(heads):
                    q_ref[k * group + i, h * HD:(h + 1) * HD, :] = rope(piece(i, h), k * group + i).astype(BF)

        @pl.when(n == n_q)
        def _():
            for i in range(group):
                for h in range(heads // 2):
                    kv_ref[k * group + i, 0, :, h * HD:(h + 1) * HD] = rope(piece(i, h), k * group + i).T.astype(BF)
                    kv_ref[k * group + i, 1, h * HD:(h + 1) * HD, :] = piece(i, h + heads // 2).astype(BF)

        return carry

    lax.fori_loop(0, n_in // group, one, 0)


def qkv(rows, w_all, tables, after=(), group=2):
    n_in = len(rows)
    dim = w_all.shape[0]
    tn = 512
    n_q = w_all.shape[1] // tn - 1
    (cos, sin), first_run = tables
    at = first_run // n_in
    tab = pl.BlockSpec((n_in, HD // 2, RUN), lambda n: (at, 0, 0))
    return pl.pallas_call(
        ordered(functools.partial(qkv_kernel, n_in=n_in, n_q=n_q, group=group), n_in + 3, after),
        grid=(n_q + 1,),
        in_specs=[ANY] * n_in + [pl.BlockSpec((dim, tn), lambda n: (0, n)), tab, tab] + [ANY] * len(after),
        out_specs=[pl.BlockSpec((n_in, tn, RUN), lambda n: (0, jnp.minimum(n, n_q - 1), 0)),
                   pl.BlockSpec((n_in, 2, 256, 256), lambda n: (0, 0, 0, 0))],
        out_shape=[jax.ShapeDtypeStruct((n_in, n_q * tn, RUN), BF), jax.ShapeDtypeStruct((n_in, 2, 256, 256), BF)],
        scratch_shapes=[pltpu.VMEM((n_in * RUN, dim), BF), pltpu.SemaphoreType.DMA((n_in,))],
        name="qkv", compiler_params=params(1),
        cost_estimate=cost(2 * n_in * RUN * w_all.size, 2 * w_all.size),
    )(*rows, w_all, cos, sin, *after)


BLK = 12
LAST, FIRST, CARRY = 16, 32, 64
ST = HD + 16


def flash_kernel(tab_ref, *refs, q_src, kv_src, n_q, n_kv, st_src, n_st, base, G, n_tiles, n_heads, final):
    qs, kvs, sts = refs[:n_q], refs[n_q:n_q + n_kv], refs[n_q + n_kv:n_q + n_kv + n_st]
    n_out = n_tiles if final else 1
    at = n_q + n_kv + n_st
    outs = refs[at:at + n_out]
    q_scr, kv_scr, o_scr, st_scr, s_scr, mb_scr, acc_scr, m_scr, l_scr, q_sem, kv_sem, o_sem, st_sem = refs[at + n_out:]
    T = RUN
    c = (HD ** -0.5) * LOG2E
    n_blocks = tab_ref[base]
    carried = base + 1 + n_tiles
    row0 = base + 1 + 2 * n_tiles

    q_copies = [pltpu.make_async_copy(qs[a].at[i], q_scr.at[t], q_sem.at[t]) for t, (a, i) in enumerate(q_src)]
    kv_copies = [pltpu.make_async_copy(kvs[a].at[i], kv_scr.at[r], kv_sem.at[r]) for r, (a, i) in enumerate(kv_src)]
    first = 4
    q_copies[0].start()
    for cp in kv_copies[:first]:
        cp.start()
    for cp in q_copies[1:]:
        cp.start()
    for t, i in enumerate(st_src):
        if i is not None:
            @pl.when(tab_ref[carried + t] != 0)
            def _():
                pltpu.make_async_copy(sts[0].at[i], st_scr.at[t], st_sem.at[t]).start()
    for cp in kv_copies[first:]:
        cp.start()

    def block(i):
        g = lax.div(i, n_blocks)
        return row0 + BLK * (i - g * n_blocks), g

    def arrived(have, need):
        def one(r, carry):
            pltpu.make_async_copy(kv_scr.at[r], kv_scr.at[r], kv_sem.at[r]).wait()
            return carry

        lax.fori_loop(have, need, one, 0)
        return jnp.maximum(have, need)

    def put(s, h, k):
        s_scr[h, pl.ds(k * RUN, RUN), :] = s
        mb_scr[h, k] = jnp.max(s.reshape(RUN // 8, 8, T), axis=0)

    def stage_a(row, g, h):
        col = pl.multiple_of(g * HD, HD)
        qt = q_scr[tab_ref[row], pl.ds(pl.multiple_of((g * G + h) * HD, HD), HD), :]
        for k in range(4):
            put(lax.dot_general(kv_scr[tab_ref[row + 3 + k], 0, :, pl.ds(col, HD)], qt, DN, preferred_element_type=F32), h, k)

    def stage_b(row, g, h):
        col = pl.multiple_of(g * HD, HD)
        m_prev = m_scr[h]
        mb = jnp.maximum(jnp.maximum(mb_scr[h, 0], mb_scr[h, 1]), jnp.maximum(mb_scr[h, 2], mb_scr[h, 3]))
        for r in (4, 2, 1):
            mb = jnp.maximum(mb, pltpu.roll(mb, r, 0))
        m_new = jnp.maximum(m_prev, mb)
        m_scr[h] = m_new
        m_c = m_new * c
        alpha = jnp.exp2(m_prev * c - m_c)
        l, pv = l_scr[h] * alpha, None
        for k in range(4):
            p = jnp.exp2(s_scr[h, k * RUN:(k + 1) * RUN].reshape(RUN // 8, 8, T) * c - m_c[None])
            l = l + jnp.sum(p, axis=0)
            d = lax.dot_general(kv_scr[tab_ref[row + 3 + k], 1, pl.ds(col, HD), :], p.reshape(RUN, T).astype(BF), DN,
                                preferred_element_type=F32)
            pv = d if pv is None else pv + d
        l_scr[h] = l
        acc_scr[h] = (acc_scr[h].reshape(HD // 8, 8, T) * alpha[None]).reshape(HD, T) + pv

    def mask_runs(row, flags):
        qry = lax.broadcasted_iota(jnp.int32, (RUN, T), 1) + tab_ref[base + 1 + tab_ref[row]]
        key = lax.broadcasted_iota(jnp.int32, (RUN, T), 0)

        def one(k, carry):
            @pl.when((lax.shift_right_logical(flags, k) & 1) != 0)
            def _():
                mask = key + tab_ref[row + 7 + k] <= qry
                rows = pl.multiple_of(k * RUN, RUN)
                for h in range(G):
                    put(jnp.where(mask, s_scr[h, pl.ds(rows, RUN), :], NEG), h, k)

            return carry

        lax.fori_loop(0, 4, one, 0)

    def finish(tile, g, get):
        for h in range(G):
            acc, l = get(h)
            o_scr[tile, :, pl.ds(pl.multiple_of((g * G + h) * HD, HD), HD)] = (acc / jnp.sum(l, axis=0, keepdims=True)).T.astype(BF)

        @pl.when(g == n_heads - 1)
        def _():
            for k in range(n_tiles):
                @pl.when(tile == k)
                def _():
                    pltpu.make_async_copy(o_scr.at[k], outs[k], o_sem.at[k]).start()

    if final and n_st:
        def idle(i, carry):
            tile, g = lax.div(i, n_heads), lax.rem(i, n_heads)

            @pl.when(tab_ref[carried + tile] == 2)
            def _():
                @pl.when(g == 0)
                def _():
                    pltpu.make_async_copy(q_scr.at[tile], q_scr.at[tile], q_sem.at[tile]).wait()
                    pltpu.make_async_copy(st_scr.at[tile], st_scr.at[tile], st_sem.at[tile]).wait()

                finish(tile, g, lambda h: (st_scr[tile, g, h, :HD, :], st_scr[tile, g, h, HD + 8:, :]))

            return carry

        lax.fori_loop(0, n_tiles * n_heads, idle, 0)

    def query(row):
        t = tab_ref[row]
        pltpu.make_async_copy(q_scr.at[t], q_scr.at[t], q_sem.at[t]).wait()

    row, g = block(0)
    query(row)
    have = arrived(0, tab_ref[row + 2])
    for h in range(G):
        stage_a(row, g, h)

    def body(i, have):
        row, g = block(i)
        nrow, ng = block(jnp.minimum(i + 1, n_heads * n_blocks - 1))
        have = arrived(have, tab_ref[nrow + 2])
        flags = tab_ref[row + 1]
        tile = tab_ref[row]

        @pl.when((i + 1 < n_blocks) & ((tab_ref[nrow + 1] & FIRST) != 0))
        def _():
            query(nrow)

        @pl.when((flags & (FIRST | CARRY)) == FIRST)
        def _():
            acc_scr[...] = jnp.zeros_like(acc_scr)
            l_scr[...] = jnp.zeros_like(l_scr)
            m_scr[...] = jnp.full_like(m_scr, NEG)

        if n_st:
            @pl.when((flags & (FIRST | CARRY)) == (FIRST | CARRY))
            def _():
                @pl.when(g == 0)
                def _():
                    pltpu.make_async_copy(st_scr.at[tile], st_scr.at[tile], st_sem.at[tile]).wait()

                for h in range(G):
                    acc_scr[h] = st_scr[tile, g, h, :HD, :]
                    m_scr[h] = st_scr[tile, g, h, HD:HD + 8, :]
                    l_scr[h] = st_scr[tile, g, h, HD + 8:, :]

        @pl.when((flags & 15) != 0)
        def _():
            mask_runs(row, flags)

        for h in range(G):
            stage_b(row, g, h)
            stage_a(nrow, ng, h)

        @pl.when((flags & LAST) != 0)
        def _():
            if final:
                finish(tile, g, lambda h: (acc_scr[h], l_scr[h]))
            else:
                for h in range(G):
                    st_scr[tile, g, h, :HD, :] = acc_scr[h]
                    st_scr[tile, g, h, HD:HD + 8, :] = m_scr[h]
                    st_scr[tile, g, h, HD + 8:, :] = l_scr[h]

                @pl.when(g == n_heads - 1)
                def _():
                    pltpu.make_async_copy(st_scr.at[tile], outs[0].at[tile], o_sem.at[tile]).start()

        return have

    have = lax.fori_loop(0, n_heads * n_blocks, body, have)
    arrived(have, len(kv_src))
    if final:
        for k in range(n_tiles):
            pltpu.make_async_copy(o_scr.at[k], outs[k], o_sem.at[k]).wait()
    else:
        def wait_out(i, carry):
            row = row0 + BLK * i

            @pl.when((tab_ref[row + 1] & LAST) != 0)
            def _():
                t = tab_ref[row]
                pltpu.make_async_copy(st_scr.at[t], st_scr.at[t], o_sem.at[t]).wait()

            return carry

        lax.fori_loop(0, n_blocks, wait_out, 0)


def flash(tab, qs, q_src, kvs, *, base, work, st=None, st_src=None, st_tiles=None, after=()):
    nq = qs[0].shape[1]
    n_heads = 2
    G = nq // HD // n_heads
    n_tiles = len(q_src)
    final = st_tiles is None
    kv_src = [(a, i) for a, kv in enumerate(kvs) for i in range(kv.shape[0])]
    n_runs = len(kv_src)
    sts = () if st is None else (st,)
    n_in = 1 + len(qs) + len(kvs) + len(sts)
    state = (n_heads, G, ST, RUN)
    has_st = not final or sts
    return pl.pallas_call(
        ordered(functools.partial(flash_kernel, q_src=q_src, kv_src=kv_src, n_q=len(qs), n_kv=len(kvs),
                                  st_src=st_src or [None] * n_tiles, n_st=len(sts), base=base, G=G, n_tiles=n_tiles,
                                  n_heads=n_heads, final=final), n_in, after),
        grid_spec=pltpu.PrefetchScalarGridSpec(
            num_scalar_prefetch=1, grid=(),
            in_specs=[ANY] * (n_in - 1 + len(after)),
            out_specs=[ANY] * n_tiles if final else [ANY],
            scratch_shapes=[pltpu.VMEM((n_tiles, nq, RUN), BF),
                            pltpu.VMEM((n_runs, 2, 256, 256), BF),
                            pltpu.VMEM((n_tiles if final else 1, RUN, nq), BF),
                            pltpu.VMEM((n_tiles if has_st else 1, *state), F32),
                            pltpu.VMEM((G, 4 * RUN, RUN), F32),
                            pltpu.VMEM((G, 4, 8, RUN), F32),
                            pltpu.VMEM((G, HD, RUN), F32),
                            pltpu.VMEM((G, 8, RUN), F32),
                            pltpu.VMEM((G, 8, RUN), F32),
                            pltpu.SemaphoreType.DMA((n_tiles,)),
                            pltpu.SemaphoreType.DMA((n_runs,)),
                            pltpu.SemaphoreType.DMA((n_tiles,)),
                            pltpu.SemaphoreType.DMA((n_tiles,))]),
        out_shape=[jax.ShapeDtypeStruct((RUN, nq), BF)] * n_tiles if final
        else [jax.ShapeDtypeStruct((st_tiles, *state), F32)],
        input_output_aliases={n_in - 1: 0} if sts and not final else {},
        name="flash" if final else "flash_part", compiler_params=pltpu.CompilerParams(vmem_limit_bytes=VMEM),
        cost_estimate=cost(8 * work * RUN * RUN * nq, n_runs * RUN * nq),
    )(tab, *qs, *kvs, *sts, *after)


def out_kernel(*refs, blocks, n_w, n_run, at, parts):
    n_o, n_out = 4 * n_run, 2 * len(parts)
    o_refs, w_refs, x_ref, g_ref = refs[:n_o], refs[n_o:n_o + n_w], refs[n_o + n_w], refs[n_o + n_w + 1]
    outs = refs[n_o + n_w + 2:n_o + n_w + 2 + n_out]
    o_scr, w_scr, x_scr, acc_scr, o_sem, w_sem, x_sem, out_sem = refs[n_o + n_w + 2 + n_out:]
    width = o_refs[0].shape[1]
    half = width // 2
    n_slots = w_scr.shape[0]

    def fetch(k):
        for i, pieces in enumerate(blocks):
            @pl.when(k == i)
            def _():
                to = 0
                for a, r0, n in pieces:
                    pltpu.make_async_copy(w_refs[a].at[pl.ds(r0, n), :], w_scr.at[i % n_slots, pl.ds(to, n), :],
                                          w_sem.at[i % n_slots]).start()
                    to += n

    mine = lax.axis_index('cp')
    loads = [[] for _ in blocks]
    for i in range(n_run):
        rows = pl.ds(i * RUN, RUN)
        for k in range(4):
            src = o_refs[4 * i + k]
            if k < 2:
                loads[2 * k].append((src, o_scr.at[rows, pl.ds(k * width, width)]))
            else:
                for p, part in enumerate((mine, 1 - mine)):
                    loads[2 * k + p].append((src.at[:, pl.ds(pl.multiple_of(part * half, half), half)],
                                             o_scr.at[rows, pl.ds(k * width + p * half, half)]))
    copies = [[pltpu.make_async_copy(src, dst, o_sem.at[k, i]) for i, (src, dst) in enumerate(ls)] for k, ls in enumerate(loads)]
    x_copy = pltpu.make_async_copy(x_ref.at[pl.ds(at * n_run * RUN, n_run * RUN), :], x_scr, x_sem)
    for cp in copies[0]:
        cp.start()
    for i in range(n_slots - 1):
        fetch(jnp.int32(i))
    for ls in copies[1:]:
        for cp in ls:
            cp.start()
    x_copy.start()
    acc_scr[...] = jnp.zeros_like(acc_scr)

    def one(k, carry):
        fetch(k + n_slots - 1)
        for i, ls in enumerate(copies):
            if ls:
                @pl.when(k == i)
                def _():
                    for cp in ls:
                        cp.wait()
        slot = lax.rem(k, n_slots)
        pltpu.make_async_copy(w_scr.at[slot], w_scr.at[slot], w_sem.at[slot]).wait()
        acc_scr[...] += jnp.dot(o_scr[:, pl.ds(pl.multiple_of(k * half, half), half)], w_scr[slot], preferred_element_type=F32)
        return carry

    lax.fori_loop(0, len(blocks), one, 0)
    x_copy.wait()

    def rows32(r, carry):
        rows = pl.ds(pl.multiple_of(r * 32, 32), 32)
        y = (x_scr[rows, :].astype(F32) + acc_scr[rows, :].astype(BF).astype(F32)).astype(BF)
        x_scr[rows, :] = y
        o_scr[rows, :] = norm_rows(y, g_ref[...])
        return carry

    stores, r0 = [], 0
    for i, n in enumerate(parts):
        lax.fori_loop(r0 // 32, (r0 + n) // 32, rows32, 0)
        for k, scr in enumerate((x_scr, o_scr)):
            stores.append(pltpu.make_async_copy(scr.at[pl.ds(r0, n), :], outs[2 * i + k], out_sem.at[2 * i + k]))
            stores[-1].start()
        r0 += n
    for cp in stores:
        cp.wait()


def out_proj(os, ws, blocks, x_rows, gain, at, parts, after=()):
    dim = x_rows.shape[1]
    width = os[0].shape[1]
    n_run = len(os) // 4
    rows = n_run * RUN
    return pl.pallas_call(
        ordered(functools.partial(out_kernel, blocks=blocks, n_w=len(ws), n_run=n_run, at=at, parts=parts),
                len(os) + len(ws) + 2, after),
        grid=(1,),
        in_specs=[ANY] * (len(os) + len(ws) + 1) + [pl.BlockSpec((1, dim), lambda i: (0, 0))] + [ANY] * len(after),
        out_specs=[ANY] * (2 * len(parts)),
        out_shape=[jax.ShapeDtypeStruct((n, dim), BF) for n in parts for _ in range(2)],
        scratch_shapes=[pltpu.VMEM((rows, 4 * width), BF), pltpu.VMEM((3, width // 2, dim), BF), pltpu.VMEM((rows, dim), BF),
                        pltpu.VMEM((rows, dim), F32), pltpu.SemaphoreType.DMA((len(blocks), 2 * n_run)),
                        pltpu.SemaphoreType.DMA((3,)), pltpu.SemaphoreType.DMA, pltpu.SemaphoreType.DMA((2 * len(parts),))],
        name="outp", compiler_params=params(1),
        cost_estimate=cost(8 * rows * width * dim, 8 * width * dim),
    )(*os, *ws, x_rows, gain, *after)


def mlp_kernel(*refs, n_in, tn, td, nk, nd):
    b_refs = refs[:n_in]
    wg_ref, wu_ref, wd_ref, keep_ref, send_ref, b_scr, u_scr, w_scr, d_scr, b_sem, w_sem, d_sem = refs[n_in:]
    i = pl.program_id(0)
    rb = b_refs[0].shape[0]

    def fetch(j):
        @pl.when(j < nk)
        def _():
            cols = pl.ds(pl.multiple_of(j * tn, tn), tn)
            for k, w in enumerate((wg_ref, wu_ref)):
                pltpu.make_async_copy(w.at[:, cols], w_scr.at[lax.rem(j, 2), k], w_sem.at[lax.rem(j, 2)]).start()

        @pl.when((j >= nk) & (j < nk + nd))
        def _():
            n = j - nk
            pltpu.make_async_copy(wd_ref.at[:, pl.ds(pl.multiple_of(n * td, td), td)], d_scr.at[lax.rem(n, 2)],
                                  d_sem.at[lax.rem(n, 2)]).start()

    def gated(rows, cols, slot):
        b = b_scr[rows, :]
        gate = jnp.dot(b, w_scr[slot, 0], preferred_element_type=F32)
        up = jnp.dot(b, w_scr[slot, 1], preferred_element_type=F32)
        u_scr[rows, cols] = (jax.nn.silu(gate) * up).astype(BF)

    @pl.when(i == 0)
    def _():
        copies = [pltpu.make_async_copy(r, b_scr.at[pl.ds(k * rb, rb), :], b_sem.at[k]) for k, r in enumerate(b_refs)]
        copies[0].start()
        fetch(i)
        for cp in copies[1:]:
            cp.start()

    fetch(i + 1)

    @pl.when(i < nk)
    def _():
        pltpu.make_async_copy(w_scr.at[lax.rem(i, 2)], w_scr.at[lax.rem(i, 2)], w_sem.at[lax.rem(i, 2)]).wait()

    @pl.when(i == 0)
    def _():
        def one(k, carry):
            rows = pl.ds(pl.multiple_of(k * rb, rb), rb)
            pltpu.make_async_copy(b_scr.at[rows, :], b_scr.at[rows, :], b_sem.at[k]).wait()
            gated(rows, pl.ds(0, tn), 0)
            return carry

        lax.fori_loop(0, n_in, one, 0)

    @pl.when((i > 0) & (i < nk))
    def _():
        gated(slice(None), pl.ds(pl.multiple_of(i * tn, tn), tn), lax.rem(i, 2))

    @pl.when(i >= nk)
    def _():
        slot = lax.rem(i - nk, 2)
        pltpu.make_async_copy(d_scr.at[slot], d_scr.at[slot], d_sem.at[slot]).wait()
        d = jnp.dot(u_scr[...], d_scr[slot], preferred_element_type=F32).astype(BF)
        half = d.shape[0] // 2
        keep_ref[...] = d[:half]
        send_ref[...] = d[half:]


def mlp(bs, wg, wu, wd, after=()):
    rb, dim = bs[0].shape
    rows = rb * len(bs)
    ffn = wg.shape[1]
    tn, td = (256, 256) if rows > 512 else (512, 512)
    nk, nd = ffn // tn, dim // td
    dn = lambda i: (0, jnp.maximum(i - nk, 0))
    return pl.pallas_call(
        ordered(functools.partial(mlp_kernel, n_in=len(bs), tn=tn, td=td, nk=nk, nd=nd), len(bs) + 3, after),
        grid=(nk + nd,),
        in_specs=[ANY] * (len(bs) + 3 + len(after)),
        out_specs=[pl.BlockSpec((rows // 2, td), dn)] * 2,
        out_shape=[jax.ShapeDtypeStruct((rows // 2, dim), BF)] * 2,
        scratch_shapes=[pltpu.VMEM((rows, dim), BF), pltpu.VMEM((rows, ffn), BF), pltpu.VMEM((2, 2, dim, tn), BF),
                        pltpu.VMEM((2, ffn, td), BF), pltpu.SemaphoreType.DMA((len(bs),)), pltpu.SemaphoreType.DMA((2,)),
                        pltpu.SemaphoreType.DMA((2,))],
        name="mlp", compiler_params=params(1),
        cost_estimate=cost(6 * rows * dim * ffn, 6 * dim * ffn),
    )(*bs, wg, wu, wd, *after)


def sum_kernel(*refs):
    p_ref, r_ref, t_ref, y_ref, z_ref = refs[-5:]
    total = p_ref[...].astype(F32) + r_ref[...].astype(F32) + t_ref[...].astype(F32)
    z_ref[...] = (y_ref[...].astype(F32) + total.astype(BF).astype(F32)).astype(BF)


def sum_rows(z, keep, recv, far, y, first, total, after=(), tile=64):
    rows, dim = y.shape
    spec = pl.BlockSpec((tile, dim), lambda i: (i, 0))
    prev = () if z is None else (z,)
    return pl.pallas_call(
        ordered(sum_kernel, len(prev) + 4, after), grid=(rows // tile,),
        in_specs=[ANY] * len(prev) + [spec] * 4 + [ANY] * len(after),
        out_specs=pl.BlockSpec((tile, dim), lambda i: (first // tile + i, 0)),
        out_shape=jax.ShapeDtypeStruct((total, dim), BF),
        input_output_aliases={0: 0} if prev else {},
        name="zsum", compiler_params=params(1),
        cost_estimate=cost(rows * dim, 8 * rows * dim),
    )(*prev, keep, recv, far, y, *after)


def run_positions(xi, ci, y, cps, piece):
    def start(x, c):
        return (y if x == 0 else 2 * cps - 1 - y) * piece + c * (piece // 2)

    per = piece // 2 // RUN
    out = [start(xi, ci) + RUN * j for j in range(per)] + [start(xi, 1 - ci) + RUN * j for j in range(per)]
    for j in range(per):
        out += [start(1 - xi, ci) + RUN * j, start(1 - xi, 1 - ci) + RUN * j]
    return out


def block_list(tile, ids, pos, diag):
    runs = [(r, pos[r]) for r in ids]
    if diag is not None:
        n_tail = (len(runs) % 4) + 1
        tail = [(diag, pos[diag])] + runs[len(runs) - (n_tail - 1):]
        runs = runs[:len(runs) - (n_tail - 1)]
    else:
        n_tail = len(runs) % 4
        tail = runs[len(runs) - n_tail:]
        runs = runs[:len(runs) - n_tail]
    blocks = [[0, runs[i:i + 4]] for i in range(0, len(runs), 4)]
    if tail:
        full = tail + [(tail[0][0], FAR)] * (4 - len(tail))
        flags = sum(1 << k for k, (r, p) in enumerate(full) if p == FAR or r == diag)
        blocks.append([flags, full])
    blocks[-1][0] |= LAST
    blocks[0][0] |= FIRST
    return [[tile, flags, 0] + [r for r, _ in four] + [p for _, p in four] + [0] for flags, four in blocks]


def call_table(tiles, pos, pairs, carry, idle):
    rows, most = [], 0
    carry = [c if pairs[t][0] or pairs[t][1] else idle for t, c in enumerate(carry)]
    for t, tile in enumerate(tiles):
        ids, own = pairs[t]
        if ids or own:
            mine = block_list(t, ids, pos, tile if own else None)
            mine[0][1] |= CARRY if carry[t] else 0
            rows += mine
    for row in rows:
        most = max(most, max(row[3:7]) + 1)
        row[2] = most
    return [len(rows)] + [pos[t] for t in tiles] + carry + [v for row in rows for v in row], len(rows)


def work_tables(cps, piece):
    per = piece // 2 // RUN
    early = 2 * per + 2
    stage = lambda r: 0 if r < early else 1
    calls = [(0, list(range(early)))]
    calls += [(1, [j, per + j, 2 * per + 2 * j, 2 * per + 2 * j + 1]) for j in range(per)]
    tabs, all_runs, sizes = [], [], []
    for y in range(cps):
        for xi in range(2):
            for ci in range(2):
                mine = run_positions(xi, ci, y, cps, piece)
                pos = mine + run_positions(xi, ci, 1 - y, cps, piece)
                all_runs.append(mine)
                tabs.append([])
                sizes.append([])
                for now, tiles in calls:
                    pairs, carry = [], []
                    for t in tiles:
                        seen = [r for r in range(len(pos)) if pos[r] < pos[t]]
                        pairs.append(([r for r in seen if max(stage(r), stage(t)) == now], stage(t) == now))
                        carry.append(int(stage(t) < now))
                    tab, n = call_table(tiles, pos, pairs, carry, 2 if now == 1 else 0)
                    tabs[-1].append(tab)
                    sizes[-1].append(n)
    widths = [max(len(t[k]) for t in tabs) for k in range(len(calls))]
    flat = [[v for k, t in enumerate(tab) for v in t + [0] * (widths[k] - len(t))] for tab in tabs]
    bases = [sum(widths[:k]) for k in range(len(calls))]
    return np.array(flat, np.int32), np.array(all_runs, np.int32), bases, np.array(sizes).max(0) * 4


def solution(mesh):
    cps = mesh.shape['cp']
    row_spec = P('dp', ('cp', 'tp'), None)
    head_cols = P(None, 'tp', None)
    n_tp = mesh.shape['tp']

    over_core, over_x, over_both = (('tp', [(t, t ^ k) for t in range(n_tp)]) for k in (1, 2, 3))
    over_y = ('cp', [(i, i ^ 1) for i in range(cps)])

    def layer(x, g_attn, w_q, w_k, w_v, w_o, g_mlp, w_gate, w_up, w_down):
        x_rows = x[0]
        dim = x_rows.shape[1]
        n_run = x_rows.shape[0] // RUN
        piece = 2 * x_rows.shape[0]
        t_id, y_id = lax.axis_index('tp'), lax.axis_index('cp')
        np_tab, np_runs, bases, work = work_tables(cps, piece)
        dev = y_id * n_tp + t_id
        tab = lax.dynamic_index_in_dim(jnp.asarray(np_tab), dev, 0, keepdims=False)
        order = list(range(2 * n_run)) + [2 * n_run + i for i in (2, 3, 4, 5, 0, 1, 6, 7)]
        run_pos = lax.dynamic_index_in_dim(jnp.asarray(np_runs[:, order]), dev, 0, keepdims=False)

        def tied(v, *others):
            return lax.optimization_barrier((v, *others))[0]

        def send(axis_pairs, v):
            return lax.ppermute(v, *axis_pairs)

        ga, gm = g_attn.reshape(1, dim), g_mlp.reshape(1, dim)
        own = []
        for j in range(n_run):
            own.append(norm_run(x_rows, ga, j, after=own[-1:]))
        far = [send(over_x, own[j]) for j in range(n_run)]
        mate = [send(over_core, own[j]) for j in range(n_run)]

        w_all = jnp.concatenate([tied(w, own[-1]).reshape(dim, -1) for w in (w_q, w_k, w_v)], axis=1)
        tables = rope_tables(tied(run_pos, own[-1])[:, None] + jnp.arange(RUN, dtype=jnp.int32)[None, :])

        def relayed(j, after):
            here = tied(far[j], after)
            return [here, send(over_core, here)]

        q_here, kv_here = qkv(own + mate, w_all, (tables, 0))
        q_a, kv_a = qkv(relayed(0, kv_here), w_all, (tables, 2 * n_run + 4), after=(kv_here,))

        wo = w_o.reshape(-1, dim)
        half = wo.shape[0] // 2
        n_piece = n_run
        rows = half // n_piece
        wo_gated = tied(wo, kv_a)
        wo_x = [send(over_x, lax.dynamic_slice_in_dim(wo_gated, y_id * half + p * rows, rows, axis=0))
                for p in range(n_piece)]
        wo_c = send(over_core, wo_gated)
        early = relayed(1, kv_a)

        tile = lambda a, n: [(a, i) for i in range(n)]
        tiles = tile(0, 2 * n_run) + tile(1, 2)
        st, = flash(tab, [q_here, q_a], tiles, [kv_here, kv_a], base=bases[0], work=int(work[0]),
                   st_tiles=len(tiles))
        q_b, kv_b = qkv(early + relayed(2, st), w_all, (tables, 2 * n_run), after=(st,))
        q_c, kv_c = qkv(relayed(3, kv_b), w_all, (tables, 2 * n_run + 6), after=(kv_b,))
        kvs = [kv_here, kv_a, kv_b, kv_c]
        kvs = kvs + [send(over_y, kv) for kv in kvs]
        q_far = [(q_a, 0), (q_b, 0), (q_b, 2), (q_c, 0)]

        os, outs, prev = [], [], kv_c
        wo_a, wo_ya, wo_yb = {}, {}, {}

        def forward_w(p):
            here = tied(wo_x[p], prev)
            wo_ya[p] = (here, send(over_core, here))
            wo_a[p] = send(over_y, here)

        def relay_w(p):
            here = tied(wo_a[p], prev)
            wo_yb[p] = (here, send(over_core, here))

        def attend(j):
            q, at = q_far[j]
            held = 2 * n_run + 2 * j
            carried = [j, n_run + j] + ([held, held + 1] if j == 0 else [None, None])
            o_own, o_mate, o_far, o_fm = flash(
                tab, [q_here, q], [(0, j), (0, n_run + j), (1, at), (1, at + 1)], kvs,
                base=bases[1 + j], work=int(work[1 + j]), st=st, st_src=carried, after=(prev,))
            os.append([o_own, send(over_core, o_mate), send(over_x, o_far), send(over_both, o_fm)])
            return o_own

        def project(i):
            ws = [wo, wo_c]
            blocks = [[(0, 0, half)], [(0, half, half)], [(1, 0, half)], [(1, half, half)]]
            for k in range(2):
                for held in (wo_ya, wo_yb):
                    blocks.append([(len(ws) + p, 0, rows) for p in range(n_piece)])
                    ws += [held[p][k] for p in range(n_piece)]
            parts = (RUN, RUN) if i == 0 else (RUN, RUN // 2, RUN // 2)
            got = out_proj(os[2 * i] + os[2 * i + 1], ws, blocks, x_rows, gm, i, parts, after=(prev,))
            for y, b in zip(got[::2], got[1::2]):
                outs.append((y, b, send(over_x, b), send(over_core, b)))
            return got[0]

        last = n_run - 1
        for j in range(last):
            forward_w(j)
            if j:
                relay_w(j - 1)
            if j == last - 1:
                forward_w(last)
            prev = attend(j)
        for p in range(last - 1, n_piece):
            relay_w(p)
        prev = project(0)
        prev = attend(last)

        z, sums, relay = None, [], {}

        def relay_b(j):
            here = tied(outs[j][2], prev)
            relay[j] = (here, send(over_core, here))

        def finish(j):
            first = sum(o[0].shape[0] for o in outs[:j])
            return sum_rows(z, *sums[j], first, n_run * RUN, after=() if prev is z else (prev,))

        relay_b(0)
        n_part = n_run + 1
        for j in range(n_part):
            y, b, _, b_mate = outs[j]
            keep, out = mlp([b, relay[j][0], b_mate, relay[j][1]], w_gate, w_up, w_down, after=(prev,))
            recv = send(over_core, out)
            prev = keep
            if j == 0:
                relay_b(1)
                prev = project(1)
            else:
                if j + 1 < n_part:
                    relay_b(j + 1)
                if j > 1:
                    prev = z = finish(j - 2)
            kept = keep if prev is keep else tied(keep, prev)
            half = y.shape[0]
            prev = s_far = (kept[half:].astype(F32) + recv[half:].astype(F32)).astype(BF)
            sums.append((keep, recv, send(over_x, s_far), y))
        for j in (n_part - 2, n_part - 1):
            prev = z = finish(j)
        return z[None]

    return jax.shard_map(layer, mesh=mesh,
                         in_specs=(row_spec, P(), head_cols, head_cols, head_cols, P('tp', None, None),
                                   P(), P(None, 'tp'), P(None, 'tp'), P('tp', None)),
                         out_specs=row_spec, check_vma=False)
```

```python
import functools
import math
import jax
import jax.numpy as jnp
import numpy as np
from jax import lax
from jax.experimental import pallas as pl
from jax.experimental.pallas import tpu as pltpu
from jax.sharding import PartitionSpec as P

NORM_EPS = 1e-5
ROPE_THETA = 500000.0
HD = 128
RUN = 256
NEG = -1e30
FAR = 1 << 29
LOG2E = math.log2(math.e)
DN = (((1,), (0,)), ((), ()))
VMEM = 67043328
BF = jnp.bfloat16
F32 = jnp.float32
ANY = pl.BlockSpec(memory_space=pltpu.HBM)


def params(n):
    return pltpu.CompilerParams(dimension_semantics=("arbitrary",) * n, vmem_limit_bytes=VMEM)


def rope_tables(positions):
    half = HD // 2
    inv_freq = ROPE_THETA ** (-2.0 * jnp.arange(half, dtype=F32) / HD)
    angles = inv_freq[:, None] * positions.astype(F32)[..., None, :]
    return jnp.cos(angles), jnp.sin(angles)


def norm_rows(rows, gain):
    f = rows.astype(F32)
    mean_sq = jnp.mean(f * f, axis=-1, keepdims=True)
    return (f * lax.rsqrt(mean_sq + NORM_EPS) * gain.astype(F32)).astype(BF)


def cost(flops, moved):
    return pl.CostEstimate(flops=flops, transcendentals=0, bytes_accessed=moved)


def ordered(kernel, n_in, after):
    n = len(after)
    return lambda *refs: kernel(*refs[:n_in], *refs[n_in + n:])


def norm_kernel(x_ref, g_ref, o_ref):
    o_ref[...] = norm_rows(x_ref[...], g_ref[...])


def norm_run(x_rows, gain, j, after=(), tile=128):
    dim = x_rows.shape[1]
    per = RUN // tile
    return pl.pallas_call(
        ordered(norm_kernel, 2, after), grid=(per,),
        in_specs=[pl.BlockSpec((tile, dim), lambda i: (j * per + i, 0)), pl.BlockSpec((1, dim), lambda i: (0, 0))]
        + [ANY] * len(after),
        out_specs=pl.BlockSpec((tile, dim), lambda i: (i, 0)),
        out_shape=jax.ShapeDtypeStruct((RUN, dim), BF),
        name="norm", compiler_params=params(1),
        cost_estimate=cost(RUN * dim, RUN * dim),
    )(x_rows, gain, *after)


def qkv_kernel(*refs, n_in, n_q, group):
    a_refs = refs[:n_in]
    w_ref, cos_ref, sin_ref, q_ref, kv_ref, a_scr, sem = refs[n_in:]
    n = pl.program_id(0)
    heads = w_ref.shape[1] // HD

    @pl.when(n == 0)
    def _():
        for k, r in enumerate(a_refs):
            pltpu.make_async_copy(r, a_scr.at[pl.ds(k * RUN, RUN), :], sem.at[k]).start()

    def rope(f, i):
        f = f.astype(BF).astype(F32)
        lo, hi, cos, sin = f[:HD // 2], f[HD // 2:], cos_ref[i], sin_ref[i]
        return jnp.concatenate([lo * cos - hi * sin, hi * cos + lo * sin], axis=0)

    def one(k, carry):
        @pl.when(n == 0)
        def _():
            for i in range(group):
                rows = pl.ds(pl.multiple_of((k * group + i) * RUN, RUN), RUN)
                pltpu.make_async_copy(a_scr.at[rows, :], a_scr.at[rows, :], sem.at[k * group + i]).wait()

        rows = pl.ds(pl.multiple_of(k * group * RUN, group * RUN), group * RUN)
        r = jnp.dot(a_scr[rows, :], w_ref[...], preferred_element_type=F32)

        def piece(i, h):
            return r[i * RUN:(i + 1) * RUN, h * HD:(h + 1) * HD].T

        @pl.when(n < n_q)
        def _():
            for i in range(group):
                for h in range(heads):
                    q_ref[k * group + i, h * HD:(h + 1) * HD, :] = rope(piece(i, h), k * group + i).astype(BF)

        @pl.when(n == n_q)
        def _():
            for i in range(group):
                for h in range(heads // 2):
                    kv_ref[k * group + i, 0, :, h * HD:(h + 1) * HD] = rope(piece(i, h), k * group + i).T.astype(BF)
                    kv_ref[k * group + i, 1, h * HD:(h + 1) * HD, :] = piece(i, h + heads // 2).astype(BF)

        return carry

    lax.fori_loop(0, n_in // group, one, 0)


def qkv(rows, w_all, tables, after=(), group=2):
    n_in = len(rows)
    dim = w_all.shape[0]
    tn = 512
    n_q = w_all.shape[1] // tn - 1
    (cos, sin), first_run = tables
    at = first_run // n_in
    tab = pl.BlockSpec((n_in, HD // 2, RUN), lambda n: (at, 0, 0))
    return pl.pallas_call(
        ordered(functools.partial(qkv_kernel, n_in=n_in, n_q=n_q, group=group), n_in + 3, after),
        grid=(n_q + 1,),
        in_specs=[ANY] * n_in + [pl.BlockSpec((dim, tn), lambda n: (0, n)), tab, tab] + [ANY] * len(after),
        out_specs=[pl.BlockSpec((n_in, tn, RUN), lambda n: (0, jnp.minimum(n, n_q - 1), 0)),
                   pl.BlockSpec((n_in, 2, 256, 256), lambda n: (0, 0, 0, 0))],
        out_shape=[jax.ShapeDtypeStruct((n_in, n_q * tn, RUN), BF), jax.ShapeDtypeStruct((n_in, 2, 256, 256), BF)],
        scratch_shapes=[pltpu.VMEM((n_in * RUN, dim), BF), pltpu.SemaphoreType.DMA((n_in,))],
        name="qkv", compiler_params=params(1),
        cost_estimate=cost(2 * n_in * RUN * w_all.size, 2 * w_all.size),
    )(*rows, w_all, cos, sin, *after)


BLK = 12
LAST, FIRST, CARRY = 16, 32, 64
ST = HD + 16


def flash_kernel(tab_ref, *refs, q_src, kv_src, n_q, n_kv, st_src, n_st, base, G, n_tiles, n_heads, final):
    qs, kvs, sts = refs[:n_q], refs[n_q:n_q + n_kv], refs[n_q + n_kv:n_q + n_kv + n_st]
    n_out = n_tiles if final else 1
    at = n_q + n_kv + n_st
    outs = refs[at:at + n_out]
    q_scr, kv_scr, o_scr, st_scr, s_scr, mb_scr, acc_scr, m_scr, l_scr, q_sem, kv_sem, o_sem, st_sem = refs[at + n_out:]
    T = RUN
    c = (HD ** -0.5) * LOG2E
    n_blocks = tab_ref[base]
    carried = base + 1 + n_tiles
    row0 = base + 1 + 2 * n_tiles

    q_copies = [pltpu.make_async_copy(qs[a].at[i], q_scr.at[t], q_sem.at[t]) for t, (a, i) in enumerate(q_src)]
    kv_copies = [pltpu.make_async_copy(kvs[a].at[i], kv_scr.at[r], kv_sem.at[r]) for r, (a, i) in enumerate(kv_src)]
    first = 4
    q_copies[0].start()
    for cp in kv_copies[:first]:
        cp.start()
    for cp in q_copies[1:]:
        cp.start()
    for t, i in enumerate(st_src):
        if i is not None:
            @pl.when(tab_ref[carried + t] != 0)
            def _():
                pltpu.make_async_copy(sts[0].at[i], st_scr.at[t], st_sem.at[t]).start()
    for cp in kv_copies[first:]:
        cp.start()

    def block(i):
        g = lax.div(i, n_blocks)
        return row0 + BLK * (i - g * n_blocks), g

    def arrived(have, need):
        def one(r, carry):
            pltpu.make_async_copy(kv_scr.at[r], kv_scr.at[r], kv_sem.at[r]).wait()
            return carry

        lax.fori_loop(have, need, one, 0)
        return jnp.maximum(have, need)

    def put(s, h, k):
        s_scr[h, pl.ds(k * RUN, RUN), :] = s
        mb_scr[h, k] = jnp.max(s.reshape(RUN // 8, 8, T), axis=0)

    def stage_a(row, g, h):
        col = pl.multiple_of(g * HD, HD)
        qt = q_scr[tab_ref[row], pl.ds(pl.multiple_of((g * G + h) * HD, HD), HD), :]
        for k in range(4):
            put(lax.dot_general(kv_scr[tab_ref[row + 3 + k], 0, :, pl.ds(col, HD)], qt, DN, preferred_element_type=F32), h, k)

    def stage_b(row, g, h):
        col = pl.multiple_of(g * HD, HD)
        m_prev = m_scr[h]
        mb = jnp.maximum(jnp.maximum(mb_scr[h, 0], mb_scr[h, 1]), jnp.maximum(mb_scr[h, 2], mb_scr[h, 3]))
        for r in (4, 2, 1):
            mb = jnp.maximum(mb, pltpu.roll(mb, r, 0))
        m_new = jnp.maximum(m_prev, mb)
        m_scr[h] = m_new
        m_c = m_new * c
        alpha = jnp.exp2(m_prev * c - m_c)
        l, pv = l_scr[h] * alpha, None
        for k in range(4):
            p = jnp.exp2(s_scr[h, k * RUN:(k + 1) * RUN].reshape(RUN // 8, 8, T) * c - m_c[None])
            l = l + jnp.sum(p, axis=0)
            d = lax.dot_general(kv_scr[tab_ref[row + 3 + k], 1, pl.ds(col, HD), :], p.reshape(RUN, T).astype(BF), DN,
                                preferred_element_type=F32)
            pv = d if pv is None else pv + d
        l_scr[h] = l
        acc_scr[h] = (acc_scr[h].reshape(HD // 8, 8, T) * alpha[None]).reshape(HD, T) + pv

    def mask_runs(row, flags):
        qry = lax.broadcasted_iota(jnp.int32, (RUN, T), 1) + tab_ref[base + 1 + tab_ref[row]]
        key = lax.broadcasted_iota(jnp.int32, (RUN, T), 0)

        def one(k, carry):
            @pl.when((lax.shift_right_logical(flags, k) & 1) != 0)
            def _():
                mask = key + tab_ref[row + 7 + k] <= qry
                rows = pl.multiple_of(k * RUN, RUN)
                for h in range(G):
                    put(jnp.where(mask, s_scr[h, pl.ds(rows, RUN), :], NEG), h, k)

            return carry

        lax.fori_loop(0, 4, one, 0)

    def finish(tile, g, get):
        for h in range(G):
            acc, l = get(h)
            o_scr[tile, :, pl.ds(pl.multiple_of((g * G + h) * HD, HD), HD)] = (acc / jnp.sum(l, axis=0, keepdims=True)).T.astype(BF)

        @pl.when(g == n_heads - 1)
        def _():
            for k in range(n_tiles):
                @pl.when(tile == k)
                def _():
                    pltpu.make_async_copy(o_scr.at[k], outs[k], o_sem.at[k]).start()

    if final and n_st:
        def idle(i, carry):
            tile, g = lax.div(i, n_heads), lax.rem(i, n_heads)

            @pl.when(tab_ref[carried + tile] == 2)
            def _():
                @pl.when(g == 0)
                def _():
                    pltpu.make_async_copy(q_scr.at[tile], q_scr.at[tile], q_sem.at[tile]).wait()
                    pltpu.make_async_copy(st_scr.at[tile], st_scr.at[tile], st_sem.at[tile]).wait()

                finish(tile, g, lambda h: (st_scr[tile, g, h, :HD, :], st_scr[tile, g, h, HD + 8:, :]))

            return carry

        lax.fori_loop(0, n_tiles * n_heads, idle, 0)

    def query(row):
        t = tab_ref[row]
        pltpu.make_async_copy(q_scr.at[t], q_scr.at[t], q_sem.at[t]).wait()

    row, g = block(0)
    query(row)
    have = arrived(0, tab_ref[row + 2])
    for h in range(G):
        stage_a(row, g, h)

    def body(i, have):
        row, g = block(i)
        nrow, ng = block(jnp.minimum(i + 1, n_heads * n_blocks - 1))
        have = arrived(have, tab_ref[nrow + 2])
        flags = tab_ref[row + 1]
        tile = tab_ref[row]

        @pl.when((i + 1 < n_blocks) & ((tab_ref[nrow + 1] & FIRST) != 0))
        def _():
            query(nrow)

        @pl.when((flags & (FIRST | CARRY)) == FIRST)
        def _():
            acc_scr[...] = jnp.zeros_like(acc_scr)
            l_scr[...] = jnp.zeros_like(l_scr)
            m_scr[...] = jnp.full_like(m_scr, NEG)

        if n_st:
            @pl.when((flags & (FIRST | CARRY)) == (FIRST | CARRY))
            def _():
                @pl.when(g == 0)
                def _():
                    pltpu.make_async_copy(st_scr.at[tile], st_scr.at[tile], st_sem.at[tile]).wait()

                for h in range(G):
                    acc_scr[h] = st_scr[tile, g, h, :HD, :]
                    m_scr[h] = st_scr[tile, g, h, HD:HD + 8, :]
                    l_scr[h] = st_scr[tile, g, h, HD + 8:, :]

        @pl.when((flags & 15) != 0)
        def _():
            mask_runs(row, flags)

        for h in range(G):
            stage_b(row, g, h)
            stage_a(nrow, ng, h)

        @pl.when((flags & LAST) != 0)
        def _():
            if final:
                finish(tile, g, lambda h: (acc_scr[h], l_scr[h]))
            else:
                for h in range(G):
                    st_scr[tile, g, h, :HD, :] = acc_scr[h]
                    st_scr[tile, g, h, HD:HD + 8, :] = m_scr[h]
                    st_scr[tile, g, h, HD + 8:, :] = l_scr[h]

                @pl.when(g == n_heads - 1)
                def _():
                    pltpu.make_async_copy(st_scr.at[tile], outs[0].at[tile], o_sem.at[tile]).start()

        return have

    have = lax.fori_loop(0, n_heads * n_blocks, body, have)
    arrived(have, len(kv_src))
    if final:
        for k in range(n_tiles):
            pltpu.make_async_copy(o_scr.at[k], outs[k], o_sem.at[k]).wait()
    else:
        def wait_out(i, carry):
            row = row0 + BLK * i

            @pl.when((tab_ref[row + 1] & LAST) != 0)
            def _():
                t = tab_ref[row]
                pltpu.make_async_copy(st_scr.at[t], st_scr.at[t], o_sem.at[t]).wait()

            return carry

        lax.fori_loop(0, n_blocks, wait_out, 0)


def flash(tab, qs, q_src, kvs, *, base, work, st=None, st_src=None, st_tiles=None, after=()):
    nq = qs[0].shape[1]
    n_heads = 2
    G = nq // HD // n_heads
    n_tiles = len(q_src)
    final = st_tiles is None
    kv_src = [(a, i) for a, kv in enumerate(kvs) for i in range(kv.shape[0])]
    n_runs = len(kv_src)
    sts = () if st is None else (st,)
    n_in = 1 + len(qs) + len(kvs) + len(sts)
    state = (n_heads, G, ST, RUN)
    has_st = not final or sts
    return pl.pallas_call(
        ordered(functools.partial(flash_kernel, q_src=q_src, kv_src=kv_src, n_q=len(qs), n_kv=len(kvs),
                                  st_src=st_src or [None] * n_tiles, n_st=len(sts), base=base, G=G, n_tiles=n_tiles,
                                  n_heads=n_heads, final=final), n_in, after),
        grid_spec=pltpu.PrefetchScalarGridSpec(
            num_scalar_prefetch=1, grid=(),
            in_specs=[ANY] * (n_in - 1 + len(after)),
            out_specs=[ANY] * n_tiles if final else [ANY],
            scratch_shapes=[pltpu.VMEM((n_tiles, nq, RUN), BF),
                            pltpu.VMEM((n_runs, 2, 256, 256), BF),
                            pltpu.VMEM((n_tiles if final else 1, RUN, nq), BF),
                            pltpu.VMEM((n_tiles if has_st else 1, *state), F32),
                            pltpu.VMEM((G, 4 * RUN, RUN), F32),
                            pltpu.VMEM((G, 4, 8, RUN), F32),
                            pltpu.VMEM((G, HD, RUN), F32),
                            pltpu.VMEM((G, 8, RUN), F32),
                            pltpu.VMEM((G, 8, RUN), F32),
                            pltpu.SemaphoreType.DMA((n_tiles,)),
                            pltpu.SemaphoreType.DMA((n_runs,)),
                            pltpu.SemaphoreType.DMA((n_tiles,)),
                            pltpu.SemaphoreType.DMA((n_tiles,))]),
        out_shape=[jax.ShapeDtypeStruct((RUN, nq), BF)] * n_tiles if final
        else [jax.ShapeDtypeStruct((st_tiles, *state), F32)],
        input_output_aliases={n_in - 1: 0} if sts and not final else {},
        name="flash" if final else "flash_part", compiler_params=pltpu.CompilerParams(vmem_limit_bytes=VMEM),
        cost_estimate=cost(8 * work * RUN * RUN * nq, n_runs * RUN * nq),
    )(tab, *qs, *kvs, *sts, *after)


def out_kernel(*refs, blocks, n_w, n_run, at):
    n_o, n_out = 4 * n_run, 2 * n_run
    o_refs, w_refs, x_ref, g_ref = refs[:n_o], refs[n_o:n_o + n_w], refs[n_o + n_w], refs[n_o + n_w + 1]
    outs = refs[n_o + n_w + 2:n_o + n_w + 2 + n_out]
    o_scr, w_scr, x_scr, acc_scr, o_sem, w_sem, x_sem, out_sem = refs[n_o + n_w + 2 + n_out:]
    width = o_refs[0].shape[1]
    half = width // 2
    n_slots = w_scr.shape[0]

    def fetch(k):
        for i, pieces in enumerate(blocks):
            @pl.when(k == i)
            def _():
                to = 0
                for a, r0, n in pieces:
                    pltpu.make_async_copy(w_refs[a].at[pl.ds(r0, n), :], w_scr.at[i % n_slots, pl.ds(to, n), :],
                                          w_sem.at[i % n_slots]).start()
                    to += n

    mine = lax.axis_index('cp')
    loads = [[] for _ in blocks]
    for i in range(n_run):
        rows = pl.ds(i * RUN, RUN)
        for k in range(4):
            src = o_refs[4 * i + k]
            if k < 2:
                loads[2 * k].append((src, o_scr.at[rows, pl.ds(k * width, width)]))
            else:
                for p, part in enumerate((mine, 1 - mine)):
                    loads[2 * k + p].append((src.at[:, pl.ds(pl.multiple_of(part * half, half), half)],
                                             o_scr.at[rows, pl.ds(k * width + p * half, half)]))
    copies = [[pltpu.make_async_copy(src, dst, o_sem.at[k, i]) for i, (src, dst) in enumerate(ls)] for k, ls in enumerate(loads)]
    x_copy = pltpu.make_async_copy(x_ref.at[pl.ds(at * n_run * RUN, n_run * RUN), :], x_scr, x_sem)
    for cp in copies[0]:
        cp.start()
    for i in range(n_slots - 1):
        fetch(jnp.int32(i))
    for ls in copies[1:]:
        for cp in ls:
            cp.start()
    x_copy.start()
    acc_scr[...] = jnp.zeros_like(acc_scr)

    def one(k, carry):
        fetch(k + n_slots - 1)
        for i, ls in enumerate(copies):
            if ls:
                @pl.when(k == i)
                def _():
                    for cp in ls:
                        cp.wait()
        slot = lax.rem(k, n_slots)
        pltpu.make_async_copy(w_scr.at[slot], w_scr.at[slot], w_sem.at[slot]).wait()
        acc_scr[...] += jnp.dot(o_scr[:, pl.ds(pl.multiple_of(k * half, half), half)], w_scr[slot], preferred_element_type=F32)
        return carry

    lax.fori_loop(0, len(blocks), one, 0)
    x_copy.wait()

    def rows32(r, carry):
        rows = pl.ds(pl.multiple_of(r * 32, 32), 32)
        y = (x_scr[rows, :].astype(F32) + acc_scr[rows, :].astype(BF).astype(F32)).astype(BF)
        x_scr[rows, :] = y
        o_scr[rows, :] = norm_rows(y, g_ref[...])
        return carry

    stores, per = [], RUN // 32
    for i in range(n_run):
        lax.fori_loop(i * per, (i + 1) * per, rows32, 0)
        for k, scr in enumerate((x_scr, o_scr)):
            stores.append(pltpu.make_async_copy(scr.at[pl.ds(i * RUN, RUN), :], outs[2 * i + k], out_sem.at[2 * i + k]))
            stores[-1].start()
    for cp in stores:
        cp.wait()


def out_proj(os, ws, blocks, x_rows, gain, at, after=()):
    dim = x_rows.shape[1]
    width = os[0].shape[1]
    n_run = len(os) // 4
    rows = n_run * RUN
    return pl.pallas_call(
        ordered(functools.partial(out_kernel, blocks=blocks, n_w=len(ws), n_run=n_run, at=at),
                len(os) + len(ws) + 2, after),
        grid=(1,),
        in_specs=[ANY] * (len(os) + len(ws) + 1) + [pl.BlockSpec((1, dim), lambda i: (0, 0))] + [ANY] * len(after),
        out_specs=[ANY] * (2 * n_run),
        out_shape=[jax.ShapeDtypeStruct((RUN, dim), BF)] * (2 * n_run),
        scratch_shapes=[pltpu.VMEM((rows, 4 * width), BF), pltpu.VMEM((3, width // 2, dim), BF), pltpu.VMEM((rows, dim), BF),
                        pltpu.VMEM((rows, dim), F32), pltpu.SemaphoreType.DMA((len(blocks), 2 * n_run)),
                        pltpu.SemaphoreType.DMA((3,)), pltpu.SemaphoreType.DMA, pltpu.SemaphoreType.DMA((2 * n_run,))],
        name="outp", compiler_params=params(1),
        cost_estimate=cost(8 * rows * width * dim, 8 * width * dim),
    )(*os, *ws, x_rows, gain, *after)


def mlp_kernel(*refs, n_in, first, rb, tn, td, nk, nd):
    b_refs = refs[:n_in]
    wg_ref, wu_ref, wd_ref, keep_ref, send_ref, b_scr, u_scr, w_scr, d_scr, b_sem, w_sem, d_sem = refs[n_in:]
    i = pl.program_id(0)

    def fetch(j):
        def tile(src, dst, sem):
            part = src.shape[0] // 4
            for r in range(0, src.shape[0], part):
                pltpu.make_async_copy(src.at[pl.ds(r, part), :], dst.at[pl.ds(r, part), :], sem).start()

        @pl.when(j < nk)
        def _():
            cols = pl.ds(pl.multiple_of(j * tn, tn), tn)
            for k, w in enumerate((wg_ref, wu_ref)):
                tile(w.at[:, cols], w_scr.at[lax.rem(j, 2), k], w_sem.at[lax.rem(j, 2)])

        @pl.when((j >= nk) & (j < nk + nd))
        def _():
            n = j - nk
            tile(wd_ref.at[:, pl.ds(pl.multiple_of(n * td, td), td)], d_scr.at[lax.rem(n, 2)], d_sem.at[lax.rem(n, 2)])

    def gated(rows, cols, slot):
        b = b_scr[rows, :]
        gate = jnp.dot(b, w_scr[slot, 0], preferred_element_type=F32)
        up = jnp.dot(b, w_scr[slot, 1], preferred_element_type=F32)
        u_scr[rows, cols] = (jax.nn.silu(gate) * up).astype(BF)

    @pl.when(i == 0)
    def _():
        copies = [pltpu.make_async_copy(r.at[pl.ds(first, rb), :], b_scr.at[pl.ds(k * rb, rb), :], b_sem.at[k])
                  for k, r in enumerate(b_refs)]
        copies[0].start()
        fetch(i)
        for cp in copies[1:]:
            cp.start()

    fetch(i + 1)

    @pl.when(i < nk)
    def _():
        pltpu.make_async_copy(w_scr.at[lax.rem(i, 2)], w_scr.at[lax.rem(i, 2)], w_sem.at[lax.rem(i, 2)]).wait()

    @pl.when(i == 0)
    def _():
        def one(k, carry):
            rows = pl.ds(pl.multiple_of(k * rb, rb), rb)
            pltpu.make_async_copy(b_scr.at[rows, :], b_scr.at[rows, :], b_sem.at[k]).wait()
            gated(rows, pl.ds(0, tn), 0)
            return carry

        lax.fori_loop(0, n_in, one, 0)

    @pl.when((i > 0) & (i < nk))
    def _():
        gated(slice(None), pl.ds(pl.multiple_of(i * tn, tn), tn), lax.rem(i, 2))

    @pl.when(i >= nk)
    def _():
        slot = lax.rem(i - nk, 2)
        pltpu.make_async_copy(d_scr.at[slot], d_scr.at[slot], d_sem.at[slot]).wait()
        d = jnp.dot(u_scr[...], d_scr[slot], preferred_element_type=F32).astype(BF)
        half = d.shape[0] // 2
        keep_ref[...] = d[:half]
        send_ref[...] = d[half:]


def mlp(bs, first, rb, wg, wu, wd, after=()):
    dim = bs[0].shape[1]
    rows = rb * len(bs)
    ffn = wg.shape[1]
    td = 512
    tn = td if rows <= td else td // 2
    nk, nd = ffn // tn, dim // td
    dn = lambda i: (0, jnp.maximum(i - nk, 0))
    return pl.pallas_call(
        ordered(functools.partial(mlp_kernel, n_in=len(bs), first=first, rb=rb, tn=tn, td=td, nk=nk, nd=nd), len(bs) + 3, after),
        grid=(nk + nd,),
        in_specs=[ANY] * (len(bs) + 3 + len(after)),
        out_specs=[pl.BlockSpec((rows // 2, td), dn)] * 2,
        out_shape=[jax.ShapeDtypeStruct((rows // 2, dim), BF)] * 2,
        scratch_shapes=[pltpu.VMEM((rows, dim), BF), pltpu.VMEM((rows, ffn), BF), pltpu.VMEM((2, 2, dim, tn), BF),
                        pltpu.VMEM((2, ffn, td), BF), pltpu.SemaphoreType.DMA((len(bs),)), pltpu.SemaphoreType.DMA((2,)),
                        pltpu.SemaphoreType.DMA((2,))],
        name="mlp", compiler_params=params(1),
        cost_estimate=cost(6 * rows * dim * ffn, 6 * dim * ffn),
    )(*bs, wg, wu, wd, *after)


def sum_kernel(*refs):
    p_ref, r_ref, t_ref, y_ref, z_ref = refs[-5:]
    total = p_ref[...].astype(F32) + r_ref[...].astype(F32) + t_ref[...].astype(F32)
    z_ref[...] = (y_ref[...].astype(F32) + total.astype(BF).astype(F32)).astype(BF)


def sum_rows(z, keep, recv, far, y, y_first, rows, first, total, after=(), tile=64):
    dim = y.shape[1]
    at = lambda r0: pl.BlockSpec((tile, dim), lambda i: (r0 // tile + i, 0))
    prev = () if z is None else (z,)
    return pl.pallas_call(
        ordered(sum_kernel, len(prev) + 4, after), grid=(rows // tile,),
        in_specs=[ANY] * len(prev) + [at(0)] * 3 + [at(y_first)] + [ANY] * len(after),
        out_specs=at(first),
        out_shape=jax.ShapeDtypeStruct((total, dim), BF),
        input_output_aliases={0: 0} if prev else {},
        name="zsum", compiler_params=params(1),
        cost_estimate=cost(rows * dim, 8 * rows * dim),
    )(*prev, keep, recv, far, y, *after)


def run_positions(xi, ci, y, cps, piece):
    def start(x, c):
        return (y if x == 0 else 2 * cps - 1 - y) * piece + c * (piece // 2)

    per = piece // 2 // RUN
    out = [start(xi, ci) + RUN * j for j in range(per)] + [start(xi, 1 - ci) + RUN * j for j in range(per)]
    for j in range(per):
        out += [start(1 - xi, ci) + RUN * j, start(1 - xi, 1 - ci) + RUN * j]
    return out


def block_list(tile, ids, pos, diag):
    runs = [(r, pos[r]) for r in ids]
    if diag is not None:
        n_tail = (len(runs) % 4) + 1
        tail = [(diag, pos[diag])] + runs[len(runs) - (n_tail - 1):]
        runs = runs[:len(runs) - (n_tail - 1)]
    else:
        n_tail = len(runs) % 4
        tail = runs[len(runs) - n_tail:]
        runs = runs[:len(runs) - n_tail]
    blocks = [[0, runs[i:i + 4]] for i in range(0, len(runs), 4)]
    if tail:
        full = tail + [(tail[0][0], FAR)] * (4 - len(tail))
        flags = sum(1 << k for k, (r, p) in enumerate(full) if p == FAR or r == diag)
        blocks.append([flags, full])
    blocks[-1][0] |= LAST
    blocks[0][0] |= FIRST
    return [[tile, flags, 0] + [r for r, _ in four] + [p for _, p in four] + [0] for flags, four in blocks]


def call_table(tiles, pos, pairs, carry, idle):
    rows, most = [], 0
    carry = [c if pairs[t][0] or pairs[t][1] else idle for t, c in enumerate(carry)]
    for t, tile in enumerate(tiles):
        ids, own = pairs[t]
        if ids or own:
            mine = block_list(t, ids, pos, tile if own else None)
            mine[0][1] |= CARRY if carry[t] else 0
            rows += mine
    for row in rows:
        most = max(most, max(row[3:7]) + 1)
        row[2] = most
    return [len(rows)] + [pos[t] for t in tiles] + carry + [v for row in rows for v in row], len(rows)


def work_tables(cps, piece):
    per = piece // 2 // RUN
    early = 2 * per + 2
    stage = lambda r: 0 if r < early else 1
    calls = [(0, list(range(early)))]
    calls += [(1, [j, per + j, 2 * per + 2 * j, 2 * per + 2 * j + 1]) for j in range(per)]
    tabs, all_runs, sizes = [], [], []
    for y in range(cps):
        for xi in range(2):
            for ci in range(2):
                mine = run_positions(xi, ci, y, cps, piece)
                pos = mine + run_positions(xi, ci, 1 - y, cps, piece)
                all_runs.append(mine)
                tabs.append([])
                sizes.append([])
                for now, tiles in calls:
                    pairs, carry = [], []
                    for t in tiles:
                        seen = [r for r in range(len(pos)) if pos[r] < pos[t]]
                        when = {r: max(stage(r), stage(t)) for r in seen}
                        late = list(when.values()).count(1) + stage(t)
                        soon = len(seen) + 1 - late
                        if late and soon % 4 <= -late % 4:
                            for r in [r for r in seen if not when[r]][:soon % 4]:
                                when[r] = 1
                        pairs.append(([r for r in seen if when[r] == now], stage(t) == now))
                        carry.append(int(stage(t) < now))
                    tab, n = call_table(tiles, pos, pairs, carry, 2 if now == 1 else 0)
                    tabs[-1].append(tab)
                    sizes[-1].append(n)
    widths = [max(len(t[k]) for t in tabs) for k in range(len(calls))]
    flat = [[v for k, t in enumerate(tab) for v in t + [0] * (widths[k] - len(t))] for tab in tabs]
    bases = [sum(widths[:k]) for k in range(len(calls))]
    return np.array(flat, np.int32), np.array(all_runs, np.int32), bases, np.array(sizes).max(0) * 4


def solution(mesh):
    cps = mesh.shape['cp']
    row_spec = P('dp', ('cp', 'tp'), None)
    head_cols = P(None, 'tp', None)
    n_tp = mesh.shape['tp']

    over_core, over_x, over_both = (('tp', [(t, t ^ k) for t in range(n_tp)]) for k in (1, 2, 3))
    over_y = ('cp', [(i, i ^ 1) for i in range(cps)])

    def layer(x, g_attn, w_q, w_k, w_v, w_o, g_mlp, w_gate, w_up, w_down):
        x_rows = x[0]
        dim = x_rows.shape[1]
        n_run = x_rows.shape[0] // RUN
        piece = 2 * x_rows.shape[0]
        t_id, y_id = lax.axis_index('tp'), lax.axis_index('cp')
        np_tab, np_runs, bases, work = work_tables(cps, piece)
        dev = y_id * n_tp + t_id
        tab = lax.dynamic_index_in_dim(jnp.asarray(np_tab), dev, 0, keepdims=False)
        run_pos = lax.dynamic_index_in_dim(jnp.asarray(np_runs), dev, 0, keepdims=False)

        def tied(v, *others):
            return lax.optimization_barrier((v, *others))[0]

        def send(axis_pairs, v):
            return lax.ppermute(v, *axis_pairs)

        ga, gm = g_attn.reshape(1, dim), g_mlp.reshape(1, dim)
        own = []
        for j in range(n_run):
            own.append(norm_run(x_rows, ga, j, after=own[-1:]))
        far = [send(over_x, own[j]) for j in range(n_run)]
        mate = [send(over_core, own[j]) for j in range(n_run)]

        w_all = jnp.concatenate([tied(w, own[-1]).reshape(dim, -1) for w in (w_q, w_k, w_v)], axis=1)
        tables = rope_tables(tied(run_pos, own[-1])[:, None] + jnp.arange(RUN, dtype=jnp.int32)[None, :])

        q_here, kv_here = qkv(own + mate, w_all, (tables, 0))
        kvs, q_far = [kv_here], []

        def far_qkv(j, after):
            here = tied(far[j], after)
            q, kv = qkv([here, send(over_core, here)], w_all, (tables, 2 * (n_run + j)), after=(after,))
            q_far.append(q)
            kvs.append(kv)
            return kv

        far_qkv(1, far_qkv(0, kv_here))

        wo = w_o.reshape(-1, dim)
        half = wo.shape[0] // 2
        n_piece = 2
        rows = half // n_piece
        wo_gated = tied(wo, kvs[-1])
        wo_x = [send(over_x, lax.dynamic_slice_in_dim(wo_gated, y_id * half + p * rows, rows, axis=0))
                for p in range(n_piece)]
        wo_c = send(over_core, wo_gated)

        tiles = [(0, i) for i in range(2 * n_run)] + [(1, 0), (1, 1)]
        st, = flash(tab, [q_here, q_far[0]], tiles, kvs[:2], base=bases[0], work=int(work[0]),
                   st_tiles=len(tiles), after=(kvs[-1],))
        far_qkv(3, far_qkv(2, st))
        kvs = kvs + [send(over_y, kv) for kv in kvs]

        os, outs, prev = [], [], kvs[n_run]
        wo_a, wo_ya, wo_yb = {}, {}, {}

        def forward_w(p):
            here = tied(wo_x[p], prev)
            wo_ya[p] = (here, send(over_core, here))
            wo_a[p] = send(over_y, here)

        def relay_w(p):
            here = tied(wo_a[p], prev)
            wo_yb[p] = (here, send(over_core, here))

        def attend(j):
            held = 2 * n_run + 2 * j
            carried = [j, n_run + j] + ([held, held + 1] if j == 0 else [None, None])
            o_own, o_mate, o_far, o_fm = flash(
                tab, [q_here, q_far[j]], [(0, j), (0, n_run + j), (1, 0), (1, 1)], kvs,
                base=bases[1 + j], work=int(work[1 + j]), st=st, st_src=carried, after=(prev,))
            os.append([o_own, send(over_core, o_mate), send(over_x, o_far), send(over_both, o_fm)])
            return o_own

        def project(i):
            ws = [wo, wo_c]
            blocks = [[(0, 0, half)], [(0, half, half)], [(1, 0, half)], [(1, half, half)]]
            for k in range(2):
                for held in (wo_ya, wo_yb):
                    blocks.append([(len(ws) + p, 0, rows) for p in range(n_piece)])
                    ws += [held[p][k] for p in range(n_piece)]
            got = out_proj(os[2 * i] + os[2 * i + 1], ws, blocks, x_rows, gm, i, after=(prev,))
            for y, b in zip(got[::2], got[1::2]):
                outs.append((y, b, send(over_x, b), send(over_core, b)))
            return got[0]

        last = n_run - 1
        for j in range(last):
            prev = attend(j)
            if j < n_piece:
                forward_w(j)
            if j:
                relay_w(j - 1)
        prev = project(0)
        prev = attend(last)

        z, sums, relay = None, [], {}

        def relay_b(j):
            here = tied(outs[j][2], prev)
            relay[j] = (here, send(over_core, here))

        chunks = [(j, 0, RUN) for j in range(last)] + [(last, 0, RUN // 2), (last, RUN // 2, RUN // 2)]

        def finish(c):
            j, first, size = chunks[c]
            return sum_rows(z, *sums[c], outs[j][0], first, size, j * RUN + first, n_run * RUN,
                        after=() if prev is z else (prev,))

        relay_b(0)
        for c, (j, first, size) in enumerate(chunks):
            b = [outs[j][1], relay[j][0], outs[j][3], relay[j][1]]
            keep, out = mlp(b, first, size, w_gate, w_up, w_down, after=(prev,))
            recv = send(over_core, out)
            prev = keep
            if c < last:
                relay_b(c + 1)
            if c == 0:
                prev = project(1)
            elif c > 1:
                prev = z = finish(c - 2)
            kept = keep if prev is keep else tied(keep, prev)
            prev = s_far = (kept[size:].astype(F32) + recv[size:].astype(F32)).astype(BF)
            sums.append((keep, recv, send(over_x, s_far)))
        for c in (last, n_run):
            prev = z = finish(c)
        return z[None]

    return jax.shard_map(layer, mesh=mesh,
                         in_specs=(row_spec, P(), head_cols, head_cols, head_cols, P('tp', None, None),
                                   P(), P(None, 'tp'), P(None, 'tp'), P('tp', None)),
                         out_specs=row_spec, check_vma=False)
```

```python
import functools
import math
import jax
import jax.numpy as jnp
import numpy as np
from jax import lax
from jax.experimental import pallas as pl
from jax.experimental.pallas import tpu as pltpu
from jax.sharding import PartitionSpec as P

NORM_EPS = 1e-5
ROPE_THETA = 500000.0
HD = 128
RUN = 256
NEG = -1e30
FAR = 1 << 29
LOG2E = math.log2(math.e)
DN = (((1,), (0,)), ((), ()))
VMEM = 67043328
BF = jnp.bfloat16
F32 = jnp.float32
ANY = pl.BlockSpec(memory_space=pltpu.HBM)


def params(n):
    return pltpu.CompilerParams(dimension_semantics=("arbitrary",) * n, vmem_limit_bytes=VMEM)


def rope_tables(positions):
    half = HD // 2
    inv_freq = ROPE_THETA ** (-2.0 * jnp.arange(half, dtype=F32) / HD)
    angles = inv_freq[:, None] * positions.astype(F32)[..., None, :]
    return jnp.cos(angles), jnp.sin(angles)


def norm_rows(rows, gain):
    f = rows.astype(F32)
    mean_sq = jnp.mean(f * f, axis=-1, keepdims=True)
    return (f * lax.rsqrt(mean_sq + NORM_EPS) * gain.astype(F32)).astype(BF)


def cost(flops, moved):
    return pl.CostEstimate(flops=flops, transcendentals=0, bytes_accessed=moved)


def ordered(kernel, n_in, after):
    n = len(after)
    return lambda *refs: kernel(*refs[:n_in], *refs[n_in + n:])


def norm_kernel(x_ref, g_ref, o_ref):
    o_ref[...] = norm_rows(x_ref[...], g_ref[...])


def norm_run(x_rows, gain, j, after=(), tile=128):
    dim = x_rows.shape[1]
    per = RUN // tile
    return pl.pallas_call(
        ordered(norm_kernel, 2, after), grid=(per,),
        in_specs=[pl.BlockSpec((tile, dim), lambda i: (j * per + i, 0)), pl.BlockSpec((1, dim), lambda i: (0, 0))]
        + [ANY] * len(after),
        out_specs=pl.BlockSpec((tile, dim), lambda i: (i, 0)),
        out_shape=jax.ShapeDtypeStruct((RUN, dim), BF),
        name="norm", compiler_params=params(1),
        cost_estimate=cost(RUN * dim, RUN * dim),
    )(x_rows, gain, *after)


def qkv_kernel(*refs, n_in, n_q, group, first, with_q, with_kv):
    a_refs = refs[:n_in]
    w_ref, cos_ref, sin_ref, *outs, a_scr, sem = refs[n_in:]
    q_ref, kv_ref = outs[0], outs[-1]
    n = pl.program_id(0) + first
    heads = w_ref.shape[1] // HD

    @pl.when(n == first)
    def _():
        for k, r in enumerate(a_refs):
            pltpu.make_async_copy(r, a_scr.at[pl.ds(k * RUN, RUN), :], sem.at[k]).start()

    def rope(f, i):
        f = f.astype(BF).astype(F32)
        lo, hi, cos, sin = f[:HD // 2], f[HD // 2:], cos_ref[i], sin_ref[i]
        return jnp.concatenate([lo * cos - hi * sin, hi * cos + lo * sin], axis=0)

    def one(k, carry):
        @pl.when(n == first)
        def _():
            for i in range(group):
                rows = pl.ds(pl.multiple_of((k * group + i) * RUN, RUN), RUN)
                pltpu.make_async_copy(a_scr.at[rows, :], a_scr.at[rows, :], sem.at[k * group + i]).wait()

        rows = pl.ds(pl.multiple_of(k * group * RUN, group * RUN), group * RUN)
        r = jnp.dot(a_scr[rows, :], w_ref[...], preferred_element_type=F32)

        def piece(i, h):
            return r[i * RUN:(i + 1) * RUN, h * HD:(h + 1) * HD].T

        @pl.when((n < n_q) if with_q else False)
        def _():
            for i in range(group):
                for h in range(heads):
                    q_ref[k * group + i, h * HD:(h + 1) * HD, :] = rope(piece(i, h), k * group + i).astype(BF)

        @pl.when((n == n_q) if with_kv else False)
        def _():
            for i in range(group):
                for h in range(heads // 2):
                    kv_ref[k * group + i, 0, :, h * HD:(h + 1) * HD] = rope(piece(i, h), k * group + i).T.astype(BF)
                    kv_ref[k * group + i, 1, h * HD:(h + 1) * HD, :] = piece(i, h + heads // 2).astype(BF)

        return carry

    lax.fori_loop(0, n_in // group, one, 0)


def qkv(rows, w_all, tables, with_q=True, with_kv=True, after=(), group=2):
    n_in = len(rows)
    dim = w_all.shape[0]
    tn = 512
    n_q = w_all.shape[1] // tn - 1
    (cos, sin), first_run = tables
    at = first_run // n_in
    start = 0 if with_q else n_q
    kv_shape = (n_in, 2, RUN, RUN)
    tab = pl.BlockSpec((n_in, HD // 2, RUN), lambda n: (at, 0, 0))
    return pl.pallas_call(
        ordered(functools.partial(qkv_kernel, n_in=n_in, n_q=n_q, group=group, first=start, with_q=with_q, with_kv=with_kv),
                n_in + 3, after),
        grid=(n_q * with_q + with_kv,),
        in_specs=[ANY] * n_in + [pl.BlockSpec((dim, tn), lambda n: (0, n + start)), tab, tab] + [ANY] * len(after),
        out_specs=[pl.BlockSpec((n_in, tn, RUN), lambda n: (0, jnp.minimum(n, n_q - 1), 0))] * with_q
        + [pl.BlockSpec(kv_shape, lambda n: (0,) * len(kv_shape))] * with_kv,
        out_shape=[jax.ShapeDtypeStruct((n_in, n_q * tn, RUN), BF)] * with_q + [jax.ShapeDtypeStruct(kv_shape, BF)] * with_kv,
        scratch_shapes=[pltpu.VMEM((n_in * RUN, dim), BF), pltpu.SemaphoreType.DMA((n_in,))],
        name="qkv", compiler_params=params(1),
        cost_estimate=cost(2 * n_in * RUN * w_all.size, 2 * w_all.size),
    )(*rows, w_all, cos, sin, *after)


BLK = 12
LAST, FIRST, CARRY = 16, 32, 64
ST = HD + 16


def flash_kernel(tab_ref, *refs, q_src, kv_src, n_q, n_kv, st_src, n_st, base, G, n_tiles, n_heads, final):
    qs, kvs, sts = refs[:n_q], refs[n_q:n_q + n_kv], refs[n_q + n_kv:n_q + n_kv + n_st]
    n_out = n_tiles if final else 1
    at = n_q + n_kv + n_st
    outs = refs[at:at + n_out]
    q_scr, kv_scr, o_scr, st_scr, s_scr, mb_scr, acc_scr, m_scr, l_scr, q_sem, kv_sem, o_sem, st_sem = refs[at + n_out:]
    T = RUN
    c = (HD ** -0.5) * LOG2E
    n_blocks = tab_ref[base]
    carried = base + 1 + n_tiles
    row0 = base + 1 + 2 * n_tiles

    q_copies = [pltpu.make_async_copy(qs[a].at[i], q_scr.at[t], q_sem.at[t]) for t, (a, i) in enumerate(q_src)]
    kv_copies = [pltpu.make_async_copy(kvs[a].at[i], kv_scr.at[r], kv_sem.at[r]) for r, (a, i) in enumerate(kv_src)]
    first = 4
    q_copies[0].start()
    for cp in kv_copies[:first]:
        cp.start()
    for cp in q_copies[1:]:
        cp.start()
    for t, i in enumerate(st_src):
        if i is not None:
            @pl.when(tab_ref[carried + t] != 0)
            def _():
                pltpu.make_async_copy(sts[0].at[i], st_scr.at[t], st_sem.at[t]).start()
    for cp in kv_copies[first:]:
        cp.start()

    def block(i):
        g = lax.div(i, n_blocks)
        return row0 + BLK * (i - g * n_blocks), g

    def arrived(have, need):
        def one(r, carry):
            pltpu.make_async_copy(kv_scr.at[r], kv_scr.at[r], kv_sem.at[r]).wait()
            return carry

        lax.fori_loop(have, need, one, 0)
        return jnp.maximum(have, need)

    def put(s, h, k):
        s_scr[h, pl.ds(k * RUN, RUN), :] = s
        mb_scr[h, k] = jnp.max(s.reshape(RUN // 8, 8, T), axis=0)

    def stage_a(row, g, h):
        col = pl.multiple_of(g * HD, HD)
        qt = q_scr[tab_ref[row], pl.ds(pl.multiple_of((g * G + h) * HD, HD), HD), :]
        for k in range(4):
            put(lax.dot_general(kv_scr[tab_ref[row + 3 + k], 0, :, pl.ds(col, HD)], qt, DN, preferred_element_type=F32), h, k)

    def stage_b(row, g, h):
        col = pl.multiple_of(g * HD, HD)
        m_prev = m_scr[h]
        mb = jnp.maximum(jnp.maximum(mb_scr[h, 0], mb_scr[h, 1]), jnp.maximum(mb_scr[h, 2], mb_scr[h, 3]))
        for r in (4, 2, 1):
            mb = jnp.maximum(mb, pltpu.roll(mb, r, 0))
        m_new = jnp.maximum(m_prev, mb)
        m_scr[h] = m_new
        m_c = m_new * c
        alpha = jnp.exp2(m_prev * c - m_c)
        l, pv = l_scr[h] * alpha, None
        for k in range(4):
            p = jnp.exp2(s_scr[h, k * RUN:(k + 1) * RUN].reshape(RUN // 8, 8, T) * c - m_c[None])
            l = l + jnp.sum(p, axis=0)
            d = lax.dot_general(kv_scr[tab_ref[row + 3 + k], 1, pl.ds(col, HD), :], p.reshape(RUN, T).astype(BF), DN,
                                preferred_element_type=F32)
            pv = d if pv is None else pv + d
        l_scr[h] = l
        acc_scr[h] = (acc_scr[h].reshape(HD // 8, 8, T) * alpha[None]).reshape(HD, T) + pv

    def mask_runs(row, flags):
        qry = lax.broadcasted_iota(jnp.int32, (RUN, T), 1) + tab_ref[base + 1 + tab_ref[row]]
        key = lax.broadcasted_iota(jnp.int32, (RUN, T), 0)

        def one(k, carry):
            @pl.when((lax.shift_right_logical(flags, k) & 1) != 0)
            def _():
                mask = key + tab_ref[row + 7 + k] <= qry
                rows = pl.multiple_of(k * RUN, RUN)
                for h in range(G):
                    put(jnp.where(mask, s_scr[h, pl.ds(rows, RUN), :], NEG), h, k)

            return carry

        lax.fori_loop(0, 4, one, 0)

    def finish(tile, g, get):
        for h in range(G):
            acc, l = get(h)
            o_scr[tile, :, pl.ds(pl.multiple_of((g * G + h) * HD, HD), HD)] = (acc / jnp.sum(l, axis=0, keepdims=True)).T.astype(BF)

        @pl.when(g == n_heads - 1)
        def _():
            for k in range(n_tiles):
                @pl.when(tile == k)
                def _():
                    pltpu.make_async_copy(o_scr.at[k], outs[k], o_sem.at[k]).start()

    if final and n_st:
        def idle(i, carry):
            tile, g = lax.div(i, n_heads), lax.rem(i, n_heads)

            @pl.when(tab_ref[carried + tile] == 2)
            def _():
                @pl.when(g == 0)
                def _():
                    pltpu.make_async_copy(q_scr.at[tile], q_scr.at[tile], q_sem.at[tile]).wait()
                    pltpu.make_async_copy(st_scr.at[tile], st_scr.at[tile], st_sem.at[tile]).wait()

                finish(tile, g, lambda h: (st_scr[tile, g, h, :HD, :], st_scr[tile, g, h, HD + 8:, :]))

            return carry

        lax.fori_loop(0, n_tiles * n_heads, idle, 0)

    def query(row):
        t = tab_ref[row]
        pltpu.make_async_copy(q_scr.at[t], q_scr.at[t], q_sem.at[t]).wait()

    row, g = block(0)
    query(row)
    have = arrived(0, tab_ref[row + 2])
    for h in range(G):
        stage_a(row, g, h)

    def body(i, have):
        row, g = block(i)
        nrow, ng = block(jnp.minimum(i + 1, n_heads * n_blocks - 1))
        have = arrived(have, tab_ref[nrow + 2])
        flags = tab_ref[row + 1]
        tile = tab_ref[row]

        @pl.when((i + 1 < n_blocks) & ((tab_ref[nrow + 1] & FIRST) != 0))
        def _():
            query(nrow)

        @pl.when((flags & (FIRST | CARRY)) == FIRST)
        def _():
            acc_scr[...] = jnp.zeros_like(acc_scr)
            l_scr[...] = jnp.zeros_like(l_scr)
            m_scr[...] = jnp.full_like(m_scr, NEG)

        if n_st:
            @pl.when((flags & (FIRST | CARRY)) == (FIRST | CARRY))
            def _():
                @pl.when(g == 0)
                def _():
                    pltpu.make_async_copy(st_scr.at[tile], st_scr.at[tile], st_sem.at[tile]).wait()

                for h in range(G):
                    acc_scr[h] = st_scr[tile, g, h, :HD, :]
                    m_scr[h] = st_scr[tile, g, h, HD:HD + 8, :]
                    l_scr[h] = st_scr[tile, g, h, HD + 8:, :]

        @pl.when((flags & 15) != 0)
        def _():
            mask_runs(row, flags)

        for h in range(G):
            stage_b(row, g, h)
            stage_a(nrow, ng, h)

        @pl.when((flags & LAST) != 0)
        def _():
            if final:
                finish(tile, g, lambda h: (acc_scr[h], l_scr[h]))
            else:
                for h in range(G):
                    st_scr[tile, g, h, :HD, :] = acc_scr[h]
                    st_scr[tile, g, h, HD:HD + 8, :] = m_scr[h]
                    st_scr[tile, g, h, HD + 8:, :] = l_scr[h]

                @pl.when(g == n_heads - 1)
                def _():
                    pltpu.make_async_copy(st_scr.at[tile], outs[0].at[tile], o_sem.at[tile]).start()

        return have

    have = lax.fori_loop(0, n_heads * n_blocks, body, have)
    arrived(have, len(kv_src))
    if final:
        for k in range(n_tiles):
            pltpu.make_async_copy(o_scr.at[k], outs[k], o_sem.at[k]).wait()
    else:
        def wait_out(i, carry):
            row = row0 + BLK * i

            @pl.when((tab_ref[row + 1] & LAST) != 0)
            def _():
                t = tab_ref[row]
                pltpu.make_async_copy(st_scr.at[t], st_scr.at[t], o_sem.at[t]).wait()

            return carry

        lax.fori_loop(0, n_blocks, wait_out, 0)


def flash(tab, qs, q_src, kvs, *, base, work, st=None, st_src=None, st_tiles=None, after=()):
    nq = qs[0].shape[1]
    n_heads = 2
    G = nq // HD // n_heads
    n_tiles = len(q_src)
    final = st_tiles is None
    kv_src = [(a, i) for a, kv in enumerate(kvs) for i in range(kv.shape[0])]
    n_runs = len(kv_src)
    sts = () if st is None else (st,)
    n_in = 1 + len(qs) + len(kvs) + len(sts)
    state = (n_heads, G, ST, RUN)
    has_st = not final or sts
    return pl.pallas_call(
        ordered(functools.partial(flash_kernel, q_src=q_src, kv_src=kv_src, n_q=len(qs), n_kv=len(kvs),
                                  st_src=st_src or [None] * n_tiles, n_st=len(sts), base=base, G=G, n_tiles=n_tiles,
                                  n_heads=n_heads, final=final), n_in, after),
        grid_spec=pltpu.PrefetchScalarGridSpec(
            num_scalar_prefetch=1, grid=(),
            in_specs=[ANY] * (n_in - 1 + len(after)),
            out_specs=[ANY] * n_tiles if final else [ANY],
            scratch_shapes=[pltpu.VMEM((n_tiles, nq, RUN), BF),
                            pltpu.VMEM((n_runs, 2, 256, 256), BF),
                            pltpu.VMEM((n_tiles if final else 1, RUN, nq), BF),
                            pltpu.VMEM((n_tiles if has_st else 1, *state), F32),
                            pltpu.VMEM((G, 4 * RUN, RUN), F32),
                            pltpu.VMEM((G, 4, 8, RUN), F32),
                            pltpu.VMEM((G, HD, RUN), F32),
                            pltpu.VMEM((G, 8, RUN), F32),
                            pltpu.VMEM((G, 8, RUN), F32),
                            pltpu.SemaphoreType.DMA((n_tiles,)),
                            pltpu.SemaphoreType.DMA((n_runs,)),
                            pltpu.SemaphoreType.DMA((n_tiles,)),
                            pltpu.SemaphoreType.DMA((n_tiles,))]),
        out_shape=[jax.ShapeDtypeStruct((RUN, nq), BF)] * n_tiles if final
        else [jax.ShapeDtypeStruct((st_tiles, *state), F32)],
        input_output_aliases={n_in - 1: 0} if sts and not final else {},
        name="flash" if final else "flash_part", compiler_params=params(0),
        cost_estimate=cost(8 * work * RUN * RUN * nq, n_runs * RUN * nq),
    )(tab, *qs, *kvs, *sts, *after)


def out_kernel(*refs, blocks, n_w, n_run, at):
    n_o, n_out = 4 * n_run, 2 * n_run
    o_refs, w_refs, x_ref, g_ref = refs[:n_o], refs[n_o:n_o + n_w], refs[n_o + n_w], refs[n_o + n_w + 1]
    outs = refs[n_o + n_w + 2:n_o + n_w + 2 + n_out]
    o_scr, w_scr, x_scr, acc_scr, o_sem, w_sem, x_sem, out_sem = refs[n_o + n_w + 2 + n_out:]
    width = o_refs[0].shape[1]
    half = width // 2
    n_slots = w_scr.shape[0]

    def fetch(k):
        for i, pieces in enumerate(blocks):
            @pl.when(k == i)
            def _():
                to = 0
                for a, r0, n in pieces:
                    pltpu.make_async_copy(w_refs[a].at[pl.ds(r0, n), :], w_scr.at[i % n_slots, pl.ds(to, n), :],
                                          w_sem.at[i % n_slots]).start()
                    to += n

    mine = lax.axis_index('cp')
    loads = [[] for _ in blocks]
    for i in range(n_run):
        rows = pl.ds(i * RUN, RUN)
        for k in range(4):
            src = o_refs[4 * i + k]
            if k < 2:
                loads[2 * k].append((src, o_scr.at[rows, pl.ds(k * width, width)]))
            else:
                for p, part in enumerate((mine, 1 - mine)):
                    loads[2 * k + p].append((src.at[:, pl.ds(pl.multiple_of(part * half, half), half)],
                                             o_scr.at[rows, pl.ds(k * width + p * half, half)]))
    copies = [[pltpu.make_async_copy(src, dst, o_sem.at[k, i]) for i, (src, dst) in enumerate(ls)] for k, ls in enumerate(loads)]
    x_copy = pltpu.make_async_copy(x_ref.at[pl.ds(at * n_run * RUN, n_run * RUN), :], x_scr, x_sem)
    for cp in copies[0]:
        cp.start()
    for i in range(n_slots - 1):
        fetch(jnp.int32(i))
    for ls in copies[1:]:
        for cp in ls:
            cp.start()
    x_copy.start()
    acc_scr[...] = jnp.zeros_like(acc_scr)

    def one(k, carry):
        fetch(k + n_slots - 1)
        for i, ls in enumerate(copies):
            if ls:
                @pl.when(k == i)
                def _():
                    for cp in ls:
                        cp.wait()
        slot = lax.rem(k, n_slots)
        pltpu.make_async_copy(w_scr.at[slot], w_scr.at[slot], w_sem.at[slot]).wait()
        acc_scr[...] += jnp.dot(o_scr[:, pl.ds(pl.multiple_of(k * half, half), half)], w_scr[slot], preferred_element_type=F32)
        return carry

    lax.fori_loop(0, len(blocks), one, 0)
    x_copy.wait()

    def rows32(r, carry):
        rows = pl.ds(pl.multiple_of(r * 32, 32), 32)
        y = (x_scr[rows, :].astype(F32) + acc_scr[rows, :].astype(BF).astype(F32)).astype(BF)
        x_scr[rows, :] = y
        o_scr[rows, :] = norm_rows(y, g_ref[...])
        return carry

    stores, per = [], RUN // 32
    for i in range(n_run):
        lax.fori_loop(i * per, (i + 1) * per, rows32, 0)
        for k, scr in enumerate((x_scr, o_scr)):
            stores.append(pltpu.make_async_copy(scr.at[pl.ds(i * RUN, RUN), :], outs[2 * i + k], out_sem.at[2 * i + k]))
            stores[-1].start()
    for cp in stores:
        cp.wait()


def out_proj(os, ws, blocks, x_rows, gain, at, after=()):
    dim = x_rows.shape[1]
    width = os[0].shape[1]
    n_run = len(os) // 4
    rows = n_run * RUN
    return pl.pallas_call(
        ordered(functools.partial(out_kernel, blocks=blocks, n_w=len(ws), n_run=n_run, at=at),
                len(os) + len(ws) + 2, after),
        grid=(1,),
        in_specs=[ANY] * (len(os) + len(ws) + 1) + [pl.BlockSpec((1, dim), lambda i: (0, 0))] + [ANY] * len(after),
        out_specs=[ANY] * (2 * n_run),
        out_shape=[jax.ShapeDtypeStruct((RUN, dim), BF)] * (2 * n_run),
        scratch_shapes=[pltpu.VMEM((rows, 4 * width), BF), pltpu.VMEM((3, width // 2, dim), BF), pltpu.VMEM((rows, dim), BF),
                        pltpu.VMEM((rows, dim), F32), pltpu.SemaphoreType.DMA((len(blocks), 2 * n_run)),
                        pltpu.SemaphoreType.DMA((3,)), pltpu.SemaphoreType.DMA, pltpu.SemaphoreType.DMA((2 * n_run,))],
        name="outp", compiler_params=params(1),
        cost_estimate=cost(8 * rows * width * dim, 8 * width * dim),
    )(*os, *ws, x_rows, gain, *after)


def mlp_kernel(*refs, n_in, first, rb, tn, td, nk, nd):
    b_refs = refs[:n_in]
    wg_ref, wu_ref, wd_ref, keep_ref, send_ref, b_scr, u_scr, w_scr, d_scr, b_sem, w_sem, d_sem = refs[n_in:]
    i = pl.program_id(0)

    def fetch(j):
        @pl.when(j < nk)
        def _():
            slot, cols = lax.rem(j, 2), pl.ds(pl.multiple_of(j * tn, tn), tn)
            for k, w in enumerate((wg_ref, wu_ref)):
                pltpu.make_async_copy(w.at[:, cols], w_scr.at[slot, k], w_sem.at[slot]).start()

        @pl.when((j >= nk) & (j < nk + nd))
        def _():
            n, slot = j - nk, lax.rem(j - nk, 2)
            pltpu.make_async_copy(wd_ref.at[:, pl.ds(pl.multiple_of(n * td, td), td)], d_scr.at[slot], d_sem.at[slot]).start()

    def gated(rows, cols, slot):
        b = b_scr[rows, :]
        gate = jnp.dot(b, w_scr[slot, 0], preferred_element_type=F32)
        up = jnp.dot(b, w_scr[slot, 1], preferred_element_type=F32)
        u_scr[rows, cols] = (jax.nn.silu(gate) * up).astype(BF)

    @pl.when(i == 0)
    def _():
        copies = [pltpu.make_async_copy(r.at[pl.ds(first, rb), :], b_scr.at[pl.ds(k * rb, rb), :], b_sem.at[k])
                  for k, r in enumerate(b_refs)]
        copies[0].start()
        fetch(i)
        for cp in copies[1:]:
            cp.start()

    fetch(i + 1)

    @pl.when(i < nk)
    def _():
        pltpu.make_async_copy(w_scr.at[lax.rem(i, 2)], w_scr.at[lax.rem(i, 2)], w_sem.at[lax.rem(i, 2)]).wait()

    @pl.when(i == 0)
    def _():
        def one(k, carry):
            rows = pl.ds(pl.multiple_of(k * rb, rb), rb)
            pltpu.make_async_copy(b_scr.at[rows, :], b_scr.at[rows, :], b_sem.at[k]).wait()
            gated(rows, pl.ds(0, tn), 0)
            return carry

        lax.fori_loop(0, n_in, one, 0)

    @pl.when((i > 0) & (i < nk))
    def _():
        gated(slice(None), pl.ds(pl.multiple_of(i * tn, tn), tn), lax.rem(i, 2))

    @pl.when(i >= nk)
    def _():
        slot = lax.rem(i - nk, 2)
        pltpu.make_async_copy(d_scr.at[slot], d_scr.at[slot], d_sem.at[slot]).wait()
        d = jnp.dot(u_scr[...], d_scr[slot], preferred_element_type=F32).astype(BF)
        half = d.shape[0] // 2
        keep_ref[...] = d[:half]
        send_ref[...] = d[half:]


def mlp(bs, first, rb, wg, wu, wd, after=()):
    dim = bs[0].shape[1]
    rows = rb * len(bs)
    ffn = wg.shape[1]
    td = 512
    tn = td if rows <= td else td // 2
    nk, nd = ffn // tn, dim // td
    dn = lambda i: (0, jnp.maximum(i - nk, 0))
    return pl.pallas_call(
        ordered(functools.partial(mlp_kernel, n_in=len(bs), first=first, rb=rb, tn=tn, td=td, nk=nk, nd=nd), len(bs) + 3, after),
        grid=(nk + nd,),
        in_specs=[ANY] * (len(bs) + 3 + len(after)),
        out_specs=[pl.BlockSpec((rows // 2, td), dn)] * 2,
        out_shape=[jax.ShapeDtypeStruct((rows // 2, dim), BF)] * 2,
        scratch_shapes=[pltpu.VMEM((rows, dim), BF), pltpu.VMEM((rows, ffn), BF), pltpu.VMEM((2, 2, dim, tn), BF),
                        pltpu.VMEM((2, ffn, td), BF), pltpu.SemaphoreType.DMA((len(bs),)), pltpu.SemaphoreType.DMA((2,)),
                        pltpu.SemaphoreType.DMA((2,))],
        name="mlp", compiler_params=params(1),
        cost_estimate=cost(6 * rows * dim * ffn, 6 * dim * ffn),
    )(*bs, wg, wu, wd, *after)


def sum_kernel(*refs):
    p_ref, r_ref, t_ref, y_ref, z_ref = refs[-5:]
    total = p_ref[...].astype(F32) + r_ref[...].astype(F32) + t_ref[...].astype(F32)
    z_ref[...] = (y_ref[...].astype(F32) + total.astype(BF).astype(F32)).astype(BF)


def sum_rows(z, keep, recv, far, y, y_first, rows, first, total, after=(), tile=64):
    dim = y.shape[1]
    at = lambda r0: pl.BlockSpec((tile, dim), lambda i: (r0 // tile + i, 0))
    prev = () if z is None else (z,)
    return pl.pallas_call(
        ordered(sum_kernel, len(prev) + 4, after), grid=(rows // tile,),
        in_specs=[ANY] * len(prev) + [at(0)] * 3 + [at(y_first)] + [ANY] * len(after),
        out_specs=at(first),
        out_shape=jax.ShapeDtypeStruct((total, dim), BF),
        input_output_aliases={0: 0} if prev else {},
        name="zsum", compiler_params=params(1),
        cost_estimate=cost(rows * dim, 8 * rows * dim),
    )(*prev, keep, recv, far, y, *after)


def run_positions(xi, ci, y, cps, piece):
    def start(x, c):
        return (y if x == 0 else 2 * cps - 1 - y) * piece + c * (piece // 2)

    per = piece // 2 // RUN
    out = [start(xi, ci) + RUN * j for j in range(per)] + [start(xi, 1 - ci) + RUN * j for j in range(per)]
    for j in range(per):
        out += [start(1 - xi, ci) + RUN * j, start(1 - xi, 1 - ci) + RUN * j]
    return out


def block_list(tile, ids, pos, diag):
    runs = [(r, pos[r]) for r in ids]
    if diag is not None:
        n_tail = (len(runs) % 4) + 1
        tail = [(diag, pos[diag])] + runs[len(runs) - (n_tail - 1):]
        runs = runs[:len(runs) - (n_tail - 1)]
    else:
        n_tail = len(runs) % 4
        tail = runs[len(runs) - n_tail:]
        runs = runs[:len(runs) - n_tail]
    blocks = [[0, runs[i:i + 4]] for i in range(0, len(runs), 4)]
    if tail:
        full = tail + [(tail[0][0], FAR)] * (4 - len(tail))
        flags = sum(1 << k for k, (r, p) in enumerate(full) if p == FAR or r == diag)
        blocks.append([flags, full])
    blocks[-1][0] |= LAST
    blocks[0][0] |= FIRST
    return [[tile, flags, 0] + [r for r, _ in four] + [p for _, p in four] + [0] for flags, four in blocks]


def call_table(tiles, pos, pairs, carry, idle):
    rows, most = [], 0
    carry = [c if pairs[t][0] or pairs[t][1] else idle for t, c in enumerate(carry)]
    for t, tile in enumerate(tiles):
        ids, own = pairs[t]
        if ids or own:
            mine = block_list(t, ids, pos, tile if own else None)
            mine[0][1] |= CARRY if carry[t] else 0
            rows += mine
    for row in rows:
        most = max(most, max(row[3:7]) + 1)
        row[2] = most
    return [len(rows)] + [pos[t] for t in tiles] + carry + [v for row in rows for v in row], len(rows)


def work_tables(cps, piece):
    per = piece // 2 // RUN
    early = 2 * per + 2
    stage = lambda r: 0 if r < early else 1
    calls = [(0, list(range(early)))]
    calls += [(1, [j, per + j, 2 * per + 2 * j, 2 * per + 2 * j + 1]) for j in range(per)]
    tabs, all_runs, sizes = [], [], []
    for y in range(cps):
        for xi in range(2):
            for ci in range(2):
                mine = run_positions(xi, ci, y, cps, piece)
                pos = mine + run_positions(xi, ci, 1 - y, cps, piece)
                all_runs.append(mine)
                tabs.append([])
                sizes.append([])
                for now, tiles in calls:
                    pairs, carry = [], []
                    for t in tiles:
                        seen = [r for r in range(len(pos)) if pos[r] < pos[t]]
                        when = {r: max(stage(r), stage(t)) for r in seen}
                        late = list(when.values()).count(1) + stage(t)
                        soon = len(seen) + 1 - late
                        if late and soon % 4 <= -late % 4:
                            for r in [r for r in seen if not when[r]][:soon % 4]:
                                when[r] = 1
                        pairs.append(([r for r in seen if when[r] == now], stage(t) == now))
                        carry.append(int(stage(t) < now))
                    tab, n = call_table(tiles, pos, pairs, carry, 2 if now == 1 else 0)
                    tabs[-1].append(tab)
                    sizes[-1].append(n)
    widths = [max(len(t[k]) for t in tabs) for k in range(len(calls))]
    flat = [[v for k, t in enumerate(tab) for v in t + [0] * (widths[k] - len(t))] for tab in tabs]
    bases = [sum(widths[:k]) for k in range(len(calls))]
    return np.array(flat, np.int32), np.array(all_runs, np.int32), bases, np.array(sizes).max(0) * 4


def solution(mesh):
    cps = mesh.shape['cp']
    row_spec = P('dp', ('cp', 'tp'), None)
    head_cols = P(None, 'tp', None)
    n_tp = mesh.shape['tp']

    over_core, over_x, over_both = (('tp', [(t, t ^ k) for t in range(n_tp)]) for k in (1, 2, 3))
    over_y = ('cp', [(i, i ^ 1) for i in range(cps)])

    def layer(x, g_attn, w_q, w_k, w_v, w_o, g_mlp, w_gate, w_up, w_down):
        x_rows = x[0]
        dim = x_rows.shape[1]
        n_run = x_rows.shape[0] // RUN
        piece = 2 * x_rows.shape[0]
        t_id, y_id = lax.axis_index('tp'), lax.axis_index('cp')
        np_tab, np_runs, bases, work = work_tables(cps, piece)
        dev = y_id * n_tp + t_id
        tab = lax.dynamic_index_in_dim(jnp.asarray(np_tab), dev, 0, keepdims=False)
        run_pos = lax.dynamic_index_in_dim(jnp.asarray(np_runs), dev, 0, keepdims=False)

        def tied(v, *others):
            return lax.optimization_barrier((v, *others))[0]

        def send(axis_pairs, v):
            return lax.ppermute(v, *axis_pairs)

        ga, gm = g_attn.reshape(1, dim), g_mlp.reshape(1, dim)
        own = []
        for j in range(n_run):
            own.append(norm_run(x_rows, ga, j, after=own[-1:]))
        far = [send(over_x, own[j]) for j in range(n_run)]
        mate = [send(over_core, own[j]) for j in range(n_run)]

        w_all = jnp.concatenate([tied(w, own[-1]).reshape(dim, -1) for w in (w_q, w_k, w_v)], axis=1)
        tables = rope_tables(tied(run_pos, own[-1])[:, None] + jnp.arange(RUN, dtype=jnp.int32)[None, :])

        q_here, kv_here = qkv(own + mate, w_all, (tables, 0))
        kvs, q_far = [kv_here], []

        def far_qkv(j, after):
            here = tied(far[j], after)
            rows = [here, send(over_core, here)], w_all, (tables, 2 * (n_run + j))
            if j + 1 < n_run:
                q, kv = qkv(*rows, after=(after,))
            else:
                kv, = qkv(*rows, False, after=(after,))
                q, = qkv(*rows, True, False, after=(kv, gm))
            q_far.append(q)
            kvs.append(kv)
            return kv

        far_qkv(1, far_qkv(0, kv_here))

        wo = w_o.reshape(-1, dim)
        half = wo.shape[0] // 2
        n_piece = 2
        rows = half // n_piece
        wo_gated = tied(wo, kvs[-1])
        wo_x = [send(over_x, lax.dynamic_slice_in_dim(wo_gated, y_id * half + p * rows, rows, axis=0))
                for p in range(n_piece)]
        wo_c = send(over_core, wo_gated)

        tiles = [(0, i) for i in range(2 * n_run)] + [(1, 0), (1, 1)]
        st, = flash(tab, [q_here, q_far[0]], tiles, kvs[:2], base=bases[0], work=int(work[0]),
                   st_tiles=len(tiles), after=(kvs[-1],))
        far_qkv(3, far_qkv(2, st))
        kvs = kvs + [send(over_y, kv) for kv in kvs]

        os, outs, prev = [], [], q_far[-1]
        wo_a, wo_ya, wo_yb = {}, {}, {}

        def forward_w(p):
            here = tied(wo_x[p], prev)
            wo_ya[p] = (here, send(over_core, here))
            wo_a[p] = send(over_y, here)

        def relay_w(p):
            here = tied(wo_a[p], prev)
            wo_yb[p] = (here, send(over_core, here))

        def attend(j):
            held = 2 * n_run + 2 * j
            carried = [j, n_run + j] + ([held, held + 1] if j == 0 else [None, None])
            o_own, o_mate, o_far, o_fm = flash(
                tab, [q_here, q_far[j]], [(0, j), (0, n_run + j), (1, 0), (1, 1)], kvs,
                base=bases[1 + j], work=int(work[1 + j]), st=st, st_src=carried, after=(prev,))
            os.append([o_own, send(over_core, o_mate), send(over_x, o_far), send(over_both, o_fm)])
            return o_own

        def project(i):
            ws = [wo, wo_c]
            blocks = [[(0, 0, half)], [(0, half, half)], [(1, 0, half)], [(1, half, half)]]
            for k in range(2):
                for held in (wo_ya, wo_yb):
                    blocks.append([(len(ws) + p, 0, rows) for p in range(n_piece)])
                    ws += [held[p][k] for p in range(n_piece)]
            got = out_proj(os[2 * i] + os[2 * i + 1], ws, blocks, x_rows, gm, i, after=(prev,))
            for y, b in zip(got[::2], got[1::2]):
                outs.append((y, b, send(over_x, b), send(over_core, b)))
            return got[0]

        last = n_run - 1
        for j in range(last):
            prev = attend(j)
            if j < n_piece:
                forward_w(j)
            if j:
                relay_w(j - 1)
        prev = project(0)
        prev = attend(last)

        z, sums, relay = None, [], {}

        def relay_b(j):
            here = tied(outs[j][2], prev)
            relay[j] = (here, send(over_core, here))

        chunks = [(j, 0, RUN) for j in range(last)] + [(last, 0, RUN // 2), (last, RUN // 2, RUN // 2)]

        def finish(c):
            j, first, size = chunks[c]
            return sum_rows(z, *sums[c], outs[j][0], first, size, j * RUN + first, n_run * RUN,
                        after=() if prev is z else (prev,))

        relay_b(0)
        for c, (j, first, size) in enumerate(chunks):
            b = [outs[j][1], relay[j][0], outs[j][3], relay[j][1]]
            keep, out = mlp(b, first, size, w_gate, w_up, w_down, after=(prev,))
            recv = send(over_core, out)
            prev = keep
            if c < last:
                relay_b(c + 1)
            if c == 0:
                prev = project(1)
            elif c < n_run:
                prev = z = finish(c - 1)
            kept = keep if prev is keep else tied(keep, prev)
            prev = s_far = (kept[size:].astype(F32) + recv[size:].astype(F32)).astype(BF)
            sums.append((keep, recv, send(over_x, s_far)))
        for c in (last, n_run):
            prev = z = finish(c)
        return z[None]

    return jax.shard_map(layer, mesh=mesh,
                         in_specs=(row_spec, P(), head_cols, head_cols, head_cols, P('tp', None, None),
                                   P(), P(None, 'tp'), P(None, 'tp'), P('tp', None)),
                         out_specs=row_spec, check_vma=False)
```

```python
import functools
import math
import jax
import jax.numpy as jnp
import numpy as np
from jax import lax
from jax.experimental import pallas as pl
from jax.experimental.pallas import tpu as pltpu
from jax.sharding import PartitionSpec as P

NORM_EPS = 1e-5
ROPE_THETA = 500000.0
HD = 128
RUN = 256
NEG = -1e30
LOG2E = math.log2(math.e)
DN = (((1,), (0,)), ((), ()))
VMEM = 67043328
BF = jnp.bfloat16
F32 = jnp.float32
ANY = pl.BlockSpec(memory_space=pltpu.HBM)


def params(n):
    return pltpu.CompilerParams(dimension_semantics=("arbitrary",) * n, vmem_limit_bytes=VMEM)


def rope_tables(positions):
    half = HD // 2
    inv_freq = ROPE_THETA ** (-2.0 * jnp.arange(half, dtype=F32) / HD)
    angles = inv_freq[:, None] * positions.astype(F32)[..., None, :]
    return jnp.cos(angles), jnp.sin(angles)


def norm_rows(rows, gain):
    f = rows.astype(F32)
    mean_sq = jnp.mean(f * f, axis=-1, keepdims=True)
    return (f * lax.rsqrt(mean_sq + NORM_EPS) * gain.astype(F32)).astype(BF)


def cost(flops, moved):
    return pl.CostEstimate(flops=flops, transcendentals=0, bytes_accessed=moved)


def ordered(kernel, n_in, after):
    n = len(after)
    return lambda *refs: kernel(*refs[:n_in], *refs[n_in + n:])


def norm_kernel(x_ref, g_ref, o_ref):
    o_ref[...] = norm_rows(x_ref[...], g_ref[...])


def norm_run(x_rows, gain, j, after=(), tile=128):
    dim = x_rows.shape[1]
    per = RUN // tile
    return pl.pallas_call(
        ordered(norm_kernel, 2, after), grid=(per,),
        in_specs=[pl.BlockSpec((tile, dim), lambda i: (j * per + i, 0)), pl.BlockSpec((1, dim), lambda i: (0, 0))]
        + [ANY] * len(after),
        out_specs=pl.BlockSpec((tile, dim), lambda i: (i, 0)),
        out_shape=jax.ShapeDtypeStruct((RUN, dim), BF),
        name="norm", compiler_params=params(1),
        cost_estimate=cost(RUN * dim, RUN * dim),
    )(x_rows, gain, *after)


def qkv_kernel(*refs, n_in, n_q, group, first, with_q, with_kv):
    a_refs = refs[:n_in]
    w_ref, cos_ref, sin_ref, *outs, a_scr, sem = refs[n_in:]
    q_ref, kv_ref = outs[0], outs[-1]
    n = pl.program_id(0) + first
    heads = w_ref.shape[1] // HD

    @pl.when(n == first)
    def _():
        for k, r in enumerate(a_refs):
            pltpu.make_async_copy(r, a_scr.at[pl.ds(k * RUN, RUN), :], sem.at[k]).start()

    def rope(f, i):
        f = f.astype(BF).astype(F32)
        lo, hi, cos, sin = f[:HD // 2], f[HD // 2:], cos_ref[i], sin_ref[i]
        return jnp.concatenate([lo * cos - hi * sin, hi * cos + lo * sin], axis=0)

    def one(k, carry):
        @pl.when(n == first)
        def _():
            for i in range(group):
                rows = pl.ds(pl.multiple_of((k * group + i) * RUN, RUN), RUN)
                pltpu.make_async_copy(a_scr.at[rows, :], a_scr.at[rows, :], sem.at[k * group + i]).wait()

        rows = pl.ds(pl.multiple_of(k * group * RUN, group * RUN), group * RUN)
        r = jnp.dot(a_scr[rows, :], w_ref[...], preferred_element_type=F32)

        def piece(i, h):
            return r[i * RUN:(i + 1) * RUN, h * HD:(h + 1) * HD].T

        @pl.when((n < n_q) if with_q else False)
        def _():
            for i in range(group):
                for h in range(heads):
                    q_ref[k * group + i, h * HD:(h + 1) * HD, :] = rope(piece(i, h), k * group + i).astype(BF)

        @pl.when((n == n_q) if with_kv else False)
        def _():
            for i in range(group):
                for h in range(heads // 2):
                    kv_ref[k * group + i, 0, :, h * HD:(h + 1) * HD] = rope(piece(i, h), k * group + i).T.astype(BF)
                    kv_ref[k * group + i, 1, h * HD:(h + 1) * HD, :] = piece(i, h + heads // 2).astype(BF)

        return carry

    lax.fori_loop(0, n_in // group, one, 0)


def qkv(rows, w_all, tables, with_q=True, with_kv=True, after=(), group=2):
    n_in = len(rows)
    dim = w_all.shape[0]
    tn = 512
    n_q = w_all.shape[1] // tn - 1
    (cos, sin), first_run = tables
    at = first_run // n_in
    start = 0 if with_q else n_q
    kv_shape = (n_in, 2, RUN, RUN)
    tab = pl.BlockSpec((n_in, HD // 2, RUN), lambda n: (at, 0, 0))
    return pl.pallas_call(
        ordered(functools.partial(qkv_kernel, n_in=n_in, n_q=n_q, group=group, first=start, with_q=with_q, with_kv=with_kv),
                n_in + 3, after),
        grid=(n_q * with_q + with_kv,),
        in_specs=[ANY] * n_in + [pl.BlockSpec((dim, tn), lambda n: (0, n + start)), tab, tab] + [ANY] * len(after),
        out_specs=[pl.BlockSpec((n_in, tn, RUN), lambda n: (0, jnp.minimum(n, n_q - 1), 0))] * with_q
        + [pl.BlockSpec(kv_shape, lambda n: (0,) * len(kv_shape))] * with_kv,
        out_shape=[jax.ShapeDtypeStruct((n_in, n_q * tn, RUN), BF)] * with_q + [jax.ShapeDtypeStruct(kv_shape, BF)] * with_kv,
        scratch_shapes=[pltpu.VMEM((n_in * RUN, dim), BF), pltpu.SemaphoreType.DMA((n_in,))],
        name="qkv", compiler_params=params(1),
        cost_estimate=cost(2 * n_in * RUN * w_all.size, 2 * w_all.size),
    )(*rows, w_all, cos, sin, *after)


BLK = 11
LAST, FIRST, CARRY = 16, 32, 64
ST = HD + 16


def flash_kernel(tab_ref, *refs, q_src, kv_src, n_q, n_kv, st_src, n_st, n_old, n_cut, slot, base, G, n_tiles, n_heads, final):
    qs, kvs, sts = refs[:n_q], refs[n_q:n_q + n_kv], refs[n_q + n_kv:n_q + n_kv + n_st]
    n_out = n_tiles + 1 if final else 1 + n_cut
    at = n_q + n_kv + n_st + n_old
    outs = refs[at:at + n_out]
    q_scr, kv_scr, o_scr, st_scr, s_scr, mb_scr, acc_scr, m_scr, l_scr, q_sem, kv_sem, o_sem, st_sem = refs[at + n_out:][:13]
    if n_cut:
        cut_ref, (cut_scr, cut_sem) = refs[at - 1], refs[-2:]
    T = RUN
    c = (HD ** -0.5) * LOG2E
    n_blocks = tab_ref[base]
    carried = base + 1
    row0 = carried + n_tiles
    null = len(kv_src)

    q_copies = [pltpu.make_async_copy(qs[a].at[i], q_scr.at[t], q_sem.at[t]) for t, (a, i) in enumerate(q_src)]
    kv_copies = [pltpu.make_async_copy(kvs[a].at[i], kv_scr.at[r], kv_sem.at[r]) for r, (a, i) in enumerate(kv_src)]
    first = 4
    q_copies[0].start()
    for cp in kv_copies[:first]:
        cp.start()
    for cp in q_copies[1:]:
        cp.start()
    for t, i in enumerate(st_src):
        if i is not None:
            @pl.when(tab_ref[carried + t] != 0)
            def _():
                pltpu.make_async_copy(sts[0].at[i], st_scr.at[t], st_sem.at[t]).start()
    for cp in kv_copies[first:]:
        cp.start()
    kv_scr[null, 1] = jnp.zeros((256, 256), BF)
    if n_cut:
        cut_in = pltpu.make_async_copy(cut_ref.at[pl.ds(lax.axis_index('cp') * cut_scr.shape[0], cut_scr.shape[0]), :], cut_scr,
                                       cut_sem)
        part = cut_scr.shape[0] // n_cut
        cut_out = [pltpu.make_async_copy(cut_scr.at[pl.ds(k * part, part), :], outs[1 + k], cut_sem) for k in range(n_cut)]
        cut_in.start()

    def block(i):
        g = lax.div(i, n_blocks)
        return row0 + BLK * (i - g * n_blocks), g

    def arrived(have, need):
        def one(r, carry):
            pltpu.make_async_copy(kv_scr.at[r], kv_scr.at[r], kv_sem.at[r]).wait()
            return carry

        lax.fori_loop(have, need, one, 0)
        return jnp.maximum(have, need)

    def put(s, h, k):
        s_scr[h, pl.ds(k * RUN, RUN), :] = s
        mb_scr[h, k] = jnp.max(s.reshape(RUN // 8, 8, T), axis=0)

    def stage_a(row, g, h):
        col = pl.multiple_of(g * HD, HD)
        qt = q_scr[tab_ref[row], pl.ds(pl.multiple_of((g * G + h) * HD, HD), HD), :]
        for k in range(4):
            put(lax.dot_general(kv_scr[tab_ref[row + 3 + k], 0, :, pl.ds(col, HD)], qt, DN, preferred_element_type=F32), h, k)

    def stage_b(row, g, h):
        col = pl.multiple_of(g * HD, HD)
        m_prev = m_scr[h]
        mb = jnp.maximum(jnp.maximum(mb_scr[h, 0], mb_scr[h, 1]), jnp.maximum(mb_scr[h, 2], mb_scr[h, 3]))
        for r in (4, 2, 1):
            mb = jnp.maximum(mb, pltpu.roll(mb, r, 0))
        m_new = jnp.maximum(m_prev, mb)
        m_scr[h] = m_new
        m_c = m_new * c
        alpha = jnp.exp2(m_prev * c - m_c)
        l, pv = l_scr[h] * alpha, None
        for k in range(4):
            run = tab_ref[row + 7 + k]
            p = jnp.exp2(s_scr[h, k * RUN:(k + 1) * RUN].reshape(RUN // 8, 8, T) * c - m_c[None])
            l = l + jnp.sum(p, axis=0) * jnp.where(run < 0, 0.0, 1.0)
            d = lax.dot_general(kv_scr[jnp.where(run < 0, null, run), 1, pl.ds(col, HD), :], p.reshape(RUN, T).astype(BF), DN,
                                preferred_element_type=F32)
            pv = d if pv is None else pv + d
        l_scr[h] = l
        acc_scr[h] = (acc_scr[h].reshape(HD // 8, 8, T) * alpha[None]).reshape(HD, T) + pv

    def mask_runs(flags):
        seen = lax.broadcasted_iota(jnp.int32, (RUN, T), 0) <= lax.broadcasted_iota(jnp.int32, (RUN, T), 1)

        def one(k, carry):
            @pl.when((lax.shift_right_logical(flags, k) & 1) != 0)
            def _():
                rows = pl.multiple_of(k * RUN, RUN)
                for h in range(G):
                    put(jnp.where(seen, s_scr[h, pl.ds(rows, RUN), :], NEG), h, k)

            return carry

        lax.fori_loop(0, 4, one, 0)

    def finish(tile, g, get):
        for h in range(G):
            acc, l = get(h)
            o_scr[tile, :, pl.ds(pl.multiple_of((g * G + h) * HD, HD), HD)] = (acc / jnp.sum(l, axis=0, keepdims=True)).T.astype(BF)

        @pl.when(g == n_heads - 1)
        def _():
            for k in range(n_tiles):
                @pl.when(tile == k)
                def _():
                    pltpu.make_async_copy(o_scr.at[k], outs[k].at[slot], o_sem.at[k]).start()

    if final and n_st:
        def idle(i, carry):
            tile, g = lax.div(i, n_heads), lax.rem(i, n_heads)

            @pl.when(tab_ref[carried + tile] == 2)
            def _():
                @pl.when(g == 0)
                def _():
                    pltpu.make_async_copy(q_scr.at[tile], q_scr.at[tile], q_sem.at[tile]).wait()
                    pltpu.make_async_copy(st_scr.at[tile], st_scr.at[tile], st_sem.at[tile]).wait()

                finish(tile, g, lambda h: (st_scr[tile, g, h, :HD, :], st_scr[tile, g, h, HD + 8:, :]))

            return carry

        lax.fori_loop(0, n_tiles * n_heads, idle, 0)

    def query(row):
        t = tab_ref[row]
        pltpu.make_async_copy(q_scr.at[t], q_scr.at[t], q_sem.at[t]).wait()

    row, g = block(0)
    query(row)
    have = arrived(0, tab_ref[row + 2])
    for h in range(G):
        stage_a(row, g, h)

    def body(i, have):
        row, g = block(i)
        nrow, ng = block(jnp.minimum(i + 1, n_heads * n_blocks - 1))
        have = arrived(have, tab_ref[nrow + 2])
        flags = tab_ref[row + 1]
        tile = tab_ref[row]

        @pl.when((i + 1 < n_blocks) & ((tab_ref[nrow + 1] & FIRST) != 0))
        def _():
            query(nrow)

        @pl.when((flags & (FIRST | CARRY)) == FIRST)
        def _():
            acc_scr[...] = jnp.zeros_like(acc_scr)
            l_scr[...] = jnp.zeros_like(l_scr)
            m_scr[...] = jnp.full_like(m_scr, NEG)

        if n_st:
            @pl.when((flags & (FIRST | CARRY)) == (FIRST | CARRY))
            def _():
                @pl.when(g == 0)
                def _():
                    pltpu.make_async_copy(st_scr.at[tile], st_scr.at[tile], st_sem.at[tile]).wait()

                for h in range(G):
                    acc_scr[h] = st_scr[tile, g, h, :HD, :]
                    m_scr[h] = st_scr[tile, g, h, HD:HD + 8, :]
                    l_scr[h] = st_scr[tile, g, h, HD + 8:, :]

        if n_cut:
            @pl.when(i == n_blocks)
            def _():
                cut_in.wait()
                for cp in cut_out:
                    cp.start()

        @pl.when((flags & 15) != 0)
        def _():
            mask_runs(flags)

        for h in range(G):
            stage_b(row, g, h)
            stage_a(nrow, ng, h)

        @pl.when((flags & LAST) != 0)
        def _():
            if final:
                finish(tile, g, lambda h: (acc_scr[h], l_scr[h]))
            else:
                for h in range(G):
                    st_scr[tile, g, h, :HD, :] = acc_scr[h]
                    st_scr[tile, g, h, HD:HD + 8, :] = m_scr[h]
                    st_scr[tile, g, h, HD + 8:, :] = l_scr[h]

                @pl.when(g == n_heads - 1)
                def _():
                    pltpu.make_async_copy(st_scr.at[tile], outs[0].at[tile], o_sem.at[tile]).start()

        return have

    have = lax.fori_loop(0, n_heads * n_blocks, body, have)
    arrived(have, len(kv_src))
    if final:
        for k in range(n_tiles):
            pltpu.make_async_copy(o_scr.at[k], outs[k].at[slot], o_sem.at[k]).wait()
    else:
        def wait_out(i, carry):
            row = row0 + BLK * i

            @pl.when((tab_ref[row + 1] & LAST) != 0)
            def _():
                t = tab_ref[row]
                pltpu.make_async_copy(st_scr.at[t], st_scr.at[t], o_sem.at[t]).wait()

            return carry

        lax.fori_loop(0, n_blocks, wait_out, 0)
        for cp in cut_out:
            cp.wait()


def flash(tab, qs, q_src, kvs, *, base, work, st=None, st_src=None, old=None, cut=None, n_cut=0, slots=1, after=()):
    nq = qs[0].shape[1]
    n_heads = 2
    G = nq // HD // n_heads
    n_tiles = len(q_src)
    final = cut is None
    kv_src = [(a, i) for a, kv in enumerate(kvs) for i in range(kv.shape[0])]
    n_runs = len(kv_src)
    sts = () if st is None else (st,)
    old = old or ()
    more = (*old, *(() if final else (cut,)))
    n_in = 1 + len(qs) + len(kvs) + len(sts) + len(more)
    state = (n_heads, G, ST, RUN)
    has_st = not final or sts
    if final:
        out_shape = [jax.ShapeDtypeStruct((slots, RUN, nq), BF)] * n_tiles + [jax.ShapeDtypeStruct((8, HD), F32)]
        scratch = []
    else:
        half = cut.shape[0] // 2
        out_shape = [jax.ShapeDtypeStruct((n_tiles, *state), F32)]
        out_shape += [jax.ShapeDtypeStruct((half // n_cut, cut.shape[1]), BF)] * n_cut
        scratch = [pltpu.VMEM((half, cut.shape[1]), BF), pltpu.SemaphoreType.DMA]
    return pl.pallas_call(
        ordered(functools.partial(flash_kernel, q_src=q_src, kv_src=kv_src, n_q=len(qs), n_kv=len(kvs),
                                  st_src=st_src or [None] * n_tiles, n_st=len(sts), n_old=len(more), n_cut=n_cut,
                                  slot=slots - 1 if old else 0, base=base, G=G, n_tiles=n_tiles, n_heads=n_heads, final=final),
                n_in, after),
        grid_spec=pltpu.PrefetchScalarGridSpec(
            num_scalar_prefetch=1, grid=(),
            in_specs=[ANY] * (n_in - 1 + len(after)),
            out_specs=[ANY] * len(out_shape),
            scratch_shapes=[pltpu.VMEM((n_tiles, nq, RUN), BF),
                            pltpu.VMEM((n_runs + 1, 2, 256, 256), BF),
                            pltpu.VMEM((n_tiles if final else 1, RUN, nq), BF),
                            pltpu.VMEM((n_tiles if has_st else 1, *state), F32),
                            pltpu.VMEM((G, 4 * RUN, RUN), F32),
                            pltpu.VMEM((G, 4, 8, RUN), F32),
                            pltpu.VMEM((G, HD, RUN), F32),
                            pltpu.VMEM((G, 8, RUN), F32),
                            pltpu.VMEM((G, 8, RUN), F32),
                            pltpu.SemaphoreType.DMA((n_tiles,)),
                            pltpu.SemaphoreType.DMA((n_runs,)),
                            pltpu.SemaphoreType.DMA((n_tiles,)),
                            pltpu.SemaphoreType.DMA((n_tiles,)), *scratch]),
        out_shape=out_shape,
        input_output_aliases={n_in - len(old) + k: k for k in range(len(old))},
        name="flash" if final else "flash_part", compiler_params=params(0),
        cost_estimate=cost(8 * work * RUN * RUN * nq, n_runs * RUN * nq),
    )(tab, *qs, *kvs, *sts, *more, *after)


def out_kernel(*refs, blocks, n_w, n_run, at):
    n_o, n_out = 4, 2 * n_run
    o_refs, w_refs, x_ref, g_ref = refs[:n_o], refs[n_o:n_o + n_w], refs[n_o + n_w], refs[n_o + n_w + 1]
    outs = refs[n_o + n_w + 2:n_o + n_w + 2 + n_out]
    o_scr, w_scr, x_scr, acc_scr, o_sem, w_sem, x_sem, out_sem = refs[n_o + n_w + 2 + n_out:]
    width = o_refs[0].shape[-1]
    half = width // 2
    n_slots = w_scr.shape[0]

    def fetch(k):
        for i, pieces in enumerate(blocks):
            @pl.when(k == i)
            def _():
                to = 0
                for a, r0, n in pieces:
                    pltpu.make_async_copy(w_refs[a].at[pl.ds(r0, n), :], w_scr.at[i % n_slots, pl.ds(to, n), :],
                                          w_sem.at[i % n_slots]).start()
                    to += n

    mine = lax.axis_index('cp')
    loads = [[] for _ in blocks]
    for i in range(n_run):
        rows = pl.ds(i * RUN, RUN)
        for k in range(4):
            src = o_refs[k].at[i]
            if k < 2:
                loads[2 * k].append((src, o_scr.at[rows, pl.ds(k * width, width)]))
            else:
                for p, part in enumerate((mine, 1 - mine)):
                    loads[2 * k + p].append((src.at[:, pl.ds(pl.multiple_of(part * half, half), half)],
                                             o_scr.at[rows, pl.ds(k * width + p * half, half)]))
    copies = [[pltpu.make_async_copy(src, dst, o_sem.at[k, i]) for i, (src, dst) in enumerate(ls)] for k, ls in enumerate(loads)]
    x_copy = pltpu.make_async_copy(x_ref.at[pl.ds(at * n_run * RUN, n_run * RUN), :], x_scr, x_sem)
    for cp in copies[0]:
        cp.start()
    for i in range(n_slots - 1):
        fetch(jnp.int32(i))
    for ls in copies[1:]:
        for cp in ls:
            cp.start()
    x_copy.start()
    acc_scr[...] = jnp.zeros_like(acc_scr)

    def one(k, carry):
        fetch(k + n_slots - 1)
        for i, ls in enumerate(copies):
            if ls:
                @pl.when(k == i)
                def _():
                    for cp in ls:
                        cp.wait()
        slot = lax.rem(k, n_slots)
        pltpu.make_async_copy(w_scr.at[slot], w_scr.at[slot], w_sem.at[slot]).wait()
        acc_scr[...] += jnp.dot(o_scr[:, pl.ds(pl.multiple_of(k * half, half), half)], w_scr[slot], preferred_element_type=F32)
        return carry

    lax.fori_loop(0, len(blocks), one, 0)
    x_copy.wait()

    def rows32(r, carry):
        rows = pl.ds(pl.multiple_of(r * 32, 32), 32)
        y = (x_scr[rows, :].astype(F32) + acc_scr[rows, :].astype(BF).astype(F32)).astype(BF)
        x_scr[rows, :] = y
        o_scr[rows, :] = norm_rows(y, g_ref[...])
        return carry

    stores, per = [], RUN // 32
    for i in range(n_run):
        lax.fori_loop(i * per, (i + 1) * per, rows32, 0)
        for k, scr in enumerate((x_scr, o_scr)):
            stores.append(pltpu.make_async_copy(scr.at[pl.ds(i * RUN, RUN), :], outs[2 * i + k], out_sem.at[2 * i + k]))
            stores[-1].start()
    for cp in stores:
        cp.wait()


def out_proj(os, ws, blocks, x_rows, gain, at, after=()):
    dim = x_rows.shape[1]
    n_run, _, width = os[0].shape
    rows = n_run * RUN
    return pl.pallas_call(
        ordered(functools.partial(out_kernel, blocks=blocks, n_w=len(ws), n_run=n_run, at=at),
                len(os) + len(ws) + 2, after),
        grid=(1,),
        in_specs=[ANY] * (len(os) + len(ws) + 1) + [pl.BlockSpec((1, dim), lambda i: (0, 0))] + [ANY] * len(after),
        out_specs=[ANY] * (2 * n_run),
        out_shape=[jax.ShapeDtypeStruct((RUN, dim), BF)] * (2 * n_run),
        scratch_shapes=[pltpu.VMEM((rows, 4 * width), BF), pltpu.VMEM((3, width // 2, dim), BF), pltpu.VMEM((rows, dim), BF),
                        pltpu.VMEM((rows, dim), F32), pltpu.SemaphoreType.DMA((len(blocks), 2 * n_run)),
                        pltpu.SemaphoreType.DMA((3,)), pltpu.SemaphoreType.DMA, pltpu.SemaphoreType.DMA((2 * n_run,))],
        name="outp", compiler_params=params(1),
        cost_estimate=cost(8 * rows * width * dim, 8 * width * dim),
    )(*os, *ws, x_rows, gain, *after)


def mlp_kernel(*refs, n_in, first, rb, tn, td, nk, nd):
    b_refs = refs[:n_in]
    wg_ref, wu_ref, wd_ref, keep_ref, send_ref, b_scr, u_scr, w_scr, d_scr, b_sem, w_sem, d_sem = refs[n_in:]
    i = pl.program_id(0)

    def fetch(j):
        @pl.when(j < nk)
        def _():
            slot, cols = lax.rem(j, 2), pl.ds(pl.multiple_of(j * tn, tn), tn)
            for k, w in enumerate((wg_ref, wu_ref)):
                pltpu.make_async_copy(w.at[:, cols], w_scr.at[slot, k], w_sem.at[slot]).start()

        @pl.when((j >= nk) & (j < nk + nd))
        def _():
            n, slot = j - nk, lax.rem(j - nk, 2)
            pltpu.make_async_copy(wd_ref.at[:, pl.ds(pl.multiple_of(n * td, td), td)], d_scr.at[slot], d_sem.at[slot]).start()

    def gated(rows, cols, slot):
        b = b_scr[rows, :]
        gate = jnp.dot(b, w_scr[slot, 0], preferred_element_type=F32)
        up = jnp.dot(b, w_scr[slot, 1], preferred_element_type=F32)
        u_scr[rows, cols] = (jax.nn.silu(gate) * up).astype(BF)

    @pl.when(i == 0)
    def _():
        copies = [pltpu.make_async_copy(r.at[pl.ds(first, rb), :], b_scr.at[pl.ds(k * rb, rb), :], b_sem.at[k])
                  for k, r in enumerate(b_refs)]
        copies[0].start()
        fetch(i)
        for cp in copies[1:]:
            cp.start()

    fetch(i + 1)

    @pl.when(i < nk)
    def _():
        pltpu.make_async_copy(w_scr.at[lax.rem(i, 2)], w_scr.at[lax.rem(i, 2)], w_sem.at[lax.rem(i, 2)]).wait()

    @pl.when(i == 0)
    def _():
        def one(k, carry):
            rows = pl.ds(pl.multiple_of(k * rb, rb), rb)
            pltpu.make_async_copy(b_scr.at[rows, :], b_scr.at[rows, :], b_sem.at[k]).wait()
            gated(rows, pl.ds(0, tn), 0)
            return carry

        lax.fori_loop(0, n_in, one, 0)

    @pl.when((i > 0) & (i < nk))
    def _():
        gated(slice(None), pl.ds(pl.multiple_of(i * tn, tn), tn), lax.rem(i, 2))

    @pl.when(i >= nk)
    def _():
        slot = lax.rem(i - nk, 2)
        pltpu.make_async_copy(d_scr.at[slot], d_scr.at[slot], d_sem.at[slot]).wait()
        d = jnp.dot(u_scr[...], d_scr[slot], preferred_element_type=F32).astype(BF)
        half = d.shape[0] // 2
        keep_ref[...] = d[:half]
        send_ref[...] = d[half:]


def mlp(bs, first, rb, wg, wu, wd, after=()):
    dim = bs[0].shape[1]
    rows = rb * len(bs)
    ffn = wg.shape[1]
    td = 512
    tn = td if rows <= td else td // 2
    nk, nd = ffn // tn, dim // td
    dn = lambda i: (0, jnp.maximum(i - nk, 0))
    return pl.pallas_call(
        ordered(functools.partial(mlp_kernel, n_in=len(bs), first=first, rb=rb, tn=tn, td=td, nk=nk, nd=nd), len(bs) + 3, after),
        grid=(nk + nd,),
        in_specs=[ANY] * (len(bs) + 3 + len(after)),
        out_specs=[pl.BlockSpec((rows // 2, td), dn)] * 2,
        out_shape=[jax.ShapeDtypeStruct((rows // 2, dim), BF)] * 2,
        scratch_shapes=[pltpu.VMEM((rows, dim), BF), pltpu.VMEM((rows, ffn), BF), pltpu.VMEM((2, 2, dim, tn), BF),
                        pltpu.VMEM((2, ffn, td), BF), pltpu.SemaphoreType.DMA((len(bs),)), pltpu.SemaphoreType.DMA((2,)),
                        pltpu.SemaphoreType.DMA((2,))],
        name="mlp", compiler_params=params(1),
        cost_estimate=cost(6 * rows * dim * ffn, 6 * dim * ffn),
    )(*bs, wg, wu, wd, *after)


def sum_kernel(*refs):
    p_ref, r_ref, t_ref, y_ref, z_ref = refs[-5:]
    total = p_ref[...].astype(F32) + r_ref[...].astype(F32) + t_ref[...].astype(F32)
    z_ref[...] = (y_ref[...].astype(F32) + total.astype(BF).astype(F32)).astype(BF)


def sum_rows(z, keep, recv, far, y, y_first, rows, first, total, after=(), tile=64):
    dim = y.shape[1]
    at = lambda r0: pl.BlockSpec((tile, dim), lambda i: (r0 // tile + i, 0))
    prev = () if z is None else (z,)
    return pl.pallas_call(
        ordered(sum_kernel, len(prev) + 4, after), grid=(rows // tile,),
        in_specs=[ANY] * len(prev) + [at(0)] * 3 + [at(y_first)] + [ANY] * len(after),
        out_specs=at(first),
        out_shape=jax.ShapeDtypeStruct((total, dim), BF),
        input_output_aliases={0: 0} if prev else {},
        name="zsum", compiler_params=params(1),
        cost_estimate=cost(rows * dim, 8 * rows * dim),
    )(*prev, keep, recv, far, y, *after)


def run_positions(xi, ci, y, cps, piece):
    def start(x, c):
        return (y if x == 0 else 2 * cps - 1 - y) * piece + c * (piece // 2)

    per = piece // 2 // RUN
    out = [start(xi, ci) + RUN * j for j in range(per)] + [start(xi, 1 - ci) + RUN * j for j in range(per)]
    for j in range(per):
        out += [start(1 - xi, ci) + RUN * j, start(1 - xi, 1 - ci) + RUN * j]
    return out


def block_list(tile, ids, diag):
    own = [] if diag is None else [diag]
    n_tail = (len(ids) + len(own)) % 4 or 4
    n_tail -= len(own)
    head, tail = ids[:len(ids) - n_tail], own + ids[len(ids) - n_tail:]
    blocks = [[0, head[i:i + 4], head[i:i + 4]] for i in range(0, len(head), 4)]
    fill = 4 - len(tail)
    keys = tail + [ids[-1] if ids else diag] * fill
    blocks.append([sum(1 << k for k, r in enumerate(keys) if r == diag), keys, tail + [-1] * fill])
    blocks[-1][0] |= LAST
    blocks[0][0] |= FIRST
    return [[tile, flags, 0] + keys + values for flags, keys, values in blocks]


def call_table(tiles, pairs, carry, idle):
    rows, most = [], 0
    carry = [c if pairs[t][0] or pairs[t][1] else idle for t, c in enumerate(carry)]
    for t, tile in enumerate(tiles):
        ids, own = pairs[t]
        if ids or own:
            mine = block_list(t, ids, tile if own else None)
            mine[0][1] |= CARRY if carry[t] else 0
            rows += mine
    for row in rows:
        most = max(most, max(row[3:7]) + 1)
        row[2] = most
    return [len(rows)] + carry + [v for row in rows for v in row], len(rows)


def work_tables(cps, piece):
    per = piece // 2 // RUN
    early = 2 * per + 2
    stage = lambda r: 0 if r < early else 1
    calls = [(0, list(range(early)))]
    calls += [(1, [j, per + j, 2 * per + 2 * j, 2 * per + 2 * j + 1]) for j in range(per)]
    tabs, all_runs, sizes = [], [], []
    for y in range(cps):
        for xi in range(2):
            for ci in range(2):
                mine = run_positions(xi, ci, y, cps, piece)
                pos = mine + run_positions(xi, ci, 1 - y, cps, piece)
                all_runs.append(mine)
                tabs.append([])
                sizes.append([])
                for now, tiles in calls:
                    pairs, carry = [], []
                    for t in tiles:
                        seen = [r for r in range(len(pos)) if pos[r] < pos[t]]
                        when = {r: max(stage(r), stage(t)) for r in seen}
                        late = list(when.values()).count(1) + stage(t)
                        soon = len(seen) + 1 - late
                        if late and soon % 4 <= -late % 4:
                            for r in [r for r in seen if not when[r]][:soon % 4]:
                                when[r] = 1
                        pairs.append(([r for r in seen if when[r] == now], stage(t) == now))
                        carry.append(int(stage(t) < now))
                    tab, n = call_table(tiles, pairs, carry, 2 if now == 1 else 0)
                    tabs[-1].append(tab)
                    sizes[-1].append(n)
    widths = [max(len(t[k]) for t in tabs) for k in range(len(calls))]
    flat = [[v for k, t in enumerate(tab) for v in t + [0] * (widths[k] - len(t))] for tab in tabs]
    bases = [sum(widths[:k]) for k in range(len(calls))]
    return np.array(flat, np.int32), np.array(all_runs, np.int32), bases, np.array(sizes).max(0) * 4


def solution(mesh):
    cps = mesh.shape['cp']
    row_spec = P('dp', ('cp', 'tp'), None)
    head_cols = P(None, 'tp', None)
    n_tp = mesh.shape['tp']

    over_core, over_x, over_both = (('tp', [(t, t ^ k) for t in range(n_tp)]) for k in (1, 2, 3))
    over_y = ('cp', [(i, i ^ 1) for i in range(cps)])

    def layer(x, g_attn, w_q, w_k, w_v, w_o, g_mlp, w_gate, w_up, w_down):
        x_rows = x[0]
        dim = x_rows.shape[1]
        n_run = x_rows.shape[0] // RUN
        piece = 2 * x_rows.shape[0]
        t_id, y_id = lax.axis_index('tp'), lax.axis_index('cp')
        np_tab, np_runs, bases, work = work_tables(cps, piece)
        dev = y_id * n_tp + t_id
        tab = lax.dynamic_index_in_dim(jnp.asarray(np_tab), dev, 0, keepdims=False)
        run_pos = lax.dynamic_index_in_dim(jnp.asarray(np_runs), dev, 0, keepdims=False)

        def tied(v, *others):
            return lax.optimization_barrier((v, *others))[0]

        def send(axis_pairs, v):
            return lax.ppermute(v, *axis_pairs)

        ga, gm = g_attn.reshape(1, dim), g_mlp.reshape(1, dim)
        own = []
        for j in range(n_run):
            own.append(norm_run(x_rows, ga, j, after=own[-1:]))
        far = [send(over_x, own[j]) for j in range(n_run)]
        mate = [send(over_core, own[j]) for j in range(n_run)]

        w_all = jnp.concatenate([tied(w, own[-1]).reshape(dim, -1) for w in (w_q, w_k, w_v)], axis=1)
        tables = rope_tables(tied(run_pos, own[-1])[:, None] + jnp.arange(RUN, dtype=jnp.int32)[None, :])

        q_here, kv_here = qkv(own + mate, w_all, (tables, 0))
        kvs, q_far = [kv_here], []

        def far_qkv(j, after):
            here = tied(far[j], after)
            rows = [here, send(over_core, here)], w_all, (tables, 2 * (n_run + j))
            if j + 1 < n_run:
                q, kv = qkv(*rows, after=(after,))
            else:
                kv, = qkv(*rows, False, after=(after,))
                q, = qkv(*rows, True, False, after=(kv, gm))
            q_far.append(q)
            kvs.append(kv)
            return kv

        far_qkv(1, far_qkv(0, kv_here))

        wo = w_o.reshape(-1, dim)
        half = wo.shape[0] // 2
        n_piece = 2
        rows = half // n_piece
        wo_c = send(over_core, tied(wo, kvs[-1]))

        tiles = [(0, i) for i in range(2 * n_run)] + [(1, 0), (1, 1)]
        st, *wo_x = flash(tab, [q_here, q_far[0]], tiles, kvs[:2], base=bases[0], work=int(work[0]), cut=wo,
                         n_cut=n_piece, after=(kvs[-1],))
        wo_x = [send(over_x, w) for w in wo_x]
        far_qkv(3, far_qkv(2, st))
        kvs = kvs + [send(over_y, kv) for kv in kvs]

        os, outs, prev = [], [], q_far[-1]
        wo_a, wo_ya, wo_yb = {}, {}, {}

        def forward_w(p):
            here = tied(wo_x[p], prev)
            wo_ya[p] = (here, send(over_core, here))
            wo_a[p] = send(over_y, here)

        def relay_w(p):
            here = tied(wo_a[p], prev)
            wo_yb[p] = (here, send(over_core, here))

        def attend(j):
            held = 2 * n_run + 2 * j
            carried = [j, n_run + j] + ([held, held + 1] if j == 0 else [None, None])
            pair = j % 2
            *o, done = flash(
                tab, [q_here, q_far[j]], [(0, j), (0, n_run + j), (1, 0), (1, 1)], kvs,
                base=bases[1 + j], work=int(work[1 + j]), st=st, st_src=carried, old=os.pop() if pair else None, slots=2,
                after=(prev,))
            if pair:
                o = [o[0], send(over_core, o[1]), send(over_x, o[2]), send(over_both, o[3])]
            os.append(o)
            return done

        def project(i):
            ws = [wo, wo_c]
            blocks = [[(0, 0, half)], [(0, half, half)], [(1, 0, half)], [(1, half, half)]]
            for k in range(2):
                for held in (wo_ya, wo_yb):
                    blocks.append([(len(ws) + p, 0, rows) for p in range(n_piece)])
                    ws += [held[p][k] for p in range(n_piece)]
            got = out_proj(os[i], ws, blocks, x_rows, gm, i, after=(prev,))
            for y, b in zip(got[::2], got[1::2]):
                outs.append((y, b, send(over_x, b), send(over_core, b)))
            return got[0]

        last = n_run - 1
        for j in range(last):
            prev = attend(j)
            if j < n_piece:
                forward_w(j)
            if j:
                relay_w(j - 1)
        prev = project(0)
        prev = attend(last)

        z, sums, relay = None, [], {}

        def relay_b(j):
            here = tied(outs[j][2], prev)
            relay[j] = (here, send(over_core, here))

        chunks = [(j, 0, RUN) for j in range(last)] + [(last, 0, RUN // 2), (last, RUN // 2, RUN // 2)]

        def finish(c):
            j, first, size = chunks[c]
            return sum_rows(z, *sums[c], outs[j][0], first, size, j * RUN + first, n_run * RUN,
                        after=() if prev is z else (prev,))

        relay_b(0)
        for c, (j, first, size) in enumerate(chunks):
            b = [outs[j][1], relay[j][0], outs[j][3], relay[j][1]]
            keep, out = mlp(b, first, size, w_gate, w_up, w_down, after=(prev,))
            recv = send(over_core, out)
            prev = keep
            if c < last:
                relay_b(c + 1)
            if c == 0:
                prev = project(1)
            elif c < n_run:
                prev = z = finish(c - 1)
            kept = keep if prev is keep else tied(keep, prev)
            prev = s_far = (kept[size:].astype(F32) + recv[size:].astype(F32)).astype(BF)
            sums.append((keep, recv, send(over_x, s_far)))
        for c in (last, n_run):
            prev = z = finish(c)
        return z[None]

    return jax.shard_map(layer, mesh=mesh,
                         in_specs=(row_spec, P(), head_cols, head_cols, head_cols, P('tp', None, None),
                                   P(), P(None, 'tp'), P(None, 'tp'), P('tp', None)),
                         out_specs=row_spec, check_vma=False)
```

```python
import functools
import math
import jax
import jax.numpy as jnp
import numpy as np
from jax import lax
from jax.experimental import pallas as pl
from jax.experimental.pallas import tpu as pltpu
from jax.sharding import PartitionSpec as P

NORM_EPS = 1e-5
ROPE_THETA = 500000.0
HD = 128
RUN = 256
NEG = -1e30
LOG2E = math.log2(math.e)
DN = (((1,), (0,)), ((), ()))
VMEM = 67043328
BF = jnp.bfloat16
F32 = jnp.float32
ANY = pl.BlockSpec(memory_space=pltpu.HBM)


def params(n):
    return pltpu.CompilerParams(dimension_semantics=("arbitrary",) * n, vmem_limit_bytes=VMEM)


def rope_tables(positions):
    half = HD // 2
    inv_freq = ROPE_THETA ** (-2.0 * jnp.arange(half, dtype=F32) / HD)
    angles = inv_freq[:, None] * positions.astype(F32)[..., None, :]
    return jnp.cos(angles), jnp.sin(angles)


def norm_rows(rows, gain):
    f = rows.astype(F32)
    mean_sq = jnp.mean(f * f, axis=-1, keepdims=True)
    return (f * lax.rsqrt(mean_sq + NORM_EPS) * gain.astype(F32)).astype(BF)


def cost(flops, moved):
    return pl.CostEstimate(flops=flops, transcendentals=0, bytes_accessed=moved)


def ordered(kernel, n_in, after):
    n = len(after)
    return lambda *refs: kernel(*refs[:n_in], *refs[n_in + n:])


def norm_kernel(x_ref, g_ref, o_ref):
    o_ref[...] = norm_rows(x_ref[...], g_ref[...])


def norm_run(x_rows, gain, j, after=(), tile=128):
    dim = x_rows.shape[1]
    per = RUN // tile
    return pl.pallas_call(
        ordered(norm_kernel, 2, after), grid=(per,),
        in_specs=[pl.BlockSpec((tile, dim), lambda i: (j * per + i, 0)), pl.BlockSpec((1, dim), lambda i: (0, 0))]
        + [ANY] * len(after),
        out_specs=pl.BlockSpec((tile, dim), lambda i: (i, 0)),
        out_shape=jax.ShapeDtypeStruct((RUN, dim), BF),
        name="norm", compiler_params=params(1),
        cost_estimate=cost(RUN * dim, RUN * dim),
    )(x_rows, gain, *after)


def qkv_kernel(*refs, n_in, n_q, group, first, with_q, with_kv):
    a_refs = refs[:n_in]
    w_ref, cos_ref, sin_ref, *outs, a_scr, sem = refs[n_in:]
    q_ref, kv_ref = outs[0], outs[-1]
    n = pl.program_id(0) + first
    heads = w_ref.shape[1] // HD

    @pl.when(n == first)
    def _():
        for k, r in enumerate(a_refs):
            pltpu.make_async_copy(r, a_scr.at[pl.ds(k * RUN, RUN), :], sem.at[k]).start()

    def rope(f, i):
        f = f.astype(BF).astype(F32)
        lo, hi, cos, sin = f[:HD // 2], f[HD // 2:], cos_ref[i], sin_ref[i]
        return jnp.concatenate([lo * cos - hi * sin, hi * cos + lo * sin], axis=0)

    def one(k, carry):
        @pl.when(n == first)
        def _():
            for i in range(group):
                rows = pl.ds(pl.multiple_of((k * group + i) * RUN, RUN), RUN)
                pltpu.make_async_copy(a_scr.at[rows, :], a_scr.at[rows, :], sem.at[k * group + i]).wait()

        rows = pl.ds(pl.multiple_of(k * group * RUN, group * RUN), group * RUN)
        r = jnp.dot(a_scr[rows, :], w_ref[...], preferred_element_type=F32)

        def piece(i, h):
            return r[i * RUN:(i + 1) * RUN, h * HD:(h + 1) * HD].T

        @pl.when((n < n_q) if with_q else False)
        def _():
            for i in range(group):
                for h in range(heads):
                    q_ref[k * group + i, h * HD:(h + 1) * HD, :] = rope(piece(i, h), k * group + i).astype(BF)

        @pl.when((n == n_q) if with_kv else False)
        def _():
            for i in range(group):
                for h in range(heads // 2):
                    kv_ref[k * group + i, 0, :, h * HD:(h + 1) * HD] = rope(piece(i, h), k * group + i).T.astype(BF)
                    kv_ref[k * group + i, 1, h * HD:(h + 1) * HD, :] = piece(i, h + heads // 2).astype(BF)

        return carry

    lax.fori_loop(0, n_in // group, one, 0)


def qkv(rows, w_all, tables, with_q=True, with_kv=True, after=(), group=2):
    n_in = len(rows)
    dim = w_all.shape[0]
    tn = 512
    n_q = w_all.shape[1] // tn - 1
    (cos, sin), first_run = tables
    at = first_run // n_in
    start = 0 if with_q else n_q
    kv_shape = (n_in, 2, RUN, RUN)
    tab = pl.BlockSpec((n_in, HD // 2, RUN), lambda n: (at, 0, 0))
    return pl.pallas_call(
        ordered(functools.partial(qkv_kernel, n_in=n_in, n_q=n_q, group=group, first=start, with_q=with_q, with_kv=with_kv),
                n_in + 3, after),
        grid=(n_q * with_q + with_kv,),
        in_specs=[ANY] * n_in + [pl.BlockSpec((dim, tn), lambda n: (0, n + start)), tab, tab] + [ANY] * len(after),
        out_specs=[pl.BlockSpec((n_in, tn, RUN), lambda n: (0, jnp.minimum(n, n_q - 1), 0))] * with_q
        + [pl.BlockSpec(kv_shape, lambda n: (0,) * len(kv_shape))] * with_kv,
        out_shape=[jax.ShapeDtypeStruct((n_in, n_q * tn, RUN), BF)] * with_q + [jax.ShapeDtypeStruct(kv_shape, BF)] * with_kv,
        scratch_shapes=[pltpu.VMEM((n_in * RUN, dim), BF), pltpu.SemaphoreType.DMA((n_in,))],
        name="qkv", compiler_params=params(1),
        cost_estimate=cost(2 * n_in * RUN * w_all.size, 2 * w_all.size),
    )(*rows, w_all, cos, sin, *after)


BLK = 11
LAST, FIRST, CARRY = 16, 32, 64
ST = HD + 16


def flash_kernel(tab_ref, *refs, q_src, kv_src, n_q, n_kv, st_src, n_st, n_old, n_cut, slot, base, G, n_tiles, n_heads, final):
    qs, kvs, sts = refs[:n_q], refs[n_q:n_q + n_kv], refs[n_q + n_kv:n_q + n_kv + n_st]
    n_out = n_tiles + 1 if final else 1 + n_cut
    at = n_q + n_kv + n_st + n_old
    outs = refs[at:at + n_out]
    q_scr, kv_scr, o_scr, st_scr, s_scr, mb_scr, acc_scr, m_scr, l_scr, q_sem, kv_sem, o_sem, st_sem = refs[at + n_out:][:13]
    if n_cut:
        cut_ref, (cut_scr, cut_sem) = refs[at - 1], refs[-2:]
    T = RUN
    c = (HD ** -0.5) * LOG2E
    n_blocks = tab_ref[base]
    carried = base + 1
    row0 = carried + n_tiles
    null = len(kv_src)

    q_copies = [pltpu.make_async_copy(qs[a].at[i], q_scr.at[t], q_sem.at[t]) for t, (a, i) in enumerate(q_src)]
    kv_copies = [pltpu.make_async_copy(kvs[a].at[i], kv_scr.at[r], kv_sem.at[r]) for r, (a, i) in enumerate(kv_src)]
    first = 4
    q_copies[0].start()
    for cp in kv_copies[:first]:
        cp.start()
    for cp in q_copies[1:]:
        cp.start()
    for t, i in enumerate(st_src):
        if i is not None:
            @pl.when(tab_ref[carried + t] != 0)
            def _():
                pltpu.make_async_copy(sts[0].at[i], st_scr.at[t], st_sem.at[t]).start()
    for cp in kv_copies[first:]:
        cp.start()
    kv_scr[null, 1] = jnp.zeros((256, 256), BF)
    if n_cut:
        cut_in = pltpu.make_async_copy(cut_ref.at[pl.ds(lax.axis_index('cp') * cut_scr.shape[0], cut_scr.shape[0]), :], cut_scr,
                                       cut_sem)
        part = cut_scr.shape[0] // n_cut
        cut_out = [pltpu.make_async_copy(cut_scr.at[pl.ds(k * part, part), :], outs[1 + k], cut_sem) for k in range(n_cut)]
        cut_in.start()

    def block(i):
        g = lax.div(i, n_blocks)
        return row0 + BLK * (i - g * n_blocks), g

    def arrived(have, need):
        def one(r, carry):
            pltpu.make_async_copy(kv_scr.at[r], kv_scr.at[r], kv_sem.at[r]).wait()
            return carry

        lax.fori_loop(have, need, one, 0)
        return jnp.maximum(have, need)

    def put(s, h, k):
        s_scr[h, pl.ds(k * RUN, RUN), :] = s
        mb_scr[h, k] = jnp.max(s.reshape(RUN // 8, 8, T), axis=0)

    def stage_a(row, g, h):
        col = pl.multiple_of(g * HD, HD)
        qt = q_scr[tab_ref[row], pl.ds(pl.multiple_of((g * G + h) * HD, HD), HD), :]
        for k in range(4):
            put(lax.dot_general(kv_scr[tab_ref[row + 3 + k], 0, :, pl.ds(col, HD)], qt, DN, preferred_element_type=F32), h, k)

    def stage_b(row, g, h):
        col = pl.multiple_of(g * HD, HD)
        m_prev = m_scr[h]
        mb = jnp.maximum(jnp.maximum(mb_scr[h, 0], mb_scr[h, 1]), jnp.maximum(mb_scr[h, 2], mb_scr[h, 3]))
        for r in (4, 2, 1):
            mb = jnp.maximum(mb, pltpu.roll(mb, r, 0))
        m_new = jnp.maximum(m_prev, mb)
        m_scr[h] = m_new
        m_c = m_new * c
        alpha = jnp.exp2(m_prev * c - m_c)
        l, pv = l_scr[h] * alpha, None
        for k in range(4):
            run = tab_ref[row + 7 + k]
            p = jnp.exp2(s_scr[h, k * RUN:(k + 1) * RUN].reshape(RUN // 8, 8, T) * c - m_c[None])
            l = l + jnp.sum(p, axis=0) * jnp.where(run < 0, 0.0, 1.0)
            d = lax.dot_general(kv_scr[jnp.where(run < 0, null, run), 1, pl.ds(col, HD), :], p.reshape(RUN, T).astype(BF), DN,
                                preferred_element_type=F32)
            pv = d if pv is None else pv + d
        l_scr[h] = l
        acc_scr[h] = (acc_scr[h].reshape(HD // 8, 8, T) * alpha[None]).reshape(HD, T) + pv

    def mask_runs(flags):
        seen = lax.broadcasted_iota(jnp.int32, (RUN, T), 0) <= lax.broadcasted_iota(jnp.int32, (RUN, T), 1)

        def one(k, carry):
            @pl.when((lax.shift_right_logical(flags, k) & 1) != 0)
            def _():
                rows = pl.multiple_of(k * RUN, RUN)
                for h in range(G):
                    put(jnp.where(seen, s_scr[h, pl.ds(rows, RUN), :], NEG), h, k)

            return carry

        lax.fori_loop(0, 4, one, 0)

    def finish(tile, g, get):
        for h in range(G):
            acc, l = get(h)
            o_scr[tile, :, pl.ds(pl.multiple_of((g * G + h) * HD, HD), HD)] = (acc / jnp.sum(l, axis=0, keepdims=True)).T.astype(BF)

        @pl.when(g == n_heads - 1)
        def _():
            for k in range(n_tiles):
                @pl.when(tile == k)
                def _():
                    pltpu.make_async_copy(o_scr.at[k], outs[k].at[slot], o_sem.at[k]).start()

    if final and n_st:
        def idle(i, carry):
            tile, g = lax.div(i, n_heads), lax.rem(i, n_heads)

            @pl.when(tab_ref[carried + tile] == 2)
            def _():
                @pl.when(g == 0)
                def _():
                    pltpu.make_async_copy(q_scr.at[tile], q_scr.at[tile], q_sem.at[tile]).wait()
                    pltpu.make_async_copy(st_scr.at[tile], st_scr.at[tile], st_sem.at[tile]).wait()

                finish(tile, g, lambda h: (st_scr[tile, g, h, :HD, :], st_scr[tile, g, h, HD + 8:, :]))

            return carry

        lax.fori_loop(0, n_tiles * n_heads, idle, 0)

    def query(row):
        t = tab_ref[row]
        pltpu.make_async_copy(q_scr.at[t], q_scr.at[t], q_sem.at[t]).wait()

    row, g = block(0)
    query(row)
    have = arrived(0, tab_ref[row + 2])
    for h in range(G):
        stage_a(row, g, h)

    def body(i, have):
        row, g = block(i)
        nrow, ng = block(jnp.minimum(i + 1, n_heads * n_blocks - 1))
        have = arrived(have, tab_ref[nrow + 2])
        flags = tab_ref[row + 1]
        tile = tab_ref[row]

        @pl.when((i + 1 < n_blocks) & ((tab_ref[nrow + 1] & FIRST) != 0))
        def _():
            query(nrow)

        @pl.when((flags & (FIRST | CARRY)) == FIRST)
        def _():
            acc_scr[...] = jnp.zeros_like(acc_scr)
            l_scr[...] = jnp.zeros_like(l_scr)
            m_scr[...] = jnp.full_like(m_scr, NEG)

        if n_st:
            @pl.when((flags & (FIRST | CARRY)) == (FIRST | CARRY))
            def _():
                @pl.when(g == 0)
                def _():
                    pltpu.make_async_copy(st_scr.at[tile], st_scr.at[tile], st_sem.at[tile]).wait()

                for h in range(G):
                    acc_scr[h] = st_scr[tile, g, h, :HD, :]
                    m_scr[h] = st_scr[tile, g, h, HD:HD + 8, :]
                    l_scr[h] = st_scr[tile, g, h, HD + 8:, :]

        if n_cut:
            @pl.when(i == n_blocks)
            def _():
                cut_in.wait()
                for cp in cut_out:
                    cp.start()

        @pl.when((flags & 15) != 0)
        def _():
            mask_runs(flags)

        for h in range(G):
            stage_b(row, g, h)
            stage_a(nrow, ng, h)

        @pl.when((flags & LAST) != 0)
        def _():
            if final:
                finish(tile, g, lambda h: (acc_scr[h], l_scr[h]))
            else:
                for h in range(G):
                    st_scr[tile, g, h, :HD, :] = acc_scr[h]
                    st_scr[tile, g, h, HD:HD + 8, :] = m_scr[h]
                    st_scr[tile, g, h, HD + 8:, :] = l_scr[h]

                @pl.when(g == n_heads - 1)
                def _():
                    pltpu.make_async_copy(st_scr.at[tile], outs[0].at[tile], o_sem.at[tile]).start()

        return have

    have = lax.fori_loop(0, n_heads * n_blocks, body, have)
    arrived(have, len(kv_src))
    if final:
        for k in range(n_tiles):
            pltpu.make_async_copy(o_scr.at[k], outs[k].at[slot], o_sem.at[k]).wait()
    else:
        def wait_out(i, carry):
            row = row0 + BLK * i

            @pl.when((tab_ref[row + 1] & LAST) != 0)
            def _():
                t = tab_ref[row]
                pltpu.make_async_copy(st_scr.at[t], st_scr.at[t], o_sem.at[t]).wait()

            return carry

        lax.fori_loop(0, n_blocks, wait_out, 0)
        for cp in cut_out:
            cp.wait()


def flash(tab, qs, q_src, kvs, *, base, work, st=None, st_src=None, old=None, cut=None, n_cut=0, slots=1, after=()):
    nq = qs[0].shape[1]
    n_heads = 2
    G = nq // HD // n_heads
    n_tiles = len(q_src)
    final = cut is None
    kv_src = [(a, i) for a, kv in enumerate(kvs) for i in range(kv.shape[0])]
    n_runs = len(kv_src)
    sts = () if st is None else (st,)
    old = old or ()
    more = (*old, *(() if final else (cut,)))
    n_in = 1 + len(qs) + len(kvs) + len(sts) + len(more)
    state = (n_heads, G, ST, RUN)
    has_st = not final or sts
    if final:
        out_shape = [jax.ShapeDtypeStruct((slots, RUN, nq), BF)] * n_tiles + [jax.ShapeDtypeStruct((8, HD), F32)]
        scratch = []
    else:
        half = cut.shape[0] // 2
        out_shape = [jax.ShapeDtypeStruct((n_tiles, *state), F32)]
        out_shape += [jax.ShapeDtypeStruct((half // n_cut, cut.shape[1]), BF)] * n_cut
        scratch = [pltpu.VMEM((half, cut.shape[1]), BF), pltpu.SemaphoreType.DMA]
    return pl.pallas_call(
        ordered(functools.partial(flash_kernel, q_src=q_src, kv_src=kv_src, n_q=len(qs), n_kv=len(kvs),
                                  st_src=st_src or [None] * n_tiles, n_st=len(sts), n_old=len(more), n_cut=n_cut,
                                  slot=slots - 1 if old else 0, base=base, G=G, n_tiles=n_tiles, n_heads=n_heads, final=final),
                n_in, after),
        grid_spec=pltpu.PrefetchScalarGridSpec(
            num_scalar_prefetch=1, grid=(),
            in_specs=[ANY] * (n_in - 1 + len(after)),
            out_specs=[ANY] * len(out_shape),
            scratch_shapes=[pltpu.VMEM((n_tiles, nq, RUN), BF),
                            pltpu.VMEM((n_runs + 1, 2, 256, 256), BF),
                            pltpu.VMEM((n_tiles if final else 1, RUN, nq), BF),
                            pltpu.VMEM((n_tiles if has_st else 1, *state), F32),
                            pltpu.VMEM((G, 4 * RUN, RUN), F32),
                            pltpu.VMEM((G, 4, 8, RUN), F32),
                            pltpu.VMEM((G, HD, RUN), F32),
                            pltpu.VMEM((G, 8, RUN), F32),
                            pltpu.VMEM((G, 8, RUN), F32),
                            pltpu.SemaphoreType.DMA((n_tiles,)),
                            pltpu.SemaphoreType.DMA((n_runs,)),
                            pltpu.SemaphoreType.DMA((n_tiles,)),
                            pltpu.SemaphoreType.DMA((n_tiles,)), *scratch]),
        out_shape=out_shape,
        input_output_aliases={n_in - len(old) + k: k for k in range(len(old))},
        name="flash" if final else "flash_part", compiler_params=params(0),
        cost_estimate=cost(8 * work * RUN * RUN * nq, n_runs * RUN * nq),
    )(tab, *qs, *kvs, *sts, *more, *after)


def out_kernel(*refs, blocks, n_w, runs):
    n_run = len(runs)
    n_o, n_out = 4, 2 * n_run
    o_refs, w_refs, x_ref, g_ref = refs[:n_o], refs[n_o:n_o + n_w], refs[n_o + n_w], refs[n_o + n_w + 1]
    outs = refs[n_o + n_w + 2:n_o + n_w + 2 + n_out]
    o_scr, w_scr, x_scr, acc_scr, o_sem, w_sem, x_sem, out_sem = refs[n_o + n_w + 2 + n_out:]
    width = o_refs[0].shape[-1]
    half = width // 2
    n_slots = w_scr.shape[0]

    def fetch(k):
        for i, pieces in enumerate(blocks):
            @pl.when(k == i)
            def _():
                to = 0
                for a, r0, n in pieces:
                    pltpu.make_async_copy(w_refs[a].at[pl.ds(r0, n), :], w_scr.at[i % n_slots, pl.ds(to, n), :],
                                          w_sem.at[i % n_slots]).start()
                    to += n

    mine = lax.axis_index('cp')
    loads = [[] for _ in blocks]
    for i in range(n_run):
        rows = pl.ds(i * RUN, RUN)
        for k in range(4):
            src = o_refs[k].at[i]
            if k < 2:
                loads[2 * k].append((src, o_scr.at[rows, pl.ds(k * width, width)]))
            else:
                for p, part in enumerate((mine, 1 - mine)):
                    loads[2 * k + p].append((src.at[:, pl.ds(pl.multiple_of(part * half, half), half)],
                                             o_scr.at[rows, pl.ds(k * width + p * half, half)]))
    copies = [[pltpu.make_async_copy(src, dst, o_sem.at[k, i]) for i, (src, dst) in enumerate(ls)] for k, ls in enumerate(loads)]
    for cp in copies[0]:
        cp.start()
    for i in range(n_slots - 1):
        fetch(jnp.int32(i))
    for ls in copies[1:]:
        for cp in ls:
            cp.start()
    for i, run in enumerate(runs):
        pltpu.make_async_copy(x_ref.at[pl.ds(run * RUN, RUN), :], x_scr.at[pl.ds(i * RUN, RUN), :], x_sem).start()
    acc_scr[...] = jnp.zeros_like(acc_scr)

    def one(k, carry):
        fetch(k + n_slots - 1)
        for i, ls in enumerate(copies):
            if ls:
                @pl.when(k == i)
                def _():
                    for cp in ls:
                        cp.wait()
        slot = lax.rem(k, n_slots)
        pltpu.make_async_copy(w_scr.at[slot], w_scr.at[slot], w_sem.at[slot]).wait()
        acc_scr[...] += jnp.dot(o_scr[:, pl.ds(pl.multiple_of(k * half, half), half)], w_scr[slot], preferred_element_type=F32)
        return carry

    lax.fori_loop(0, len(blocks), one, 0)
    pltpu.make_async_copy(x_scr, x_scr, x_sem).wait()

    def rows32(r, carry):
        rows = pl.ds(pl.multiple_of(r * 32, 32), 32)
        y = (x_scr[rows, :].astype(F32) + acc_scr[rows, :].astype(BF).astype(F32)).astype(BF)
        x_scr[rows, :] = y
        o_scr[rows, :] = norm_rows(y, g_ref[...])
        return carry

    stores, per = [], RUN // 32
    for i in range(n_run):
        lax.fori_loop(i * per, (i + 1) * per, rows32, 0)
        for k, scr in enumerate((x_scr, o_scr)):
            stores.append(pltpu.make_async_copy(scr.at[pl.ds(i * RUN, RUN), :], outs[2 * i + k], out_sem.at[2 * i + k]))
            stores[-1].start()
    for cp in stores:
        cp.wait()


def out_proj(os, ws, blocks, x_rows, gain, runs, after=()):
    dim = x_rows.shape[1]
    n_run, _, width = os[0].shape
    rows = n_run * RUN
    return pl.pallas_call(
        ordered(functools.partial(out_kernel, blocks=blocks, n_w=len(ws), runs=runs),
                len(os) + len(ws) + 2, after),
        grid=(1,),
        in_specs=[ANY] * (len(os) + len(ws) + 1) + [pl.BlockSpec((1, dim), lambda i: (0, 0))] + [ANY] * len(after),
        out_specs=[ANY] * (2 * n_run),
        out_shape=[jax.ShapeDtypeStruct((RUN, dim), BF)] * (2 * n_run),
        scratch_shapes=[pltpu.VMEM((rows, 4 * width), BF), pltpu.VMEM((3, width // 2, dim), BF), pltpu.VMEM((rows, dim), BF),
                        pltpu.VMEM((rows, dim), F32), pltpu.SemaphoreType.DMA((len(blocks), 2 * n_run)),
                        pltpu.SemaphoreType.DMA((3,)), pltpu.SemaphoreType.DMA, pltpu.SemaphoreType.DMA((2 * n_run,))],
        name="outp", compiler_params=params(1),
        cost_estimate=cost(8 * rows * width * dim, 8 * width * dim),
    )(*os, *ws, x_rows, gain, *after)


def mlp_kernel(*refs, n_in, first, rb, tn, td, nk, nd):
    b_refs = refs[:n_in]
    wg_ref, wu_ref, wd_ref, keep_ref, send_ref, b_scr, u_scr, w_scr, d_scr, b_sem, w_sem, d_sem = refs[n_in:]
    i = pl.program_id(0)

    def fetch(j):
        @pl.when(j < nk)
        def _():
            slot, cols = lax.rem(j, 2), pl.ds(pl.multiple_of(j * tn, tn), tn)
            for k, w in enumerate((wg_ref, wu_ref)):
                pltpu.make_async_copy(w.at[:, cols], w_scr.at[slot, k], w_sem.at[slot]).start()

        @pl.when((j >= nk) & (j < nk + nd))
        def _():
            n, slot = j - nk, lax.rem(j - nk, 2)
            pltpu.make_async_copy(wd_ref.at[:, pl.ds(pl.multiple_of(n * td, td), td)], d_scr.at[slot], d_sem.at[slot]).start()

    def gated(rows, cols, slot):
        b = b_scr[rows, :]
        gate = jnp.dot(b, w_scr[slot, 0], preferred_element_type=F32)
        up = jnp.dot(b, w_scr[slot, 1], preferred_element_type=F32)
        u_scr[rows, cols] = (jax.nn.silu(gate) * up).astype(BF)

    @pl.when(i == 0)
    def _():
        copies = [pltpu.make_async_copy(r.at[pl.ds(first, rb), :], b_scr.at[pl.ds(k * rb, rb), :], b_sem.at[k])
                  for k, r in enumerate(b_refs)]
        copies[0].start()
        fetch(i)
        for cp in copies[1:]:
            cp.start()

    fetch(i + 1)

    @pl.when(i < nk)
    def _():
        pltpu.make_async_copy(w_scr.at[lax.rem(i, 2)], w_scr.at[lax.rem(i, 2)], w_sem.at[lax.rem(i, 2)]).wait()

    @pl.when(i == 0)
    def _():
        def one(k, carry):
            rows = pl.ds(pl.multiple_of(k * rb, rb), rb)
            pltpu.make_async_copy(b_scr.at[rows, :], b_scr.at[rows, :], b_sem.at[k]).wait()
            gated(rows, pl.ds(0, tn), 0)
            return carry

        lax.fori_loop(0, n_in, one, 0)

    @pl.when((i > 0) & (i < nk))
    def _():
        gated(slice(None), pl.ds(pl.multiple_of(i * tn, tn), tn), lax.rem(i, 2))

    @pl.when(i >= nk)
    def _():
        slot = lax.rem(i - nk, 2)
        pltpu.make_async_copy(d_scr.at[slot], d_scr.at[slot], d_sem.at[slot]).wait()
        d = jnp.dot(u_scr[...], d_scr[slot], preferred_element_type=F32).astype(BF)
        half = d.shape[0] // 2
        keep_ref[...] = d[:half]
        send_ref[...] = d[half:]


def mlp(bs, first, rb, wg, wu, wd, after=()):
    dim = bs[0].shape[1]
    rows = rb * len(bs)
    ffn = wg.shape[1]
    td = 512
    tn = td if rows <= td else td // 2
    nk, nd = ffn // tn, dim // td
    dn = lambda i: (0, jnp.maximum(i - nk, 0))
    return pl.pallas_call(
        ordered(functools.partial(mlp_kernel, n_in=len(bs), first=first, rb=rb, tn=tn, td=td, nk=nk, nd=nd), len(bs) + 3, after),
        grid=(nk + nd,),
        in_specs=[ANY] * (len(bs) + 3 + len(after)),
        out_specs=[pl.BlockSpec((rows // 2, td), dn)] * 2,
        out_shape=[jax.ShapeDtypeStruct((rows // 2, dim), BF)] * 2,
        scratch_shapes=[pltpu.VMEM((rows, dim), BF), pltpu.VMEM((rows, ffn), BF), pltpu.VMEM((2, 2, dim, tn), BF),
                        pltpu.VMEM((2, ffn, td), BF), pltpu.SemaphoreType.DMA((len(bs),)), pltpu.SemaphoreType.DMA((2,)),
                        pltpu.SemaphoreType.DMA((2,))],
        name="mlp", compiler_params=params(1),
        cost_estimate=cost(6 * rows * dim * ffn, 6 * dim * ffn),
    )(*bs, wg, wu, wd, *after)


def sum_kernel(*refs):
    p_ref, r_ref, t_ref, y_ref, z_ref = refs[-5:]
    total = p_ref[...].astype(F32) + r_ref[...].astype(F32) + t_ref[...].astype(F32)
    z_ref[...] = (y_ref[...].astype(F32) + total.astype(BF).astype(F32)).astype(BF)


def sum_rows(z, keep, recv, far, y, y_first, rows, first, total, after=(), tile=64):
    dim = y.shape[1]
    at = lambda r0: pl.BlockSpec((tile, dim), lambda i: (r0 // tile + i, 0))
    prev = () if z is None else (z,)
    return pl.pallas_call(
        ordered(sum_kernel, len(prev) + 4, after), grid=(rows // tile,),
        in_specs=[ANY] * len(prev) + [at(0)] * 3 + [at(y_first)] + [ANY] * len(after),
        out_specs=at(first),
        out_shape=jax.ShapeDtypeStruct((total, dim), BF),
        input_output_aliases={0: 0} if prev else {},
        name="zsum", compiler_params=params(1),
        cost_estimate=cost(rows * dim, 8 * rows * dim),
    )(*prev, keep, recv, far, y, *after)


def run_positions(xi, ci, y, cps, piece):
    def start(x, c):
        return (y if x == 0 else 2 * cps - 1 - y) * piece + c * (piece // 2)

    per = piece // 2 // RUN
    out = [start(xi, ci) + RUN * j for j in range(per)] + [start(xi, 1 - ci) + RUN * j for j in range(per)]
    for j in range(per):
        out += [start(1 - xi, ci) + RUN * j, start(1 - xi, 1 - ci) + RUN * j]
    return out


def block_list(tile, ids, diag):
    own = [] if diag is None else [diag]
    n_tail = (len(ids) + len(own)) % 4 or 4
    n_tail -= len(own)
    head, tail = ids[:len(ids) - n_tail], own + ids[len(ids) - n_tail:]
    blocks = [[0, head[i:i + 4], head[i:i + 4]] for i in range(0, len(head), 4)]
    fill = 4 - len(tail)
    keys = tail + [ids[-1] if ids else diag] * fill
    blocks.append([sum(1 << k for k, r in enumerate(keys) if r == diag), keys, tail + [-1] * fill])
    blocks[-1][0] |= LAST
    blocks[0][0] |= FIRST
    return [[tile, flags, 0] + keys + values for flags, keys, values in blocks]


def call_table(tiles, pairs, carry, idle):
    rows, most = [], 0
    carry = [c if pairs[t][0] or pairs[t][1] else idle for t, c in enumerate(carry)]
    for t, tile in enumerate(tiles):
        ids, own = pairs[t]
        if ids or own:
            mine = block_list(t, ids, tile if own else None)
            mine[0][1] |= CARRY if carry[t] else 0
            rows += mine
    for row in rows:
        most = max(most, max(row[3:7]) + 1)
        row[2] = most
    return [len(rows)] + carry + [v for row in rows for v in row], len(rows)


def work_tables(cps, piece):
    per = piece // 2 // RUN
    early = 3 * per
    stage = lambda r: 0 if r < early else 1
    calls = [(0, list(range(early)))]
    calls += [(1, [j, per + j, 2 * per + 2 * j, 2 * per + 2 * j + 1]) for j in range(per)]
    tabs, all_runs, sizes = [], [], []
    for y in range(cps):
        for xi in range(2):
            for ci in range(2):
                mine = run_positions(xi, ci, y, cps, piece)
                pos = mine + run_positions(xi, ci, 1 - y, cps, piece)
                all_runs.append(mine)
                tabs.append([])
                sizes.append([])
                for now, tiles in calls:
                    pairs, carry = [], []
                    for t in tiles:
                        seen = [r for r in range(len(pos)) if pos[r] < pos[t]]
                        when = {r: max(stage(r), stage(t)) for r in seen}
                        late = list(when.values()).count(1) + stage(t)
                        soon = len(seen) + 1 - late
                        if late and soon % 4 <= -late % 4:
                            for r in [r for r in seen if not when[r]][:soon % 4]:
                                when[r] = 1
                        pairs.append(([r for r in seen if when[r] == now], stage(t) == now))
                        carry.append(int(stage(t) < now))
                    tab, n = call_table(tiles, pairs, carry, 2 if now == 1 else 0)
                    tabs[-1].append(tab)
                    sizes[-1].append(n)
    widths = [max(len(t[k]) for t in tabs) for k in range(len(calls))]
    flat = [[v for k, t in enumerate(tab) for v in t + [0] * (widths[k] - len(t))] for tab in tabs]
    bases = [sum(widths[:k]) for k in range(len(calls))]
    return np.array(flat, np.int32), np.array(all_runs, np.int32), bases, np.array(sizes).max(0) * 4


def solution(mesh):
    cps = mesh.shape['cp']
    row_spec = P('dp', ('cp', 'tp'), None)
    head_cols = P(None, 'tp', None)
    n_tp = mesh.shape['tp']

    over_core, over_x, over_both = (('tp', [(t, t ^ k) for t in range(n_tp)]) for k in (1, 2, 3))
    over_y = ('cp', [(i, i ^ 1) for i in range(cps)])

    def layer(x, g_attn, w_q, w_k, w_v, w_o, g_mlp, w_gate, w_up, w_down):
        x_rows = x[0]
        dim = x_rows.shape[1]
        n_run = x_rows.shape[0] // RUN
        piece = 2 * x_rows.shape[0]
        t_id, y_id = lax.axis_index('tp'), lax.axis_index('cp')
        np_tab, np_runs, bases, work = work_tables(cps, piece)
        dev = y_id * n_tp + t_id
        tab = lax.dynamic_index_in_dim(jnp.asarray(np_tab), dev, 0, keepdims=False)
        run_pos = lax.dynamic_index_in_dim(jnp.asarray(np_runs), dev, 0, keepdims=False)

        def tied(v, *others):
            return lax.optimization_barrier((v, *others))[0]

        def send(axis_pairs, v):
            return lax.ppermute(v, *axis_pairs)

        ga, gm = g_attn.reshape(1, dim), g_mlp.reshape(1, dim)
        own = []
        for j in range(n_run):
            own.append(norm_run(x_rows, ga, j, after=own[-1:]))
        far = [send(over_x, own[j]) for j in range(n_run)]
        mate = [send(over_core, own[j]) for j in range(n_run)]

        w_all = jnp.concatenate([tied(w, own[-1]).reshape(dim, -1) for w in (w_q, w_k, w_v)], axis=1)
        tables = rope_tables(tied(run_pos, own[-1])[:, None] + jnp.arange(RUN, dtype=jnp.int32)[None, :])

        q_here, kv_here = qkv(own + mate, w_all, (tables, 0))
        kvs, q_far = [kv_here], []

        def far_qkv(j, after):
            here = tied(far[j], after)
            rows = [here, send(over_core, here)], w_all, (tables, 2 * (n_run + j))
            if j + 1 < n_run:
                q, kv = qkv(*rows, after=(after,))
            else:
                kv, = qkv(*rows, False, after=(after,))
                q, = qkv(*rows, True, False, after=(kv, gm))
            q_far.append(q)
            kvs.append(kv)
            return kv

        far_qkv(1, far_qkv(0, kv_here))

        wo = w_o.reshape(-1, dim)
        half = wo.shape[0] // 2
        n_piece = 2
        rows = half // n_piece
        wo_c = send(over_core, tied(wo, kvs[-1]))

        tiles = [(0, i) for i in range(2 * n_run)] + [(a, i) for a in (1, 2) for i in range(2)]
        st, *wo_x = flash(tab, [q_here, *q_far], tiles, kvs, base=bases[0], work=int(work[0]), cut=wo,
                         n_cut=n_piece)
        wo_x = [send(over_x, w) for w in wo_x]
        far_qkv(3, far_qkv(2, st))
        kvs = kvs + [send(over_y, kv) for kv in kvs]

        os, outs, prev = [], [], q_far[-1]
        wo_a, wo_ya, wo_yb = {}, {}, {}

        def forward_w(p):
            here = tied(wo_x[p], prev)
            wo_ya[p] = (here, send(over_core, here))
            wo_a[p] = send(over_y, here)

        def relay_w(p):
            here = tied(wo_a[p], prev)
            wo_yb[p] = (here, send(over_core, here))

        order = (0, 3, 1, 2)

        def attend(at):
            j = order[at]
            held = 2 * n_run + 2 * j
            carried = [j, n_run + j] + ([held, held + 1] if held < len(tiles) else [None, None])
            pair = at % 2
            *o, done = flash(
                tab, [q_here, q_far[j]], [(0, j), (0, n_run + j), (1, 0), (1, 1)], kvs,
                base=bases[1 + j], work=int(work[1 + j]), st=st, st_src=carried, old=os.pop() if pair else None, slots=2,
                after=(prev,))
            if pair:
                o = [o[0], send(over_core, o[1]), send(over_x, o[2]), send(over_both, o[3])]
            os.append(o)
            return done

        def project(i):
            ws = [wo, wo_c]
            blocks = [[(0, 0, half)], [(0, half, half)], [(1, 0, half)], [(1, half, half)]]
            for k in range(2):
                for held in (wo_ya, wo_yb):
                    blocks.append([(len(ws) + p, 0, rows) for p in range(n_piece)])
                    ws += [held[p][k] for p in range(n_piece)]
            got = out_proj(os[i], ws, blocks, x_rows, gm, order[2 * i:2 * i + 2], after=(prev,))
            for y, b in zip(got[::2], got[1::2]):
                outs.append((y, b, send(over_x, b), send(over_core, b)))
            return got[0]

        last = n_run - 1
        for j in range(last):
            prev = attend(j)
            if j < n_piece:
                forward_w(j)
            if j:
                relay_w(j - 1)
        prev = project(0)
        prev = attend(last)

        z, sums, relay = None, [], {}

        def relay_b(j):
            here = tied(outs[j][2], prev)
            relay[j] = (here, send(over_core, here))

        chunks = [(j, 0, RUN) for j in range(last)] + [(last, 0, RUN // 2), (last, RUN // 2, RUN // 2)]

        def finish(c):
            j, first, size = chunks[c]
            return sum_rows(z, *sums[c], outs[j][0], first, size, order[j] * RUN + first, n_run * RUN,
                        after=() if prev is z else (prev,))

        relay_b(0)
        for c, (j, first, size) in enumerate(chunks):
            b = [outs[j][1], relay[j][0], outs[j][3], relay[j][1]]
            keep, out = mlp(b, first, size, w_gate, w_up, w_down, after=(prev,))
            recv = send(over_core, out)
            prev = keep
            if c < last:
                relay_b(c + 1)
            if c == 0:
                prev = project(1)
            elif c < n_run:
                prev = z = finish(c - 1)
            kept = keep if prev is keep else tied(keep, prev)
            prev = s_far = (kept[size:].astype(F32) + recv[size:].astype(F32)).astype(BF)
            sums.append((keep, recv, send(over_x, s_far)))
        for c in (last, n_run):
            prev = z = finish(c)
        return z[None]

    return jax.shard_map(layer, mesh=mesh,
                         in_specs=(row_spec, P(), head_cols, head_cols, head_cols, P('tp', None, None),
                                   P(), P(None, 'tp'), P(None, 'tp'), P('tp', None)),
                         out_specs=row_spec, check_vma=False)
```

```python
import functools
import math
import jax
import jax.numpy as jnp
import numpy as np
from jax import lax
from jax.experimental import pallas as pl
from jax.experimental.pallas import tpu as pltpu
from jax.sharding import PartitionSpec as P

NORM_EPS = 1e-5
ROPE_THETA = 500000.0
HD = 128
RUN = 256
NEG = -1e30
LOG2E = math.log2(math.e)
DN = (((1,), (0,)), ((), ()))
BF = jnp.bfloat16
F32 = jnp.float32
ANY = pl.BlockSpec(memory_space=pltpu.HBM)


PARAMS = pltpu.CompilerParams(vmem_limit_bytes=67043328)


def rope_tables(positions):
    half = HD // 2
    inv_freq = ROPE_THETA ** (-2.0 * jnp.arange(half, dtype=F32) / HD)
    angles = inv_freq[:, None] * positions.astype(F32)[..., None, :]
    return jnp.cos(angles), jnp.sin(angles)


def norm_rows(rows, gain):
    f = rows.astype(F32)
    mean_sq = jnp.mean(f * f, axis=-1, keepdims=True)
    return (f * lax.rsqrt(mean_sq + NORM_EPS) * gain.astype(F32)).astype(BF)


def cost(flops, moved):
    return pl.CostEstimate(flops=flops, transcendentals=0, bytes_accessed=moved)


def ordered(kernel, n_in, after):
    n = len(after)
    return lambda *refs: kernel(*refs[:n_in], *refs[n_in + n:])


def norm_kernel(x_ref, g_ref, o_ref):
    o_ref[...] = norm_rows(x_ref[...], g_ref[...])


def norm_run(x_rows, gain, j, after=(), tile=128):
    dim = x_rows.shape[1]
    per = RUN // tile
    return pl.pallas_call(
        ordered(norm_kernel, 2, after), grid=(per,),
        in_specs=[pl.BlockSpec((tile, dim), lambda i: (j * per + i, 0)), pl.BlockSpec((1, dim), lambda i: (0, 0))]
        + [ANY] * len(after),
        out_specs=pl.BlockSpec((tile, dim), lambda i: (i, 0)),
        out_shape=jax.ShapeDtypeStruct((RUN, dim), BF),
        name="norm", compiler_params=PARAMS,
        cost_estimate=cost(RUN * dim, RUN * dim),
    )(x_rows, gain, *after)


def qkv_kernel(*refs, n_in, n_q, group, first, with_q, with_kv):
    a_refs = refs[:n_in]
    w_ref, cos_ref, sin_ref, *outs, a_scr, sem = refs[n_in:]
    q_ref, kv_ref = outs[0], outs[-1]
    n = pl.program_id(0) + first
    heads = w_ref.shape[1] // HD

    @pl.when(n == first)
    def _():
        for k, r in enumerate(a_refs):
            pltpu.make_async_copy(r, a_scr.at[pl.ds(k * RUN, RUN), :], sem.at[k]).start()

    def rope(f, i):
        f = f.astype(BF).astype(F32)
        lo, hi, cos, sin = f[:HD // 2], f[HD // 2:], cos_ref[i], sin_ref[i]
        return jnp.concatenate([lo * cos - hi * sin, hi * cos + lo * sin], axis=0)

    def one(k, carry):
        @pl.when(n == first)
        def _():
            for i in range(group):
                rows = pl.ds(pl.multiple_of((k * group + i) * RUN, RUN), RUN)
                pltpu.make_async_copy(a_scr.at[rows, :], a_scr.at[rows, :], sem.at[k * group + i]).wait()

        runs = [k * group + i for i in range(group)]

        def products():
            return [jnp.dot(a_scr[pl.ds(pl.multiple_of(run * RUN, RUN), RUN), :], w_ref[...], preferred_element_type=F32)
                    for run in runs]

        if with_q:
            @pl.when(n < n_q)
            def _():
                for run, r in zip(runs, products()):
                    for h in range(heads):
                        cols = slice(h * HD, (h + 1) * HD)
                        q_ref[run, cols, :] = rope(r[:, cols].T, run).astype(BF)

        if with_kv:
            @pl.when(n == n_q)
            def _():
                for run, r in zip(runs, products()):
                    for h in range(heads // 2):
                        cols, past = slice(h * HD, (h + 1) * HD), heads // 2 * HD
                        kv_ref[run, 0, :, cols] = rope(r[:, cols].T, run).T.astype(BF)
                        kv_ref[run, 1, cols, :] = r[:, past + h * HD:past + (h + 1) * HD].T.astype(BF)
        return carry

    lax.fori_loop(0, n_in // group, one, 0)


def qkv(rows, w_all, tables, with_q=True, with_kv=True, after=(), group=2):
    n_in = len(rows)
    dim = w_all.shape[0]
    tn = 512
    n_q = w_all.shape[1] // tn - 1
    (cos, sin), first_run = tables
    at = first_run // n_in
    start = 0 if with_q else n_q
    kv_shape = (n_in, 2, RUN, RUN)
    tab = pl.BlockSpec((n_in, HD // 2, RUN), lambda n: (at, 0, 0))
    return pl.pallas_call(
        ordered(functools.partial(qkv_kernel, n_in=n_in, n_q=n_q, group=group, first=start, with_q=with_q, with_kv=with_kv),
                n_in + 3, after),
        grid=(n_q * with_q + with_kv,),
        in_specs=[ANY] * n_in + [pl.BlockSpec((dim, tn), lambda n: (0, n + start)), tab, tab] + [ANY] * len(after),
        out_specs=[pl.BlockSpec((n_in, tn, RUN), lambda n: (0, jnp.minimum(n, n_q - 1), 0))] * with_q
        + [pl.BlockSpec(kv_shape, lambda n: (0,) * len(kv_shape))] * with_kv,
        out_shape=[jax.ShapeDtypeStruct((n_in, n_q * tn, RUN), BF)] * with_q + [jax.ShapeDtypeStruct(kv_shape, BF)] * with_kv,
        scratch_shapes=[pltpu.VMEM((n_in * RUN, dim), BF), pltpu.SemaphoreType.DMA((n_in,))],
        name="qkv", compiler_params=PARAMS,
        cost_estimate=cost(2 * n_in * RUN * w_all.size, 2 * w_all.size),
    )(*rows, w_all, cos, sin, *after)


BLK = 11
LAST, FIRST, CARRY = 16, 32, 64
ST = HD + 16


def flash_kernel(tab_ref, *refs, q_src, kv_src, n_q, n_kv, st_src, n_st, n_old, n_cut, slot, base, G, n_tiles, n_heads, final):
    qs, kvs, sts = refs[:n_q], refs[n_q:n_q + n_kv], refs[n_q + n_kv:n_q + n_kv + n_st]
    n_out = n_tiles + 1 if final else 1 + n_cut
    at = n_q + n_kv + n_st + n_old
    outs = refs[at:at + n_out]
    q_scr, kv_scr, o_scr, st_scr, s_scr, mb_scr, acc_scr, m_scr, l_scr, q_sem, kv_sem, o_sem, st_sem = refs[at + n_out:][:13]
    if n_cut:
        cut_ref, (cut_scr, cut_sem) = refs[at - 1], refs[-2:]
    T = RUN
    c = (HD ** -0.5) * LOG2E
    n_blocks = tab_ref[base]
    carried = base + 1
    row0 = carried + n_tiles
    null = len(kv_src)

    q_copies = [pltpu.make_async_copy(qs[a].at[i], q_scr.at[t], q_sem.at[t]) for t, (a, i) in enumerate(q_src)]
    kv_copies = [pltpu.make_async_copy(kvs[a].at[i], kv_scr.at[r], kv_sem.at[r]) for r, (a, i) in enumerate(kv_src)]
    first = 4
    q_copies[0].start()
    for cp in kv_copies[:first]:
        cp.start()
    for cp in q_copies[1:]:
        cp.start()
    for t, i in enumerate(st_src):
        if i is not None:
            @pl.when(tab_ref[carried + t] != 0)
            def _():
                pltpu.make_async_copy(sts[0].at[i], st_scr.at[t], st_sem.at[t]).start()
    for cp in kv_copies[first:]:
        cp.start()
    kv_scr[null, 1] = jnp.zeros((256, 256), BF)
    if n_cut:
        cut_in = pltpu.make_async_copy(cut_ref.at[pl.ds(lax.axis_index('cp') * cut_scr.shape[0], cut_scr.shape[0]), :], cut_scr,
                                       cut_sem)
        part = cut_scr.shape[0] // n_cut
        cut_out = [pltpu.make_async_copy(cut_scr.at[pl.ds(k * part, part), :], outs[1 + k], cut_sem) for k in range(n_cut)]
        cut_in.start()

    def block(i):
        g = lax.div(i, n_blocks)
        return row0 + BLK * (i - g * n_blocks), g

    def arrived(have, need):
        def one(r, carry):
            pltpu.make_async_copy(kv_scr.at[r], kv_scr.at[r], kv_sem.at[r]).wait()
            return carry

        lax.fori_loop(have, need, one, 0)
        return jnp.maximum(have, need)

    def put(s, h, k):
        s_scr[h, pl.ds(k * RUN, RUN), :] = s
        mb_scr[h, k] = jnp.max(s.reshape(RUN // 8, 8, T), axis=0)

    def stage_a(row, g, h):
        col = pl.multiple_of(g * HD, HD)
        qt = q_scr[tab_ref[row], pl.ds(pl.multiple_of((g * G + h) * HD, HD), HD), :]
        for k in range(4):
            put(lax.dot_general(kv_scr[tab_ref[row + 3 + k], 0, :, pl.ds(col, HD)], qt, DN, preferred_element_type=F32), h, k)

    def stage_b(row, g, h):
        col = pl.multiple_of(g * HD, HD)
        m_prev = m_scr[h]
        mb = jnp.maximum(jnp.maximum(mb_scr[h, 0], mb_scr[h, 1]), jnp.maximum(mb_scr[h, 2], mb_scr[h, 3]))
        for r in (4, 2, 1):
            mb = jnp.maximum(mb, pltpu.roll(mb, r, 0))
        m_new = jnp.maximum(m_prev, mb)
        m_scr[h] = m_new
        m_c = m_new * c
        alpha = jnp.exp2(m_prev * c - m_c)
        l, pv = l_scr[h] * alpha, None
        for k in range(4):
            run = tab_ref[row + 7 + k]
            p = jnp.exp2(s_scr[h, k * RUN:(k + 1) * RUN].reshape(RUN // 8, 8, T) * c - m_c[None])
            l = l + jnp.sum(p, axis=0) * jnp.where(run < 0, 0.0, 1.0)
            d = lax.dot_general(kv_scr[jnp.where(run < 0, null, run), 1, pl.ds(col, HD), :], p.reshape(RUN, T).astype(BF), DN,
                                preferred_element_type=F32)
            pv = d if pv is None else pv + d
        l_scr[h] = l
        acc_scr[h] = (acc_scr[h].reshape(HD // 8, 8, T) * alpha[None]).reshape(HD, T) + pv

    def mask_runs(flags):
        seen = lax.broadcasted_iota(jnp.int32, (RUN, T), 0) <= lax.broadcasted_iota(jnp.int32, (RUN, T), 1)

        def one(k, carry):
            @pl.when((lax.shift_right_logical(flags, k) & 1) != 0)
            def _():
                rows = pl.multiple_of(k * RUN, RUN)
                for h in range(G):
                    put(jnp.where(seen, s_scr[h, pl.ds(rows, RUN), :], NEG), h, k)

            return carry

        lax.fori_loop(0, 4, one, 0)

    def finish(tile, g, get):
        for h in range(G):
            acc, l = get(h)
            o_scr[tile, :, pl.ds(pl.multiple_of((g * G + h) * HD, HD), HD)] = (acc / jnp.sum(l, axis=0, keepdims=True)).T.astype(BF)

        @pl.when(g == n_heads - 1)
        def _():
            for k in range(n_tiles):
                @pl.when(tile == k)
                def _():
                    pltpu.make_async_copy(o_scr.at[k], outs[k].at[slot], o_sem.at[k]).start()

    if final and n_st:
        def idle(i, carry):
            tile, g = lax.div(i, n_heads), lax.rem(i, n_heads)

            @pl.when(tab_ref[carried + tile] == 2)
            def _():
                @pl.when(g == 0)
                def _():
                    pltpu.make_async_copy(q_scr.at[tile], q_scr.at[tile], q_sem.at[tile]).wait()
                    pltpu.make_async_copy(st_scr.at[tile], st_scr.at[tile], st_sem.at[tile]).wait()

                finish(tile, g, lambda h: (st_scr[tile, g, h, :HD, :], st_scr[tile, g, h, HD + 8:, :]))

            return carry

        lax.fori_loop(0, n_tiles * n_heads, idle, 0)

    def query(row):
        t = tab_ref[row]
        pltpu.make_async_copy(q_scr.at[t], q_scr.at[t], q_sem.at[t]).wait()

    row, g = block(0)
    query(row)
    have = arrived(0, tab_ref[row + 2])
    for h in range(G):
        stage_a(row, g, h)

    def body(i, have):
        row, g = block(i)
        nrow, ng = block(jnp.minimum(i + 1, n_heads * n_blocks - 1))
        have = arrived(have, tab_ref[nrow + 2])
        flags = tab_ref[row + 1]
        tile = tab_ref[row]

        @pl.when((i + 1 < n_blocks) & ((tab_ref[nrow + 1] & FIRST) != 0))
        def _():
            query(nrow)

        @pl.when((flags & (FIRST | CARRY)) == FIRST)
        def _():
            acc_scr[...] = jnp.zeros_like(acc_scr)
            l_scr[...] = jnp.zeros_like(l_scr)
            m_scr[...] = jnp.full_like(m_scr, NEG)

        if n_st:
            @pl.when((flags & (FIRST | CARRY)) == (FIRST | CARRY))
            def _():
                @pl.when(g == 0)
                def _():
                    pltpu.make_async_copy(st_scr.at[tile], st_scr.at[tile], st_sem.at[tile]).wait()

                for h in range(G):
                    acc_scr[h] = st_scr[tile, g, h, :HD, :]
                    m_scr[h] = st_scr[tile, g, h, HD:HD + 8, :]
                    l_scr[h] = st_scr[tile, g, h, HD + 8:, :]

        if n_cut:
            @pl.when(i == n_blocks)
            def _():
                cut_in.wait()
                for cp in cut_out:
                    cp.start()

        @pl.when((flags & 15) != 0)
        def _():
            mask_runs(flags)

        for h in range(G):
            stage_b(row, g, h)
            stage_a(nrow, ng, h)

        @pl.when((flags & LAST) != 0)
        def _():
            if final:
                finish(tile, g, lambda h: (acc_scr[h], l_scr[h]))
            else:
                for h in range(G):
                    st_scr[tile, g, h, :HD, :] = acc_scr[h]
                    st_scr[tile, g, h, HD:HD + 8, :] = m_scr[h]
                    st_scr[tile, g, h, HD + 8:, :] = l_scr[h]

                @pl.when(g == n_heads - 1)
                def _():
                    pltpu.make_async_copy(st_scr.at[tile], outs[0].at[tile], o_sem.at[tile]).start()

        return have

    have = lax.fori_loop(0, n_heads * n_blocks, body, have)
    arrived(have, len(kv_src))
    if final:
        for k in range(n_tiles):
            pltpu.make_async_copy(o_scr.at[k], outs[k].at[slot], o_sem.at[k]).wait()
    else:
        def wait_out(i, carry):
            row = row0 + BLK * i

            @pl.when((tab_ref[row + 1] & LAST) != 0)
            def _():
                t = tab_ref[row]
                pltpu.make_async_copy(st_scr.at[t], st_scr.at[t], o_sem.at[t]).wait()

            return carry

        lax.fori_loop(0, n_blocks, wait_out, 0)
        for cp in cut_out:
            cp.wait()


def flash(tab, qs, q_src, kvs, *, base, work, st=None, st_src=None, old=None, cut=None, n_cut=0, slots=1, after=()):
    nq = qs[0].shape[1]
    n_heads = 2
    G = nq // HD // n_heads
    n_tiles = len(q_src)
    final = cut is None
    kv_src = [(a, i) for a, kv in enumerate(kvs) for i in range(kv.shape[0])]
    n_runs = len(kv_src)
    sts = () if st is None else (st,)
    old = old or ()
    more = (*old, *(() if final else (cut,)))
    n_in = 1 + len(qs) + len(kvs) + len(sts) + len(more)
    state = (n_heads, G, ST, RUN)
    has_st = not final or sts
    if final:
        out_shape = [jax.ShapeDtypeStruct((slots, RUN, nq), BF)] * n_tiles + [jax.ShapeDtypeStruct((8, HD), F32)]
        scratch = []
    else:
        half = cut.shape[0] // 2
        out_shape = [jax.ShapeDtypeStruct((n_tiles, *state), F32)]
        out_shape += [jax.ShapeDtypeStruct((half // n_cut, cut.shape[1]), BF)] * n_cut
        scratch = [pltpu.VMEM((half, cut.shape[1]), BF), pltpu.SemaphoreType.DMA]
    return pl.pallas_call(
        ordered(functools.partial(flash_kernel, q_src=q_src, kv_src=kv_src, n_q=len(qs), n_kv=len(kvs),
                                  st_src=st_src or [None] * n_tiles, n_st=len(sts), n_old=len(more), n_cut=n_cut,
                                  slot=slots - 1 if old else 0, base=base, G=G, n_tiles=n_tiles, n_heads=n_heads, final=final),
                n_in, after),
        grid_spec=pltpu.PrefetchScalarGridSpec(
            num_scalar_prefetch=1, grid=(),
            in_specs=[ANY] * (n_in - 1 + len(after)),
            out_specs=[ANY] * len(out_shape),
            scratch_shapes=[pltpu.VMEM((n_tiles, nq, RUN), BF),
                            pltpu.VMEM((n_runs + 1, 2, 256, 256), BF),
                            pltpu.VMEM((n_tiles if final else 1, RUN, nq), BF),
                            pltpu.VMEM((n_tiles if has_st else 1, *state), F32),
                            pltpu.VMEM((G, 4 * RUN, RUN), F32),
                            pltpu.VMEM((G, 4, 8, RUN), F32),
                            pltpu.VMEM((G, HD, RUN), F32),
                            pltpu.VMEM((G, 8, RUN), F32),
                            pltpu.VMEM((G, 8, RUN), F32),
                            pltpu.SemaphoreType.DMA((n_tiles,)),
                            pltpu.SemaphoreType.DMA((n_runs,)),
                            pltpu.SemaphoreType.DMA((n_tiles,)),
                            pltpu.SemaphoreType.DMA((n_tiles,)), *scratch]),
        out_shape=out_shape,
        input_output_aliases={n_in - len(old) + k: k for k in range(len(old))},
        name="flash" if final else "flash_part", compiler_params=PARAMS,
        cost_estimate=cost(8 * work * RUN * RUN * nq, n_runs * RUN * nq),
    )(tab, *qs, *kvs, *sts, *more, *after)


def out_kernel(*refs, blocks, n_w, n_run, at):
    n_o, n_out = 4, 2 * n_run
    o_refs, w_refs, x_ref, g_ref = refs[:n_o], refs[n_o:n_o + n_w], refs[n_o + n_w], refs[n_o + n_w + 1]
    outs = refs[n_o + n_w + 2:n_o + n_w + 2 + n_out]
    o_scr, w_scr, x_scr, acc_scr, o_sem, w_sem, x_sem, out_sem = refs[n_o + n_w + 2 + n_out:]
    width = o_refs[0].shape[-1]
    half = width // 2
    n_slots = w_scr.shape[0]

    def fetch(k):
        for i, pieces in enumerate(blocks):
            @pl.when(k == i)
            def _():
                to = 0
                for a, r0, n in pieces:
                    pltpu.make_async_copy(w_refs[a].at[pl.ds(r0, n), :], w_scr.at[i % n_slots, pl.ds(to, n), :],
                                          w_sem.at[i % n_slots]).start()
                    to += n

    mine = lax.axis_index('cp')
    loads = [[] for _ in blocks]
    for i in range(n_run):
        rows = pl.ds(i * RUN, RUN)
        for k in range(4):
            src = o_refs[k].at[i]
            if k < 2:
                loads[2 * k].append((src, o_scr.at[rows, pl.ds(k * width, width)]))
            else:
                for p, part in enumerate((mine, 1 - mine)):
                    loads[2 * k + p].append((src.at[:, pl.ds(pl.multiple_of(part * half, half), half)],
                                             o_scr.at[rows, pl.ds(k * width + p * half, half)]))
    copies = [[pltpu.make_async_copy(src, dst, o_sem.at[k, i]) for i, (src, dst) in enumerate(ls)] for k, ls in enumerate(loads)]
    x_copy = pltpu.make_async_copy(x_ref.at[pl.ds(at * n_run * RUN, n_run * RUN), :], x_scr, x_sem)
    for cp in copies[0]:
        cp.start()
    for i in range(n_slots - 1):
        fetch(jnp.int32(i))
    for ls in copies[1:]:
        for cp in ls:
            cp.start()
    x_copy.start()
    acc_scr[...] = jnp.zeros_like(acc_scr)

    def one(k, carry):
        fetch(k + n_slots - 1)
        for i, ls in enumerate(copies):
            if ls:
                @pl.when(k == i)
                def _():
                    for cp in ls:
                        cp.wait()
        slot = lax.rem(k, n_slots)
        pltpu.make_async_copy(w_scr.at[slot], w_scr.at[slot], w_sem.at[slot]).wait()
        acc_scr[...] += jnp.dot(o_scr[:, pl.ds(pl.multiple_of(k * half, half), half)], w_scr[slot], preferred_element_type=F32)
        return carry

    lax.fori_loop(0, len(blocks), one, 0)
    x_copy.wait()

    def rows32(r, carry):
        rows = pl.ds(pl.multiple_of(r * 32, 32), 32)
        y = (x_scr[rows, :].astype(F32) + acc_scr[rows, :].astype(BF).astype(F32)).astype(BF)
        x_scr[rows, :] = y
        o_scr[rows, :] = norm_rows(y, g_ref[...])
        return carry

    stores, per = [], RUN // 32
    for i in range(n_run):
        lax.fori_loop(i * per, (i + 1) * per, rows32, 0)
        for k, scr in enumerate((x_scr, o_scr)):
            stores.append(pltpu.make_async_copy(scr.at[pl.ds(i * RUN, RUN), :], outs[2 * i + k], out_sem.at[2 * i + k]))
            stores[-1].start()
    for cp in stores:
        cp.wait()


def out_proj(os, ws, blocks, x_rows, gain, at, after=()):
    dim = x_rows.shape[1]
    n_run, _, width = os[0].shape
    rows = n_run * RUN
    return pl.pallas_call(
        ordered(functools.partial(out_kernel, blocks=blocks, n_w=len(ws), n_run=n_run, at=at),
                len(os) + len(ws) + 2, after),
        grid=(1,),
        in_specs=[ANY] * (len(os) + len(ws) + 1) + [pl.BlockSpec((1, dim), lambda i: (0, 0))] + [ANY] * len(after),
        out_specs=[ANY] * (2 * n_run),
        out_shape=[jax.ShapeDtypeStruct((RUN, dim), BF)] * (2 * n_run),
        scratch_shapes=[pltpu.VMEM((rows, 4 * width), BF), pltpu.VMEM((3, width // 2, dim), BF), pltpu.VMEM((rows, dim), BF),
                        pltpu.VMEM((rows, dim), F32), pltpu.SemaphoreType.DMA((len(blocks), 2 * n_run)),
                        pltpu.SemaphoreType.DMA((3,)), pltpu.SemaphoreType.DMA, pltpu.SemaphoreType.DMA((2 * n_run,))],
        name="outp", compiler_params=PARAMS,
        cost_estimate=cost(8 * rows * width * dim, 8 * width * dim),
    )(*os, *ws, x_rows, gain, *after)


def mlp_kernel(*refs, n_in, first, rb, tn, td, nk, nd):
    b_refs = refs[:n_in]
    wg_ref, wu_ref, wd_ref, keep_ref, send_ref, b_scr, u_scr, w_scr, d_scr, b_sem, w_sem, d_sem = refs[n_in:]
    i = pl.program_id(0)

    def fetch(j):
        @pl.when(j < nk)
        def _():
            slot, cols = lax.rem(j, 2), pl.ds(pl.multiple_of(j * tn, tn), tn)
            for k, w in enumerate((wg_ref, wu_ref)):
                pltpu.make_async_copy(w.at[:, cols], w_scr.at[slot, k], w_sem.at[slot]).start()

        @pl.when((j >= nk) & (j < nk + nd))
        def _():
            n, slot = j - nk, lax.rem(j - nk, 2)
            pltpu.make_async_copy(wd_ref.at[:, pl.ds(pl.multiple_of(n * td, td), td)], d_scr.at[slot], d_sem.at[slot]).start()

    def gated(rows, cols, slot):
        b = b_scr[rows, :]
        gate = jnp.dot(b, w_scr[slot, 0], preferred_element_type=F32)
        up = jnp.dot(b, w_scr[slot, 1], preferred_element_type=F32)
        u_scr[rows, cols] = (jax.nn.silu(gate) * up).astype(BF)

    @pl.when(i == 0)
    def _():
        copies = [pltpu.make_async_copy(r.at[pl.ds(first, rb), :], b_scr.at[pl.ds(k * rb, rb), :], b_sem.at[k])
                  for k, r in enumerate(b_refs)]
        copies[0].start()
        fetch(i)
        for cp in copies[1:]:
            cp.start()

    fetch(i + 1)

    @pl.when(i < nk)
    def _():
        pltpu.make_async_copy(w_scr.at[lax.rem(i, 2)], w_scr.at[lax.rem(i, 2)], w_sem.at[lax.rem(i, 2)]).wait()

    @pl.when(i == 0)
    def _():
        def one(k, carry):
            rows = pl.ds(pl.multiple_of(k * rb, rb), rb)
            pltpu.make_async_copy(b_scr.at[rows, :], b_scr.at[rows, :], b_sem.at[k]).wait()
            gated(rows, pl.ds(0, tn), 0)
            return carry

        lax.fori_loop(0, n_in, one, 0)

    @pl.when((i > 0) & (i < nk))
    def _():
        gated(slice(None), pl.ds(pl.multiple_of(i * tn, tn), tn), lax.rem(i, 2))

    @pl.when(i >= nk)
    def _():
        slot = lax.rem(i - nk, 2)
        pltpu.make_async_copy(d_scr.at[slot], d_scr.at[slot], d_sem.at[slot]).wait()
        d = jnp.dot(u_scr[...], d_scr[slot], preferred_element_type=F32).astype(BF)
        half = d.shape[0] // 2
        keep_ref[...] = d[:half]
        send_ref[...] = d[half:]


def mlp(bs, first, rb, wg, wu, wd, after=()):
    dim = bs[0].shape[1]
    rows = rb * len(bs)
    ffn = wg.shape[1]
    td = 512
    tn = td if rows <= td else td // 2
    nk, nd = ffn // tn, dim // td
    dn = lambda i: (0, jnp.maximum(i - nk, 0))
    return pl.pallas_call(
        ordered(functools.partial(mlp_kernel, n_in=len(bs), first=first, rb=rb, tn=tn, td=td, nk=nk, nd=nd), len(bs) + 3, after),
        grid=(nk + nd,),
        in_specs=[ANY] * (len(bs) + 3 + len(after)),
        out_specs=[pl.BlockSpec((rows // 2, td), dn)] * 2,
        out_shape=[jax.ShapeDtypeStruct((rows // 2, dim), BF)] * 2,
        scratch_shapes=[pltpu.VMEM((rows, dim), BF), pltpu.VMEM((rows, ffn), BF), pltpu.VMEM((2, 2, dim, tn), BF),
                        pltpu.VMEM((2, ffn, td), BF), pltpu.SemaphoreType.DMA((len(bs),)), pltpu.SemaphoreType.DMA((2,)),
                        pltpu.SemaphoreType.DMA((2,))],
        name="mlp", compiler_params=PARAMS,
        cost_estimate=cost(6 * rows * dim * ffn, 6 * dim * ffn),
    )(*bs, wg, wu, wd, *after)


def sum_kernel(*refs):
    p_ref, r_ref, t_ref, y_ref, z_ref = refs[-5:]
    total = p_ref[...].astype(F32) + r_ref[...].astype(F32) + t_ref[...].astype(F32)
    z_ref[...] = (y_ref[...].astype(F32) + total.astype(BF).astype(F32)).astype(BF)


def sum_rows(z, keep, recv, far, y, y_first, rows, first, total, after=(), tile=64):
    dim = y.shape[1]
    at = lambda r0: pl.BlockSpec((tile, dim), lambda i: (r0 // tile + i, 0))
    prev = () if z is None else (z,)
    return pl.pallas_call(
        ordered(sum_kernel, len(prev) + 4, after), grid=(rows // tile,),
        in_specs=[ANY] * len(prev) + [at(0)] * 3 + [at(y_first)] + [ANY] * len(after),
        out_specs=at(first),
        out_shape=jax.ShapeDtypeStruct((total, dim), BF),
        input_output_aliases={0: 0} if prev else {},
        name="zsum", compiler_params=PARAMS,
        cost_estimate=cost(rows * dim, 8 * rows * dim),
    )(*prev, keep, recv, far, y, *after)


def run_positions(xi, ci, y, cps, piece):
    def start(x, c):
        return (y if x == 0 else 2 * cps - 1 - y) * piece + c * (piece // 2)

    per = piece // 2 // RUN
    out = [start(xi, ci) + RUN * j for j in range(per)] + [start(xi, 1 - ci) + RUN * j for j in range(per)]
    for j in range(per):
        out += [start(1 - xi, ci) + RUN * j, start(1 - xi, 1 - ci) + RUN * j]
    return out


def block_list(tile, ids, diag):
    own = [] if diag is None else [diag]
    n_tail = (len(ids) + len(own)) % 4 or 4
    n_tail -= len(own)
    head, tail = ids[:len(ids) - n_tail], own + ids[len(ids) - n_tail:]
    blocks = [[0, head[i:i + 4], head[i:i + 4]] for i in range(0, len(head), 4)]
    fill = 4 - len(tail)
    keys = tail + [ids[-1] if ids else diag] * fill
    blocks.append([sum(1 << k for k, r in enumerate(keys) if r == diag), keys, tail + [-1] * fill])
    blocks[-1][0] |= LAST
    blocks[0][0] |= FIRST
    return [[tile, flags, 0] + keys + values for flags, keys, values in blocks]


def call_table(tiles, pairs, carry, idle):
    rows, most = [], 0
    carry = [c if pairs[t][0] or pairs[t][1] else idle for t, c in enumerate(carry)]
    for t, tile in enumerate(tiles):
        ids, own = pairs[t]
        if ids or own:
            mine = block_list(t, ids, tile if own else None)
            mine[0][1] |= CARRY if carry[t] else 0
            rows += mine
    for row in rows:
        most = max(most, max(row[3:7]) + 1)
        row[2] = most
    return [len(rows)] + carry + [v for row in rows for v in row], len(rows)


def work_tables(cps, piece):
    per = piece // 2 // RUN
    early, more = 2 * per + 2, 2 * per + 4
    stage = lambda r: 0 if r < early else 1
    soon_pair = lambda r, t: r < early and t < early or r < more and t in (0, 1, per, per + 1)
    calls = [(0, list(range(early)))]
    calls += [(1, [j, per + j, 2 * per + 2 * j, 2 * per + 2 * j + 1]) for j in range(per)]
    tabs, all_runs, sizes = [], [], []
    for y in range(cps):
        for xi in range(2):
            for ci in range(2):
                mine = run_positions(xi, ci, y, cps, piece)
                pos = mine + run_positions(xi, ci, 1 - y, cps, piece)
                all_runs.append(mine)
                tabs.append([])
                sizes.append([])
                for now, tiles in calls:
                    pairs, carry = [], []
                    for t in tiles:
                        seen = [r for r in range(len(pos)) if pos[r] < pos[t]]
                        when = {r: 0 if soon_pair(r, t) else 1 for r in seen}
                        late = list(when.values()).count(1) + stage(t)
                        soon = len(seen) + 1 - late
                        if late and soon % 4 <= -late % 4:
                            for r in [r for r in seen if not when[r]][:soon % 4]:
                                when[r] = 1
                        pairs.append(([r for r in seen if when[r] == now], stage(t) == now))
                        carry.append(int(stage(t) < now))
                    tab, n = call_table(tiles, pairs, carry, 2 if now == 1 else 0)
                    tabs[-1].append(tab)
                    sizes[-1].append(n)
    widths = [max(len(t[k]) for t in tabs) for k in range(len(calls))]
    flat = [[v for k, t in enumerate(tab) for v in t + [0] * (widths[k] - len(t))] for tab in tabs]
    bases = [sum(widths[:k]) for k in range(len(calls))]
    return np.array(flat, np.int32), np.array(all_runs, np.int32), bases, np.array(sizes).max(0) * 4


def solution(mesh):
    cps = mesh.shape['cp']
    row_spec = P('dp', ('cp', 'tp'), None)
    head_cols = P(None, 'tp', None)
    n_tp = mesh.shape['tp']

    over_core, over_x, over_both = (('tp', [(t, t ^ k) for t in range(n_tp)]) for k in (1, 2, 3))
    over_y = ('cp', [(i, i ^ 1) for i in range(cps)])

    def layer(x, g_attn, w_q, w_k, w_v, w_o, g_mlp, w_gate, w_up, w_down):
        x_rows = x[0]
        dim = x_rows.shape[1]
        n_run = x_rows.shape[0] // RUN
        piece = 2 * x_rows.shape[0]
        t_id, y_id = lax.axis_index('tp'), lax.axis_index('cp')
        np_tab, np_runs, bases, work = work_tables(cps, piece)
        dev = y_id * n_tp + t_id
        tab = lax.dynamic_index_in_dim(jnp.asarray(np_tab), dev, 0, keepdims=False)
        run_pos = lax.dynamic_index_in_dim(jnp.asarray(np_runs), dev, 0, keepdims=False)

        def tied(v, *others):
            return lax.optimization_barrier((v, *others))[0]

        def send(axis_pairs, v):
            return lax.ppermute(v, *axis_pairs)

        ga, gm = g_attn.reshape(1, dim), g_mlp.reshape(1, dim)
        own = []
        for j in range(n_run):
            own.append(norm_run(x_rows, ga, j, after=own[-1:]))
        far = [send(over_x, own[j]) for j in range(n_run)]
        mate = [send(over_core, own[j]) for j in range(n_run)]

        w_all = jnp.concatenate([tied(w, own[-1]).reshape(dim, -1) for w in (w_q, w_k, w_v)], axis=1)
        tables = rope_tables(tied(run_pos, own[-1])[:, None] + jnp.arange(RUN, dtype=jnp.int32)[None, :])

        q_here, kv_here = qkv(own + mate, w_all, (tables, 0))
        kvs, q_far = [kv_here], []

        def far_qkv(j, after):
            here = tied(far[j], after)
            rows = [here, send(over_core, here)], w_all, (tables, 2 * (n_run + j))
            if j + 1 < n_run:
                q, kv = qkv(*rows, after=(after,))
            else:
                kv, = qkv(*rows, False, after=(after,))
                q, = qkv(*rows, True, False, after=(kv, gm))
            q_far.append(q)
            kvs.append(kv)
            return kv

        far_qkv(1, far_qkv(0, kv_here))

        wo = w_o.reshape(-1, dim)
        half = wo.shape[0] // 2
        n_piece = 2
        rows = half // n_piece
        wo_c = send(over_core, tied(wo, kvs[-1]))

        tiles = [(0, i) for i in range(2 * n_run)] + [(1, 0), (1, 1)]
        st, *wo_x = flash(tab, [q_here, q_far[0]], tiles, kvs, base=bases[0], work=int(work[0]), cut=wo,
                         n_cut=n_piece)
        wo_x = [send(over_x, w) for w in wo_x]
        far_qkv(3, far_qkv(2, st))
        kvs = kvs + [send(over_y, kv) for kv in kvs]

        os, outs, prev = [], [], q_far[-1]
        wo_a, wo_ya, wo_yb = {}, {}, {}

        def forward_w(p):
            here = tied(wo_x[p], prev)
            wo_ya[p] = (here, send(over_core, here))
            wo_a[p] = send(over_y, here)

        def relay_w(p):
            here = tied(wo_a[p], prev)
            wo_yb[p] = (here, send(over_core, here))

        def attend(j):
            held = 2 * n_run + 2 * j
            carried = [j, n_run + j] + ([held, held + 1] if j == 0 else [None, None])
            pair = j % 2
            *o, done = flash(
                tab, [q_here, q_far[j]], [(0, j), (0, n_run + j), (1, 0), (1, 1)], kvs,
                base=bases[1 + j], work=int(work[1 + j]), st=st, st_src=carried, old=os.pop() if pair else None, slots=2,
                after=(prev,))
            if pair:
                o = [o[0], send(over_core, o[1]), send(over_x, o[2]), send(over_both, o[3])]
            os.append(o)
            return done

        def project(i):
            ws = [wo, wo_c]
            blocks = [[(0, 0, half)], [(0, half, half)], [(1, 0, half)], [(1, half, half)]]
            for k in range(2):
                for held in (wo_ya, wo_yb):
                    blocks.append([(len(ws) + p, 0, rows) for p in range(n_piece)])
                    ws += [held[p][k] for p in range(n_piece)]
            got = out_proj(os[i], ws, blocks, x_rows, gm, i, after=(prev,))
            for y, b in zip(got[::2], got[1::2]):
                outs.append((y, b, send(over_x, b), send(over_core, b)))
            return got[0]

        last = n_run - 1
        for j in range(last):
            prev = attend(j)
            if j < n_piece:
                forward_w(j)
            if j:
                relay_w(j - 1)
        prev = project(0)
        prev = attend(last)

        z, sums, relay = None, [], {}

        def relay_b(j):
            here = tied(outs[j][2], prev)
            relay[j] = (here, send(over_core, here))

        chunks = [(j, 0, RUN) for j in range(last)] + [(last, 0, RUN // 2), (last, RUN // 2, RUN // 2)]

        def finish(c):
            j, first, size = chunks[c]
            return sum_rows(z, *sums[c], outs[j][0], first, size, j * RUN + first, n_run * RUN,
                        after=() if prev is z else (prev,))

        relay_b(0)
        for c, (j, first, size) in enumerate(chunks):
            b = [outs[j][1], relay[j][0], outs[j][3], relay[j][1]]
            keep, out = mlp(b, first, size, w_gate, w_up, w_down, after=(prev,))
            recv = send(over_core, out)
            prev = keep
            if c < last:
                relay_b(c + 1)
            if c == 0:
                prev = project(1)
            elif c < n_run:
                prev = z = finish(c - 1)
            kept = keep if prev is keep else tied(keep, prev)
            prev = s_far = (kept[size:].astype(F32) + recv[size:].astype(F32)).astype(BF)
            sums.append((keep, recv, send(over_x, s_far)))
        for c in (last, n_run):
            prev = z = finish(c)
        return z[None]

    return jax.shard_map(layer, mesh=mesh,
                         in_specs=(row_spec, P(), head_cols, head_cols, head_cols, P('tp', None, None),
                                   P(), P(None, 'tp'), P(None, 'tp'), P('tp', None)),
                         out_specs=row_spec, check_vma=False)
```

```python
import functools
import math
import jax
import jax.numpy as jnp
import numpy as np
from jax import lax
from jax.experimental import pallas as pl
from jax.experimental.pallas import tpu as pltpu
from jax.sharding import PartitionSpec as P

NORM_EPS = 1e-5
ROPE_THETA = 500000.0
HD = 128
RUN = 256
NEG = -1e30
LOG2E = math.log2(math.e)
DN = (((1,), (0,)), ((), ()))
BF = jnp.bfloat16
F32 = jnp.float32
ANY = pl.BlockSpec(memory_space=pltpu.HBM)


PARAMS = pltpu.CompilerParams(vmem_limit_bytes=67043328)


def rope_tables(positions):
    half = HD // 2
    inv_freq = ROPE_THETA ** (-2.0 * jnp.arange(half, dtype=F32) / HD)
    angles = inv_freq[:, None] * positions.astype(F32)[..., None, :]
    return jnp.cos(angles), jnp.sin(angles)


def norm_rows(rows, gain):
    f = rows.astype(F32)
    mean_sq = jnp.mean(f * f, axis=-1, keepdims=True)
    return (f * lax.rsqrt(mean_sq + NORM_EPS) * gain.astype(F32)).astype(BF)


def cost(flops, moved):
    return pl.CostEstimate(flops=flops, transcendentals=0, bytes_accessed=moved)


def ordered(kernel, n_in, after):
    n = len(after)
    return lambda *refs: kernel(*refs[:n_in], *refs[n_in + n:])


def norm_kernel(x_ref, g_ref, *refs, per):
    for k, o_ref in enumerate(refs):
        @pl.when(lax.div(pl.program_id(0), per) == k)
        def _():
            o_ref[...] = norm_rows(x_ref[...], g_ref[...])


def norm_runs(x_rows, gain, runs, after=(), tile=128):
    dim = x_rows.shape[1]
    per = RUN // tile
    n = len(runs)
    return pl.pallas_call(
        ordered(functools.partial(norm_kernel, per=per), 2, after), grid=(n * per,),
        in_specs=[pl.BlockSpec((tile, dim), lambda i: (runs[0] * per + i, 0)), pl.BlockSpec((1, dim), lambda i: (0, 0))]
        + [ANY] * len(after),
        out_specs=[pl.BlockSpec((tile, dim), lambda i, k=k: (jnp.clip(i - k * per, 0, per - 1), 0)) for k in range(n)],
        out_shape=[jax.ShapeDtypeStruct((RUN, dim), BF)] * n,
        name="norm", compiler_params=PARAMS,
        cost_estimate=cost(n * RUN * dim, n * RUN * dim),
    )(x_rows, gain, *after)


def qkv_kernel(*refs, n_in, n_q, group, first, with_q, with_kv):
    a_refs = refs[:n_in]
    w_ref, cos_ref, sin_ref, *outs, a_scr, sem = refs[n_in:]
    q_ref, kv_ref = outs[0], outs[-1]
    n = pl.program_id(0) + first
    heads = w_ref.shape[1] // HD

    @pl.when(n == first)
    def _():
        for k, r in enumerate(a_refs):
            pltpu.make_async_copy(r, a_scr.at[pl.ds(k * RUN, RUN), :], sem.at[k]).start()

    def rope(f, i):
        f = f.astype(BF).astype(F32)
        lo, hi, cos, sin = f[:HD // 2], f[HD // 2:], cos_ref[i], sin_ref[i]
        return jnp.concatenate([lo * cos - hi * sin, hi * cos + lo * sin], axis=0)

    def one(k, carry):
        @pl.when(n == first)
        def _():
            for i in range(group):
                rows = pl.ds(pl.multiple_of((k * group + i) * RUN, RUN), RUN)
                pltpu.make_async_copy(a_scr.at[rows, :], a_scr.at[rows, :], sem.at[k * group + i]).wait()

        runs = [k * group + i for i in range(group)]

        def products():
            return [jnp.dot(a_scr[pl.ds(pl.multiple_of(run * RUN, RUN), RUN), :], w_ref[...], preferred_element_type=F32)
                    for run in runs]

        if with_q:
            @pl.when(n < n_q)
            def _():
                for run, r in zip(runs, products()):
                    for h in range(heads):
                        cols = slice(h * HD, (h + 1) * HD)
                        q_ref[run, cols, :] = rope(r[:, cols].T, run).astype(BF)

        if with_kv:
            @pl.when(n == n_q)
            def _():
                for run, r in zip(runs, products()):
                    for h in range(heads // 2):
                        cols, past = slice(h * HD, (h + 1) * HD), heads // 2 * HD
                        kv_ref[run, 0, :, cols] = rope(r[:, cols].T, run).T.astype(BF)
                        kv_ref[run, 1, cols, :] = r[:, past + h * HD:past + (h + 1) * HD].T.astype(BF)
        return carry

    lax.fori_loop(0, n_in // group, one, 0)


def qkv(rows, w_all, tables, with_q=True, with_kv=True, after=(), group=2):
    n_in = len(rows)
    dim = w_all.shape[0]
    tn = 512
    n_q = w_all.shape[1] // tn - 1
    (cos, sin), first_run = tables
    at = first_run // n_in
    start = 0 if with_q else n_q
    kv_shape = (n_in, 2, RUN, RUN)
    tab = pl.BlockSpec((n_in, HD // 2, RUN), lambda n: (at, 0, 0))
    return pl.pallas_call(
        ordered(functools.partial(qkv_kernel, n_in=n_in, n_q=n_q, group=group, first=start, with_q=with_q, with_kv=with_kv),
                n_in + 3, after),
        grid=(n_q * with_q + with_kv,),
        in_specs=[ANY] * n_in + [pl.BlockSpec((dim, tn), lambda n: (0, n + start)), tab, tab] + [ANY] * len(after),
        out_specs=[pl.BlockSpec((n_in, tn, RUN), lambda n: (0, jnp.minimum(n, n_q - 1), 0))] * with_q
        + [pl.BlockSpec(kv_shape, lambda n: (0,) * len(kv_shape))] * with_kv,
        out_shape=[jax.ShapeDtypeStruct((n_in, n_q * tn, RUN), BF)] * with_q + [jax.ShapeDtypeStruct(kv_shape, BF)] * with_kv,
        scratch_shapes=[pltpu.VMEM((n_in * RUN, dim), BF), pltpu.SemaphoreType.DMA((n_in,))],
        name="qkv", compiler_params=PARAMS,
        cost_estimate=cost(2 * n_in * RUN * w_all.size, 2 * w_all.size),
    )(*rows, w_all, cos, sin, *after)


BLK = 11
LAST, FIRST, CARRY = 16, 32, 64
ST = HD + 16


def flash_kernel(tab_ref, *refs, q_src, kv_src, n_q, n_kv, st_src, n_st, n_old, n_cut, slot, base, G, n_tiles, n_heads, final):
    qs, kvs, sts = refs[:n_q], refs[n_q:n_q + n_kv], refs[n_q + n_kv:n_q + n_kv + n_st]
    n_out = n_tiles + 1 if final else 1 + n_cut
    at = n_q + n_kv + n_st + n_old
    outs = refs[at:at + n_out]
    q_scr, kv_scr, o_scr, st_scr, s_scr, mb_scr, acc_scr, m_scr, l_scr, q_sem, kv_sem, o_sem, st_sem = refs[at + n_out:][:13]
    if n_cut:
        cut_ref, (cut_scr, cut_sem) = refs[at - 1], refs[-2:]
    T = RUN
    c = (HD ** -0.5) * LOG2E
    n_blocks = tab_ref[base]
    carried = base + 1
    row0 = carried + n_tiles
    null = len(kv_src)

    q_copies = [pltpu.make_async_copy(qs[a].at[i], q_scr.at[t], q_sem.at[t]) for t, (a, i) in enumerate(q_src)]
    kv_copies = [pltpu.make_async_copy(kvs[a].at[i], kv_scr.at[r], kv_sem.at[r]) for r, (a, i) in enumerate(kv_src)]

    def load_state(t):
        if st_src[t] is not None:
            @pl.when(tab_ref[carried + t] != 0)
            def _():
                pltpu.make_async_copy(sts[0].at[st_src[t]], st_scr.at[t], st_sem.at[t]).start()

    q_copies[0].start()
    for cp in kv_copies[:4]:
        cp.start()
    load_state(0)
    for cp in kv_copies[4:]:
        cp.start()
    for t in range(1, n_tiles):
        q_copies[t].start()
        load_state(t)
    kv_scr[null, 1] = jnp.zeros((256, 256), BF)
    if n_cut:
        cut_in = pltpu.make_async_copy(cut_ref.at[pl.ds(lax.axis_index('cp') * cut_scr.shape[0], cut_scr.shape[0]), :], cut_scr,
                                       cut_sem)
        part = cut_scr.shape[0] // n_cut
        cut_out = [pltpu.make_async_copy(cut_scr.at[pl.ds(k * part, part), :], outs[1 + k], cut_sem) for k in range(n_cut)]
        cut_in.start()

    def block(i):
        g = lax.div(i, n_blocks)
        return row0 + BLK * (i - g * n_blocks), g

    def arrived(have, need):
        def one(r, carry):
            pltpu.make_async_copy(kv_scr.at[r], kv_scr.at[r], kv_sem.at[r]).wait()
            return carry

        lax.fori_loop(have, need, one, 0)
        return jnp.maximum(have, need)

    def put(s, h, k):
        s_scr[h, pl.ds(k * RUN, RUN), :] = s
        mb_scr[h, k] = jnp.max(s.reshape(RUN // 8, 8, T), axis=0)

    def stage_a(row, g, h):
        col = pl.multiple_of(g * HD, HD)
        qt = q_scr[tab_ref[row], pl.ds(pl.multiple_of((g * G + h) * HD, HD), HD), :]
        for k in range(4):
            put(lax.dot_general(kv_scr[tab_ref[row + 3 + k], 0, :, pl.ds(col, HD)], qt, DN, preferred_element_type=F32), h, k)

    def stage_b(row, g, h):
        col = pl.multiple_of(g * HD, HD)
        m_prev = m_scr[h]
        mb = jnp.maximum(jnp.maximum(mb_scr[h, 0], mb_scr[h, 1]), jnp.maximum(mb_scr[h, 2], mb_scr[h, 3]))
        for r in (4, 2, 1):
            mb = jnp.maximum(mb, pltpu.roll(mb, r, 0))
        m_new = jnp.maximum(m_prev, mb)
        m_scr[h] = m_new
        m_c = m_new * c
        alpha = jnp.exp2(m_prev * c - m_c)
        l, pv = l_scr[h] * alpha, None
        for k in range(4):
            run = tab_ref[row + 7 + k]
            p = jnp.exp2(s_scr[h, k * RUN:(k + 1) * RUN].reshape(RUN // 8, 8, T) * c - m_c[None])
            l = l + jnp.sum(p, axis=0) * jnp.where(run < 0, 0.0, 1.0)
            d = lax.dot_general(kv_scr[jnp.where(run < 0, null, run), 1, pl.ds(col, HD), :], p.reshape(RUN, T).astype(BF), DN,
                                preferred_element_type=F32)
            pv = d if pv is None else pv + d
        l_scr[h] = l
        acc_scr[h] = (acc_scr[h].reshape(HD // 8, 8, T) * alpha[None]).reshape(HD, T) + pv

    def mask_runs(flags):
        seen = lax.broadcasted_iota(jnp.int32, (RUN, T), 0) <= lax.broadcasted_iota(jnp.int32, (RUN, T), 1)

        def one(k, carry):
            @pl.when((lax.shift_right_logical(flags, k) & 1) != 0)
            def _():
                rows = pl.multiple_of(k * RUN, RUN)
                for h in range(G):
                    put(jnp.where(seen, s_scr[h, pl.ds(rows, RUN), :], NEG), h, k)

            return carry

        lax.fori_loop(0, 4, one, 0)

    def finish(tile, g, get):
        for h in range(G):
            acc, l = get(h)
            o_scr[tile, :, pl.ds(pl.multiple_of((g * G + h) * HD, HD), HD)] = (acc / jnp.sum(l, axis=0, keepdims=True)).T.astype(BF)

        @pl.when(g == n_heads - 1)
        def _():
            for k in range(n_tiles):
                @pl.when(tile == k)
                def _():
                    pltpu.make_async_copy(o_scr.at[k], outs[k].at[slot], o_sem.at[k]).start()

    if final and n_st:
        def idle(i, carry):
            tile, g = lax.div(i, n_heads), lax.rem(i, n_heads)

            @pl.when(tab_ref[carried + tile] == 2)
            def _():
                @pl.when(g == 0)
                def _():
                    pltpu.make_async_copy(q_scr.at[tile], q_scr.at[tile], q_sem.at[tile]).wait()
                    pltpu.make_async_copy(st_scr.at[tile], st_scr.at[tile], st_sem.at[tile]).wait()

                finish(tile, g, lambda h: (st_scr[tile, g, h, :HD, :], st_scr[tile, g, h, HD + 8:, :]))

            return carry

        lax.fori_loop(0, n_tiles * n_heads, idle, 0)

    def query(row):
        t = tab_ref[row]
        pltpu.make_async_copy(q_scr.at[t], q_scr.at[t], q_sem.at[t]).wait()

    row, g = block(0)
    query(row)
    have = arrived(0, tab_ref[row + 2])
    for h in range(G):
        stage_a(row, g, h)

    def body(i, have):
        row, g = block(i)
        nrow, ng = block(jnp.minimum(i + 1, n_heads * n_blocks - 1))
        have = arrived(have, tab_ref[nrow + 2])
        flags = tab_ref[row + 1]
        tile = tab_ref[row]

        @pl.when((i + 1 < n_blocks) & ((tab_ref[nrow + 1] & FIRST) != 0))
        def _():
            query(nrow)

        @pl.when((flags & (FIRST | CARRY)) == FIRST)
        def _():
            acc_scr[...] = jnp.zeros_like(acc_scr)
            l_scr[...] = jnp.zeros_like(l_scr)
            m_scr[...] = jnp.full_like(m_scr, NEG)

        if n_st:
            @pl.when((flags & (FIRST | CARRY)) == (FIRST | CARRY))
            def _():
                @pl.when(g == 0)
                def _():
                    pltpu.make_async_copy(st_scr.at[tile], st_scr.at[tile], st_sem.at[tile]).wait()

                for h in range(G):
                    acc_scr[h] = st_scr[tile, g, h, :HD, :]
                    m_scr[h] = st_scr[tile, g, h, HD:HD + 8, :]
                    l_scr[h] = st_scr[tile, g, h, HD + 8:, :]

        if n_cut:
            @pl.when(i == n_blocks)
            def _():
                cut_in.wait()
                for cp in cut_out:
                    cp.start()

        @pl.when((flags & 15) != 0)
        def _():
            mask_runs(flags)

        for h in range(G):
            stage_b(row, g, h)
            stage_a(nrow, ng, h)

        @pl.when((flags & LAST) != 0)
        def _():
            if final:
                finish(tile, g, lambda h: (acc_scr[h], l_scr[h]))
            else:
                for h in range(G):
                    st_scr[tile, g, h, :HD, :] = acc_scr[h]
                    st_scr[tile, g, h, HD:HD + 8, :] = m_scr[h]
                    st_scr[tile, g, h, HD + 8:, :] = l_scr[h]

                @pl.when(g == n_heads - 1)
                def _():
                    pltpu.make_async_copy(st_scr.at[tile], outs[0].at[tile], o_sem.at[tile]).start()

        return have

    have = lax.fori_loop(0, n_heads * n_blocks, body, have)
    arrived(have, len(kv_src))
    if final:
        for k in range(n_tiles):
            pltpu.make_async_copy(o_scr.at[k], outs[k].at[slot], o_sem.at[k]).wait()
    else:
        def wait_out(i, carry):
            row = row0 + BLK * i

            @pl.when((tab_ref[row + 1] & LAST) != 0)
            def _():
                t = tab_ref[row]
                pltpu.make_async_copy(st_scr.at[t], st_scr.at[t], o_sem.at[t]).wait()

            return carry

        lax.fori_loop(0, n_blocks, wait_out, 0)
        for cp in cut_out:
            cp.wait()


def flash(tab, qs, q_src, kvs, *, base, work, st=None, st_src=None, old=None, cut=None, n_cut=0, slots=1, after=()):
    nq = qs[0].shape[1]
    n_heads = 2
    G = nq // HD // n_heads
    n_tiles = len(q_src)
    final = cut is None
    kv_src = [(a, i) for a, kv in enumerate(kvs) for i in range(kv.shape[0])]
    n_runs = len(kv_src)
    sts = () if st is None else (st,)
    old = old or ()
    more = (*old, *(() if final else (cut,)))
    n_in = 1 + len(qs) + len(kvs) + len(sts) + len(more)
    state = (n_heads, G, ST, RUN)
    has_st = not final or sts
    if final:
        out_shape = [jax.ShapeDtypeStruct((slots, RUN, nq), BF)] * n_tiles + [jax.ShapeDtypeStruct((8, HD), F32)]
        scratch = []
    else:
        half = cut.shape[0] // 2
        out_shape = [jax.ShapeDtypeStruct((n_tiles, *state), F32)]
        out_shape += [jax.ShapeDtypeStruct((half // n_cut, cut.shape[1]), BF)] * n_cut
        scratch = [pltpu.VMEM((half, cut.shape[1]), BF), pltpu.SemaphoreType.DMA]
    return pl.pallas_call(
        ordered(functools.partial(flash_kernel, q_src=q_src, kv_src=kv_src, n_q=len(qs), n_kv=len(kvs),
                                  st_src=st_src or [None] * n_tiles, n_st=len(sts), n_old=len(more), n_cut=n_cut,
                                  slot=slots - 1 if old else 0, base=base, G=G, n_tiles=n_tiles, n_heads=n_heads, final=final),
                n_in, after),
        grid_spec=pltpu.PrefetchScalarGridSpec(
            num_scalar_prefetch=1, grid=(),
            in_specs=[ANY] * (n_in - 1 + len(after)),
            out_specs=[ANY] * len(out_shape),
            scratch_shapes=[pltpu.VMEM((n_tiles, nq, RUN), BF),
                            pltpu.VMEM((n_runs + 1, 2, 256, 256), BF),
                            pltpu.VMEM((n_tiles if final else 1, RUN, nq), BF),
                            pltpu.VMEM((n_tiles if has_st else 1, *state), F32),
                            pltpu.VMEM((G, 4 * RUN, RUN), F32),
                            pltpu.VMEM((G, 4, 8, RUN), F32),
                            pltpu.VMEM((G, HD, RUN), F32),
                            pltpu.VMEM((G, 8, RUN), F32),
                            pltpu.VMEM((G, 8, RUN), F32),
                            pltpu.SemaphoreType.DMA((n_tiles,)),
                            pltpu.SemaphoreType.DMA((n_runs,)),
                            pltpu.SemaphoreType.DMA((n_tiles,)),
                            pltpu.SemaphoreType.DMA((n_tiles,)), *scratch]),
        out_shape=out_shape,
        input_output_aliases={n_in - len(old) + k: k for k in range(len(old))},
        name="flash" if final else "flash_part", compiler_params=PARAMS,
        cost_estimate=cost(8 * work * RUN * RUN * nq, n_runs * RUN * nq),
    )(tab, *qs, *kvs, *sts, *more, *after)


def out_kernel(*refs, blocks, n_w, n_run, at):
    n_o, n_out = 4, 2 * n_run
    o_refs, w_refs, x_ref, g_ref = refs[:n_o], refs[n_o:n_o + n_w], refs[n_o + n_w], refs[n_o + n_w + 1]
    outs = refs[n_o + n_w + 2:n_o + n_w + 2 + n_out]
    o_scr, w_scr, x_scr, acc_scr, o_sem, w_sem, x_sem, out_sem = refs[n_o + n_w + 2 + n_out:]
    width = o_refs[0].shape[-1]
    half = width // 2
    n_slots = w_scr.shape[0]

    def fetch(k):
        for i, pieces in enumerate(blocks):
            @pl.when(k == i)
            def _():
                to = 0
                for a, r0, n in pieces:
                    pltpu.make_async_copy(w_refs[a].at[pl.ds(r0, n), :], w_scr.at[i % n_slots, pl.ds(to, n), :],
                                          w_sem.at[i % n_slots]).start()
                    to += n

    mine = lax.axis_index('cp')
    loads = [[] for _ in blocks]
    for i in range(n_run):
        rows = pl.ds(i * RUN, RUN)
        for k in range(4):
            src = o_refs[k].at[i]
            if k < 2:
                loads[2 * k].append((src, o_scr.at[rows, pl.ds(k * width, width)]))
            else:
                for p, part in enumerate((mine, 1 - mine)):
                    loads[2 * k + p].append((src.at[:, pl.ds(pl.multiple_of(part * half, half), half)],
                                             o_scr.at[rows, pl.ds(k * width + p * half, half)]))
    copies = [[pltpu.make_async_copy(src, dst, o_sem.at[k, i]) for i, (src, dst) in enumerate(ls)] for k, ls in enumerate(loads)]
    x_copy = pltpu.make_async_copy(x_ref.at[pl.ds(at * n_run * RUN, n_run * RUN), :], x_scr, x_sem)
    for cp in copies[0]:
        cp.start()
    for i in range(n_slots - 1):
        fetch(jnp.int32(i))
    for ls in copies[1:]:
        for cp in ls:
            cp.start()
    x_copy.start()
    acc_scr[...] = jnp.zeros_like(acc_scr)

    def one(k, carry):
        fetch(k + n_slots - 1)
        for i, ls in enumerate(copies):
            if ls:
                @pl.when(k == i)
                def _():
                    for cp in ls:
                        cp.wait()
        slot = lax.rem(k, n_slots)
        pltpu.make_async_copy(w_scr.at[slot], w_scr.at[slot], w_sem.at[slot]).wait()
        acc_scr[...] += jnp.dot(o_scr[:, pl.ds(pl.multiple_of(k * half, half), half)], w_scr[slot], preferred_element_type=F32)
        return carry

    lax.fori_loop(0, len(blocks), one, 0)
    x_copy.wait()

    def rows32(r, carry):
        rows = pl.ds(pl.multiple_of(r * 32, 32), 32)
        y = (x_scr[rows, :].astype(F32) + acc_scr[rows, :].astype(BF).astype(F32)).astype(BF)
        x_scr[rows, :] = y
        o_scr[rows, :] = norm_rows(y, g_ref[...])
        return carry

    stores, per = [], RUN // 32
    for i in range(n_run):
        lax.fori_loop(i * per, (i + 1) * per, rows32, 0)
        for k, scr in enumerate((x_scr, o_scr)):
            stores.append(pltpu.make_async_copy(scr.at[pl.ds(i * RUN, RUN), :], outs[2 * i + k], out_sem.at[2 * i + k]))
            stores[-1].start()
    for cp in stores:
        cp.wait()


def out_proj(os, ws, blocks, x_rows, gain, at, after=()):
    dim = x_rows.shape[1]
    n_run, _, width = os[0].shape
    rows = n_run * RUN
    return pl.pallas_call(
        ordered(functools.partial(out_kernel, blocks=blocks, n_w=len(ws), n_run=n_run, at=at),
                len(os) + len(ws) + 2, after),
        grid=(1,),
        in_specs=[ANY] * (len(os) + len(ws) + 1) + [pl.BlockSpec((1, dim), lambda i: (0, 0))] + [ANY] * len(after),
        out_specs=[ANY] * (2 * n_run),
        out_shape=[jax.ShapeDtypeStruct((RUN, dim), BF)] * (2 * n_run),
        scratch_shapes=[pltpu.VMEM((rows, 4 * width), BF), pltpu.VMEM((3, width // 2, dim), BF), pltpu.VMEM((rows, dim), BF),
                        pltpu.VMEM((rows, dim), F32), pltpu.SemaphoreType.DMA((len(blocks), 2 * n_run)),
                        pltpu.SemaphoreType.DMA((3,)), pltpu.SemaphoreType.DMA, pltpu.SemaphoreType.DMA((2 * n_run,))],
        name="outp", compiler_params=PARAMS,
        cost_estimate=cost(8 * rows * width * dim, 8 * width * dim),
    )(*os, *ws, x_rows, gain, *after)


def mlp_kernel(*refs, n_in, first, rb, tn, td, nk, nd):
    b_refs = refs[:n_in]
    wg_ref, wu_ref, wd_ref, keep_ref, send_ref, b_scr, u_scr, w_scr, d_scr, b_sem, w_sem, d_sem = refs[n_in:]
    i = pl.program_id(0)

    def fetch(j):
        @pl.when(j < nk)
        def _():
            slot, cols = lax.rem(j, 2), pl.ds(pl.multiple_of(j * tn, tn), tn)
            for k, w in enumerate((wg_ref, wu_ref)):
                pltpu.make_async_copy(w.at[:, cols], w_scr.at[slot, k], w_sem.at[slot]).start()

        @pl.when((j >= nk) & (j < nk + nd))
        def _():
            n, slot = j - nk, lax.rem(j - nk, 2)
            pltpu.make_async_copy(wd_ref.at[:, pl.ds(pl.multiple_of(n * td, td), td)], d_scr.at[slot], d_sem.at[slot]).start()

    def gated(rows, cols, slot):
        b = b_scr[rows, :]
        gate = jnp.dot(b, w_scr[slot, 0], preferred_element_type=F32)
        up = jnp.dot(b, w_scr[slot, 1], preferred_element_type=F32)
        u_scr[rows, cols] = (jax.nn.silu(gate) * up).astype(BF)

    @pl.when(i == 0)
    def _():
        copies = [pltpu.make_async_copy(r.at[pl.ds(first, rb), :], b_scr.at[pl.ds(k * rb, rb), :], b_sem.at[k])
                  for k, r in enumerate(b_refs)]
        copies[0].start()
        fetch(i)
        for cp in copies[1:]:
            cp.start()

    fetch(i + 1)

    @pl.when(i < nk)
    def _():
        pltpu.make_async_copy(w_scr.at[lax.rem(i, 2)], w_scr.at[lax.rem(i, 2)], w_sem.at[lax.rem(i, 2)]).wait()

    @pl.when(i == 0)
    def _():
        def one(k, carry):
            rows = pl.ds(pl.multiple_of(k * rb, rb), rb)
            pltpu.make_async_copy(b_scr.at[rows, :], b_scr.at[rows, :], b_sem.at[k]).wait()
            gated(rows, pl.ds(0, tn), 0)
            return carry

        lax.fori_loop(0, n_in, one, 0)

    @pl.when((i > 0) & (i < nk))
    def _():
        gated(slice(None), pl.ds(pl.multiple_of(i * tn, tn), tn), lax.rem(i, 2))

    @pl.when(i >= nk)
    def _():
        slot = lax.rem(i - nk, 2)
        pltpu.make_async_copy(d_scr.at[slot], d_scr.at[slot], d_sem.at[slot]).wait()
        d = jnp.dot(u_scr[...], d_scr[slot], preferred_element_type=F32).astype(BF)
        half = d.shape[0] // 2
        keep_ref[...] = d[:half]
        send_ref[...] = d[half:]


def mlp(bs, first, rb, wg, wu, wd, after=()):
    dim = bs[0].shape[1]
    rows = rb * len(bs)
    ffn = wg.shape[1]
    td = 512
    tn = td if rows <= td else td // 2
    nk, nd = ffn // tn, dim // td
    dn = lambda i: (0, jnp.maximum(i - nk, 0))
    return pl.pallas_call(
        ordered(functools.partial(mlp_kernel, n_in=len(bs), first=first, rb=rb, tn=tn, td=td, nk=nk, nd=nd), len(bs) + 3, after),
        grid=(nk + nd,),
        in_specs=[ANY] * (len(bs) + 3 + len(after)),
        out_specs=[pl.BlockSpec((rows // 2, td), dn)] * 2,
        out_shape=[jax.ShapeDtypeStruct((rows // 2, dim), BF)] * 2,
        scratch_shapes=[pltpu.VMEM((rows, dim), BF), pltpu.VMEM((rows, ffn), BF), pltpu.VMEM((2, 2, dim, tn), BF),
                        pltpu.VMEM((2, ffn, td), BF), pltpu.SemaphoreType.DMA((len(bs),)), pltpu.SemaphoreType.DMA((2,)),
                        pltpu.SemaphoreType.DMA((2,))],
        name="mlp", compiler_params=PARAMS,
        cost_estimate=cost(6 * rows * dim * ffn, 6 * dim * ffn),
    )(*bs, wg, wu, wd, *after)


def sum_kernel(*refs):
    p_ref, r_ref, t_ref, y_ref, z_ref = refs[-5:]
    total = p_ref[...].astype(F32) + r_ref[...].astype(F32) + t_ref[...].astype(F32)
    z_ref[...] = (y_ref[...].astype(F32) + total.astype(BF).astype(F32)).astype(BF)


def sum_rows(z, keep, recv, far, y, y_first, rows, first, total, after=(), tile=64):
    dim = y.shape[1]
    at = lambda r0: pl.BlockSpec((tile, dim), lambda i: (r0 // tile + i, 0))
    prev = () if z is None else (z,)
    return pl.pallas_call(
        ordered(sum_kernel, len(prev) + 4, after), grid=(rows // tile,),
        in_specs=[ANY] * len(prev) + [at(0)] * 3 + [at(y_first)] + [ANY] * len(after),
        out_specs=at(first),
        out_shape=jax.ShapeDtypeStruct((total, dim), BF),
        input_output_aliases={0: 0} if prev else {},
        name="zsum", compiler_params=PARAMS,
        cost_estimate=cost(rows * dim, 8 * rows * dim),
    )(*prev, keep, recv, far, y, *after)


def run_positions(xi, ci, y, cps, piece):
    def start(x, c):
        return (y if x == 0 else 2 * cps - 1 - y) * piece + c * (piece // 2)

    per = piece // 2 // RUN
    out = [start(xi, ci) + RUN * j for j in range(per)] + [start(xi, 1 - ci) + RUN * j for j in range(per)]
    for j in range(per):
        out += [start(1 - xi, ci) + RUN * j, start(1 - xi, 1 - ci) + RUN * j]
    return out


def block_list(tile, ids, diag):
    own = [] if diag is None else [diag]
    n_tail = (len(ids) + len(own)) % 4 or 4
    n_tail -= len(own)
    head, tail = ids[:len(ids) - n_tail], own + ids[len(ids) - n_tail:]
    blocks = [[0, head[i:i + 4], head[i:i + 4]] for i in range(0, len(head), 4)]
    fill = 4 - len(tail)
    keys = tail + [ids[-1] if ids else diag] * fill
    blocks.append([sum(1 << k for k, r in enumerate(keys) if r == diag), keys, tail + [-1] * fill])
    blocks[-1][0] |= LAST
    blocks[0][0] |= FIRST
    return [[tile, flags, 0] + keys + values for flags, keys, values in blocks]


def call_table(tiles, pairs, carry, idle):
    rows, most = [], 0
    carry = [c if pairs[t][0] or pairs[t][1] else idle for t, c in enumerate(carry)]
    for t, tile in enumerate(tiles):
        ids, own = pairs[t]
        if ids or own:
            mine = block_list(t, ids, tile if own else None)
            mine[0][1] |= CARRY if carry[t] else 0
            rows += mine
    for row in rows:
        most = max(most, max(row[3:7]) + 1)
        row[2] = most
    return [len(rows)] + carry + [v for row in rows for v in row], len(rows)


def work_tables(cps, piece):
    per = piece // 2 // RUN
    early, more = 2 * per + 2, 2 * per + 4
    stage = lambda r: 0 if r < early else 1
    soon_pair = lambda r, t: r < early and t < early or r < more and t in (0, 1, per, per + 1)
    calls = [(0, list(range(early)))]
    calls += [(1, [j, per + j, 2 * per + 2 * j, 2 * per + 2 * j + 1]) for j in range(per)]
    tabs, all_runs, sizes = [], [], []
    for y in range(cps):
        for xi in range(2):
            for ci in range(2):
                mine = run_positions(xi, ci, y, cps, piece)
                pos = mine + run_positions(xi, ci, 1 - y, cps, piece)
                all_runs.append(mine)
                tabs.append([])
                sizes.append([])
                for now, tiles in calls:
                    pairs, carry = [], []
                    for t in tiles:
                        seen = [r for r in range(len(pos)) if pos[r] < pos[t]]
                        when = {r: 0 if soon_pair(r, t) else 1 for r in seen}
                        late = list(when.values()).count(1) + stage(t)
                        soon = len(seen) + 1 - late
                        if late and soon % 4 <= -late % 4:
                            for r in [r for r in seen if not when[r]][:soon % 4]:
                                when[r] = 1
                        pairs.append(([r for r in seen if when[r] == now], stage(t) == now))
                        carry.append(int(stage(t) < now))
                    tab, n = call_table(tiles, pairs, carry, 2 if now == 1 else 0)
                    tabs[-1].append(tab)
                    sizes[-1].append(n)
    widths = [max(len(t[k]) for t in tabs) for k in range(len(calls))]
    flat = [[v for k, t in enumerate(tab) for v in t + [0] * (widths[k] - len(t))] for tab in tabs]
    bases = [sum(widths[:k]) for k in range(len(calls))]
    return np.array(flat, np.int32), np.array(all_runs, np.int32), bases, np.array(sizes).max(0) * 4


def solution(mesh):
    cps = mesh.shape['cp']
    row_spec = P('dp', ('cp', 'tp'), None)
    head_cols = P(None, 'tp', None)
    n_tp = mesh.shape['tp']

    over_core, over_x, over_both = (('tp', [(t, t ^ k) for t in range(n_tp)]) for k in (1, 2, 3))
    over_y = ('cp', [(i, i ^ 1) for i in range(cps)])

    def layer(x, g_attn, w_q, w_k, w_v, w_o, g_mlp, w_gate, w_up, w_down):
        x_rows = x[0]
        dim = x_rows.shape[1]
        n_run = x_rows.shape[0] // RUN
        piece = 2 * x_rows.shape[0]
        t_id, y_id = lax.axis_index('tp'), lax.axis_index('cp')
        np_tab, np_runs, bases, work = work_tables(cps, piece)
        dev = y_id * n_tp + t_id
        tab = lax.dynamic_index_in_dim(jnp.asarray(np_tab), dev, 0, keepdims=False)
        run_pos = lax.dynamic_index_in_dim(jnp.asarray(np_runs), dev, 0, keepdims=False)

        def tied(v, *others):
            return lax.optimization_barrier((v, *others))[0]

        def send(axis_pairs, v):
            return lax.ppermute(v, *axis_pairs)

        ga, gm = g_attn.reshape(1, dim), g_mlp.reshape(1, dim)
        own = list(norm_runs(x_rows, ga, [0]))
        own += norm_runs(x_rows, ga, list(range(1, n_run)), after=own)
        far = [send(over_x, own[j]) for j in range(n_run)]
        mate = [send(over_core, own[j]) for j in range(n_run)]

        w_all = jnp.concatenate([tied(w, own[-1]).reshape(dim, -1) for w in (w_q, w_k, w_v)], axis=1)
        row_pos = run_pos[:, None] + jnp.arange(RUN, dtype=jnp.int32)[None, :]
        tables = rope_tables(tied(row_pos[:2 * n_run], own[-1]))

        q_here, kv_here = qkv(own + mate, w_all, (tables, 0))
        kvs, q_far = [kv_here], []
        far_tables = rope_tables(tied(row_pos[2 * n_run:], kv_here))

        def far_qkv(j, after):
            here = tied(far[j], after)
            rows = [here, send(over_core, here)], w_all, (far_tables, 2 * j)
            if j + 1 < n_run:
                q, kv = qkv(*rows, after=(after,))
            else:
                kv, = qkv(*rows, False, after=(after,))
                q, = qkv(*rows, True, False, after=(kv, gm))
            q_far.append(q)
            kvs.append(kv)
            return kv

        far_qkv(1, far_qkv(0, kv_here))

        wo = w_o.reshape(-1, dim)
        half = wo.shape[0] // 2
        n_piece = 2
        rows = half // n_piece
        wo_c = send(over_core, tied(wo, kvs[-1]))

        tiles = [(0, i) for i in range(2 * n_run)] + [(1, 0), (1, 1)]
        st, *wo_x = flash(tab, [q_here, q_far[0]], tiles, kvs, base=bases[0], work=int(work[0]), cut=wo,
                         n_cut=n_piece)
        wo_x = [send(over_x, w) for w in wo_x]
        far_qkv(3, far_qkv(2, st))
        kvs = kvs + [send(over_y, kv) for kv in kvs]

        os, outs, prev = [], [], q_far[-1]
        wo_a, wo_ya, wo_yb = {}, {}, {}

        def forward_w(p):
            here = tied(wo_x[p], prev)
            wo_ya[p] = (here, send(over_core, here))
            wo_a[p] = send(over_y, here)

        def relay_w(p):
            here = tied(wo_a[p], prev)
            wo_yb[p] = (here, send(over_core, here))

        def attend(j):
            held = 2 * n_run + 2 * j
            carried = [j, n_run + j] + ([held, held + 1] if j == 0 else [None, None])
            pair = j % 2
            *o, done = flash(
                tab, [q_here, q_far[j]], [(0, j), (0, n_run + j), (1, 0), (1, 1)], kvs,
                base=bases[1 + j], work=int(work[1 + j]), st=st, st_src=carried, old=os.pop() if pair else None, slots=2,
                after=(prev,))
            if pair:
                o = [o[0], send(over_core, o[1]), send(over_x, o[2]), send(over_both, o[3])]
            os.append(o)
            return done

        def project(i):
            ws = [wo, wo_c]
            blocks = [[(0, 0, half)], [(0, half, half)], [(1, 0, half)], [(1, half, half)]]
            for k in range(2):
                for held in (wo_ya, wo_yb):
                    blocks.append([(len(ws) + p, 0, rows) for p in range(n_piece)])
                    ws += [held[p][k] for p in range(n_piece)]
            got = out_proj(os[i], ws, blocks, x_rows, gm, i, after=(prev,))
            for y, b in zip(got[::2], got[1::2]):
                outs.append((y, b, send(over_x, b), send(over_core, b)))
            return got[0]

        last = n_run - 1
        for j in range(last):
            prev = attend(j)
            if j < n_piece:
                forward_w(j)
            if j:
                relay_w(j - 1)
        prev = project(0)
        prev = attend(last)

        z, sums, relay = None, [], {}

        def relay_b(j):
            here = tied(outs[j][2], prev)
            relay[j] = (here, send(over_core, here))

        chunks = [(j, 0, RUN) for j in range(last)] + [(last, 0, RUN // 2), (last, RUN // 2, RUN // 2)]

        def finish(c):
            j, first, size = chunks[c]
            return sum_rows(z, *sums[c], outs[j][0], first, size, j * RUN + first, n_run * RUN,
                        after=() if prev is z else (prev,))

        relay_b(0)
        for c, (j, first, size) in enumerate(chunks):
            b = [outs[j][1], relay[j][0], outs[j][3], relay[j][1]]
            keep, out = mlp(b, first, size, w_gate, w_up, w_down, after=(prev,))
            recv = send(over_core, out)
            prev = keep
            if c < last:
                relay_b(c + 1)
            if c == 0:
                prev = project(1)
            elif c < n_run:
                prev = z = finish(c - 1)
            kept = keep if prev is keep else tied(keep, prev)
            prev = s_far = (kept[size:].astype(F32) + recv[size:].astype(F32)).astype(BF)
            sums.append((keep, recv, send(over_x, s_far)))
        for c in (last, n_run):
            prev = z = finish(c)
        return z[None]

    return jax.shard_map(layer, mesh=mesh,
                         in_specs=(row_spec, P(), head_cols, head_cols, head_cols, P('tp', None, None),
                                   P(), P(None, 'tp'), P(None, 'tp'), P('tp', None)),
                         out_specs=row_spec, check_vma=False)
```

```python
import functools
import math
import jax
import jax.numpy as jnp
import numpy as np
from jax import lax
from jax.experimental import pallas as pl
from jax.experimental.pallas import tpu as pltpu
from jax.sharding import PartitionSpec as P

NORM_EPS = 1e-5
ROPE_THETA = 500000.0
HD = 128
RUN = 256
NEG = -1e30
LOG2E = math.log2(math.e)
DN = (((1,), (0,)), ((), ()))
BF = jnp.bfloat16
F32 = jnp.float32
ANY = pl.BlockSpec(memory_space=pltpu.HBM)


VMEM = 67043328
PARAMS = pltpu.CompilerParams(vmem_limit_bytes=VMEM)


def rope_tables(positions):
    half = HD // 2
    inv_freq = ROPE_THETA ** (-2.0 * jnp.arange(half, dtype=F32) / HD)
    angles = inv_freq[:, None] * positions.astype(F32)[..., None, :]
    return jnp.cos(angles), jnp.sin(angles)


def norm_rows(rows, gain):
    f = rows.astype(F32)
    mean_sq = jnp.mean(f * f, axis=-1, keepdims=True)
    return (f * lax.rsqrt(mean_sq + NORM_EPS) * gain.astype(F32)).astype(BF)


def cost(flops, moved):
    return pl.CostEstimate(flops=flops, transcendentals=0, bytes_accessed=moved)


def ordered(kernel, n_in, after):
    n = len(after)
    return lambda *refs: kernel(*refs[:n_in], *refs[n_in + n:])


def norm_kernel(x_ref, g_ref, *refs, per):
    for k, o_ref in enumerate(refs):
        @pl.when(lax.div(pl.program_id(0), per) == k)
        def _():
            o_ref[:] = norm_rows(x_ref[:], g_ref[:])


def norm_runs(x_rows, gain, runs, after=(), tile=128):
    dim = x_rows.shape[1]
    per = RUN // tile
    n = len(runs)
    return pl.pallas_call(
        ordered(functools.partial(norm_kernel, per=per), 2, after), grid=(n * per,),
        in_specs=[pl.BlockSpec((tile, dim), lambda i: (runs[0] * per + i, 0)), pl.BlockSpec((1, dim), lambda i: (0, 0))]
        + [ANY] * len(after),
        out_specs=[pl.BlockSpec((tile, dim), lambda i, k=k: (jnp.clip(i - k * per, 0, per - 1), 0)) for k in range(n)],
        out_shape=[jax.ShapeDtypeStruct((RUN, dim), BF)] * n,
        name="norm", compiler_params=PARAMS,
        cost_estimate=cost(n * RUN * dim, n * RUN * dim),
    )(x_rows, gain, *after)


def qkv_kernel(*refs, n_in, n_q, group, first, with_q, with_kv):
    a_refs = refs[:n_in]
    w_ref, cos_ref, sin_ref, *outs, a_scr, sem = refs[n_in:]
    q_ref, kv_ref = outs[0], outs[-1]
    n = pl.program_id(0) + first
    heads = w_ref.shape[1] // HD

    @pl.when(n == first)
    def _():
        for k, r in enumerate(a_refs):
            pltpu.make_async_copy(r, a_scr.at[pl.ds(k * RUN, RUN), :], sem.at[k]).start()

    def rope(f, i):
        f = f.astype(BF).astype(F32)
        lo, hi, cos, sin = f[:HD // 2], f[HD // 2:], cos_ref[i], sin_ref[i]
        return jnp.concatenate([lo * cos - hi * sin, hi * cos + lo * sin], axis=0)

    def one(k, carry):
        @pl.when(n == first)
        def _():
            for i in range(group):
                rows = pl.ds(pl.multiple_of((k * group + i) * RUN, RUN), RUN)
                pltpu.make_async_copy(a_scr.at[rows, :], a_scr.at[rows, :], sem.at[k * group + i]).wait()

        runs = [k * group + i for i in range(group)]

        def products():
            return [jnp.dot(a_scr[pl.ds(pl.multiple_of(run * RUN, RUN), RUN), :], w_ref[:], preferred_element_type=F32)
                    for run in runs]

        if with_q:
            @pl.when(n < n_q)
            def _():
                for run, r in zip(runs, products()):
                    for h in range(heads):
                        cols = slice(h * HD, (h + 1) * HD)
                        q_ref[run, cols, :] = rope(r[:, cols].T, run).astype(BF)

        if with_kv:
            @pl.when(n == n_q)
            def _():
                for run, r in zip(runs, products()):
                    for h in range(heads // 2):
                        cols, past = slice(h * HD, (h + 1) * HD), heads // 2 * HD
                        kv_ref[run, 0, :, cols] = rope(r[:, cols].T, run).T.astype(BF)
                        kv_ref[run, 1, cols, :] = r[:, past + h * HD:past + (h + 1) * HD].T.astype(BF)
        return carry

    lax.fori_loop(0, n_in // group, one, 0)


def qkv(rows, w_all, tables, with_q=True, with_kv=True, after=(), group=2):
    n_in = len(rows)
    dim = w_all.shape[0]
    tn = 512
    n_q = w_all.shape[1] // tn - 1
    (cos, sin), first_run = tables
    at = first_run // n_in
    start = 0 if with_q else n_q
    kv_shape = (n_in, 2, RUN, RUN)
    tab = pl.BlockSpec((n_in, HD // 2, RUN), lambda n: (at, 0, 0))
    return pl.pallas_call(
        ordered(functools.partial(qkv_kernel, n_in=n_in, n_q=n_q, group=group, first=start, with_q=with_q, with_kv=with_kv),
                n_in + 3, after),
        grid=(n_q * with_q + with_kv,),
        in_specs=[ANY] * n_in + [pl.BlockSpec((dim, tn), lambda n: (0, n + start)), tab, tab] + [ANY] * len(after),
        out_specs=[pl.BlockSpec((n_in, tn, RUN), lambda n: (0, jnp.minimum(n, n_q - 1), 0))] * with_q
        + [pl.BlockSpec(kv_shape, lambda n: (0,) * len(kv_shape))] * with_kv,
        out_shape=[jax.ShapeDtypeStruct((n_in, n_q * tn, RUN), BF)] * with_q + [jax.ShapeDtypeStruct(kv_shape, BF)] * with_kv,
        scratch_shapes=[pltpu.VMEM((n_in * RUN, dim), BF), pltpu.SemaphoreType.DMA((n_in,))],
        name="qkv", compiler_params=PARAMS,
        cost_estimate=cost(2 * n_in * RUN * w_all.size, 2 * w_all.size),
    )(*rows, w_all, cos, sin, *after)


BLK = 11
LAST, FIRST, CARRY = 16, 32, 64
ST = HD + 16


def flash_kernel(tab_ref, *refs, q_src, kv_src, n_q, n_kv, st_src, n_st, n_old, n_cut, slot, base, G, n_tiles, n_heads, final):
    qs, kvs, sts = refs[:n_q], refs[n_q:n_q + n_kv], refs[n_q + n_kv:n_q + n_kv + n_st]
    n_out = n_tiles + 1 if final else 1 + n_cut
    at = n_q + n_kv + n_st + n_old
    outs = refs[at:at + n_out]
    q_scr, kv_scr, o_scr, st_scr, s_scr, mb_scr, acc_scr, m_scr, l_scr, q_sem, kv_sem, o_sem, st_sem = refs[at + n_out:][:13]
    if n_cut:
        cut_ref, (cut_scr, cut_sem) = refs[at - 1], refs[-2:]
    T = RUN
    c = (HD ** -0.5) * LOG2E
    n_blocks = tab_ref[base]
    carried = base + 1
    row0 = carried + n_tiles
    null = len(kv_src)

    q_copies = [pltpu.make_async_copy(qs[a].at[i], q_scr.at[t], q_sem.at[t]) for t, (a, i) in enumerate(q_src)]
    kv_copies = [pltpu.make_async_copy(kvs[a].at[i], kv_scr.at[r], kv_sem.at[r]) for r, (a, i) in enumerate(kv_src)]

    def load_state(t):
        if st_src[t] is not None:
            @pl.when(tab_ref[carried + t] != 0)
            def _():
                pltpu.make_async_copy(sts[0].at[st_src[t]], st_scr.at[t], st_sem.at[t]).start()

    q_copies[0].start()
    for cp in kv_copies[:4]:
        cp.start()
    load_state(0)
    for cp in kv_copies[4:]:
        cp.start()
    for t in range(1, n_tiles):
        q_copies[t].start()
        load_state(t)
    kv_scr[null, 1] = jnp.zeros((256, 256), BF)
    if n_cut:
        cut_in = pltpu.make_async_copy(cut_ref.at[pl.ds(lax.axis_index('cp') * cut_scr.shape[0], cut_scr.shape[0]), :], cut_scr,
                                       cut_sem)
        part = cut_scr.shape[0] // n_cut
        cut_out = [pltpu.make_async_copy(cut_scr.at[pl.ds(k * part, part), :], outs[1 + k], cut_sem) for k in range(n_cut)]
        cut_in.start()

    def block(i):
        g = lax.div(i, n_blocks)
        return row0 + BLK * (i - g * n_blocks), g

    def arrived(have, need):
        def one(r, carry):
            pltpu.make_async_copy(kv_scr.at[r], kv_scr.at[r], kv_sem.at[r]).wait()
            return carry

        lax.fori_loop(have, need, one, 0)
        return jnp.maximum(have, need)

    def put(s, h, k):
        s_scr[h, pl.ds(k * RUN, RUN), :] = s
        mb_scr[h, k] = jnp.max(s.reshape(RUN // 8, 8, T), axis=0)

    def stage_a(row, g, h):
        col = pl.multiple_of(g * HD, HD)
        qt = q_scr[tab_ref[row], pl.ds(pl.multiple_of((g * G + h) * HD, HD), HD), :]
        for k in range(4):
            put(lax.dot_general(kv_scr[tab_ref[row + 3 + k], 0, :, pl.ds(col, HD)], qt, DN, preferred_element_type=F32), h, k)

    def stage_b(row, g, h):
        col = pl.multiple_of(g * HD, HD)
        m_prev = m_scr[h]
        mb = jnp.maximum(jnp.maximum(mb_scr[h, 0], mb_scr[h, 1]), jnp.maximum(mb_scr[h, 2], mb_scr[h, 3]))
        for r in (4, 2, 1):
            mb = jnp.maximum(mb, pltpu.roll(mb, r, 0))
        m_new = jnp.maximum(m_prev, mb)
        m_scr[h] = m_new
        m_c = m_new * c
        alpha = jnp.exp2(m_prev * c - m_c)
        l, pv = l_scr[h] * alpha, None
        for k in range(4):
            run = tab_ref[row + 7 + k]
            p = jnp.exp2(s_scr[h, k * RUN:(k + 1) * RUN].reshape(RUN // 8, 8, T) * c - m_c[None])
            l = l + jnp.sum(p, axis=0) * jnp.where(run < 0, 0.0, 1.0)
            d = lax.dot_general(kv_scr[jnp.where(run < 0, null, run), 1, pl.ds(col, HD), :], p.reshape(RUN, T).astype(BF), DN,
                                preferred_element_type=F32)
            pv = d if pv is None else pv + d
        l_scr[h] = l
        acc_scr[h] = (acc_scr[h].reshape(HD // 8, 8, T) * alpha[None]).reshape(HD, T) + pv

    def mask_runs(flags):
        seen = lax.broadcasted_iota(jnp.int32, (RUN, T), 0) <= lax.broadcasted_iota(jnp.int32, (RUN, T), 1)

        def one(k, carry):
            @pl.when((lax.shift_right_logical(flags, k) & 1) != 0)
            def _():
                rows = pl.multiple_of(k * RUN, RUN)
                for h in range(G):
                    put(jnp.where(seen, s_scr[h, pl.ds(rows, RUN), :], NEG), h, k)

            return carry

        lax.fori_loop(0, 4, one, 0)

    def finish(tile, g, get):
        for h in range(G):
            acc, l = get(h)
            o_scr[tile, :, pl.ds(pl.multiple_of((g * G + h) * HD, HD), HD)] = (acc / jnp.sum(l, axis=0, keepdims=True)).T.astype(BF)

        @pl.when(g == n_heads - 1)
        def _():
            for k in range(n_tiles):
                @pl.when(tile == k)
                def _():
                    pltpu.make_async_copy(o_scr.at[k], outs[k].at[slot], o_sem.at[k]).start()

    if final and n_st:
        def idle(i, carry):
            tile, g = lax.div(i, n_heads), lax.rem(i, n_heads)

            @pl.when(tab_ref[carried + tile] == 2)
            def _():
                @pl.when(g == 0)
                def _():
                    pltpu.make_async_copy(q_scr.at[tile], q_scr.at[tile], q_sem.at[tile]).wait()
                    pltpu.make_async_copy(st_scr.at[tile], st_scr.at[tile], st_sem.at[tile]).wait()

                finish(tile, g, lambda h: (st_scr[tile, g, h, :HD, :], st_scr[tile, g, h, HD + 8:, :]))

            return carry

        lax.fori_loop(0, n_tiles * n_heads, idle, 0)

    def query(row):
        t = tab_ref[row]
        pltpu.make_async_copy(q_scr.at[t], q_scr.at[t], q_sem.at[t]).wait()

    row, g = block(0)
    query(row)
    have = arrived(0, tab_ref[row + 2])
    for h in range(G):
        stage_a(row, g, h)

    def body(i, have):
        row, g = block(i)
        nrow, ng = block(jnp.minimum(i + 1, n_heads * n_blocks - 1))
        have = arrived(have, tab_ref[nrow + 2])
        flags = tab_ref[row + 1]
        tile = tab_ref[row]

        @pl.when((i + 1 < n_blocks) & ((tab_ref[nrow + 1] & FIRST) != 0))
        def _():
            query(nrow)

        @pl.when((flags & (FIRST | CARRY)) == FIRST)
        def _():
            acc_scr[:] = jnp.zeros_like(acc_scr)
            l_scr[:] = jnp.zeros_like(l_scr)
            m_scr[:] = jnp.full_like(m_scr, NEG)

        if n_st:
            @pl.when((flags & (FIRST | CARRY)) == (FIRST | CARRY))
            def _():
                @pl.when(g == 0)
                def _():
                    pltpu.make_async_copy(st_scr.at[tile], st_scr.at[tile], st_sem.at[tile]).wait()

                for h in range(G):
                    acc_scr[h] = st_scr[tile, g, h, :HD, :]
                    m_scr[h] = st_scr[tile, g, h, HD:HD + 8, :]
                    l_scr[h] = st_scr[tile, g, h, HD + 8:, :]

        if n_cut:
            @pl.when(i == n_blocks)
            def _():
                cut_in.wait()
                for cp in cut_out:
                    cp.start()

        @pl.when((flags & 15) != 0)
        def _():
            mask_runs(flags)

        for h in range(G):
            stage_b(row, g, h)
            stage_a(nrow, ng, h)

        @pl.when((flags & LAST) != 0)
        def _():
            if final:
                finish(tile, g, lambda h: (acc_scr[h], l_scr[h]))
            else:
                for h in range(G):
                    st_scr[tile, g, h, :HD, :] = acc_scr[h]
                    st_scr[tile, g, h, HD:HD + 8, :] = m_scr[h]
                    st_scr[tile, g, h, HD + 8:, :] = l_scr[h]

                @pl.when(g == n_heads - 1)
                def _():
                    pltpu.make_async_copy(st_scr.at[tile], outs[0].at[tile], o_sem.at[tile]).start()

        return have

    have = lax.fori_loop(0, n_heads * n_blocks, body, have)
    arrived(have, len(kv_src))
    if final:
        for k in range(n_tiles):
            pltpu.make_async_copy(o_scr.at[k], outs[k].at[slot], o_sem.at[k]).wait()
    else:
        def wait_out(i, carry):
            row = row0 + BLK * i

            @pl.when((tab_ref[row + 1] & LAST) != 0)
            def _():
                t = tab_ref[row]
                pltpu.make_async_copy(st_scr.at[t], st_scr.at[t], o_sem.at[t]).wait()

            return carry

        lax.fori_loop(0, n_blocks, wait_out, 0)
        for cp in cut_out:
            cp.wait()


def flash(tab, qs, q_src, kvs, *, base, work, st=None, st_src=None, old=None, cut=None, n_cut=0, slots=1, after=()):
    nq = qs[0].shape[1]
    n_heads = 2
    G = nq // HD // n_heads
    n_tiles = len(q_src)
    final = cut is None
    kv_src = [(a, i) for a, kv in enumerate(kvs) for i in range(kv.shape[0])]
    n_runs = len(kv_src)
    sts = () if st is None else (st,)
    old = old or ()
    more = (*old, *(() if final else (cut,)))
    n_in = 1 + len(qs) + len(kvs) + len(sts) + len(more)
    state = (n_heads, G, ST, RUN)
    has_st = not final or sts
    if final:
        out_shape = [jax.ShapeDtypeStruct((slots, RUN, nq), BF)] * n_tiles + [jax.ShapeDtypeStruct((8, HD), F32)]
        scratch = []
    else:
        half = cut.shape[0] // 2
        out_shape = [jax.ShapeDtypeStruct((n_tiles, *state), F32)]
        out_shape += [jax.ShapeDtypeStruct((half // n_cut, cut.shape[1]), BF)] * n_cut
        scratch = [pltpu.VMEM((half, cut.shape[1]), BF), pltpu.SemaphoreType.DMA]
    return pl.pallas_call(
        ordered(functools.partial(flash_kernel, q_src=q_src, kv_src=kv_src, n_q=len(qs), n_kv=len(kvs),
                                  st_src=st_src or [None] * n_tiles, n_st=len(sts), n_old=len(more), n_cut=n_cut,
                                  slot=slots - 1 if old else 0, base=base, G=G, n_tiles=n_tiles, n_heads=n_heads, final=final),
                n_in, after),
        grid_spec=pltpu.PrefetchScalarGridSpec(
            num_scalar_prefetch=1, grid=(),
            in_specs=[ANY] * (n_in - 1 + len(after)),
            out_specs=[ANY] * len(out_shape),
            scratch_shapes=[pltpu.VMEM((n_tiles, nq, RUN), BF),
                            pltpu.VMEM((n_runs + 1, 2, 256, 256), BF),
                            pltpu.VMEM((n_tiles if final else 1, RUN, nq), BF),
                            pltpu.VMEM((n_tiles if has_st else 1, *state), F32),
                            pltpu.VMEM((G, 4 * RUN, RUN), F32),
                            pltpu.VMEM((G, 4, 8, RUN), F32),
                            pltpu.VMEM((G, HD, RUN), F32),
                            pltpu.VMEM((G, 8, RUN), F32),
                            pltpu.VMEM((G, 8, RUN), F32),
                            pltpu.SemaphoreType.DMA((n_tiles,)),
                            pltpu.SemaphoreType.DMA((n_runs,)),
                            pltpu.SemaphoreType.DMA((n_tiles,)),
                            pltpu.SemaphoreType.DMA((n_tiles,)), *scratch]),
        out_shape=out_shape,
        input_output_aliases={n_in - len(old) + k: k for k in range(len(old))},
        name="flash" if final else "flash_part", compiler_params=PARAMS,
        cost_estimate=cost(8 * work * RUN * RUN * nq, n_runs * RUN * nq),
    )(tab, *qs, *kvs, *sts, *more, *after)


def out_kernel(*refs, blocks, n_w, n_run, at):
    n_o, n_out = 4, 2 * n_run
    o_refs, w_refs, x_ref, g_ref = refs[:n_o], refs[n_o:n_o + n_w], refs[n_o + n_w], refs[n_o + n_w + 1]
    outs = refs[n_o + n_w + 2:n_o + n_w + 2 + n_out]
    o_scr, w_scr, x_scr, acc_scr, o_sem, w_sem, x_sem, out_sem = refs[n_o + n_w + 2 + n_out:]
    width = o_refs[0].shape[-1]
    half = width // 2
    n_slots = w_scr.shape[0]

    def fetch(k):
        for i, pieces in enumerate(blocks):
            @pl.when(k == i)
            def _():
                to = 0
                for a, r0, n in pieces:
                    pltpu.make_async_copy(w_refs[a].at[pl.ds(r0, n), :], w_scr.at[i % n_slots, pl.ds(to, n), :],
                                          w_sem.at[i % n_slots]).start()
                    to += n

    mine = lax.axis_index('cp')
    loads = [[] for _ in blocks]
    for i in range(n_run):
        rows = pl.ds(i * RUN, RUN)
        for k in range(4):
            src = o_refs[k].at[i]
            if k < 2:
                loads[2 * k].append((src, o_scr.at[rows, pl.ds(k * width, width)]))
            else:
                for p, part in enumerate((mine, 1 - mine)):
                    loads[2 * k + p].append((src.at[:, pl.ds(pl.multiple_of(part * half, half), half)],
                                             o_scr.at[rows, pl.ds(k * width + p * half, half)]))
    copies = [[pltpu.make_async_copy(src, dst, o_sem.at[k, i]) for i, (src, dst) in enumerate(ls)] for k, ls in enumerate(loads)]
    x_copy = pltpu.make_async_copy(x_ref.at[pl.ds(at * n_run * RUN, n_run * RUN), :], x_scr, x_sem)
    for cp in copies[0]:
        cp.start()
    for i in range(n_slots - 1):
        fetch(jnp.int32(i))
    for ls in copies[1:]:
        for cp in ls:
            cp.start()
    x_copy.start()
    acc_scr[:] = jnp.zeros_like(acc_scr)

    def one(k, carry):
        fetch(k + n_slots - 1)
        for i, ls in enumerate(copies):
            if ls:
                @pl.when(k == i)
                def _():
                    for cp in ls:
                        cp.wait()
        slot = lax.rem(k, n_slots)
        pltpu.make_async_copy(w_scr.at[slot], w_scr.at[slot], w_sem.at[slot]).wait()
        acc_scr[:] += jnp.dot(o_scr[:, pl.ds(pl.multiple_of(k * half, half), half)], w_scr[slot], preferred_element_type=F32)
        return carry

    lax.fori_loop(0, len(blocks), one, 0)
    x_copy.wait()

    def rows32(r, carry):
        rows = pl.ds(pl.multiple_of(r * 32, 32), 32)
        y = (x_scr[rows, :].astype(F32) + acc_scr[rows, :].astype(BF).astype(F32)).astype(BF)
        x_scr[rows, :] = y
        o_scr[rows, :] = norm_rows(y, g_ref[:])
        return carry

    stores, per = [], RUN // 32
    for i in range(n_run):
        lax.fori_loop(i * per, (i + 1) * per, rows32, 0)
        for k, scr in enumerate((x_scr, o_scr)):
            stores.append(pltpu.make_async_copy(scr.at[pl.ds(i * RUN, RUN), :], outs[2 * i + k], out_sem.at[2 * i + k]))
            stores[-1].start()
    for cp in stores:
        cp.wait()


def out_proj(os, ws, blocks, x_rows, gain, at, after=()):
    dim = x_rows.shape[1]
    n_run, _, width = os[0].shape
    rows = n_run * RUN
    return pl.pallas_call(
        ordered(functools.partial(out_kernel, blocks=blocks, n_w=len(ws), n_run=n_run, at=at),
                len(os) + len(ws) + 2, after),
        grid=(1,),
        in_specs=[ANY] * (len(os) + len(ws) + 1) + [pl.BlockSpec((1, dim), lambda i: (0, 0))] + [ANY] * len(after),
        out_specs=[ANY] * (2 * n_run),
        out_shape=[jax.ShapeDtypeStruct((RUN, dim), BF)] * (2 * n_run),
        scratch_shapes=[pltpu.VMEM((rows, 4 * width), BF), pltpu.VMEM((3, width // 2, dim), BF), pltpu.VMEM((rows, dim), BF),
                        pltpu.VMEM((rows, dim), F32), pltpu.SemaphoreType.DMA((len(blocks), 2 * n_run)),
                        pltpu.SemaphoreType.DMA((3,)), pltpu.SemaphoreType.DMA, pltpu.SemaphoreType.DMA((2 * n_run,))],
        name="outp", compiler_params=PARAMS,
        cost_estimate=cost(8 * rows * width * dim, 8 * width * dim),
    )(*os, *ws, x_rows, gain, *after)


def mlp_kernel(*refs, n_in, first, rb, tn, td, nk, nd):
    b_refs = refs[:n_in]
    (wg_ref, wu_ref, wd_ref, own_ref, far_ref, b_scr, u_scr, w_scr, d_scr, keep_scr, out_scr, in_scr, b_sem, w_sem, d_sem,
     out_sem, in_sem) = refs[n_in:]
    i = pl.program_id(0)
    me = lax.axis_index('tp')
    mate = {'tp': me + 1 - 2 * lax.rem(me, 2)}
    barrier = pltpu.get_barrier_semaphore()

    def fetch(j):
        @pl.when(j < nk)
        def _():
            slot, cols = lax.rem(j, 2), pl.ds(pl.multiple_of(j * tn, tn), tn)
            for k, w in enumerate((wg_ref, wu_ref)):
                pltpu.make_async_copy(w.at[:, cols], w_scr.at[slot, k], w_sem.at[slot]).start()

        @pl.when((j >= nk) & (j < nk + nd))
        def _():
            n, slot = j - nk, lax.rem(j - nk, 2)
            pltpu.make_async_copy(wd_ref.at[:, pl.ds(pl.multiple_of(n * td, td), td)], d_scr.at[slot], d_sem.at[slot]).start()

    def gated(rows, cols, slot):
        b = b_scr[rows, :]
        gate = jnp.dot(b, w_scr[slot, 0], preferred_element_type=F32)
        up = jnp.dot(b, w_scr[slot, 1], preferred_element_type=F32)
        u_scr[rows, cols] = (jax.nn.silu(gate) * up).astype(BF)

    def to_mate(n):
        return pltpu.make_async_remote_copy(src_ref=out_scr.at[n], dst_ref=in_scr.at[n], send_sem=out_sem.at[n],
                                            recv_sem=in_sem.at[n], device_id=mate, device_id_type=pl.DeviceIdType.MESH)

    @pl.when(i == 0)
    def _():
        copies = [pltpu.make_async_copy(r.at[pl.ds(first, rb), :], b_scr.at[pl.ds(k * rb, rb), :], b_sem.at[k])
                  for k, r in enumerate(b_refs)]
        copies[0].start()
        fetch(i)
        for cp in copies[1:]:
            cp.start()
        pl.semaphore_signal(barrier, inc=1, device_id=mate, device_id_type=pl.DeviceIdType.MESH)

    @pl.when(i == 1)
    def _():
        pl.semaphore_wait(barrier, 1)

    fetch(i + 1)

    @pl.when(i < nk)
    def _():
        pltpu.make_async_copy(w_scr.at[lax.rem(i, 2)], w_scr.at[lax.rem(i, 2)], w_sem.at[lax.rem(i, 2)]).wait()

    @pl.when(i == 0)
    def _():
        def one(k, carry):
            rows = pl.ds(pl.multiple_of(k * rb, rb), rb)
            pltpu.make_async_copy(b_scr.at[rows, :], b_scr.at[rows, :], b_sem.at[k]).wait()
            gated(rows, pl.ds(0, tn), 0)
            return carry

        lax.fori_loop(0, n_in, one, 0)

    @pl.when((i > 0) & (i < nk))
    def _():
        gated(slice(None), pl.ds(pl.multiple_of(i * tn, tn), tn), lax.rem(i, 2))

    n = i - nk

    @pl.when(n > 1)
    def _():
        m = n - 2
        to_mate(m).wait_recv()
        total = (keep_scr[lax.rem(m, 2)].astype(F32) + in_scr[m].astype(F32)).astype(BF)
        size = total.shape[0] // 2
        own_ref[:] = total[:size]
        far_ref[:] = total[size:]

    @pl.when((n > 0) & (n <= nd))
    def _():
        to_mate(n - 1).start()

    @pl.when((n >= 0) & (n < nd))
    def _():
        slot = lax.rem(n, 2)
        pltpu.make_async_copy(d_scr.at[slot], d_scr.at[slot], d_sem.at[slot]).wait()
        d = jnp.dot(u_scr[:], d_scr[slot], preferred_element_type=F32).astype(BF)
        half = d.shape[0] // 2
        keep_scr[slot] = d[:half]
        out_scr[n] = d[half:]

    @pl.when(n > nd)
    def _():
        def sent(k, carry):
            to_mate(k).wait_send()
            return carry

        lax.fori_loop(0, nd, sent, 0)


def mlp(bs, first, rb, wg, wu, wd, call, after=()):
    dim = bs[0].shape[1]
    rows = rb * len(bs)
    ffn = wg.shape[1]
    td = 512
    tn = td if rows <= td else td // 2
    nk, nd = ffn // tn, dim // td
    half = rows // 2
    dn = lambda i: (0, jnp.clip(i - nk - 2, 0, nd - 1))
    return pl.pallas_call(
        ordered(functools.partial(mlp_kernel, n_in=len(bs), first=first, rb=rb, tn=tn, td=td, nk=nk, nd=nd), len(bs) + 3, after),
        grid=(nk + nd + 2,),
        in_specs=[ANY] * (len(bs) + 3 + len(after)),
        out_specs=[pl.BlockSpec((half // 2, td), dn)] * 2,
        out_shape=[jax.ShapeDtypeStruct((half // 2, dim), BF)] * 2,
        scratch_shapes=[pltpu.VMEM((rows, dim), BF), pltpu.VMEM((rows, ffn), BF), pltpu.VMEM((2, 2, dim, tn), BF),
                        pltpu.VMEM((2, ffn, td), BF), pltpu.VMEM((2, half, td), BF)]
        + [pltpu.VMEM((nd, half, td), BF)] * 2 + [pltpu.SemaphoreType.DMA((n,)) for n in (len(bs), 2, 2, nd, nd)],
        name="mlp",
        compiler_params=pltpu.CompilerParams(vmem_limit_bytes=VMEM, collective_id=call, has_side_effects=True),
        cost_estimate=cost(6 * rows * dim * ffn, 6 * dim * ffn),
    )(*bs, wg, wu, wd, *after)


def sum_kernel(*refs):
    p_ref, t_ref, y_ref, z_ref = refs[-4:]
    total = (p_ref[:].astype(F32) + t_ref[:].astype(F32)).astype(BF)
    z_ref[:] = (y_ref[:].astype(F32) + total.astype(F32)).astype(BF)


def sum_rows(z, mine, far, y, y_first, first, total, after=(), tile=64):
    rows, dim = mine.shape
    at = lambda r0: pl.BlockSpec((tile, dim), lambda i: (r0 // tile + i, 0))
    prev = () if z is None else (z,)
    return pl.pallas_call(
        ordered(sum_kernel, len(prev) + 3, after), grid=(rows // tile,),
        in_specs=[ANY] * len(prev) + [at(0), at(0), at(y_first)] + [ANY] * len(after),
        out_specs=at(first),
        out_shape=jax.ShapeDtypeStruct((total, dim), BF),
        input_output_aliases={0: 0} if prev else {},
        name="zsum", compiler_params=PARAMS,
        cost_estimate=cost(rows * dim, 8 * rows * dim),
    )(*prev, mine, far, y, *after)


def run_positions(xi, ci, y, cps, piece):
    def start(x, c):
        return (y if x == 0 else 2 * cps - 1 - y) * piece + c * (piece // 2)

    per = piece // 2 // RUN
    out = [start(xi, ci) + RUN * j for j in range(per)] + [start(xi, 1 - ci) + RUN * j for j in range(per)]
    for j in range(per):
        out += [start(1 - xi, ci) + RUN * j, start(1 - xi, 1 - ci) + RUN * j]
    return out


def block_list(tile, ids, diag):
    own = [] if diag is None else [diag]
    n_tail = (len(ids) + len(own)) % 4 or 4
    n_tail -= len(own)
    head, tail = ids[:len(ids) - n_tail], own + ids[len(ids) - n_tail:]
    blocks = [[0, head[i:i + 4], head[i:i + 4]] for i in range(0, len(head), 4)]
    fill = 4 - len(tail)
    keys = tail + [ids[-1] if ids else diag] * fill
    blocks.append([sum(1 << k for k, r in enumerate(keys) if r == diag), keys, tail + [-1] * fill])
    blocks[-1][0] |= LAST
    blocks[0][0] |= FIRST
    return [[tile, flags, 0] + keys + values for flags, keys, values in blocks]


def call_table(tiles, pairs, carry, idle):
    rows, most = [], 0
    carry = [c if pairs[t][0] or pairs[t][1] else idle for t, c in enumerate(carry)]
    for t, tile in enumerate(tiles):
        ids, own = pairs[t]
        if ids or own:
            mine = block_list(t, ids, tile if own else None)
            mine[0][1] |= CARRY if carry[t] else 0
            rows += mine
    for row in rows:
        most = max(most, max(row[3:7]) + 1)
        row[2] = most
    return [len(rows)] + carry + [v for row in rows for v in row], len(rows)


def work_tables(cps, piece):
    per = piece // 2 // RUN
    early, more = 2 * per + 2, 2 * per + 4
    stage = lambda r: 0 if r < early else 1
    soon_pair = lambda r, t: r < early and t < early or r < more and t in (0, 1, per, per + 1)
    calls = [(0, list(range(early)))]
    calls += [(1, [j, per + j, 2 * per + 2 * j, 2 * per + 2 * j + 1]) for j in range(per)]
    tabs, all_runs, sizes = [], [], []
    for y in range(cps):
        for xi in range(2):
            for ci in range(2):
                mine = run_positions(xi, ci, y, cps, piece)
                pos = mine + run_positions(xi, ci, 1 - y, cps, piece)
                all_runs.append(mine)
                tabs.append([])
                sizes.append([])
                for now, tiles in calls:
                    pairs, carry = [], []
                    for t in tiles:
                        seen = [r for r in range(len(pos)) if pos[r] < pos[t]]
                        when = {r: 0 if soon_pair(r, t) else 1 for r in seen}
                        late = list(when.values()).count(1) + stage(t)
                        soon = len(seen) + 1 - late
                        if late and soon % 4 <= -late % 4:
                            for r in [r for r in seen if not when[r]][:soon % 4]:
                                when[r] = 1
                        pairs.append(([r for r in seen if when[r] == now], stage(t) == now))
                        carry.append(int(stage(t) < now))
                    tab, n = call_table(tiles, pairs, carry, 2 if now == 1 else 0)
                    tabs[-1].append(tab)
                    sizes[-1].append(n)
    widths = [max(len(t[k]) for t in tabs) for k in range(len(calls))]
    flat = [[v for k, t in enumerate(tab) for v in t + [0] * (widths[k] - len(t))] for tab in tabs]
    bases = [sum(widths[:k]) for k in range(len(calls))]
    return np.array(flat, np.int32), np.array(all_runs, np.int32), bases, np.array(sizes).max(0) * 4


def solution(mesh):
    cps = mesh.shape['cp']
    row_spec = P('dp', ('cp', 'tp'), None)
    head_cols = P(None, 'tp', None)
    n_tp = mesh.shape['tp']

    over_core, over_x, over_both = (('tp', [(t, t ^ k) for t in range(n_tp)]) for k in (1, 2, 3))
    over_y = ('cp', [(i, i ^ 1) for i in range(cps)])

    def layer(x, g_attn, w_q, w_k, w_v, w_o, g_mlp, w_gate, w_up, w_down):
        x_rows = x[0]
        dim = x_rows.shape[1]
        n_run = x_rows.shape[0] // RUN
        piece = 2 * x_rows.shape[0]
        t_id, y_id = lax.axis_index('tp'), lax.axis_index('cp')
        np_tab, np_runs, bases, work = work_tables(cps, piece)
        dev = y_id * n_tp + t_id
        tab = lax.dynamic_index_in_dim(jnp.asarray(np_tab), dev, 0, keepdims=False)
        run_pos = lax.dynamic_index_in_dim(jnp.asarray(np_runs), dev, 0, keepdims=False)

        def tied(v, *others):
            return lax.optimization_barrier((v, *others))[0]

        def send(axis_pairs, v):
            return lax.ppermute(v, *axis_pairs)

        ga, gm = g_attn.reshape(1, dim), g_mlp.reshape(1, dim)
        own = list(norm_runs(x_rows, ga, [0]))
        own += norm_runs(x_rows, ga, list(range(1, n_run)), after=own)
        far = [send(over_x, own[j]) for j in range(n_run)]
        mate = [send(over_core, own[j]) for j in range(n_run)]

        w_all = jnp.concatenate([tied(w, own[-1]).reshape(dim, -1) for w in (w_q, w_k, w_v)], axis=1)
        row_pos = run_pos[:, None] + jnp.arange(RUN, dtype=jnp.int32)[None, :]
        tables = rope_tables(tied(row_pos[:2 * n_run], own[-1]))

        q_here, kv_here = qkv(own + mate, w_all, (tables, 0))
        kvs, q_far = [kv_here], []
        far_tables = rope_tables(tied(row_pos[2 * n_run:], kv_here))

        def far_qkv(j, after):
            here = tied(far[j], after)
            rows = [here, send(over_core, here)], w_all, (far_tables, 2 * j)
            if j + 1 < n_run:
                q, kv = qkv(*rows, after=(after,))
            else:
                kv, = qkv(*rows, False, after=(after,))
                q, = qkv(*rows, True, False, after=(kv, gm))
            q_far.append(q)
            kvs.append(kv)
            return kv

        far_qkv(1, far_qkv(0, kv_here))

        wo = w_o.reshape(-1, dim)
        half = wo.shape[0] // 2
        n_piece = 2
        rows = half // n_piece
        wo_c = send(over_core, tied(wo, kvs[-1]))

        tiles = [(0, i) for i in range(2 * n_run)] + [(1, 0), (1, 1)]
        st, *wo_x = flash(tab, [q_here, q_far[0]], tiles, kvs, base=bases[0], work=int(work[0]), cut=wo,
                         n_cut=n_piece)
        wo_x = [send(over_x, w) for w in wo_x]
        far_qkv(3, far_qkv(2, st))
        kvs = kvs + [send(over_y, kv) for kv in kvs]

        os, outs, prev = [], [], q_far[-1]
        wo_a, wo_ya, wo_yb = {}, {}, {}

        def forward_w(p):
            here = tied(wo_x[p], prev)
            wo_ya[p] = (here, send(over_core, here))
            wo_a[p] = send(over_y, here)

        def relay_w(p):
            here = tied(wo_a[p], prev)
            wo_yb[p] = (here, send(over_core, here))

        def attend(j):
            held = 2 * n_run + 2 * j
            carried = [j, n_run + j] + ([held, held + 1] if j == 0 else [None, None])
            pair = j % 2
            *o, done = flash(
                tab, [q_here, q_far[j]], [(0, j), (0, n_run + j), (1, 0), (1, 1)], kvs,
                base=bases[1 + j], work=int(work[1 + j]), st=st, st_src=carried, old=os.pop() if pair else None, slots=2,
                after=(prev,))
            if pair:
                o = [o[0], send(over_core, o[1]), send(over_x, o[2]), send(over_both, o[3])]
            os.append(o)
            return done

        def project(i):
            ws = [wo, wo_c]
            blocks = [[(0, 0, half)], [(0, half, half)], [(1, 0, half)], [(1, half, half)]]
            for k in range(2):
                for held in (wo_ya, wo_yb):
                    blocks.append([(len(ws) + p, 0, rows) for p in range(n_piece)])
                    ws += [held[p][k] for p in range(n_piece)]
            got = out_proj(os[i], ws, blocks, x_rows, gm, i, after=(prev,))
            for y, b in zip(got[::2], got[1::2]):
                outs.append((y, b, send(over_x, b), send(over_core, b)))
            return got[0]

        last = n_run - 1
        for j in range(last):
            prev = attend(j)
            if j < n_piece:
                forward_w(j)
            if j:
                relay_w(j - 1)
        prev = project(0)
        prev = attend(last)

        z, sums, relay = None, [], {}

        def relay_b(j):
            here = tied(outs[j][2], prev)
            relay[j] = (here, send(over_core, here))

        chunks = [(j, 0, RUN) for j in range(last)] + [(last, 0, RUN // 2), (last, RUN // 2, RUN // 2)]

        def finish(c):
            j, first, _ = chunks[c]
            return sum_rows(z, *sums[c], outs[j][0], first, j * RUN + first, n_run * RUN,
                        after=() if prev is z else (prev,))

        relay_b(0)
        for c, (j, first, size) in enumerate(chunks):
            b = [outs[j][1], relay[j][0], outs[j][3], relay[j][1]]
            prev, s_far = mlp(b, first, size, w_gate, w_up, w_down, c, after=(prev,))
            sums.append((prev, send(over_x, s_far)))
            if c < last:
                relay_b(c + 1)
            if c == 0:
                prev = project(1)
            elif c < n_run:
                prev = z = finish(c - 1)
        for c in (last, n_run):
            prev = z = finish(c)
        return z[None]

    return jax.shard_map(layer, mesh=mesh,
                         in_specs=(row_spec, P(), head_cols, head_cols, head_cols, P('tp', None, None),
                                   P(), P(None, 'tp'), P(None, 'tp'), P('tp', None)),
                         out_specs=row_spec, check_vma=False)
```

```python
import functools
import math
import jax
import jax.numpy as jnp
import numpy as np
from jax import lax
from jax.experimental import pallas as pl
from jax.experimental.pallas import tpu as pltpu
from jax.sharding import PartitionSpec as P

NORM_EPS = 1e-5
ROPE_THETA = 500000.0
HD = 128
RUN = 256
NEG = -1e30
LOG2E = math.log2(math.e)
DN = (((1,), (0,)), ((), ()))
BF = jnp.bfloat16
F32 = jnp.float32
ANY = pl.BlockSpec(memory_space=pltpu.HBM)


VMEM = 67043328
PARAMS = pltpu.CompilerParams(vmem_limit_bytes=VMEM)


def rope_tables(positions):
    half = HD // 2
    inv_freq = ROPE_THETA ** (-2.0 * jnp.arange(half, dtype=F32) / HD)
    angles = inv_freq[:, None] * positions.astype(F32)[..., None, :]
    return jnp.cos(angles), jnp.sin(angles)


def norm_rows(rows, gain):
    f = rows.astype(F32)
    mean_sq = jnp.mean(f * f, axis=-1, keepdims=True)
    return (f * lax.rsqrt(mean_sq + NORM_EPS) * gain.astype(F32)).astype(BF)


def cost(flops, moved):
    return pl.CostEstimate(flops=flops, transcendentals=0, bytes_accessed=moved)


def ordered(kernel, n_in, after):
    n = len(after)
    return lambda *refs: kernel(*refs[:n_in], *refs[n_in + n:])


def norm_kernel(x_ref, g_ref, *refs, per):
    for k, o_ref in enumerate(refs):
        @pl.when(lax.div(pl.program_id(0), per) == k)
        def _():
            o_ref[:] = norm_rows(x_ref[:], g_ref[:])


def norm_runs(x_rows, gain, runs, after=(), tile=128):
    dim = x_rows.shape[1]
    per = RUN // tile
    n = len(runs)
    return pl.pallas_call(
        ordered(functools.partial(norm_kernel, per=per), 2, after), grid=(n * per,),
        in_specs=[pl.BlockSpec((tile, dim), lambda i: (runs[0] * per + i, 0)), pl.BlockSpec((1, dim), lambda i: (0, 0))]
        + [ANY] * len(after),
        out_specs=[pl.BlockSpec((tile, dim), lambda i, k=k: (jnp.clip(i - k * per, 0, per - 1), 0)) for k in range(n)],
        out_shape=[jax.ShapeDtypeStruct((RUN, dim), BF)] * n,
        name="norm", compiler_params=PARAMS,
        cost_estimate=cost(n * RUN * dim, n * RUN * dim),
    )(x_rows, gain, *after)


def qkv_kernel(*refs, n_in, n_q, group, first, with_q, with_kv):
    a_refs = refs[:n_in]
    w_ref, cos_ref, sin_ref, *outs, a_scr, sem = refs[n_in:]
    q_ref, kv_ref = outs[0], outs[-1]
    n = pl.program_id(0) + first
    heads = w_ref.shape[1] // HD

    @pl.when(n == first)
    def _():
        for k, r in enumerate(a_refs):
            pltpu.make_async_copy(r, a_scr.at[pl.ds(k * RUN, RUN), :], sem.at[k]).start()

    def rope(f, i):
        f = f.astype(BF).astype(F32)
        lo, hi, cos, sin = f[:HD // 2], f[HD // 2:], cos_ref[i], sin_ref[i]
        return jnp.concatenate([lo * cos - hi * sin, hi * cos + lo * sin], axis=0)

    def one(k, carry):
        @pl.when(n == first)
        def _():
            for i in range(group):
                rows = pl.ds(pl.multiple_of((k * group + i) * RUN, RUN), RUN)
                pltpu.make_async_copy(a_scr.at[rows, :], a_scr.at[rows, :], sem.at[k * group + i]).wait()

        runs = [k * group + i for i in range(group)]

        def products():
            return [jnp.dot(a_scr[pl.ds(pl.multiple_of(run * RUN, RUN), RUN), :], w_ref[:], preferred_element_type=F32)
                    for run in runs]

        if with_q:
            @pl.when(n < n_q)
            def _():
                for run, r in zip(runs, products()):
                    for h in range(heads):
                        cols = slice(h * HD, (h + 1) * HD)
                        q_ref[run, cols, :] = rope(r[:, cols].T, run).astype(BF)

        if with_kv:
            @pl.when(n == n_q)
            def _():
                for run, r in zip(runs, products()):
                    for h in range(heads // 2):
                        cols, past = slice(h * HD, (h + 1) * HD), heads // 2 * HD
                        kv_ref[run, 0, :, cols] = rope(r[:, cols].T, run).T.astype(BF)
                        kv_ref[run, 1, cols, :] = r[:, past + h * HD:past + (h + 1) * HD].T.astype(BF)
        return carry

    lax.fori_loop(0, n_in // group, one, 0)


def qkv(rows, w_all, tables, with_q=True, with_kv=True, after=(), group=2):
    n_in = len(rows)
    dim = w_all.shape[0]
    tn = 512
    n_q = w_all.shape[1] // tn - 1
    (cos, sin), first_run = tables
    at = first_run // n_in
    start = 0 if with_q else n_q
    kv_shape = (n_in, 2, RUN, RUN)
    tab = pl.BlockSpec((n_in, HD // 2, RUN), lambda n: (at, 0, 0))
    return pl.pallas_call(
        ordered(functools.partial(qkv_kernel, n_in=n_in, n_q=n_q, group=group, first=start, with_q=with_q, with_kv=with_kv),
                n_in + 3, after),
        grid=(n_q * with_q + with_kv,),
        in_specs=[ANY] * n_in + [pl.BlockSpec((dim, tn), lambda n: (0, n + start)), tab, tab] + [ANY] * len(after),
        out_specs=[pl.BlockSpec((n_in, tn, RUN), lambda n: (0, jnp.minimum(n, n_q - 1), 0))] * with_q
        + [pl.BlockSpec(kv_shape, lambda n: (0,) * len(kv_shape))] * with_kv,
        out_shape=[jax.ShapeDtypeStruct((n_in, n_q * tn, RUN), BF)] * with_q + [jax.ShapeDtypeStruct(kv_shape, BF)] * with_kv,
        scratch_shapes=[pltpu.VMEM((n_in * RUN, dim), BF), pltpu.SemaphoreType.DMA((n_in,))],
        name="qkv", compiler_params=PARAMS,
        cost_estimate=cost(2 * n_in * RUN * w_all.size, 2 * w_all.size),
    )(*rows, w_all, cos, sin, *after)


BLK = 11
LAST, FIRST, CARRY = 16, 32, 64
ST = HD + 16


def flash_kernel(tab_ref, *refs, q_src, kv_src, n_q, n_kv, st_src, n_st, n_old, n_cut, slot, base, G, n_tiles, n_heads, final):
    qs, kvs, sts = refs[:n_q], refs[n_q:n_q + n_kv], refs[n_q + n_kv:n_q + n_kv + n_st]
    n_out = n_tiles + 1 if final else 1 + n_cut
    at = n_q + n_kv + n_st + n_old
    outs = refs[at:at + n_out]
    q_scr, kv_scr, o_scr, st_scr, s_scr, mb_scr, acc_scr, m_scr, l_scr, q_sem, kv_sem, o_sem, st_sem = refs[at + n_out:][:13]
    if n_cut:
        cut_ref, (cut_scr, cut_sem) = refs[at - 1], refs[-2:]
    T = RUN
    c = (HD ** -0.5) * LOG2E
    n_blocks = tab_ref[base]
    carried = base + 1
    row0 = carried + n_tiles
    null = len(kv_src)

    q_copies = [pltpu.make_async_copy(qs[a].at[i], q_scr.at[t], q_sem.at[t]) for t, (a, i) in enumerate(q_src)]
    kv_copies = [pltpu.make_async_copy(kvs[a].at[i], kv_scr.at[r], kv_sem.at[r]) for r, (a, i) in enumerate(kv_src)]

    def load_state(t):
        if st_src[t] is not None:
            @pl.when(tab_ref[carried + t] != 0)
            def _():
                pltpu.make_async_copy(sts[0].at[st_src[t]], st_scr.at[t], st_sem.at[t]).start()

    q_copies[0].start()
    for cp in kv_copies[:4]:
        cp.start()
    load_state(0)
    for cp in kv_copies[4:]:
        cp.start()
    for t in range(1, n_tiles):
        q_copies[t].start()
        load_state(t)
    kv_scr[null, 1] = jnp.zeros((RUN, RUN), BF)
    if n_cut:
        cut_in = pltpu.make_async_copy(cut_ref.at[pl.ds(lax.axis_index('cp') * cut_scr.shape[0], cut_scr.shape[0]), :], cut_scr,
                                       cut_sem)
        part = cut_scr.shape[0] // n_cut
        cut_out = [pltpu.make_async_copy(cut_scr.at[pl.ds(k * part, part), :], outs[1 + k], cut_sem) for k in range(n_cut)]
        cut_in.start()

    def block(i):
        g = lax.div(i, n_blocks)
        return row0 + BLK * (i - g * n_blocks), g

    def arrived(have, need):
        def one(r, carry):
            pltpu.make_async_copy(kv_scr.at[r], kv_scr.at[r], kv_sem.at[r]).wait()
            return carry

        lax.fori_loop(have, need, one, 0)
        return jnp.maximum(have, need)

    def put(s, h, k):
        s_scr[h, pl.ds(k * RUN, RUN), :] = s
        mb_scr[h, k] = jnp.max(s.reshape(RUN // 8, 8, T), axis=0)

    def stage_a(row, g, h):
        col = pl.multiple_of(g * HD, HD)
        qt = q_scr[tab_ref[row], pl.ds(pl.multiple_of((g * G + h) * HD, HD), HD), :]
        for k in range(4):
            put(lax.dot_general(kv_scr[tab_ref[row + 3 + k], 0, :, pl.ds(col, HD)], qt, DN, preferred_element_type=F32), h, k)

    def stage_b(row, g, h):
        col = pl.multiple_of(g * HD, HD)
        m_prev = m_scr[h]
        mb = jnp.maximum(jnp.maximum(mb_scr[h, 0], mb_scr[h, 1]), jnp.maximum(mb_scr[h, 2], mb_scr[h, 3]))
        for r in (4, 2, 1):
            mb = jnp.maximum(mb, pltpu.roll(mb, r, 0))
        m_new = jnp.maximum(m_prev, mb)
        m_scr[h] = m_new
        m_c = m_new * c
        alpha = jnp.exp2(m_prev * c - m_c)
        l, pv = l_scr[h] * alpha, None
        for k in range(4):
            run = tab_ref[row + 7 + k]
            p = jnp.exp2(s_scr[h, k * RUN:(k + 1) * RUN].reshape(RUN // 8, 8, T) * c - m_c[None])
            l = l + jnp.sum(p, axis=0) * jnp.where(run < 0, 0.0, 1.0)
            d = lax.dot_general(kv_scr[jnp.where(run < 0, null, run), 1, pl.ds(col, HD), :], p.reshape(RUN, T).astype(BF), DN,
                                preferred_element_type=F32)
            pv = d if pv is None else pv + d
        l_scr[h] = l
        acc_scr[h] = (acc_scr[h].reshape(HD // 8, 8, T) * alpha[None]).reshape(HD, T) + pv

    def mask_runs(flags):
        seen = lax.broadcasted_iota(jnp.int32, (RUN, T), 0) <= lax.broadcasted_iota(jnp.int32, (RUN, T), 1)

        def one(k, carry):
            @pl.when((lax.shift_right_logical(flags, k) & 1) != 0)
            def _():
                rows = pl.multiple_of(k * RUN, RUN)
                for h in range(G):
                    put(jnp.where(seen, s_scr[h, pl.ds(rows, RUN), :], NEG), h, k)

            return carry

        lax.fori_loop(0, 4, one, 0)

    def finish(tile, g, get):
        for h in range(G):
            acc, l = get(h)
            o_scr[tile, :, pl.ds(pl.multiple_of((g * G + h) * HD, HD), HD)] = (acc / jnp.sum(l, axis=0, keepdims=True)).T.astype(BF)

        @pl.when(g == n_heads - 1)
        def _():
            for k in range(n_tiles):
                @pl.when(tile == k)
                def _():
                    pltpu.make_async_copy(o_scr.at[k], outs[k].at[slot], o_sem.at[k]).start()

    if final and n_st:
        def idle(i, carry):
            tile, g = lax.div(i, n_heads), lax.rem(i, n_heads)

            @pl.when(tab_ref[carried + tile] == 2)
            def _():
                @pl.when(g == 0)
                def _():
                    pltpu.make_async_copy(q_scr.at[tile], q_scr.at[tile], q_sem.at[tile]).wait()
                    pltpu.make_async_copy(st_scr.at[tile], st_scr.at[tile], st_sem.at[tile]).wait()

                finish(tile, g, lambda h: (st_scr[tile, g, h, :HD, :], st_scr[tile, g, h, HD + 8:, :]))

            return carry

        lax.fori_loop(0, n_tiles * n_heads, idle, 0)

    def query(row):
        t = tab_ref[row]
        pltpu.make_async_copy(q_scr.at[t], q_scr.at[t], q_sem.at[t]).wait()

    row, g = block(0)
    query(row)
    have = arrived(0, tab_ref[row + 2])
    for h in range(G):
        stage_a(row, g, h)

    def body(i, have):
        row, g = block(i)
        nrow, ng = block(jnp.minimum(i + 1, n_heads * n_blocks - 1))
        have = arrived(have, tab_ref[nrow + 2])
        flags = tab_ref[row + 1]
        tile = tab_ref[row]

        @pl.when((i + 1 < n_blocks) & ((tab_ref[nrow + 1] & FIRST) != 0))
        def _():
            query(nrow)

        @pl.when((flags & (FIRST | CARRY)) == FIRST)
        def _():
            acc_scr[:] = jnp.zeros_like(acc_scr)
            l_scr[:] = jnp.zeros_like(l_scr)
            m_scr[:] = jnp.full_like(m_scr, NEG)

        if n_st:
            @pl.when((flags & (FIRST | CARRY)) == (FIRST | CARRY))
            def _():
                @pl.when(g == 0)
                def _():
                    pltpu.make_async_copy(st_scr.at[tile], st_scr.at[tile], st_sem.at[tile]).wait()

                for h in range(G):
                    acc_scr[h] = st_scr[tile, g, h, :HD, :]
                    m_scr[h] = st_scr[tile, g, h, HD:HD + 8, :]
                    l_scr[h] = st_scr[tile, g, h, HD + 8:, :]

        if n_cut:
            @pl.when(i == n_blocks)
            def _():
                cut_in.wait()
                for cp in cut_out:
                    cp.start()

        @pl.when((flags & 15) != 0)
        def _():
            mask_runs(flags)

        for h in range(G):
            stage_b(row, g, h)
            stage_a(nrow, ng, h)

        @pl.when((flags & LAST) != 0)
        def _():
            if final:
                finish(tile, g, lambda h: (acc_scr[h], l_scr[h]))
            else:
                for h in range(G):
                    st_scr[tile, g, h, :HD, :] = acc_scr[h]
                    st_scr[tile, g, h, HD:HD + 8, :] = m_scr[h]
                    st_scr[tile, g, h, HD + 8:, :] = l_scr[h]

                @pl.when(g == n_heads - 1)
                def _():
                    pltpu.make_async_copy(st_scr.at[tile], outs[0].at[tile], o_sem.at[tile]).start()

        return have

    have = lax.fori_loop(0, n_heads * n_blocks, body, have)
    arrived(have, len(kv_src))
    if final:
        for k in range(n_tiles):
            pltpu.make_async_copy(o_scr.at[k], outs[k].at[slot], o_sem.at[k]).wait()
    else:
        def wait_out(i, carry):
            row = row0 + BLK * i

            @pl.when((tab_ref[row + 1] & LAST) != 0)
            def _():
                t = tab_ref[row]
                pltpu.make_async_copy(st_scr.at[t], st_scr.at[t], o_sem.at[t]).wait()

            return carry

        lax.fori_loop(0, n_blocks, wait_out, 0)
        for cp in cut_out:
            cp.wait()


def flash(tab, qs, q_src, kvs, *, base, work, st=None, st_src=None, old=None, cut=None, n_cut=0, slots=1, after=()):
    nq = qs[0].shape[1]
    n_heads = 2
    G = nq // HD // n_heads
    n_tiles = len(q_src)
    final = cut is None
    kv_src = [(a, i) for a, kv in enumerate(kvs) for i in range(kv.shape[0])]
    n_runs = len(kv_src)
    sts = () if st is None else (st,)
    old = old or ()
    more = (*old, *(() if final else (cut,)))
    n_in = 1 + len(qs) + len(kvs) + len(sts) + len(more)
    state = (n_heads, G, ST, RUN)
    has_st = not final or sts
    if final:
        out_shape = [jax.ShapeDtypeStruct((slots, RUN, nq), BF)] * n_tiles + [jax.ShapeDtypeStruct((8, HD), F32)]
        scratch = []
    else:
        half = cut.shape[0] // 2
        out_shape = [jax.ShapeDtypeStruct((n_tiles, *state), F32)]
        out_shape += [jax.ShapeDtypeStruct((half // n_cut, cut.shape[1]), BF)] * n_cut
        scratch = [pltpu.VMEM((half, cut.shape[1]), BF), pltpu.SemaphoreType.DMA]
    return pl.pallas_call(
        ordered(functools.partial(flash_kernel, q_src=q_src, kv_src=kv_src, n_q=len(qs), n_kv=len(kvs),
                                  st_src=st_src or [None] * n_tiles, n_st=len(sts), n_old=len(more), n_cut=n_cut,
                                  slot=slots - 1 if old else 0, base=base, G=G, n_tiles=n_tiles, n_heads=n_heads, final=final),
                n_in, after),
        grid_spec=pltpu.PrefetchScalarGridSpec(
            num_scalar_prefetch=1, grid=(),
            in_specs=[ANY] * (n_in - 1 + len(after)),
            out_specs=[ANY] * len(out_shape),
            scratch_shapes=[pltpu.VMEM((n_tiles, nq, RUN), BF),
                            pltpu.VMEM((n_runs + 1, 2, RUN, RUN), BF),
                            pltpu.VMEM((n_tiles if final else 1, RUN, nq), BF),
                            pltpu.VMEM((n_tiles if has_st else 1, *state), F32),
                            pltpu.VMEM((G, 4 * RUN, RUN), F32),
                            pltpu.VMEM((G, 4, 8, RUN), F32),
                            pltpu.VMEM((G, HD, RUN), F32),
                            pltpu.VMEM((G, 8, RUN), F32),
                            pltpu.VMEM((G, 8, RUN), F32),
                            pltpu.SemaphoreType.DMA((n_tiles,)),
                            pltpu.SemaphoreType.DMA((n_runs,)),
                            pltpu.SemaphoreType.DMA((n_tiles,)),
                            pltpu.SemaphoreType.DMA((n_tiles,)), *scratch]),
        out_shape=out_shape,
        input_output_aliases={n_in - len(old) + k: k for k in range(len(old))},
        name="flash" if final else "flash_part", compiler_params=PARAMS,
        cost_estimate=cost(8 * work * RUN * RUN * nq, n_runs * RUN * nq),
    )(tab, *qs, *kvs, *sts, *more, *after)


def out_kernel(*refs, blocks, n_w, n_run, at):
    n_o, n_out = 4, 2 * n_run
    o_refs, w_refs, x_ref, g_ref = refs[:n_o], refs[n_o:n_o + n_w], refs[n_o + n_w], refs[n_o + n_w + 1]
    outs = refs[n_o + n_w + 2:n_o + n_w + 2 + n_out]
    o_scr, w_scr, x_scr, acc_scr, o_sem, w_sem, x_sem, out_sem = refs[n_o + n_w + 2 + n_out:]
    width = o_refs[0].shape[-1]
    half = width // 2
    n_slots = w_scr.shape[0]

    def fetch(k):
        for i, pieces in enumerate(blocks):
            @pl.when(k == i)
            def _():
                to = 0
                for a, r0, n in pieces:
                    pltpu.make_async_copy(w_refs[a].at[pl.ds(r0, n), :], w_scr.at[i % n_slots, pl.ds(to, n), :],
                                          w_sem.at[i % n_slots]).start()
                    to += n

    mine = lax.axis_index('cp')
    loads = [[] for _ in blocks]
    for i in range(n_run):
        rows = pl.ds(i * RUN, RUN)
        for k in range(4):
            src = o_refs[k].at[i]
            if k < 2:
                loads[2 * k].append((src, o_scr.at[rows, pl.ds(k * width, width)]))
            else:
                for p, part in enumerate((mine, 1 - mine)):
                    loads[2 * k + p].append((src.at[:, pl.ds(pl.multiple_of(part * half, half), half)],
                                             o_scr.at[rows, pl.ds(k * width + p * half, half)]))
    copies = [[pltpu.make_async_copy(src, dst, o_sem.at[k, i]) for i, (src, dst) in enumerate(ls)] for k, ls in enumerate(loads)]
    x_copy = pltpu.make_async_copy(x_ref.at[pl.ds(at * n_run * RUN, n_run * RUN), :], x_scr, x_sem)
    for cp in copies[0]:
        cp.start()
    for i in range(n_slots - 1):
        fetch(jnp.int32(i))
    for ls in copies[1:]:
        for cp in ls:
            cp.start()
    x_copy.start()
    acc_scr[:] = jnp.zeros_like(acc_scr)

    def one(k, carry):
        fetch(k + n_slots - 1)
        for i, ls in enumerate(copies):
            if ls:
                @pl.when(k == i)
                def _():
                    for cp in ls:
                        cp.wait()
        slot = lax.rem(k, n_slots)
        pltpu.make_async_copy(w_scr.at[slot], w_scr.at[slot], w_sem.at[slot]).wait()
        acc_scr[:] += jnp.dot(o_scr[:, pl.ds(pl.multiple_of(k * half, half), half)], w_scr[slot], preferred_element_type=F32)
        return carry

    lax.fori_loop(0, len(blocks), one, 0)
    x_copy.wait()

    strip = 32

    def one_strip(r, carry):
        rows = pl.ds(pl.multiple_of(r * strip, strip), strip)
        y = (x_scr[rows, :].astype(F32) + acc_scr[rows, :].astype(BF).astype(F32)).astype(BF)
        x_scr[rows, :] = y
        o_scr[rows, :] = norm_rows(y, g_ref[:])
        return carry

    stores, per = [], RUN // strip
    for i in range(n_run):
        lax.fori_loop(i * per, (i + 1) * per, one_strip, 0)
        for k, scr in enumerate((x_scr, o_scr)):
            stores.append(pltpu.make_async_copy(scr.at[pl.ds(i * RUN, RUN), :], outs[2 * i + k], out_sem.at[2 * i + k]))
            stores[-1].start()
    for cp in stores:
        cp.wait()


def out_proj(os, ws, blocks, x_rows, gain, at, after=()):
    dim = x_rows.shape[1]
    n_run, _, width = os[0].shape
    rows = n_run * RUN
    return pl.pallas_call(
        ordered(functools.partial(out_kernel, blocks=blocks, n_w=len(ws), n_run=n_run, at=at),
                len(os) + len(ws) + 2, after),
        grid=(1,),
        in_specs=[ANY] * (len(os) + len(ws) + 1) + [pl.BlockSpec((1, dim), lambda i: (0, 0))] + [ANY] * len(after),
        out_specs=[ANY] * (2 * n_run),
        out_shape=[jax.ShapeDtypeStruct((RUN, dim), BF)] * (2 * n_run),
        scratch_shapes=[pltpu.VMEM((rows, 4 * width), BF), pltpu.VMEM((3, width // 2, dim), BF), pltpu.VMEM((rows, dim), BF),
                        pltpu.VMEM((rows, dim), F32), pltpu.SemaphoreType.DMA((len(blocks), 2 * n_run)),
                        pltpu.SemaphoreType.DMA((3,)), pltpu.SemaphoreType.DMA, pltpu.SemaphoreType.DMA((2 * n_run,))],
        name="outp", compiler_params=PARAMS,
        cost_estimate=cost(8 * rows * width * dim, 8 * width * dim),
    )(*os, *ws, x_rows, gain, *after)


def mlp_kernel(*refs, n_in, first, rb, tn, td, nk, nd, cross):
    b_refs = refs[:n_in]
    wg_ref, wu_ref, wd_ref, *outs = refs[n_in:n_in + (4 if cross else 5)]
    (b_scr, u_scr, w_scr, d_scr, keep_scr, out_scr, in_scr, b_sem, w_sem, d_sem, out_sem, in_sem,
     *more) = refs[n_in + (4 if cross else 5):]
    i = pl.program_id(0)
    me = lax.axis_index('tp')
    mate = {'tp': me + 1 - 2 * lax.rem(me, 2)}
    peers = [mate]
    if cross:
        own_scr, far_scr, back_scr, far_sem, back_sem = more
        half_tp = lax.axis_size('tp') // 2
        peers.append({'tp': lax.rem(me + half_tp, 2 * half_tp)})
    barrier = pltpu.get_barrier_semaphore()

    def fetch(j):
        @pl.when(j < nk)
        def _():
            slot, cols = lax.rem(j, 2), pl.ds(pl.multiple_of(j * tn, tn), tn)
            for k, w in enumerate((wg_ref, wu_ref)):
                pltpu.make_async_copy(w.at[:, cols], w_scr.at[slot, k], w_sem.at[slot]).start()

        @pl.when((j >= nk) & (j < nk + nd))
        def _():
            n, slot = j - nk, lax.rem(j - nk, 2)
            pltpu.make_async_copy(wd_ref.at[:, pl.ds(pl.multiple_of(n * td, td), td)], d_scr.at[slot], d_sem.at[slot]).start()

    def gated(rows, cols, slot):
        b = b_scr[rows, :]
        gate = jnp.dot(b, w_scr[slot, 0], preferred_element_type=F32)
        up = jnp.dot(b, w_scr[slot, 1], preferred_element_type=F32)
        u_scr[rows, cols] = (jax.nn.silu(gate) * up).astype(BF)

    def to_mate(n):
        return pltpu.make_async_remote_copy(src_ref=out_scr.at[n], dst_ref=in_scr.at[n], send_sem=out_sem.at[n],
                                            recv_sem=in_sem.at[n], device_id=mate, device_id_type=pl.DeviceIdType.MESH)

    def to_far(n):
        return pltpu.make_async_remote_copy(src_ref=far_scr.at[n], dst_ref=back_scr.at[n], send_sem=far_sem.at[n],
                                            recv_sem=back_sem.at[n], device_id=peers[-1], device_id_type=pl.DeviceIdType.MESH)

    @pl.when(i == 0)
    def _():
        copies = [pltpu.make_async_copy(r.at[pl.ds(first, rb), :], b_scr.at[pl.ds(k * rb, rb), :], b_sem.at[k])
                  for k, r in enumerate(b_refs)]
        copies[0].start()
        fetch(i)
        for cp in copies[1:]:
            cp.start()
        for peer in peers:
            pl.semaphore_signal(barrier, inc=1, device_id=peer, device_id_type=pl.DeviceIdType.MESH)

    @pl.when(i == 1)
    def _():
        pl.semaphore_wait(barrier, len(peers))

    fetch(i + 1)

    @pl.when(i < nk)
    def _():
        slot = lax.rem(i, 2)
        pltpu.make_async_copy(w_scr.at[slot], w_scr.at[slot], w_sem.at[slot]).wait()

    @pl.when(i == 0)
    def _():
        def one(k, carry):
            rows = pl.ds(pl.multiple_of(k * rb, rb), rb)
            pltpu.make_async_copy(b_scr.at[rows, :], b_scr.at[rows, :], b_sem.at[k]).wait()
            gated(rows, pl.ds(0, tn), 0)
            return carry

        lax.fori_loop(0, n_in, one, 0)

    @pl.when((i > 0) & (i < nk))
    def _():
        gated(slice(None), pl.ds(pl.multiple_of(i * tn, tn), tn), lax.rem(i, 2))

    n = i - nk

    @pl.when((n > 0) & (n <= nd))
    def _():
        to_mate(n - 1).start()

    if cross:
        @pl.when((n > 1) & (n <= nd + 1))
        def _():
            to_far(n - 2).start()

    @pl.when((n >= 0) & (n < nd))
    def _():
        slot = lax.rem(n, 2)
        pltpu.make_async_copy(d_scr.at[slot], d_scr.at[slot], d_sem.at[slot]).wait()
        d = jnp.dot(u_scr[:], d_scr[slot], preferred_element_type=F32).astype(BF)
        half = d.shape[0] // 2
        keep_scr[slot] = d[:half]
        out_scr[n] = d[half:]

    @pl.when((n > 0) & (n <= nd))
    def _():
        m = n - 1
        to_mate(m).wait_recv()
        total = (keep_scr[lax.rem(m, 2)].astype(F32) + in_scr[m].astype(F32)).astype(BF)
        size = total.shape[0] // 2
        if cross:
            own_scr[m] = total[:size]
            far_scr[m] = total[size:]
        else:
            outs[0][:] = total[:size]
            outs[1][:] = total[size:]

    if cross:
        @pl.when(n > nd)
        def _():
            m = n - nd - 1
            to_far(m).wait_recv()
            outs[0][:] = (own_scr[m].astype(F32) + back_scr[m].astype(F32)).astype(BF)

    @pl.when(i == pl.num_programs(0) - 1)
    def _():
        def sent(k, carry):
            to_mate(k).wait_send()
            if cross:
                to_far(k).wait_send()
            return carry

        lax.fori_loop(0, nd, sent, 0)


def mlp(bs, first, rb, wg, wu, wd, call, cross=False, after=()):
    dim = bs[0].shape[1]
    rows = rb * len(bs)
    ffn = wg.shape[1]
    td = 512
    tn = td if rows <= td else td // 2
    nk, nd = ffn // tn, dim // td
    half = rows // 2
    lag = nk + 1 + nd * cross
    n_out = 1 if cross else 2
    tiles = pltpu.VMEM((nd, half, td), BF)
    sem = pltpu.SemaphoreType.DMA
    return pl.pallas_call(
        ordered(functools.partial(mlp_kernel, n_in=len(bs), first=first, rb=rb, tn=tn, td=td, nk=nk, nd=nd, cross=cross),
                len(bs) + 3, after),
        grid=(nd + lag,),
        in_specs=[ANY] * (len(bs) + 3 + len(after)),
        out_specs=[pl.BlockSpec((rb, td), lambda i: (0, jnp.clip(i - lag, 0, nd - 1)))] * n_out,
        out_shape=[jax.ShapeDtypeStruct((rb, dim), BF)] * n_out,
        scratch_shapes=[pltpu.VMEM((rows, dim), BF), pltpu.VMEM((rows, ffn), BF), pltpu.VMEM((2, 2, dim, tn), BF),
                        pltpu.VMEM((2, ffn, td), BF), pltpu.VMEM((2, half, td), BF), tiles, tiles]
        + [sem((n,)) for n in (len(bs), 2, 2, nd, nd)]
        + ([pltpu.VMEM((nd, rb, td), BF)] * 3 + [sem((nd,))] * 2 if cross else []),
        name="mlp",
        compiler_params=pltpu.CompilerParams(vmem_limit_bytes=VMEM, collective_id=call, has_side_effects=True),
        cost_estimate=cost(6 * rows * dim * ffn, 6 * dim * ffn),
    )(*bs, wg, wu, wd, *after)


def sum_kernel(*refs, n):
    *parts, y_ref, z_ref = refs[-2 - n:]
    total = sum(p[:].astype(F32) for p in parts).astype(BF)
    z_ref[:] = (y_ref[:].astype(F32) + total.astype(F32)).astype(BF)


def sum_rows(z, parts, y, y_first, first, total, after=(), tile=64):
    rows, dim = parts[0].shape
    at = lambda r0: pl.BlockSpec((tile, dim), lambda i: (r0 // tile + i, 0))
    prev = () if z is None else (z,)
    n = len(parts)
    return pl.pallas_call(
        ordered(functools.partial(sum_kernel, n=n), len(prev) + n + 1, after), grid=(rows // tile,),
        in_specs=[ANY] * len(prev) + [at(0)] * n + [at(y_first)] + [ANY] * len(after),
        out_specs=at(first),
        out_shape=jax.ShapeDtypeStruct((total, dim), BF),
        input_output_aliases={0: 0} if prev else {},
        name="zsum", compiler_params=PARAMS,
        cost_estimate=cost(rows * dim, rows * dim),
    )(*prev, *parts, y, *after)


def run_positions(xi, ci, y, cps, piece):
    def start(x, c):
        return (y if x == 0 else 2 * cps - 1 - y) * piece + c * (piece // 2)

    per = piece // 2 // RUN
    out = [start(xi, ci) + RUN * j for j in range(per)] + [start(xi, 1 - ci) + RUN * j for j in range(per)]
    for j in range(per):
        out += [start(1 - xi, ci) + RUN * j, start(1 - xi, 1 - ci) + RUN * j]
    return out


def block_list(tile, ids, diag):
    own = [] if diag is None else [diag]
    n_tail = (len(ids) + len(own)) % 4 or 4
    n_tail -= len(own)
    head, tail = ids[:len(ids) - n_tail], own + ids[len(ids) - n_tail:]
    blocks = [[0, head[i:i + 4], head[i:i + 4]] for i in range(0, len(head), 4)]
    fill = 4 - len(tail)
    keys = tail + [ids[-1] if ids else diag] * fill
    blocks.append([sum(1 << k for k, r in enumerate(keys) if r == diag), keys, tail + [-1] * fill])
    blocks[-1][0] |= LAST
    blocks[0][0] |= FIRST
    return [[tile, flags, 0] + keys + values for flags, keys, values in blocks]


def call_table(tiles, pairs, carry, idle):
    rows, most = [], 0
    carry = [c if pairs[t][0] or pairs[t][1] else idle for t, c in enumerate(carry)]
    for t, tile in enumerate(tiles):
        ids, own = pairs[t]
        if ids or own:
            mine = block_list(t, ids, tile if own else None)
            mine[0][1] |= CARRY if carry[t] else 0
            rows += mine
    for row in rows:
        most = max(most, max(row[3:7]) + 1)
        row[2] = most
    return [len(rows)] + carry + [v for row in rows for v in row], len(rows)


def work_tables(cps, piece):
    per = piece // 2 // RUN
    early, more = 2 * per + 2, 2 * per + 4
    stage = lambda r: 0 if r < early else 1
    soon_pair = lambda r, t: r < early and t < early or r < more and t in (0, 1, per, per + 1)
    calls = [(0, list(range(early)))]
    calls += [(1, [j, per + j, 2 * per + 2 * j, 2 * per + 2 * j + 1]) for j in range(per)]
    tabs, all_runs, sizes = [], [], []
    for y in range(cps):
        for xi in range(2):
            for ci in range(2):
                mine = run_positions(xi, ci, y, cps, piece)
                pos = mine + run_positions(xi, ci, 1 - y, cps, piece)
                all_runs.append(mine)
                tabs.append([])
                sizes.append([])
                for now, tiles in calls:
                    pairs, carry = [], []
                    for t in tiles:
                        seen = [r for r in range(len(pos)) if pos[r] < pos[t]]
                        when = {r: 0 if soon_pair(r, t) else 1 for r in seen}
                        late = list(when.values()).count(1) + stage(t)
                        soon = len(seen) + 1 - late
                        if late and soon % 4 <= -late % 4:
                            for r in [r for r in seen if not when[r]][:soon % 4]:
                                when[r] = 1
                        pairs.append(([r for r in seen if when[r] == now], stage(t) == now))
                        carry.append(int(stage(t) < now))
                    tab, n = call_table(tiles, pairs, carry, 2 if now == 1 else 0)
                    tabs[-1].append(tab)
                    sizes[-1].append(n)
    widths = [max(len(t[k]) for t in tabs) for k in range(len(calls))]
    flat = [[v for k, t in enumerate(tab) for v in t + [0] * (widths[k] - len(t))] for tab in tabs]
    bases = [sum(widths[:k]) for k in range(len(calls))]
    return np.array(flat, np.int32), np.array(all_runs, np.int32), bases, np.array(sizes).max(0) * 4


def solution(mesh):
    cps = mesh.shape['cp']
    row_spec = P('dp', ('cp', 'tp'), None)
    head_cols = P(None, 'tp', None)
    n_tp = mesh.shape['tp']

    over_core, over_x, over_both = (('tp', [(t, t ^ k) for t in range(n_tp)]) for k in (1, 2, 3))
    over_y = ('cp', [(i, i ^ 1) for i in range(cps)])

    def layer(x, g_attn, w_q, w_k, w_v, w_o, g_mlp, w_gate, w_up, w_down):
        x_rows = x[0]
        dim = x_rows.shape[1]
        n_run = x_rows.shape[0] // RUN
        piece = 2 * x_rows.shape[0]
        t_id, y_id = lax.axis_index('tp'), lax.axis_index('cp')
        np_tab, np_runs, bases, work = work_tables(cps, piece)
        dev = y_id * n_tp + t_id
        tab = lax.dynamic_index_in_dim(jnp.asarray(np_tab), dev, 0, keepdims=False)
        run_pos = lax.dynamic_index_in_dim(jnp.asarray(np_runs), dev, 0, keepdims=False)

        def tied(v, *others):
            return lax.optimization_barrier((v, *others))[0]

        def send(axis_pairs, v):
            return lax.ppermute(v, *axis_pairs)

        ga, gm = g_attn.reshape(1, dim), g_mlp.reshape(1, dim)
        own = list(norm_runs(x_rows, ga, [0]))
        own += norm_runs(x_rows, ga, list(range(1, n_run)), after=own)
        far = [send(over_x, own[j]) for j in range(n_run)]
        mate = [send(over_core, own[j]) for j in range(n_run)]

        w_all = jnp.concatenate([tied(w, own[-1]).reshape(dim, -1) for w in (w_q, w_k, w_v)], axis=1)
        row_pos = run_pos[:, None] + jnp.arange(RUN, dtype=jnp.int32)[None, :]
        tables = rope_tables(tied(row_pos[:2 * n_run], own[-1]))

        q_here, kv_here = qkv(own + mate, w_all, (tables, 0))
        kvs, q_far = [kv_here], []
        far_tables = rope_tables(tied(row_pos[2 * n_run:], kv_here))

        def far_qkv(j, after):
            here = tied(far[j], after)
            rows = [here, send(over_core, here)], w_all, (far_tables, 2 * j)
            if j + 1 < n_run:
                q, kv = qkv(*rows, after=(after,))
            else:
                kv, = qkv(*rows, False, after=(after,))
                q, = qkv(*rows, True, False, after=(kv, gm))
            q_far.append(q)
            kvs.append(kv)
            return kv

        far_qkv(1, far_qkv(0, kv_here))

        wo = w_o.reshape(-1, dim)
        half = wo.shape[0] // 2
        n_piece = 2
        rows = half // n_piece
        wo_c = send(over_core, tied(wo, kvs[-1]))

        tiles = [(0, i) for i in range(2 * n_run)] + [(1, i) for i in (0, 1)]
        st, *wo_x = flash(tab, [q_here, q_far[0]], tiles, kvs, base=bases[0], work=int(work[0]), cut=wo,
                         n_cut=n_piece)
        wo_x = [send(over_x, w) for w in wo_x]
        far_qkv(3, far_qkv(2, st))
        kvs = kvs + [send(over_y, kv) for kv in kvs]

        os, outs, prev = [], [], q_far[-1]
        wo_a, wo_ya, wo_yb = {}, {}, {}

        def forward_w(p):
            here = tied(wo_x[p], prev)
            wo_ya[p] = (here, send(over_core, here))
            wo_a[p] = send(over_y, here)

        def relay_w(p):
            here = tied(wo_a[p], prev)
            wo_yb[p] = (here, send(over_core, here))

        def attend(j):
            held = 2 * n_run + 2 * j
            carried = [j, n_run + j] + ([held, held + 1] if j == 0 else [None, None])
            pair = j % 2
            *o, done = flash(
                tab, [q_here, q_far[j]], [(0, j), (0, n_run + j), (1, 0), (1, 1)], kvs,
                base=bases[1 + j], work=int(work[1 + j]), st=st, st_src=carried, old=os.pop() if pair else None, slots=2,
                after=(prev,))
            if pair:
                o = [o[0], send(over_core, o[1]), send(over_x, o[2]), send(over_both, o[3])]
            os.append(o)
            return done

        def project(i):
            ws = [wo, wo_c]
            blocks = [[(a, r, half)] for a in (0, 1) for r in (0, half)]
            for k in range(2):
                for held in (wo_ya, wo_yb):
                    blocks.append([(len(ws) + p, 0, rows) for p in range(n_piece)])
                    ws += [held[p][k] for p in range(n_piece)]
            got = out_proj(os[i], ws, blocks, x_rows, gm, i, after=(prev,))
            for y, b in zip(got[::2], got[1::2]):
                outs.append((y, b, send(over_x, b), send(over_core, b)))
            return got[0]

        last = n_run - 1
        for j in range(last):
            prev = attend(j)
            if j < n_piece:
                forward_w(j)
            if j:
                relay_w(j - 1)
        prev = project(0)
        prev = attend(last)

        z, sums, relay = None, [], {}

        def relay_b(j):
            here = tied(outs[j][2], prev)
            relay[j] = (here, send(over_core, here))

        chunks = [(j, 0, RUN) for j in range(last)] + [(last, 0, RUN // 2), (last, RUN // 2, RUN // 2)]

        def finish(c):
            j, first, _ = chunks[c]
            return sum_rows(z, sums[c], outs[j][0], first, j * RUN + first, n_run * RUN,
                        after=() if prev is z else (prev,))

        relay_b(0)
        for c, (j, first, size) in enumerate(chunks):
            b = [outs[j][1], relay[j][0], outs[j][3], relay[j][1]]
            prev, *s_far = mlp(b, first, size, w_gate, w_up, w_down, c, c == n_run, after=(prev,))
            sums.append([prev] + [send(over_x, v) for v in s_far])
            if c < last:
                relay_b(c + 1)
            if c == 0:
                prev = project(1)
            elif c < n_run:
                prev = z = finish(c - 1)
        for c in (last, n_run):
            prev = z = finish(c)
        return z[None]

    return jax.shard_map(layer, mesh=mesh,
                         in_specs=(row_spec, P(), head_cols, head_cols, head_cols, P('tp', None, None),
                                   P(), P(None, 'tp'), P(None, 'tp'), P('tp', None)),
                         out_specs=row_spec, check_vma=False)
```

```python
import functools
import math
import jax
import jax.numpy as jnp
import numpy as np
from jax import lax
from jax.experimental import pallas as pl
from jax.experimental.pallas import tpu as pltpu
from jax.sharding import PartitionSpec as P

NORM_EPS = 1e-5
ROPE_THETA = 500000.0
HD = 128
RUN = 256
NEG = -1e30
LOG2E = math.log2(math.e)
DN = (((1,), (0,)), ((), ()))
BF = jnp.bfloat16
F32 = jnp.float32
ANY = pl.BlockSpec(memory_space=pltpu.HBM)


VMEM = 67043328
PARAMS = pltpu.CompilerParams(vmem_limit_bytes=VMEM)


def rope_tables(positions):
    half = HD // 2
    inv_freq = ROPE_THETA ** (-2.0 * jnp.arange(half, dtype=F32) / HD)
    angles = inv_freq[:, None] * positions.astype(F32)[..., None, :]
    return jnp.cos(angles), jnp.sin(angles)


def norm_rows(rows, gain):
    f = rows.astype(F32)
    mean_sq = jnp.mean(f * f, axis=-1, keepdims=True)
    return (f * lax.rsqrt(mean_sq + NORM_EPS) * gain.astype(F32)).astype(BF)


def cost(flops, moved):
    return pl.CostEstimate(flops=flops, transcendentals=0, bytes_accessed=moved)


def ordered(kernel, n_in, after):
    n = len(after)
    return lambda *refs: kernel(*refs[:n_in], *refs[n_in + n:])


def norm_kernel(x_ref, g_ref, *refs, per):
    for k, o_ref in enumerate(refs):
        @pl.when(lax.div(pl.program_id(0), per) == k)
        def _():
            o_ref[:] = norm_rows(x_ref[:], g_ref[:])


def norm_runs(x_rows, gain, runs, after=(), tile=128):
    dim = x_rows.shape[1]
    per = RUN // tile
    n = len(runs)
    return pl.pallas_call(
        ordered(functools.partial(norm_kernel, per=per), 2, after), grid=(n * per,),
        in_specs=[pl.BlockSpec((tile, dim), lambda i: (runs[0] * per + i, 0)), pl.BlockSpec((1, dim), lambda i: (0, 0))]
        + [ANY] * len(after),
        out_specs=[pl.BlockSpec((tile, dim), lambda i, k=k: (jnp.clip(i - k * per, 0, per - 1), 0)) for k in range(n)],
        out_shape=[jax.ShapeDtypeStruct((RUN, dim), BF)] * n,
        name="norm", compiler_params=PARAMS,
        cost_estimate=cost(n * RUN * dim, n * RUN * dim),
    )(x_rows, gain, *after)


def qkv_kernel(*refs, n_in, n_q, group, first, with_q, with_kv):
    a_refs = refs[:n_in]
    w_ref, cos_ref, sin_ref, *outs, a_scr, sem = refs[n_in:]
    q_ref, kv_ref = outs[0], outs[-1]
    n = pl.program_id(0) + first
    heads = w_ref.shape[1] // HD

    @pl.when(n == first)
    def _():
        for k, r in enumerate(a_refs):
            pltpu.make_async_copy(r, a_scr.at[pl.ds(k * RUN, RUN), :], sem.at[k]).start()

    def rope(f, i):
        f = f.astype(BF).astype(F32)
        lo, hi, cos, sin = f[:HD // 2], f[HD // 2:], cos_ref[i], sin_ref[i]
        return jnp.concatenate([lo * cos - hi * sin, hi * cos + lo * sin], axis=0)

    def one(k, carry):
        @pl.when(n == first)
        def _():
            for i in range(group):
                rows = pl.ds(pl.multiple_of((k * group + i) * RUN, RUN), RUN)
                pltpu.make_async_copy(a_scr.at[rows, :], a_scr.at[rows, :], sem.at[k * group + i]).wait()

        runs = [k * group + i for i in range(group)]

        def products():
            return [jnp.dot(a_scr[pl.ds(pl.multiple_of(run * RUN, RUN), RUN), :], w_ref[:], preferred_element_type=F32)
                    for run in runs]

        if with_q:
            @pl.when(n < n_q)
            def _():
                for run, r in zip(runs, products()):
                    for h in range(heads):
                        cols = slice(h * HD, (h + 1) * HD)
                        q_ref[run, cols, :] = rope(r[:, cols].T, run).astype(BF)

        if with_kv:
            @pl.when(n == n_q)
            def _():
                for run, r in zip(runs, products()):
                    for h in range(heads // 2):
                        cols, past = slice(h * HD, (h + 1) * HD), heads // 2 * HD
                        kv_ref[run, 0, :, cols] = rope(r[:, cols].T, run).T.astype(BF)
                        kv_ref[run, 1, cols, :] = r[:, past + h * HD:past + (h + 1) * HD].T.astype(BF)
        return carry

    lax.fori_loop(0, n_in // group, one, 0)


def qkv(rows, w_all, tables, with_q=True, with_kv=True, after=(), group=2):
    n_in = len(rows)
    dim = w_all.shape[0]
    tn = 512
    n_q = w_all.shape[1] // tn - 1
    (cos, sin), first_run = tables
    at = first_run // n_in
    start = 0 if with_q else n_q
    kv_shape = (n_in, 2, RUN, RUN)
    tab = pl.BlockSpec((n_in, HD // 2, RUN), lambda n: (at, 0, 0))
    return pl.pallas_call(
        ordered(functools.partial(qkv_kernel, n_in=n_in, n_q=n_q, group=group, first=start, with_q=with_q, with_kv=with_kv),
                n_in + 3, after),
        grid=(n_q * with_q + with_kv,),
        in_specs=[ANY] * n_in + [pl.BlockSpec((dim, tn), lambda n: (0, n + start)), tab, tab] + [ANY] * len(after),
        out_specs=[pl.BlockSpec((n_in, tn, RUN), lambda n: (0, jnp.minimum(n, n_q - 1), 0))] * with_q
        + [pl.BlockSpec(kv_shape, lambda n: (0,) * len(kv_shape))] * with_kv,
        out_shape=[jax.ShapeDtypeStruct((n_in, n_q * tn, RUN), BF)] * with_q + [jax.ShapeDtypeStruct(kv_shape, BF)] * with_kv,
        scratch_shapes=[pltpu.VMEM((n_in * RUN, dim), BF), pltpu.SemaphoreType.DMA((n_in,))],
        name="qkv", compiler_params=PARAMS,
        cost_estimate=cost(2 * n_in * RUN * w_all.size, 2 * w_all.size),
    )(*rows, w_all, cos, sin, *after)


BLK = 11
LAST, FIRST, CARRY = 16, 32, 64
ST = HD + 16


def flash_kernel(tab_ref, *refs, q_src, kv_src, n_q, n_kv, st_src, n_st, n_old, n_cut, slot, base, G, n_tiles, n_heads, final):
    qs, kvs, sts = refs[:n_q], refs[n_q:n_q + n_kv], refs[n_q + n_kv:n_q + n_kv + n_st]
    n_out = n_tiles + 1 if final else 1 + n_cut
    at = n_q + n_kv + n_st + n_old
    outs = refs[at:at + n_out]
    q_scr, kv_scr, o_scr, st_scr, s_scr, mb_scr, acc_scr, m_scr, l_scr, q_sem, kv_sem, o_sem, st_sem = refs[at + n_out:][:13]
    if n_cut:
        cut_ref, (cut_scr, cut_sem) = refs[at - 1], refs[-2:]
    T = RUN
    c = (HD ** -0.5) * LOG2E
    n_blocks = tab_ref[base]
    carried = base + 1
    row0 = carried + n_tiles
    null = len(kv_src)

    q_copies = [pltpu.make_async_copy(qs[a].at[i], q_scr.at[t], q_sem.at[t]) for t, (a, i) in enumerate(q_src)]
    kv_copies = [pltpu.make_async_copy(kvs[a].at[i], kv_scr.at[r], kv_sem.at[r]) for r, (a, i) in enumerate(kv_src)]

    def load_state(t):
        if st_src[t] is not None:
            @pl.when(tab_ref[carried + t] != 0)
            def _():
                pltpu.make_async_copy(sts[0].at[st_src[t]], st_scr.at[t], st_sem.at[t]).start()

    q_copies[0].start()
    for cp in kv_copies[:4]:
        cp.start()
    load_state(0)
    for cp in kv_copies[4:]:
        cp.start()
    for t in range(1, n_tiles):
        q_copies[t].start()
        load_state(t)
    kv_scr[null, 1] = jnp.zeros((RUN, RUN), BF)
    if n_cut:
        cut_in = pltpu.make_async_copy(cut_ref.at[pl.ds(lax.axis_index('cp') * cut_scr.shape[0], cut_scr.shape[0]), :], cut_scr,
                                       cut_sem)
        part = cut_scr.shape[0] // n_cut
        cut_out = [pltpu.make_async_copy(cut_scr.at[pl.ds(k * part, part), :], outs[1 + k], cut_sem) for k in range(n_cut)]
        cut_in.start()

    def block(i):
        g = lax.div(i, n_blocks)
        return row0 + BLK * (i - g * n_blocks), g

    def arrived(have, need):
        def one(r, carry):
            pltpu.make_async_copy(kv_scr.at[r], kv_scr.at[r], kv_sem.at[r]).wait()
            return carry

        lax.fori_loop(have, need, one, 0)
        return jnp.maximum(have, need)

    def put(s, h, k):
        s_scr[h, pl.ds(k * RUN, RUN), :] = s
        mb_scr[h, k] = jnp.max(s.reshape(RUN // 8, 8, T), axis=0)

    def stage_a(row, g, h):
        col = pl.multiple_of(g * HD, HD)
        qt = q_scr[tab_ref[row], pl.ds(pl.multiple_of((g * G + h) * HD, HD), HD), :]
        for k in range(4):
            put(lax.dot_general(kv_scr[tab_ref[row + 3 + k], 0, :, pl.ds(col, HD)], qt, DN, preferred_element_type=F32), h, k)

    def stage_b(row, g, h):
        col = pl.multiple_of(g * HD, HD)
        m_prev = m_scr[h]
        mb = jnp.maximum(jnp.maximum(mb_scr[h, 0], mb_scr[h, 1]), jnp.maximum(mb_scr[h, 2], mb_scr[h, 3]))
        for r in (4, 2, 1):
            mb = jnp.maximum(mb, pltpu.roll(mb, r, 0))
        m_new = jnp.maximum(m_prev, mb)
        m_scr[h] = m_new
        m_c = m_new * c
        alpha = jnp.exp2(m_prev * c - m_c)
        l, pv = l_scr[h] * alpha, None
        for k in range(4):
            run = tab_ref[row + 7 + k]
            p = jnp.exp2(s_scr[h, k * RUN:(k + 1) * RUN].reshape(RUN // 8, 8, T) * c - m_c[None])
            l = l + jnp.sum(p, axis=0) * jnp.where(run < 0, 0.0, 1.0)
            d = lax.dot_general(kv_scr[jnp.where(run < 0, null, run), 1, pl.ds(col, HD), :], p.reshape(RUN, T).astype(BF), DN,
                                preferred_element_type=F32)
            pv = d if pv is None else pv + d
        l_scr[h] = l
        acc_scr[h] = (acc_scr[h].reshape(HD // 8, 8, T) * alpha[None]).reshape(HD, T) + pv

    def mask_runs(flags):
        seen = lax.broadcasted_iota(jnp.int32, (RUN, T), 0) <= lax.broadcasted_iota(jnp.int32, (RUN, T), 1)

        def one(k, carry):
            @pl.when((lax.shift_right_logical(flags, k) & 1) != 0)
            def _():
                rows = pl.multiple_of(k * RUN, RUN)
                for h in range(G):
                    put(jnp.where(seen, s_scr[h, pl.ds(rows, RUN), :], NEG), h, k)

            return carry

        lax.fori_loop(0, 4, one, 0)

    def finish(tile, g, get):
        for h in range(G):
            acc, l = get(h)
            o_scr[tile, :, pl.ds(pl.multiple_of((g * G + h) * HD, HD), HD)] = (acc / jnp.sum(l, axis=0, keepdims=True)).T.astype(BF)

        @pl.when(g == n_heads - 1)
        def _():
            for k in range(n_tiles):
                @pl.when(tile == k)
                def _():
                    pltpu.make_async_copy(o_scr.at[k], outs[k].at[slot], o_sem.at[k]).start()

    if final and n_st:
        def idle(i, carry):
            tile, g = lax.div(i, n_heads), lax.rem(i, n_heads)

            @pl.when(tab_ref[carried + tile] == 2)
            def _():
                @pl.when(g == 0)
                def _():
                    pltpu.make_async_copy(q_scr.at[tile], q_scr.at[tile], q_sem.at[tile]).wait()
                    pltpu.make_async_copy(st_scr.at[tile], st_scr.at[tile], st_sem.at[tile]).wait()

                finish(tile, g, lambda h: (st_scr[tile, g, h, :HD, :], st_scr[tile, g, h, HD + 8:, :]))

            return carry

        lax.fori_loop(0, n_tiles * n_heads, idle, 0)

    def query(row):
        t = tab_ref[row]
        pltpu.make_async_copy(q_scr.at[t], q_scr.at[t], q_sem.at[t]).wait()

    row, g = block(0)
    query(row)
    have = arrived(0, tab_ref[row + 2])
    for h in range(G):
        stage_a(row, g, h)

    def body(i, have):
        row, g = block(i)
        nrow, ng = block(jnp.minimum(i + 1, n_heads * n_blocks - 1))
        have = arrived(have, tab_ref[nrow + 2])
        flags = tab_ref[row + 1]
        tile = tab_ref[row]

        @pl.when((i + 1 < n_blocks) & ((tab_ref[nrow + 1] & FIRST) != 0))
        def _():
            query(nrow)

        @pl.when((flags & (FIRST | CARRY)) == FIRST)
        def _():
            acc_scr[:] = jnp.zeros_like(acc_scr)
            l_scr[:] = jnp.zeros_like(l_scr)
            m_scr[:] = jnp.full_like(m_scr, NEG)

        if n_st:
            @pl.when((flags & (FIRST | CARRY)) == (FIRST | CARRY))
            def _():
                @pl.when(g == 0)
                def _():
                    pltpu.make_async_copy(st_scr.at[tile], st_scr.at[tile], st_sem.at[tile]).wait()

                for h in range(G):
                    acc_scr[h] = st_scr[tile, g, h, :HD, :]
                    m_scr[h] = st_scr[tile, g, h, HD:HD + 8, :]
                    l_scr[h] = st_scr[tile, g, h, HD + 8:, :]

        if n_cut:
            @pl.when(i == n_blocks)
            def _():
                cut_in.wait()
                for cp in cut_out:
                    cp.start()

        @pl.when((flags & 15) != 0)
        def _():
            mask_runs(flags)

        for h in range(G):
            stage_b(row, g, h)
            stage_a(nrow, ng, h)

        @pl.when((flags & LAST) != 0)
        def _():
            if final:
                finish(tile, g, lambda h: (acc_scr[h], l_scr[h]))
            else:
                for h in range(G):
                    st_scr[tile, g, h, :HD, :] = acc_scr[h]
                    st_scr[tile, g, h, HD:HD + 8, :] = m_scr[h]
                    st_scr[tile, g, h, HD + 8:, :] = l_scr[h]

                @pl.when(g == n_heads - 1)
                def _():
                    pltpu.make_async_copy(st_scr.at[tile], outs[0].at[tile], o_sem.at[tile]).start()

        return have

    have = lax.fori_loop(0, n_heads * n_blocks, body, have)
    arrived(have, len(kv_src))
    if final:
        for k in range(n_tiles):
            pltpu.make_async_copy(o_scr.at[k], outs[k].at[slot], o_sem.at[k]).wait()
    else:
        def wait_out(i, carry):
            row = row0 + BLK * i

            @pl.when((tab_ref[row + 1] & LAST) != 0)
            def _():
                t = tab_ref[row]
                pltpu.make_async_copy(st_scr.at[t], st_scr.at[t], o_sem.at[t]).wait()

            return carry

        lax.fori_loop(0, n_blocks, wait_out, 0)
        for cp in cut_out:
            cp.wait()


def flash(tab, qs, q_src, kvs, *, base, work, st=None, st_src=None, old=None, cut=None, n_cut=0, slots=1, after=()):
    nq = qs[0].shape[1]
    n_heads = 2
    G = nq // HD // n_heads
    n_tiles = len(q_src)
    final = cut is None
    kv_src = [(a, i) for a, kv in enumerate(kvs) for i in range(kv.shape[0])]
    n_runs = len(kv_src)
    sts = () if st is None else (st,)
    old = old or ()
    more = (*old, *(() if final else (cut,)))
    n_in = 1 + len(qs) + len(kvs) + len(sts) + len(more)
    state = (n_heads, G, ST, RUN)
    has_st = not final or sts
    if final:
        out_shape = [jax.ShapeDtypeStruct((slots, RUN, nq), BF)] * n_tiles + [jax.ShapeDtypeStruct((8, HD), F32)]
        scratch = []
    else:
        half = cut.shape[0] // 2
        out_shape = [jax.ShapeDtypeStruct((n_tiles, *state), F32)]
        out_shape += [jax.ShapeDtypeStruct((half // n_cut, cut.shape[1]), BF)] * n_cut
        scratch = [pltpu.VMEM((half, cut.shape[1]), BF), pltpu.SemaphoreType.DMA]
    return pl.pallas_call(
        ordered(functools.partial(flash_kernel, q_src=q_src, kv_src=kv_src, n_q=len(qs), n_kv=len(kvs),
                                  st_src=st_src or [None] * n_tiles, n_st=len(sts), n_old=len(more), n_cut=n_cut,
                                  slot=slots - 1 if old else 0, base=base, G=G, n_tiles=n_tiles, n_heads=n_heads, final=final),
                n_in, after),
        grid_spec=pltpu.PrefetchScalarGridSpec(
            num_scalar_prefetch=1, grid=(),
            in_specs=[ANY] * (n_in - 1 + len(after)),
            out_specs=[ANY] * len(out_shape),
            scratch_shapes=[pltpu.VMEM((n_tiles, nq, RUN), BF),
                            pltpu.VMEM((n_runs + 1, 2, RUN, RUN), BF),
                            pltpu.VMEM((n_tiles if final else 1, RUN, nq), BF),
                            pltpu.VMEM((n_tiles if has_st else 1, *state), F32),
                            pltpu.VMEM((G, 4 * RUN, RUN), F32),
                            pltpu.VMEM((G, 4, 8, RUN), F32),
                            pltpu.VMEM((G, HD, RUN), F32),
                            pltpu.VMEM((G, 8, RUN), F32),
                            pltpu.VMEM((G, 8, RUN), F32),
                            pltpu.SemaphoreType.DMA((n_tiles,)),
                            pltpu.SemaphoreType.DMA((n_runs,)),
                            pltpu.SemaphoreType.DMA((n_tiles,)),
                            pltpu.SemaphoreType.DMA((n_tiles,)), *scratch]),
        out_shape=out_shape,
        input_output_aliases={n_in - len(old) + k: k for k in range(len(old))},
        name="flash" if final else "flash_part", compiler_params=PARAMS,
        cost_estimate=cost(8 * work * RUN * RUN * nq, n_runs * RUN * nq),
    )(tab, *qs, *kvs, *sts, *more, *after)


def out_kernel(*refs, blocks, n_w, n_run, at):
    n_o, n_out = 4, 2 * n_run
    o_refs, w_refs, x_ref, g_ref = refs[:n_o], refs[n_o:n_o + n_w], refs[n_o + n_w], refs[n_o + n_w + 1]
    outs = refs[n_o + n_w + 2:n_o + n_w + 2 + n_out]
    o_scr, w_scr, x_scr, acc_scr, o_sem, w_sem, x_sem, out_sem = refs[n_o + n_w + 2 + n_out:]
    width = o_refs[0].shape[-1]
    half = width // 2
    n_slots = w_scr.shape[0]

    def fetch(k):
        for i, pieces in enumerate(blocks):
            @pl.when(k == i)
            def _():
                to = 0
                for a, r0, n in pieces:
                    pltpu.make_async_copy(w_refs[a].at[pl.ds(r0, n), :], w_scr.at[i % n_slots, pl.ds(to, n), :],
                                          w_sem.at[i % n_slots]).start()
                    to += n

    mine = lax.axis_index('cp')
    loads = [[] for _ in blocks]
    for i in range(n_run):
        rows = pl.ds(i * RUN, RUN)
        for k in range(4):
            src = o_refs[k].at[i]
            if k < 2:
                loads[2 * k].append((src, o_scr.at[rows, pl.ds(k * width, width)]))
            else:
                for p, part in enumerate((mine, 1 - mine)):
                    loads[2 * k + p].append((src.at[:, pl.ds(pl.multiple_of(part * half, half), half)],
                                             o_scr.at[rows, pl.ds(k * width + p * half, half)]))
    copies = [[pltpu.make_async_copy(src, dst, o_sem.at[k, i]) for i, (src, dst) in enumerate(ls)] for k, ls in enumerate(loads)]
    x_copy = pltpu.make_async_copy(x_ref.at[pl.ds(at * n_run * RUN, n_run * RUN), :], x_scr, x_sem)
    for cp in copies[0]:
        cp.start()
    for i in range(n_slots - 1):
        fetch(jnp.int32(i))
    for ls in copies[1:]:
        for cp in ls:
            cp.start()
    x_copy.start()
    acc_scr[:] = jnp.zeros_like(acc_scr)

    def one(k, carry):
        fetch(k + n_slots - 1)
        for i, ls in enumerate(copies):
            if ls:
                @pl.when(k == i)
                def _():
                    for cp in ls:
                        cp.wait()
        slot = lax.rem(k, n_slots)
        pltpu.make_async_copy(w_scr.at[slot], w_scr.at[slot], w_sem.at[slot]).wait()
        acc_scr[:] += jnp.dot(o_scr[:, pl.ds(pl.multiple_of(k * half, half), half)], w_scr[slot], preferred_element_type=F32)
        return carry

    lax.fori_loop(0, len(blocks), one, 0)
    x_copy.wait()

    strip = 32

    def one_strip(r, carry):
        rows = pl.ds(pl.multiple_of(r * strip, strip), strip)
        y = (x_scr[rows, :].astype(F32) + acc_scr[rows, :].astype(BF).astype(F32)).astype(BF)
        x_scr[rows, :] = y
        o_scr[rows, :] = norm_rows(y, g_ref[:])
        return carry

    stores, per = [], RUN // strip
    for i in range(n_run):
        lax.fori_loop(i * per, (i + 1) * per, one_strip, 0)
        for k, scr in enumerate((x_scr, o_scr)):
            stores.append(pltpu.make_async_copy(scr.at[pl.ds(i * RUN, RUN), :], outs[2 * i + k], out_sem.at[2 * i + k]))
            stores[-1].start()
    for cp in stores:
        cp.wait()


def out_proj(os, ws, blocks, x_rows, gain, at, after=()):
    dim = x_rows.shape[1]
    n_run, _, width = os[0].shape
    rows = n_run * RUN
    return pl.pallas_call(
        ordered(functools.partial(out_kernel, blocks=blocks, n_w=len(ws), n_run=n_run, at=at),
                len(os) + len(ws) + 2, after),
        grid=(1,),
        in_specs=[ANY] * (len(os) + len(ws) + 1) + [pl.BlockSpec((1, dim), lambda i: (0, 0))] + [ANY] * len(after),
        out_specs=[ANY] * (2 * n_run),
        out_shape=[jax.ShapeDtypeStruct((RUN, dim), BF)] * (2 * n_run),
        scratch_shapes=[pltpu.VMEM((rows, 4 * width), BF), pltpu.VMEM((3, width // 2, dim), BF), pltpu.VMEM((rows, dim), BF),
                        pltpu.VMEM((rows, dim), F32), pltpu.SemaphoreType.DMA((len(blocks), 2 * n_run)),
                        pltpu.SemaphoreType.DMA((3,)), pltpu.SemaphoreType.DMA, pltpu.SemaphoreType.DMA((2 * n_run,))],
        name="outp", compiler_params=PARAMS,
        cost_estimate=cost(8 * rows * width * dim, 8 * width * dim),
    )(*os, *ws, x_rows, gain, *after)


def mlp_kernel(*refs, n_in, first, rb, tn, td, nk, nd, cross):
    b_refs = refs[:n_in]
    wg_ref, wu_ref, wd_ref, *outs = refs[n_in:n_in + (4 if cross else 5)]
    (b_scr, u_scr, w_scr, d_scr, keep_scr, out_scr, in_scr, b_sem, w_sem, d_sem, out_sem, in_sem,
     rows_sem, *more) = refs[n_in + (4 if cross else 5):]
    i = pl.program_id(0)
    me = lax.axis_index('tp')
    mate = {'tp': me + 1 - 2 * lax.rem(me, 2)}
    peers = [mate]
    if cross:
        own_scr, far_scr, back_scr, far_sem, back_sem = more
        half_tp = lax.axis_size('tp') // 2
        peers.append({'tp': lax.rem(me + half_tp, 2 * half_tp)})
    barrier = pltpu.get_barrier_semaphore()

    def fetch(j):
        @pl.when(j < nk)
        def _():
            slot, cols = lax.rem(j, 2), pl.ds(pl.multiple_of(j * tn, tn), tn)
            for k, w in enumerate((wg_ref, wu_ref)):
                pltpu.make_async_copy(w.at[:, cols], w_scr.at[slot, k], w_sem.at[slot]).start()

        @pl.when((j >= nk) & (j < nk + nd))
        def _():
            n, slot = j - nk, lax.rem(j - nk, 2)
            pltpu.make_async_copy(wd_ref.at[:, pl.ds(pl.multiple_of(n * td, td), td)], d_scr.at[slot], d_sem.at[slot]).start()

    def gated(rows, cols, slot):
        b = b_scr[rows, :]
        gate = jnp.dot(b, w_scr[slot, 0], preferred_element_type=F32)
        up = jnp.dot(b, w_scr[slot, 1], preferred_element_type=F32)
        u_scr[rows, cols] = (jax.nn.silu(gate) * up).astype(BF)

    def to_mate(n):
        return pltpu.make_async_remote_copy(src_ref=out_scr.at[n], dst_ref=in_scr.at[n], send_sem=out_sem.at[n],
                                            recv_sem=in_sem.at[n], device_id=mate, device_id_type=pl.DeviceIdType.MESH)

    def to_far(n):
        return pltpu.make_async_remote_copy(src_ref=far_scr.at[n], dst_ref=back_scr.at[n], send_sem=far_sem.at[n],
                                            recv_sem=back_sem.at[n], device_id=peers[-1], device_id_type=pl.DeviceIdType.MESH)

    def rows_to_mate(n):
        return pltpu.make_async_remote_copy(
            src_ref=b_refs[n].at[pl.ds(first, rb), :], dst_ref=b_scr.at[pl.ds((n_in + n) * rb, rb), :],
            send_sem=rows_sem.at[n], recv_sem=b_sem.at[n_in + n], device_id=mate, device_id_type=pl.DeviceIdType.MESH)

    @pl.when(i == 0)
    def _():
        copies = [pltpu.make_async_copy(r.at[pl.ds(first, rb), :], b_scr.at[pl.ds(k * rb, rb), :], b_sem.at[k])
                  for k, r in enumerate(b_refs)]
        for peer in peers:
            pl.semaphore_signal(barrier, inc=1, device_id=peer, device_id_type=pl.DeviceIdType.MESH)
        copies[0].start()
        fetch(i)
        for cp in copies[1:]:
            cp.start()
        pl.semaphore_wait(barrier, len(peers))
        for n in range(n_in):
            rows_to_mate(n).start()

    fetch(i + 1)

    @pl.when(i < nk)
    def _():
        slot = lax.rem(i, 2)
        pltpu.make_async_copy(w_scr.at[slot], w_scr.at[slot], w_sem.at[slot]).wait()

    @pl.when(i == 0)
    def _():
        def one(k, carry):
            rows = pl.ds(pl.multiple_of(k * rb, rb), rb)
            pltpu.make_async_copy(b_scr.at[rows, :], b_scr.at[rows, :], b_sem.at[k]).wait()
            gated(rows, pl.ds(0, tn), 0)
            return carry

        lax.fori_loop(0, 2 * n_in, one, 0)

    @pl.when((i > 0) & (i < nk))
    def _():
        gated(slice(None), pl.ds(pl.multiple_of(i * tn, tn), tn), lax.rem(i, 2))

    n = i - nk

    @pl.when((n > 0) & (n <= nd))
    def _():
        to_mate(n - 1).start()

    if cross:
        @pl.when((n > 1) & (n <= nd + 1))
        def _():
            to_far(n - 2).start()

    @pl.when((n >= 0) & (n < nd))
    def _():
        slot = lax.rem(n, 2)
        pltpu.make_async_copy(d_scr.at[slot], d_scr.at[slot], d_sem.at[slot]).wait()
        d = jnp.dot(u_scr[:], d_scr[slot], preferred_element_type=F32).astype(BF)
        half = d.shape[0] // 2
        keep_scr[slot] = d[:half]
        out_scr[n] = d[half:]

    @pl.when((n > 0) & (n <= nd))
    def _():
        m = n - 1
        to_mate(m).wait_recv()
        total = (keep_scr[lax.rem(m, 2)].astype(F32) + in_scr[m].astype(F32)).astype(BF)
        size = total.shape[0] // 2
        if cross:
            own_scr[m] = total[:size]
            far_scr[m] = total[size:]
        else:
            outs[0][:] = total[:size]
            outs[1][:] = total[size:]

    if cross:
        @pl.when(n > nd)
        def _():
            m = n - nd - 1
            to_far(m).wait_recv()
            outs[0][:] = (own_scr[m].astype(F32) + back_scr[m].astype(F32)).astype(BF)

    @pl.when(i == pl.num_programs(0) - 1)
    def _():
        def sent(k, carry):
            to_mate(k).wait_send()
            if cross:
                to_far(k).wait_send()
            return carry

        lax.fori_loop(0, nd, sent, 0)
        for k in range(n_in):
            rows_to_mate(k).wait_send()


def mlp(bs, first, rb, wg, wu, wd, call, cross=False, after=()):
    dim = bs[0].shape[1]
    rows = 2 * rb * len(bs)
    ffn = wg.shape[1]
    td = 512
    tn = td if rows <= td else td // 2
    nk, nd = ffn // tn, dim // td
    half = rows // 2
    lag = nk + 1 + nd * cross
    n_out = 1 if cross else 2
    tiles = pltpu.VMEM((nd, half, td), BF)
    sem = pltpu.SemaphoreType.DMA
    return pl.pallas_call(
        ordered(functools.partial(mlp_kernel, n_in=len(bs), first=first, rb=rb, tn=tn, td=td, nk=nk, nd=nd, cross=cross),
                len(bs) + 3, after),
        grid=(nd + lag,),
        in_specs=[ANY] * (len(bs) + 3 + len(after)),
        out_specs=[pl.BlockSpec((rb, td), lambda i: (0, jnp.clip(i - lag, 0, nd - 1)))] * n_out,
        out_shape=[jax.ShapeDtypeStruct((rb, dim), BF)] * n_out,
        scratch_shapes=[pltpu.VMEM((rows, dim), BF), pltpu.VMEM((rows, ffn), BF), pltpu.VMEM((2, 2, dim, tn), BF),
                        pltpu.VMEM((2, ffn, td), BF), pltpu.VMEM((2, half, td), BF), tiles, tiles]
        + [sem((n,)) for n in (2 * len(bs), 2, 2, nd, nd, len(bs))]
        + ([pltpu.VMEM((nd, rb, td), BF)] * 3 + [sem((nd,))] * 2 if cross else []),
        name="mlp",
        compiler_params=pltpu.CompilerParams(vmem_limit_bytes=VMEM, collective_id=call, has_side_effects=True),
        cost_estimate=cost(6 * rows * dim * ffn, 6 * dim * ffn),
    )(*bs, wg, wu, wd, *after)


def sum_kernel(*refs, n):
    *parts, y_ref, z_ref = refs[-2 - n:]
    total = sum(p[:].astype(F32) for p in parts).astype(BF)
    z_ref[:] = (y_ref[:].astype(F32) + total.astype(F32)).astype(BF)


def sum_rows(z, parts, y, y_first, first, total, after=(), tile=64):
    rows, dim = parts[0].shape
    at = lambda r0: pl.BlockSpec((tile, dim), lambda i: (r0 // tile + i, 0))
    prev = () if z is None else (z,)
    n = len(parts)
    return pl.pallas_call(
        ordered(functools.partial(sum_kernel, n=n), len(prev) + n + 1, after), grid=(rows // tile,),
        in_specs=[ANY] * len(prev) + [at(0)] * n + [at(y_first)] + [ANY] * len(after),
        out_specs=at(first),
        out_shape=jax.ShapeDtypeStruct((total, dim), BF),
        input_output_aliases={0: 0} if prev else {},
        name="zsum", compiler_params=PARAMS,
        cost_estimate=cost(rows * dim, rows * dim),
    )(*prev, *parts, y, *after)


def run_positions(xi, ci, y, cps, piece):
    def start(x, c):
        return (y if x == 0 else 2 * cps - 1 - y) * piece + c * (piece // 2)

    per = piece // 2 // RUN
    out = [start(xi, ci) + RUN * j for j in range(per)] + [start(xi, 1 - ci) + RUN * j for j in range(per)]
    for j in range(per):
        out += [start(1 - xi, ci) + RUN * j, start(1 - xi, 1 - ci) + RUN * j]
    return out


def block_list(tile, ids, diag):
    own = [] if diag is None else [diag]
    n_tail = (len(ids) + len(own)) % 4 or 4
    n_tail -= len(own)
    head, tail = ids[:len(ids) - n_tail], own + ids[len(ids) - n_tail:]
    blocks = [[0, head[i:i + 4], head[i:i + 4]] for i in range(0, len(head), 4)]
    fill = 4 - len(tail)
    keys = tail + [ids[-1] if ids else diag] * fill
    blocks.append([sum(1 << k for k, r in enumerate(keys) if r == diag), keys, tail + [-1] * fill])
    blocks[-1][0] |= LAST
    blocks[0][0] |= FIRST
    return [[tile, flags, 0] + keys + values for flags, keys, values in blocks]


def call_table(tiles, pairs, carry, idle):
    rows, most = [], 0
    carry = [c if pairs[t][0] or pairs[t][1] else idle for t, c in enumerate(carry)]
    for t, tile in enumerate(tiles):
        ids, own = pairs[t]
        if ids or own:
            mine = block_list(t, ids, tile if own else None)
            mine[0][1] |= CARRY if carry[t] else 0
            rows += mine
    for row in rows:
        most = max(most, max(row[3:7]) + 1)
        row[2] = most
    return [len(rows)] + carry + [v for row in rows for v in row], len(rows)


def work_tables(cps, piece):
    per = piece // 2 // RUN
    early, more = 2 * per + 2, 2 * per + 4
    stage = lambda r: 0 if r < early else 1
    soon_pair = lambda r, t: r < early and t < early or r < more and t in (0, 1, per, per + 1)
    calls = [(0, list(range(early)))]
    calls += [(1, [j, per + j, 2 * per + 2 * j, 2 * per + 2 * j + 1]) for j in range(per)]
    tabs, all_runs, sizes = [], [], []
    for y in range(cps):
        for xi in range(2):
            for ci in range(2):
                mine = run_positions(xi, ci, y, cps, piece)
                pos = mine + run_positions(xi, ci, 1 - y, cps, piece)
                all_runs.append(mine)
                tabs.append([])
                sizes.append([])
                for now, tiles in calls:
                    pairs, carry = [], []
                    for t in tiles:
                        seen = [r for r in range(len(pos)) if pos[r] < pos[t]]
                        when = {r: 0 if soon_pair(r, t) else 1 for r in seen}
                        late = list(when.values()).count(1) + stage(t)
                        soon = len(seen) + 1 - late
                        if late and soon % 4 <= -late % 4:
                            for r in [r for r in seen if not when[r]][:soon % 4]:
                                when[r] = 1
                        pairs.append(([r for r in seen if when[r] == now], stage(t) == now))
                        carry.append(int(stage(t) < now))
                    tab, n = call_table(tiles, pairs, carry, 2 if now == 1 else 0)
                    tabs[-1].append(tab)
                    sizes[-1].append(n)
    widths = [max(len(t[k]) for t in tabs) for k in range(len(calls))]
    flat = [[v for k, t in enumerate(tab) for v in t + [0] * (widths[k] - len(t))] for tab in tabs]
    bases = [sum(widths[:k]) for k in range(len(calls))]
    return np.array(flat, np.int32), np.array(all_runs, np.int32), bases, np.array(sizes).max(0) * 4


def solution(mesh):
    cps = mesh.shape['cp']
    row_spec = P('dp', ('cp', 'tp'), None)
    head_cols = P(None, 'tp', None)
    n_tp = mesh.shape['tp']

    over_core, over_x, over_both = (('tp', [(t, t ^ k) for t in range(n_tp)]) for k in (1, 2, 3))
    over_y = ('cp', [(i, i ^ 1) for i in range(cps)])

    def layer(x, g_attn, w_q, w_k, w_v, w_o, g_mlp, w_gate, w_up, w_down):
        x_rows = x[0]
        dim = x_rows.shape[1]
        n_run = x_rows.shape[0] // RUN
        piece = 2 * x_rows.shape[0]
        t_id, y_id = lax.axis_index('tp'), lax.axis_index('cp')
        np_tab, np_runs, bases, work = work_tables(cps, piece)
        dev = y_id * n_tp + t_id
        tab = lax.dynamic_index_in_dim(jnp.asarray(np_tab), dev, 0, keepdims=False)
        run_pos = lax.dynamic_index_in_dim(jnp.asarray(np_runs), dev, 0, keepdims=False)

        def tied(v, *others):
            return lax.optimization_barrier((v, *others))[0]

        def send(axis_pairs, v):
            return lax.ppermute(v, *axis_pairs)

        ga, gm = g_attn.reshape(1, dim), g_mlp.reshape(1, dim)
        own = list(norm_runs(x_rows, ga, [0]))
        own += norm_runs(x_rows, ga, list(range(1, n_run)), after=own)
        far = [send(over_x, own[j]) for j in range(n_run)]
        mate = [send(over_core, own[j]) for j in range(n_run)]

        w_all = jnp.concatenate([tied(w, own[-1]).reshape(dim, -1) for w in (w_q, w_k, w_v)], axis=1)
        row_pos = run_pos[:, None] + jnp.arange(RUN, dtype=jnp.int32)[None, :]
        tables = rope_tables(tied(row_pos[:2 * n_run], own[-1]))

        q_here, kv_here = qkv(own + mate, w_all, (tables, 0))
        kvs, q_far = [kv_here], []
        far_tables = rope_tables(tied(row_pos[2 * n_run:], kv_here))

        def far_qkv(j, after):
            here = tied(far[j], after)
            rows = [here, send(over_core, here)], w_all, (far_tables, 2 * j)
            if j + 1 < n_run:
                q, kv = qkv(*rows, after=(after,))
            else:
                kv, = qkv(*rows, False, after=(after,))
                q, = qkv(*rows, True, False, after=(kv, gm))
            q_far.append(q)
            kvs.append(kv)
            return kv

        far_qkv(1, far_qkv(0, kv_here))

        wo = w_o.reshape(-1, dim)
        half = wo.shape[0] // 2
        n_piece = 2
        rows = half // n_piece
        wo_c = send(over_core, tied(wo, kvs[-1]))

        tiles = [(0, i) for i in range(2 * n_run)] + [(1, i) for i in (0, 1)]
        st, *wo_x = flash(tab, [q_here, q_far[0]], tiles, kvs, base=bases[0], work=int(work[0]), cut=wo,
                         n_cut=n_piece)
        wo_x = [send(over_x, w) for w in wo_x]
        far_qkv(3, far_qkv(2, st))
        kvs = kvs + [send(over_y, kv) for kv in kvs]

        os, outs, prev = [], [], q_far[-1]
        wo_a, wo_ya, wo_yb = {}, {}, {}

        def forward_w(p):
            here = tied(wo_x[p], prev)
            wo_ya[p] = (here, send(over_core, here))
            wo_a[p] = send(over_y, here)

        def relay_w(p):
            here = tied(wo_a[p], prev)
            wo_yb[p] = (here, send(over_core, here))

        def attend(j):
            held = 2 * n_run + 2 * j
            carried = [j, n_run + j] + ([held, held + 1] if j == 0 else [None, None])
            pair = j % 2
            *o, done = flash(
                tab, [q_here, q_far[j]], [(0, j), (0, n_run + j), (1, 0), (1, 1)], kvs,
                base=bases[1 + j], work=int(work[1 + j]), st=st, st_src=carried, old=os.pop() if pair else None, slots=2,
                after=(prev,))
            if pair:
                o = [o[0], send(over_core, o[1]), send(over_x, o[2]), send(over_both, o[3])]
            os.append(o)
            return done

        def project(i):
            ws = [wo, wo_c]
            blocks = [[(a, r, half)] for a in (0, 1) for r in (0, half)]
            for k in range(2):
                for held in (wo_ya, wo_yb):
                    blocks.append([(len(ws) + p, 0, rows) for p in range(n_piece)])
                    ws += [held[p][k] for p in range(n_piece)]
            got = out_proj(os[i], ws, blocks, x_rows, gm, i, after=(prev,))
            for y, b in zip(got[::2], got[1::2]):
                outs.append((y, b, send(over_x, b)))
            return got[0]

        last = n_run - 1
        for j in range(last):
            prev = attend(j)
            if j < n_piece:
                forward_w(j)
            if j:
                relay_w(j - 1)
        prev = project(0)
        prev = attend(last)

        z, sums = None, []

        chunks = [(j, 0, RUN) for j in range(last)] + [(last, 0, RUN // 2), (last, RUN // 2, RUN // 2)]

        def finish(c):
            j, first, _ = chunks[c]
            return sum_rows(z, sums[c], outs[j][0], first, j * RUN + first, n_run * RUN,
                        after=() if prev is z else (prev,))

        for c, (j, first, size) in enumerate(chunks):
            prev, *s_far = mlp(outs[j][1:], first, size, w_gate, w_up, w_down, c, c == n_run, after=(prev,))
            sums.append([prev] + [send(over_x, v) for v in s_far])
            if c == 0:
                prev = project(1)
            elif c < n_run:
                prev = z = finish(c - 1)
        for c in (last, n_run):
            prev = z = finish(c)
        return z[None]

    return jax.shard_map(layer, mesh=mesh,
                         in_specs=(row_spec, P(), head_cols, head_cols, head_cols, P('tp', None, None),
                                   P(), P(None, 'tp'), P(None, 'tp'), P('tp', None)),
                         out_specs=row_spec, check_vma=False)
```

```python
import functools
import math
import jax
import jax.numpy as jnp
import numpy as np
from jax import lax
from jax.experimental import pallas as pl
from jax.experimental.pallas import tpu as pltpu
from jax.sharding import PartitionSpec as P

NORM_EPS = 1e-5
ROPE_THETA = 500000.0
HD = 128
RUN = 256
NEG = -1e30
LOG2E = math.log2(math.e)
DN = (((1,), (0,)), ((), ()))
BF = jnp.bfloat16
F32 = jnp.float32
ANY = pl.BlockSpec(memory_space=pltpu.HBM)


VMEM = 67043328
PAIR = (0, 1)
PARAMS = pltpu.CompilerParams(vmem_limit_bytes=VMEM)


def rope_tables(positions):
    half = HD // 2
    inv_freq = ROPE_THETA ** (-2.0 * jnp.arange(half, dtype=F32) / HD)
    angles = inv_freq[:, None] * positions.astype(F32)[..., None, :]
    return jnp.cos(angles), jnp.sin(angles)


def norm_rows(rows, gain):
    f = rows.astype(F32)
    mean_sq = jnp.mean(f * f, axis=-1, keepdims=True)
    return (f * lax.rsqrt(mean_sq + NORM_EPS) * gain.astype(F32)).astype(BF)


def other_core():
    me = lax.axis_index('tp')
    return {'tp': me + 1 - 2 * lax.rem(me, 2)}


def cost(flops, moved):
    return pl.CostEstimate(flops=flops, transcendentals=0, bytes_accessed=moved)


def ordered(kernel, n_in, after):
    n = len(after)
    return lambda *refs: kernel(*refs[:n_in], *refs[n_in + n:])


def norm_kernel(x_ref, g_ref, *refs, per):
    for k, o_ref in enumerate(refs):
        @pl.when(lax.div(pl.program_id(0), per) == k)
        def _():
            o_ref[:] = norm_rows(x_ref[:], g_ref[:])


def norm_runs(x_rows, gain, runs, after=(), tile=128):
    dim = x_rows.shape[1]
    per = RUN // tile
    n = len(runs)
    return pl.pallas_call(
        ordered(functools.partial(norm_kernel, per=per), 2, after), grid=(n * per,),
        in_specs=[pl.BlockSpec((tile, dim), lambda i: (runs[0] * per + i, 0)), pl.BlockSpec((1, dim), lambda i: (0, 0))]
        + [ANY] * len(after),
        out_specs=[pl.BlockSpec((tile, dim), lambda i, k=k: (jnp.clip(i - k * per, 0, per - 1), 0)) for k in range(n)],
        out_shape=[jax.ShapeDtypeStruct((RUN, dim), BF)] * n,
        name="norm", compiler_params=PARAMS,
        cost_estimate=cost(n * RUN * dim, n * RUN * dim),
    )(x_rows, gain, *after)


def qkv_kernel(*refs, n_in, n_q, group, first, with_q, with_kv):
    a_refs = refs[:n_in]
    w_ref, cos_ref, sin_ref, *outs, a_scr, sem = refs[n_in:]
    q_ref, kv_ref = outs[0], outs[-1]
    n = pl.program_id(0) + first
    heads = w_ref.shape[1] // HD

    @pl.when(n == first)
    def _():
        for k, r in enumerate(a_refs):
            pltpu.make_async_copy(r, a_scr.at[pl.ds(k * RUN, RUN), :], sem.at[k]).start()

    def rope(f, i):
        f = f.astype(BF).astype(F32)
        lo, hi, cos, sin = f[:HD // 2], f[HD // 2:], cos_ref[i], sin_ref[i]
        return jnp.concatenate([lo * cos - hi * sin, hi * cos + lo * sin], axis=0)

    def one(k, carry):
        @pl.when(n == first)
        def _():
            for i in range(group):
                rows = pl.ds(pl.multiple_of((k * group + i) * RUN, RUN), RUN)
                pltpu.make_async_copy(a_scr.at[rows, :], a_scr.at[rows, :], sem.at[k * group + i]).wait()

        runs = [k * group + i for i in range(group)]

        def products():
            return [jnp.dot(a_scr[pl.ds(pl.multiple_of(run * RUN, RUN), RUN), :], w_ref[:], preferred_element_type=F32)
                    for run in runs]

        if with_q:
            @pl.when(n < n_q)
            def _():
                for run, r in zip(runs, products()):
                    for h in range(heads):
                        cols = slice(h * HD, (h + 1) * HD)
                        q_ref[run, cols, :] = rope(r[:, cols].T, run).astype(BF)

        if with_kv:
            @pl.when(n == n_q)
            def _():
                for run, r in zip(runs, products()):
                    for h in range(heads // 2):
                        cols, past = slice(h * HD, (h + 1) * HD), heads // 2 * HD
                        kv_ref[run, 0, :, cols] = rope(r[:, cols].T, run).T.astype(BF)
                        kv_ref[run, 1, cols, :] = r[:, past + h * HD:past + (h + 1) * HD].T.astype(BF)
        return carry

    lax.fori_loop(0, n_in // group, one, 0)


def qkv(rows, w_all, tables, with_q=True, with_kv=True, after=()):
    n_in = len(rows)
    dim = w_all.shape[0]
    tn = 512
    n_q = w_all.shape[1] // tn - 1
    (cos, sin), first_run = tables
    group = 2
    at = first_run // n_in
    start = 0 if with_q else n_q
    kv_shape = (n_in, 2, RUN, RUN)
    tab = pl.BlockSpec((n_in, HD // 2, RUN), lambda n: (at, 0, 0))
    return pl.pallas_call(
        ordered(functools.partial(qkv_kernel, n_in=n_in, n_q=n_q, group=group, first=start, with_q=with_q, with_kv=with_kv),
                n_in + 3, after),
        grid=(n_q * with_q + with_kv,),
        in_specs=[ANY] * n_in + [pl.BlockSpec((dim, tn), lambda n: (0, n + start)), tab, tab] + [ANY] * len(after),
        out_specs=[pl.BlockSpec((n_in, tn, RUN), lambda n: (0, jnp.minimum(n, n_q - 1), 0))] * with_q
        + [pl.BlockSpec(kv_shape, lambda n: (0,) * len(kv_shape))] * with_kv,
        out_shape=[jax.ShapeDtypeStruct((n_in, n_q * tn, RUN), BF)] * with_q + [jax.ShapeDtypeStruct(kv_shape, BF)] * with_kv,
        scratch_shapes=[pltpu.VMEM((n_in * RUN, dim), BF), pltpu.SemaphoreType.DMA((n_in,))],
        name="qkv", compiler_params=PARAMS,
        cost_estimate=cost(2 * n_in * RUN * w_all.size, 2 * w_all.size),
    )(*rows, w_all, cos, sin, *after)


BLK = 11
LAST, FIRST, CARRY = 16, 32, 64
ST = HD + 16


def flash_kernel(tab_ref, *refs, q_src, kv_src, n_q, n_kv, st_src, n_st, n_old, n_cut, slot, base, G, n_tiles, n_heads, final):
    qs, kvs, sts = refs[:n_q], refs[n_q:n_q + n_kv], refs[n_q + n_kv:n_q + n_kv + n_st]
    n_out = n_tiles + 1 if final else 1 + n_cut
    at = n_q + n_kv + n_st + n_old
    outs = refs[at:at + n_out]
    q_scr, kv_scr, o_scr, st_scr, s_scr, mb_scr, acc_scr, m_scr, l_scr, q_sem, kv_sem, o_sem, st_sem = refs[at + n_out:][:13]
    if n_cut:
        cut_ref, (cut_scr, cut_sem) = refs[at - 1], refs[-2:]
    T = RUN
    c = (HD ** -0.5) * LOG2E
    n_blocks = tab_ref[base]
    carried = base + 1
    row0 = carried + n_tiles
    null = len(kv_src)

    q_copies = [pltpu.make_async_copy(qs[a].at[i], q_scr.at[t], q_sem.at[t]) for t, (a, i) in enumerate(q_src)]
    kv_copies = [pltpu.make_async_copy(kvs[a].at[i], kv_scr.at[r], kv_sem.at[r]) for r, (a, i) in enumerate(kv_src)]

    def load_state(t):
        if st_src[t] is not None:
            @pl.when(tab_ref[carried + t] != 0)
            def _():
                pltpu.make_async_copy(sts[0].at[st_src[t]], st_scr.at[t], st_sem.at[t]).start()

    q_copies[0].start()
    for cp in kv_copies[:4]:
        cp.start()
    load_state(0)
    for cp in kv_copies[4:]:
        cp.start()
    for t in range(1, n_tiles):
        q_copies[t].start()
        load_state(t)
    kv_scr[null, 1] = jnp.zeros((RUN, RUN), BF)
    if n_cut:
        cut_in = pltpu.make_async_copy(cut_ref.at[pl.ds(lax.axis_index('cp') * cut_scr.shape[0], cut_scr.shape[0]), :], cut_scr,
                                       cut_sem)
        part = cut_scr.shape[0] // n_cut
        cut_out = [pltpu.make_async_copy(cut_scr.at[pl.ds(k * part, part), :], outs[1 + k], cut_sem) for k in range(n_cut)]
        cut_in.start()

    def block(i):
        g = lax.div(i, n_blocks)
        return row0 + BLK * (i - g * n_blocks), g

    def arrived(have, need):
        def one(r, carry):
            pltpu.make_async_copy(kv_scr.at[r], kv_scr.at[r], kv_sem.at[r]).wait()
            return carry

        lax.fori_loop(have, need, one, 0)
        return jnp.maximum(have, need)

    def put(s, h, k):
        s_scr[h, pl.ds(k * RUN, RUN), :] = s
        mb_scr[h, k] = jnp.max(s.reshape(RUN // 8, 8, T), axis=0)

    def stage_a(row, g, h):
        col = pl.multiple_of(g * HD, HD)
        qt = q_scr[tab_ref[row], pl.ds(pl.multiple_of((g * G + h) * HD, HD), HD), :]
        for k in range(4):
            put(lax.dot_general(kv_scr[tab_ref[row + 3 + k], 0, :, pl.ds(col, HD)], qt, DN, preferred_element_type=F32), h, k)

    def stage_b(row, g, h):
        col = pl.multiple_of(g * HD, HD)
        m_prev = m_scr[h]
        mb = jnp.maximum(jnp.maximum(mb_scr[h, 0], mb_scr[h, 1]), jnp.maximum(mb_scr[h, 2], mb_scr[h, 3]))
        for r in (4, 2, 1):
            mb = jnp.maximum(mb, pltpu.roll(mb, r, 0))
        m_new = jnp.maximum(m_prev, mb)
        m_scr[h] = m_new
        m_c = m_new * c
        alpha = jnp.exp2(m_prev * c - m_c)
        l, pv = l_scr[h] * alpha, None
        for k in range(4):
            run = tab_ref[row + 7 + k]
            p = jnp.exp2(s_scr[h, k * RUN:(k + 1) * RUN].reshape(RUN // 8, 8, T) * c - m_c[None])
            l = l + jnp.sum(p, axis=0) * jnp.where(run < 0, 0.0, 1.0)
            d = lax.dot_general(kv_scr[jnp.where(run < 0, null, run), 1, pl.ds(col, HD), :], p.reshape(RUN, T).astype(BF), DN,
                                preferred_element_type=F32)
            pv = d if pv is None else pv + d
        l_scr[h] = l
        acc_scr[h] = (acc_scr[h].reshape(HD // 8, 8, T) * alpha[None]).reshape(HD, T) + pv

    def mask_runs(flags):
        seen = lax.broadcasted_iota(jnp.int32, (RUN, T), 0) <= lax.broadcasted_iota(jnp.int32, (RUN, T), 1)

        def one(k, carry):
            @pl.when((lax.shift_right_logical(flags, k) & 1) != 0)
            def _():
                rows = pl.multiple_of(k * RUN, RUN)
                for h in range(G):
                    put(jnp.where(seen, s_scr[h, pl.ds(rows, RUN), :], NEG), h, k)

            return carry

        lax.fori_loop(0, 4, one, 0)

    def finish(tile, g, get):
        for h in range(G):
            acc, l = get(h)
            o_scr[tile, :, pl.ds(pl.multiple_of((g * G + h) * HD, HD), HD)] = (acc / jnp.sum(l, axis=0, keepdims=True)).T.astype(BF)

        @pl.when(g == n_heads - 1)
        def _():
            for k in range(n_tiles):
                @pl.when(tile == k)
                def _():
                    pltpu.make_async_copy(o_scr.at[k], outs[k].at[slot], o_sem.at[k]).start()

    if final and n_st:
        def idle(i, carry):
            tile, g = lax.div(i, n_heads), lax.rem(i, n_heads)

            @pl.when(tab_ref[carried + tile] == 2)
            def _():
                @pl.when(g == 0)
                def _():
                    pltpu.make_async_copy(q_scr.at[tile], q_scr.at[tile], q_sem.at[tile]).wait()
                    pltpu.make_async_copy(st_scr.at[tile], st_scr.at[tile], st_sem.at[tile]).wait()

                finish(tile, g, lambda h: (st_scr[tile, g, h, :HD, :], st_scr[tile, g, h, HD + 8:, :]))

            return carry

        lax.fori_loop(0, n_tiles * n_heads, idle, 0)

    def query(row):
        t = tab_ref[row]
        pltpu.make_async_copy(q_scr.at[t], q_scr.at[t], q_sem.at[t]).wait()

    row, g = block(0)
    query(row)
    have = arrived(0, tab_ref[row + 2])
    for h in range(G):
        stage_a(row, g, h)

    def body(i, have):
        row, g = block(i)
        nrow, ng = block(jnp.minimum(i + 1, n_heads * n_blocks - 1))
        have = arrived(have, tab_ref[nrow + 2])
        flags = tab_ref[row + 1]
        tile = tab_ref[row]

        @pl.when((i + 1 < n_blocks) & ((tab_ref[nrow + 1] & FIRST) != 0))
        def _():
            query(nrow)

        @pl.when((flags & (FIRST | CARRY)) == FIRST)
        def _():
            acc_scr[:] = jnp.zeros_like(acc_scr)
            l_scr[:] = jnp.zeros_like(l_scr)
            m_scr[:] = jnp.full_like(m_scr, NEG)

        if n_st:
            @pl.when((flags & (FIRST | CARRY)) == (FIRST | CARRY))
            def _():
                @pl.when(g == 0)
                def _():
                    pltpu.make_async_copy(st_scr.at[tile], st_scr.at[tile], st_sem.at[tile]).wait()

                for h in range(G):
                    acc_scr[h] = st_scr[tile, g, h, :HD, :]
                    m_scr[h] = st_scr[tile, g, h, HD:HD + 8, :]
                    l_scr[h] = st_scr[tile, g, h, HD + 8:, :]

        if n_cut:
            @pl.when(i == n_blocks)
            def _():
                cut_in.wait()
                for cp in cut_out:
                    cp.start()

        @pl.when((flags & 15) != 0)
        def _():
            mask_runs(flags)

        for h in range(G):
            stage_b(row, g, h)
            stage_a(nrow, ng, h)

        @pl.when((flags & LAST) != 0)
        def _():
            if final:
                finish(tile, g, lambda h: (acc_scr[h], l_scr[h]))
            else:
                for h in range(G):
                    st_scr[tile, g, h, :HD, :] = acc_scr[h]
                    st_scr[tile, g, h, HD:HD + 8, :] = m_scr[h]
                    st_scr[tile, g, h, HD + 8:, :] = l_scr[h]

                @pl.when(g == n_heads - 1)
                def _():
                    pltpu.make_async_copy(st_scr.at[tile], outs[0].at[tile], o_sem.at[tile]).start()

        return have

    have = lax.fori_loop(0, n_heads * n_blocks, body, have)
    arrived(have, len(kv_src))
    if final:
        for k in range(n_tiles):
            pltpu.make_async_copy(o_scr.at[k], outs[k].at[slot], o_sem.at[k]).wait()
    else:
        def wait_out(i, carry):
            row = row0 + BLK * i

            @pl.when((tab_ref[row + 1] & LAST) != 0)
            def _():
                t = tab_ref[row]
                pltpu.make_async_copy(st_scr.at[t], st_scr.at[t], o_sem.at[t]).wait()

            return carry

        lax.fori_loop(0, n_blocks, wait_out, 0)
        for cp in cut_out:
            cp.wait()


def flash(tab, qs, q_src, kvs, *, base, work, st=None, st_src=None, old=None, cut=None, n_cut=0, slots=1, after=()):
    nq = qs[0].shape[1]
    n_heads = 2
    G = nq // HD // n_heads
    n_tiles = len(q_src)
    final = cut is None
    kv_src = [(a, i) for a, kv in enumerate(kvs) for i in range(kv.shape[0])]
    n_runs = len(kv_src)
    sts = () if st is None else (st,)
    old = old or ()
    more = (*old, *(() if final else (cut,)))
    n_in = 1 + len(qs) + len(kvs) + len(sts) + len(more)
    state = (n_heads, G, ST, RUN)
    has_st = not final or sts
    if final:
        out_shape = [jax.ShapeDtypeStruct((slots, RUN, nq), BF)] * n_tiles + [jax.ShapeDtypeStruct((8, HD), F32)]
        scratch = []
    else:
        half = cut.shape[0] // 2
        out_shape = [jax.ShapeDtypeStruct((n_tiles, *state), F32)]
        out_shape += [jax.ShapeDtypeStruct((half // n_cut, cut.shape[1]), BF)] * n_cut
        scratch = [pltpu.VMEM((half, cut.shape[1]), BF), pltpu.SemaphoreType.DMA]
    return pl.pallas_call(
        ordered(functools.partial(flash_kernel, q_src=q_src, kv_src=kv_src, n_q=len(qs), n_kv=len(kvs),
                                  st_src=st_src or [None] * n_tiles, n_st=len(sts), n_old=len(more), n_cut=n_cut,
                                  slot=slots - 1 if old else 0, base=base, G=G, n_tiles=n_tiles, n_heads=n_heads, final=final),
                n_in, after),
        grid_spec=pltpu.PrefetchScalarGridSpec(
            num_scalar_prefetch=1, grid=(),
            in_specs=[ANY] * (n_in - 1 + len(after)),
            out_specs=[ANY] * len(out_shape),
            scratch_shapes=[pltpu.VMEM((n_tiles, nq, RUN), BF),
                            pltpu.VMEM((n_runs + 1, 2, RUN, RUN), BF),
                            pltpu.VMEM((n_tiles if final else 1, RUN, nq), BF),
                            pltpu.VMEM((n_tiles if has_st else 1, *state), F32),
                            pltpu.VMEM((G, 4 * RUN, RUN), F32),
                            pltpu.VMEM((G, 4, 8, RUN), F32),
                            pltpu.VMEM((G, HD, RUN), F32),
                            pltpu.VMEM((G, 8, RUN), F32),
                            pltpu.VMEM((G, 8, RUN), F32),
                            pltpu.SemaphoreType.DMA((n_tiles,)),
                            pltpu.SemaphoreType.DMA((n_runs,)),
                            pltpu.SemaphoreType.DMA((n_tiles,)),
                            pltpu.SemaphoreType.DMA((n_tiles,)), *scratch]),
        out_shape=out_shape,
        input_output_aliases={n_in - len(old) + k: k for k in range(len(old))},
        name="flash" if final else "flash_part", compiler_params=PARAMS,
        cost_estimate=cost(8 * work * RUN * RUN * nq, n_runs * RUN * nq),
    )(tab, *qs, *kvs, *sts, *more, *after)


def out_kernel(*refs, blocks, n_w, n_run, at, n_shared):
    n_o, n_out = 4, 2 * n_run
    o_refs, w_refs, x_ref, g_ref = refs[:n_o], refs[n_o:n_o + n_w], refs[n_o + n_w], refs[n_o + n_w + 1]
    outs = refs[n_o + n_w + 2:n_o + n_w + 2 + n_out]
    o_scr, w_scr, x_scr, acc_scr, o_sem, w_sem, x_sem, out_sem, sent_sem = refs[n_o + n_w + 2 + n_out:]
    width = o_refs[0].shape[-1]
    half = width // 2
    n_slots = w_scr.shape[0] - n_shared
    n_local = len(blocks)
    mate = other_core()
    barrier = pltpu.get_barrier_semaphore()
    pl.semaphore_signal(barrier, inc=1, device_id=mate, device_id_type=pl.DeviceIdType.MESH)

    def fetch(k):
        for i, pieces in enumerate(blocks):
            @pl.when(k == i)
            def _():
                to = 0
                for a, r0, n in pieces:
                    pltpu.make_async_copy(w_refs[a].at[pl.ds(r0, n), :], w_scr.at[i % n_slots, pl.ds(to, n), :],
                                          w_sem.at[i % n_slots]).start()
                    to += n

    mine = lax.axis_index('cp')
    loads = [[] for _ in range(n_local + n_shared)]
    for i in range(n_run):
        rows = pl.ds(i * RUN, RUN)
        for k in range(4):
            src = o_refs[k].at[i]
            if k < 2:
                loads[2 * k].append((src, o_scr.at[rows, pl.ds(k * width, width)]))
            else:
                for p, part in enumerate((mine, 1 - mine)):
                    loads[2 * k + p].append((src.at[:, pl.ds(pl.multiple_of(part * half, half), half)],
                                             o_scr.at[rows, pl.ds(k * width + p * half, half)]))
    copies = [[pltpu.make_async_copy(src, dst, o_sem.at[k, i]) for i, (src, dst) in enumerate(ls)] for k, ls in enumerate(loads)]
    x_copy = pltpu.make_async_copy(x_ref.at[pl.ds(at * n_run * RUN, n_run * RUN), :], x_scr, x_sem)
    for cp in copies[0]:
        cp.start()
    for i in range(n_slots - 1):
        fetch(jnp.int32(i))
    shared = []
    pl.semaphore_wait(barrier, 1)
    for b in range(n_shared):
        to = 0
        for a, r0, n in blocks[b - n_shared]:
            shared.append(pltpu.make_async_remote_copy(
                src_ref=w_refs[a].at[pl.ds(r0, n), :], dst_ref=w_scr.at[n_slots + b, pl.ds(to, n), :],
                send_sem=sent_sem.at[len(shared)], recv_sem=w_sem.at[n_slots + b], device_id=mate,
                device_id_type=pl.DeviceIdType.MESH))
            shared[-1].start()
            to += n
    for ls in copies[1:]:
        for cp in ls:
            cp.start()
    x_copy.start()
    acc_scr[:] = jnp.zeros_like(acc_scr)

    def one(k, carry):
        fetch(k + n_slots - 1)
        for i, ls in enumerate(copies):
            if ls:
                @pl.when(k == i)
                def _():
                    for cp in ls:
                        cp.wait()
        slot = jnp.where(k < n_local, lax.rem(k, n_slots), k - n_local + n_slots)
        pltpu.make_async_copy(w_scr.at[slot], w_scr.at[slot], w_sem.at[slot]).wait()
        acc_scr[:] += jnp.dot(o_scr[:, pl.ds(pl.multiple_of(k * half, half), half)], w_scr[slot], preferred_element_type=F32)
        return carry

    lax.fori_loop(0, len(loads), one, 0)
    x_copy.wait()

    strip = 32

    def one_strip(r, carry):
        rows = pl.ds(pl.multiple_of(r * strip, strip), strip)
        y = (x_scr[rows, :].astype(F32) + acc_scr[rows, :].astype(BF).astype(F32)).astype(BF)
        x_scr[rows, :] = y
        o_scr[rows, :] = norm_rows(y, g_ref[:])
        return carry

    stores, per = [], RUN // strip
    for i in range(n_run):
        lax.fori_loop(i * per, (i + 1) * per, one_strip, 0)
        for k, scr in enumerate((x_scr, o_scr)):
            stores.append(pltpu.make_async_copy(scr.at[pl.ds(i * RUN, RUN), :], outs[2 * i + k], out_sem.at[2 * i + k]))
            stores[-1].start()
    for cp in stores:
        cp.wait()
    for cp in shared:
        cp.wait_send()


def out_proj(os, ws, blocks, n_shared, x_rows, gain, at, call, after=()):
    dim = x_rows.shape[1]
    n_run, _, width = os[0].shape
    rows = n_run * RUN
    return pl.pallas_call(
        ordered(functools.partial(out_kernel, blocks=blocks, n_w=len(ws), n_run=n_run, at=at, n_shared=n_shared),
                len(os) + len(ws) + 2, after),
        grid=(1,),
        in_specs=[ANY] * (len(os) + len(ws) + 1) + [pl.BlockSpec((1, dim), lambda i: (0, 0))] + [ANY] * len(after),
        out_specs=[ANY] * (2 * n_run),
        out_shape=[jax.ShapeDtypeStruct((RUN, dim), BF)] * (2 * n_run),
        scratch_shapes=[pltpu.VMEM((rows, 4 * width), BF), pltpu.VMEM((3 + n_shared, width // 2, dim), BF), pltpu.VMEM((rows, dim), BF),
                        pltpu.VMEM((rows, dim), F32), pltpu.SemaphoreType.DMA((len(blocks) + n_shared, 2 * n_run)),
                        pltpu.SemaphoreType.DMA((3 + n_shared,)), pltpu.SemaphoreType.DMA, pltpu.SemaphoreType.DMA((2 * n_run,)),
                        pltpu.SemaphoreType.DMA((len(ws),))],
        name="outp",
        compiler_params=pltpu.CompilerParams(vmem_limit_bytes=VMEM, collective_id=call, has_side_effects=True),
        cost_estimate=cost(8 * rows * width * dim, 8 * width * dim),
    )(*os, *ws, x_rows, gain, *after)


def mlp_kernel(*refs, n_in, first, rb, tn, td, nk, nd, cross):
    b_refs = refs[:n_in]
    wg_ref, wu_ref, wd_ref, *outs = refs[n_in:n_in + (4 if cross else 5)]
    (b_scr, u_scr, w_scr, d_scr, keep_scr, out_scr, in_scr, b_sem, w_sem, d_sem, out_sem, in_sem,
     rows_sem, *more) = refs[n_in + (4 if cross else 5):]
    i = pl.program_id(0)
    mate = other_core()
    peers = [mate]
    if cross:
        own_scr, far_scr, back_scr, far_sem, back_sem = more
        half_tp = lax.axis_size('tp') // 2
        peers.append({'tp': lax.rem(lax.axis_index('tp') + half_tp, 2 * half_tp)})
    barrier = pltpu.get_barrier_semaphore()

    def fetch(j):
        @pl.when(j < nk)
        def _():
            slot, cols = lax.rem(j, 2), pl.ds(pl.multiple_of(j * tn, tn), tn)
            for k, w in enumerate((wg_ref, wu_ref)):
                pltpu.make_async_copy(w.at[:, cols], w_scr.at[slot, k], w_sem.at[slot]).start()

        @pl.when((j >= nk) & (j < nk + nd))
        def _():
            n, slot = j - nk, lax.rem(j - nk, 2)
            pltpu.make_async_copy(wd_ref.at[:, pl.ds(pl.multiple_of(n * td, td), td)], d_scr.at[slot], d_sem.at[slot]).start()

    def gated(rows, cols, slot):
        b = b_scr[rows, :]
        gate = jnp.dot(b, w_scr[slot, 0], preferred_element_type=F32)
        up = jnp.dot(b, w_scr[slot, 1], preferred_element_type=F32)
        u_scr[rows, cols] = (jax.nn.silu(gate) * up).astype(BF)

    def to_mate(n):
        return pltpu.make_async_remote_copy(src_ref=out_scr.at[n], dst_ref=in_scr.at[n], send_sem=out_sem.at[n],
                                            recv_sem=in_sem.at[n], device_id=mate, device_id_type=pl.DeviceIdType.MESH)

    def to_far(n):
        return pltpu.make_async_remote_copy(src_ref=far_scr.at[n], dst_ref=back_scr.at[n], send_sem=far_sem.at[n],
                                            recv_sem=back_sem.at[n], device_id=peers[-1], device_id_type=pl.DeviceIdType.MESH)

    def rows_to_mate(n):
        return pltpu.make_async_remote_copy(
            src_ref=b_refs[n].at[pl.ds(first, rb), :], dst_ref=b_scr.at[pl.ds((n_in + n) * rb, rb), :],
            send_sem=rows_sem.at[n], recv_sem=b_sem.at[n_in + n], device_id=mate, device_id_type=pl.DeviceIdType.MESH)

    @pl.when(i == 0)
    def _():
        copies = [pltpu.make_async_copy(r.at[pl.ds(first, rb), :], b_scr.at[pl.ds(k * rb, rb), :], b_sem.at[k])
                  for k, r in enumerate(b_refs)]
        for peer in peers:
            pl.semaphore_signal(barrier, inc=1, device_id=peer, device_id_type=pl.DeviceIdType.MESH)
        copies[0].start()
        fetch(i)
        for cp in copies[1:]:
            cp.start()
        pl.semaphore_wait(barrier, len(peers))
        for n in range(n_in):
            rows_to_mate(n).start()

    fetch(i + 1)

    @pl.when(i < nk)
    def _():
        slot = lax.rem(i, 2)
        pltpu.make_async_copy(w_scr.at[slot], w_scr.at[slot], w_sem.at[slot]).wait()

    @pl.when(i == 0)
    def _():
        def one(k, carry):
            rows = pl.ds(pl.multiple_of(k * rb, rb), rb)
            pltpu.make_async_copy(b_scr.at[rows, :], b_scr.at[rows, :], b_sem.at[k]).wait()
            gated(rows, pl.ds(0, tn), 0)
            return carry

        lax.fori_loop(0, 2 * n_in, one, 0)

    @pl.when((i > 0) & (i < nk))
    def _():
        gated(slice(None), pl.ds(pl.multiple_of(i * tn, tn), tn), lax.rem(i, 2))

    n = i - nk

    @pl.when((n > 0) & (n <= nd))
    def _():
        to_mate(n - 1).start()

    if cross:
        @pl.when((n > 1) & (n <= nd + 1))
        def _():
            to_far(n - 2).start()

    @pl.when((n >= 0) & (n < nd))
    def _():
        slot = lax.rem(n, 2)
        pltpu.make_async_copy(d_scr.at[slot], d_scr.at[slot], d_sem.at[slot]).wait()
        d = jnp.dot(u_scr[:], d_scr[slot], preferred_element_type=F32).astype(BF)
        half = d.shape[0] // 2
        keep_scr[slot] = d[:half]
        out_scr[n] = d[half:]

    @pl.when((n > 0) & (n <= nd))
    def _():
        m = n - 1
        to_mate(m).wait_recv()
        total = (keep_scr[lax.rem(m, 2)].astype(F32) + in_scr[m].astype(F32)).astype(BF)
        size = total.shape[0] // 2
        if cross:
            own_scr[m] = total[:size]
            far_scr[m] = total[size:]
        else:
            outs[0][:] = total[:size]
            outs[1][:] = total[size:]

    if cross:
        @pl.when(n > nd)
        def _():
            m = n - nd - 1
            to_far(m).wait_recv()
            outs[0][:] = (own_scr[m].astype(F32) + back_scr[m].astype(F32)).astype(BF)

    @pl.when(i == pl.num_programs(0) - 1)
    def _():
        def sent(k, carry):
            to_mate(k).wait_send()
            if cross:
                to_far(k).wait_send()
            return carry

        lax.fori_loop(0, nd, sent, 0)
        for k in range(n_in):
            rows_to_mate(k).wait_send()


def mlp(bs, first, rb, wg, wu, wd, call, cross=False, after=()):
    dim = bs[0].shape[1]
    rows = 2 * rb * len(bs)
    ffn = wg.shape[1]
    td = 512
    tn = td if rows <= td else td // 2
    nk, nd = ffn // tn, dim // td
    half = rows // 2
    lag = nk + 1 + nd * cross
    n_out = 1 if cross else 2
    tiles = pltpu.VMEM((nd, half, td), BF)
    sem = pltpu.SemaphoreType.DMA
    return pl.pallas_call(
        ordered(functools.partial(mlp_kernel, n_in=len(bs), first=first, rb=rb, tn=tn, td=td, nk=nk, nd=nd, cross=cross),
                len(bs) + 3, after),
        grid=(nd + lag,),
        in_specs=[ANY] * (len(bs) + 3 + len(after)),
        out_specs=[pl.BlockSpec((rb, td), lambda i: (0, jnp.clip(i - lag, 0, nd - 1)))] * n_out,
        out_shape=[jax.ShapeDtypeStruct((rb, dim), BF)] * n_out,
        scratch_shapes=[pltpu.VMEM((rows, dim), BF), pltpu.VMEM((rows, ffn), BF), pltpu.VMEM((2, 2, dim, tn), BF),
                        pltpu.VMEM((2, ffn, td), BF), pltpu.VMEM((2, half, td), BF), tiles, tiles]
        + [sem((n,)) for n in (2 * len(bs), 2, 2, nd, nd, len(bs))]
        + ([pltpu.VMEM((nd, rb, td), BF)] * 3 + [sem((nd,))] * 2 if cross else []),
        name="mlp",
        compiler_params=pltpu.CompilerParams(vmem_limit_bytes=VMEM, collective_id=call, has_side_effects=True),
        cost_estimate=cost(6 * rows * dim * ffn, 6 * dim * ffn),
    )(*bs, wg, wu, wd, *after)


def sum_kernel(*refs, n):
    *parts, y_ref, z_ref = refs[-2 - n:]
    total = sum(p[:].astype(F32) for p in parts).astype(BF)
    z_ref[:] = (y_ref[:].astype(F32) + total.astype(F32)).astype(BF)


def sum_rows(z, parts, y, y_first, first, total, after=(), tile=64):
    rows, dim = parts[0].shape
    at = lambda r0: pl.BlockSpec((tile, dim), lambda i: (r0 // tile + i, 0))
    prev = () if z is None else (z,)
    n = len(parts)
    return pl.pallas_call(
        ordered(functools.partial(sum_kernel, n=n), len(prev) + n + 1, after), grid=(rows // tile,),
        in_specs=[ANY] * len(prev) + [at(0)] * n + [at(y_first)] + [ANY] * len(after),
        out_specs=at(first),
        out_shape=jax.ShapeDtypeStruct((total, dim), BF),
        input_output_aliases={0: 0} if prev else {},
        name="zsum", compiler_params=PARAMS,
        cost_estimate=cost(rows * dim, rows * dim),
    )(*prev, *parts, y, *after)


def run_positions(xi, ci, y, cps, piece):
    def start(x, c):
        return (y if x == 0 else 2 * cps - 1 - y) * piece + c * (piece // 2)

    per = piece // 2 // RUN
    out = [start(xi, ci) + RUN * j for j in range(per)] + [start(xi, 1 - ci) + RUN * j for j in range(per)]
    for j in range(per):
        out += [start(1 - xi, ci) + RUN * j, start(1 - xi, 1 - ci) + RUN * j]
    return out


def block_list(tile, ids, diag):
    own = [] if diag is None else [diag]
    n_tail = (len(ids) + len(own)) % 4 or 4
    n_tail -= len(own)
    head, tail = ids[:len(ids) - n_tail], own + ids[len(ids) - n_tail:]
    blocks = [[0, head[i:i + 4], head[i:i + 4]] for i in range(0, len(head), 4)]
    fill = 4 - len(tail)
    keys = tail + [ids[-1] if ids else diag] * fill
    blocks.append([sum(1 << k for k, r in enumerate(keys) if r == diag), keys, tail + [-1] * fill])
    blocks[-1][0] |= LAST
    blocks[0][0] |= FIRST
    return [[tile, flags, 0] + keys + values for flags, keys, values in blocks]


def call_table(tiles, pairs, carry, idle):
    rows, most = [], 0
    carry = [c if pairs[t][0] or pairs[t][1] else idle for t, c in enumerate(carry)]
    for t, tile in enumerate(tiles):
        ids, own = pairs[t]
        if ids or own:
            mine = block_list(t, ids, tile if own else None)
            mine[0][1] |= CARRY if carry[t] else 0
            rows += mine
    for row in rows:
        most = max(most, max(row[3:7]) + 1)
        row[2] = most
    return [len(rows)] + carry + [v for row in rows for v in row], len(rows)


def work_tables(cps, piece):
    per = piece // 2 // RUN
    early, more = 2 * per + 2, 2 * per + 4
    stage = lambda r: 0 if r < early else 1
    soon_pair = lambda r, t: r < early and t < early or r < more and t in (0, 1, per, per + 1)
    calls = [(0, list(range(early)))]
    calls += [(1, [j, per + j, 2 * per + 2 * j, 2 * per + 2 * j + 1]) for j in range(per)]
    tabs, all_runs, sizes = [], [], []
    for y in range(cps):
        for xi in range(2):
            for ci in range(2):
                mine = run_positions(xi, ci, y, cps, piece)
                pos = mine + run_positions(xi, ci, 1 - y, cps, piece)
                all_runs.append(mine)
                tabs.append([])
                sizes.append([])
                for now, tiles in calls:
                    pairs, carry = [], []
                    for t in tiles:
                        seen = [r for r in range(len(pos)) if pos[r] < pos[t]]
                        when = {r: 0 if soon_pair(r, t) else 1 for r in seen}
                        late = list(when.values()).count(1) + stage(t)
                        soon = len(seen) + 1 - late
                        if late and soon % 4 <= -late % 4:
                            for r in [r for r in seen if not when[r]][:soon % 4]:
                                when[r] = 1
                        pairs.append(([r for r in seen if when[r] == now], stage(t) == now))
                        carry.append(int(stage(t) < now))
                    tab, n = call_table(tiles, pairs, carry, 2 if now == 1 else 0)
                    tabs[-1].append(tab)
                    sizes[-1].append(n)
    widths = [max(len(t[k]) for t in tabs) for k in range(len(calls))]
    flat = [[v for k, t in enumerate(tab) for v in t + [0] * (widths[k] - len(t))] for tab in tabs]
    bases = [sum(widths[:k]) for k in range(len(calls))]
    return np.array(flat, np.int32), np.array(all_runs, np.int32), bases, np.array(sizes).max(0) * 4


def solution(mesh):
    cps = mesh.shape['cp']
    row_spec = P('dp', ('cp', 'tp'), None)
    head_cols = P(None, 'tp', None)
    n_tp = mesh.shape['tp']

    over_core, over_x, over_both = (('tp', [(t, t ^ k) for t in range(n_tp)]) for k in (1, 2, 3))
    over_y = ('cp', [(i, i ^ 1) for i in range(cps)])

    def layer(x, g_attn, w_q, w_k, w_v, w_o, g_mlp, w_gate, w_up, w_down):
        x_rows = x[0]
        dim = x_rows.shape[1]
        n_run = x_rows.shape[0] // RUN
        piece = 2 * x_rows.shape[0]
        t_id, y_id = lax.axis_index('tp'), lax.axis_index('cp')
        np_tab, np_runs, bases, work = work_tables(cps, piece)
        dev = y_id * n_tp + t_id
        tab = lax.dynamic_index_in_dim(jnp.asarray(np_tab), dev, 0, keepdims=False)
        run_pos = lax.dynamic_index_in_dim(jnp.asarray(np_runs), dev, 0, keepdims=False)

        def tied(v, *others):
            return lax.optimization_barrier((v, *others))[0]

        def send(axis_pairs, v):
            return lax.ppermute(v, *axis_pairs)

        ga, gm = g_attn.reshape(1, dim), g_mlp.reshape(1, dim)
        own = list(norm_runs(x_rows, ga, [0]))
        own += norm_runs(x_rows, ga, list(range(1, n_run)), after=own)
        far = [send(over_x, own[j]) for j in range(n_run)]
        mate = [send(over_core, own[j]) for j in range(n_run)]

        w_all = jnp.concatenate([tied(w, own[-1]).reshape(dim, -1) for w in (w_q, w_k, w_v)], axis=1)
        row_pos = run_pos[:, None] + jnp.arange(RUN, dtype=jnp.int32)[None, :]
        tables = rope_tables(tied(row_pos[:2 * n_run], own[-1]))

        q_here, kv_here = qkv(own + mate, w_all, (tables, 0))
        kvs, q_far = [kv_here], []
        far_tables = rope_tables(tied(row_pos[2 * n_run:], kv_here))

        def far_qkv(j, after):
            here = tied(far[j], after)
            rows = [here, send(over_core, here)], w_all, (far_tables, 2 * j)
            if j + 1 < n_run:
                q, kv = qkv(*rows, after=(after,))
            else:
                kv, = qkv(*rows, False, after=(after,))
                q, = qkv(*rows, True, False, after=(kv, gm))
            q_far.append(q)
            kvs.append(kv)
            return kv

        far_qkv(1, far_qkv(0, kv_here))

        wo = w_o.reshape(-1, dim)
        half = wo.shape[0] // 2
        n_piece = 2
        rows = half // n_piece
        wo_c = send(over_core, tied(wo, kvs[-1]))

        tiles = [(0, i) for i in range(2 * n_run)] + [(1, i) for i in PAIR]
        st, *wo_x = flash(tab, [q_here, q_far[0]], tiles, kvs, base=bases[0], work=int(work[0]), cut=wo,
                         n_cut=n_piece)
        wo_x = [send(over_x, w) for w in wo_x]
        far_qkv(3, far_qkv(2, st))
        kvs = kvs + [send(over_y, kv) for kv in kvs]

        os, outs, prev = [], [], q_far[-1]
        wo_a, wo_b = [], []

        def forward_w(p):
            wo_a.append(tied(wo_x[p], prev))
            wo_b.append(send(over_y, wo_a[p]))

        def attend(j):
            held = 2 * n_run + 2 * j
            carried = [j, n_run + j] + ([held, held + 1] if j == 0 else [None, None])
            pair = j % 2
            *o, done = flash(
                tab, [q_here, q_far[j]], [(0, j), (0, n_run + j), (1, 0), (1, 1)], kvs,
                base=bases[1 + j], work=int(work[1 + j]), st=st, st_src=carried, old=os.pop() if pair else None, slots=2,
                after=(prev,))
            if pair:
                o = [o[0], send(over_core, o[1]), send(over_x, o[2]), send(over_both, o[3])]
            os.append(o)
            return done

        def project(i):
            ws = [wo, wo_c, *wo_a, *wo_b]
            blocks = [[(a, r, half)] for a in PAIR for r in (0, half)]
            blocks += [[(2 + b * n_piece + p, 0, rows) for p in range(n_piece)] for b in PAIR]
            got = out_proj(os[i], ws, blocks, 2, x_rows, gm, i, n_run + 1 + i, after=(prev,))
            for y, b in zip(got[::2], got[1::2]):
                outs.append((y, b, send(over_x, b)))
            return got[0]

        last = n_run - 1
        for j in range(last):
            prev = attend(j)
            if j < n_piece:
                forward_w(j)
        prev = project(0)
        prev = attend(last)

        z, sums = None, []

        chunks = [(j, 0, RUN) for j in range(last)] + [(last, 0, RUN // 2), (last, RUN // 2, RUN // 2)]

        def finish(c):
            j, first, _ = chunks[c]
            return sum_rows(z, sums[c], outs[j][0], first, j * RUN + first, n_run * RUN,
                        after=() if prev is z else (prev,))

        for c, (j, first, size) in enumerate(chunks):
            prev, *s_far = mlp(outs[j][1:], first, size, w_gate, w_up, w_down, c, c == n_run, after=(prev,))
            sums.append([prev] + [send(over_x, v) for v in s_far])
            if c == 0:
                prev = project(1)
            elif c < n_run:
                prev = z = finish(c - 1)
        for c in (last, n_run):
            prev = z = finish(c)
        return z[None]

    return jax.shard_map(layer, mesh=mesh,
                         in_specs=(row_spec, P(), head_cols, head_cols, head_cols, P('tp', None, None),
                                   P(), P(None, 'tp'), P(None, 'tp'), P('tp', None)),
                         out_specs=row_spec, check_vma=False)
```

```python
import functools
import math
import jax
import jax.numpy as jnp
import numpy as np
from jax import lax
from jax.experimental import pallas as pl
from jax.experimental.pallas import tpu as pltpu
from jax.sharding import PartitionSpec as P

NORM_EPS = 1e-5
ROPE_THETA = 500000.0
HD = 128
RUN = 256
NEG = -1e30
LOG2E = math.log2(math.e)
DN = (((1,), (0,)), ((), ()))
BF = jnp.bfloat16
F32 = jnp.float32
ANY = pl.BlockSpec(memory_space=pltpu.HBM)


VMEM = 67043328
PAIR = (0, 1)
PARAMS = pltpu.CompilerParams(vmem_limit_bytes=VMEM)


def rope_tables(positions):
    half = HD // 2
    inv_freq = ROPE_THETA ** (-2.0 * jnp.arange(half, dtype=F32) / HD)
    angles = inv_freq[:, None] * positions.astype(F32)[..., None, :]
    return jnp.cos(angles), jnp.sin(angles)


def norm_rows(rows, gain):
    f = rows.astype(F32)
    mean_sq = jnp.mean(f * f, axis=-1, keepdims=True)
    return (f * lax.rsqrt(mean_sq + NORM_EPS) * gain.astype(F32)).astype(BF)


def other_core():
    me = lax.axis_index('tp')
    return {'tp': me + 1 - 2 * lax.rem(me, 2)}


def cost(flops, moved):
    return pl.CostEstimate(flops=flops, transcendentals=0, bytes_accessed=moved)


def ordered(kernel, n_in, after):
    n = len(after)
    return lambda *refs: kernel(*refs[:n_in], *refs[n_in + n:])


def norm_kernel(x_ref, g_ref, *refs, per):
    for k, o_ref in enumerate(refs):
        @pl.when(lax.div(pl.program_id(0), per) == k)
        def _():
            o_ref[:] = norm_rows(x_ref[:], g_ref[:])


def norm_runs(x_rows, gain, runs, after=(), tile=128):
    dim = x_rows.shape[1]
    per = RUN // tile
    n = len(runs)
    return pl.pallas_call(
        ordered(functools.partial(norm_kernel, per=per), 2, after), grid=(n * per,),
        in_specs=[pl.BlockSpec((tile, dim), lambda i: (runs[0] * per + i, 0)), pl.BlockSpec((1, dim), lambda i: (0, 0))]
        + [ANY] * len(after),
        out_specs=[pl.BlockSpec((tile, dim), lambda i, k=k: (jnp.clip(i - k * per, 0, per - 1), 0)) for k in range(n)],
        out_shape=[jax.ShapeDtypeStruct((RUN, dim), BF)] * n,
        name="norm", compiler_params=PARAMS,
        cost_estimate=cost(n * RUN * dim, n * RUN * dim),
    )(x_rows, gain, *after)


def qkv_kernel(*refs, n_in, n_q, group, first, with_q, with_kv):
    a_refs = refs[:n_in]
    w_ref, cos_ref, sin_ref, *outs, a_scr, sem = refs[n_in:]
    q_ref, kv_ref = outs[0], outs[-1]
    n = pl.program_id(0) + first
    heads = w_ref.shape[1] // HD

    @pl.when(n == first)
    def _():
        for k, r in enumerate(a_refs):
            pltpu.make_async_copy(r, a_scr.at[pl.ds(k * RUN, RUN), :], sem.at[k]).start()

    def rope(f, i):
        f = f.astype(BF).astype(F32)
        lo, hi, cos, sin = f[:HD // 2], f[HD // 2:], cos_ref[i], sin_ref[i]
        return jnp.concatenate([lo * cos - hi * sin, hi * cos + lo * sin], axis=0)

    def one(k, carry):
        @pl.when(n == first)
        def _():
            for i in range(group):
                rows = pl.ds(pl.multiple_of((k * group + i) * RUN, RUN), RUN)
                pltpu.make_async_copy(a_scr.at[rows, :], a_scr.at[rows, :], sem.at[k * group + i]).wait()

        runs = [k * group + i for i in range(group)]

        def products():
            return [jnp.dot(a_scr[pl.ds(pl.multiple_of(run * RUN, RUN), RUN), :], w_ref[:], preferred_element_type=F32)
                    for run in runs]

        if with_q:
            @pl.when(n < n_q)
            def _():
                for run, r in zip(runs, products()):
                    for h in range(heads):
                        cols = slice(h * HD, (h + 1) * HD)
                        q_ref[run, cols, :] = rope(r[:, cols].T, run).astype(BF)

        if with_kv:
            @pl.when(n == n_q)
            def _():
                for run, r in zip(runs, products()):
                    for h in range(heads // 2):
                        cols, past = slice(h * HD, (h + 1) * HD), heads // 2 * HD
                        kv_ref[run, 0, :, cols] = rope(r[:, cols].T, run).T.astype(BF)
                        kv_ref[run, 1, cols, :] = r[:, past + h * HD:past + (h + 1) * HD].T.astype(BF)
        return carry

    lax.fori_loop(0, n_in // group, one, 0)


def qkv(rows, w_all, tables, with_q=True, with_kv=True, after=()):
    n_in = len(rows)
    dim = w_all.shape[0]
    tn = 512
    n_q = w_all.shape[1] // tn - 1
    (cos, sin), first_run = tables
    group = 2
    at = first_run // n_in
    start = 0 if with_q else n_q
    kv_shape = (n_in, 2, RUN, RUN)
    tab = pl.BlockSpec((n_in, HD // 2, RUN), lambda n: (at, 0, 0))
    return pl.pallas_call(
        ordered(functools.partial(qkv_kernel, n_in=n_in, n_q=n_q, group=group, first=start, with_q=with_q, with_kv=with_kv),
                n_in + 3, after),
        grid=(n_q * with_q + with_kv,),
        in_specs=[ANY] * n_in + [pl.BlockSpec((dim, tn), lambda n: (0, n + start)), tab, tab] + [ANY] * len(after),
        out_specs=[pl.BlockSpec((n_in, tn, RUN), lambda n: (0, jnp.minimum(n, n_q - 1), 0))] * with_q
        + [pl.BlockSpec(kv_shape, lambda n: (0,) * len(kv_shape))] * with_kv,
        out_shape=[jax.ShapeDtypeStruct((n_in, n_q * tn, RUN), BF)] * with_q + [jax.ShapeDtypeStruct(kv_shape, BF)] * with_kv,
        scratch_shapes=[pltpu.VMEM((n_in * RUN, dim), BF), pltpu.SemaphoreType.DMA((n_in,))],
        name="qkv", compiler_params=PARAMS,
        cost_estimate=cost(2 * n_in * RUN * w_all.size, 2 * w_all.size),
    )(*rows, w_all, cos, sin, *after)


BLK = 11
LAST, FIRST, CARRY = 16, 32, 64
ST = HD + 16


def flash_kernel(tab_ref, *refs, q_src, kv_src, n_q, n_kv, st_src, n_st, n_old, n_cut, slot, base, G, n_tiles, n_heads, final):
    qs, kvs, sts = refs[:n_q], refs[n_q:n_q + n_kv], refs[n_q + n_kv:n_q + n_kv + n_st]
    n_out = n_tiles + 1 if final else 1 + n_cut
    at = n_q + n_kv + n_st + n_old
    outs = refs[at:at + n_out]
    q_scr, kv_scr, o_scr, st_scr, s_scr, mb_scr, acc_scr, m_scr, l_scr, q_sem, kv_sem, o_sem, st_sem = refs[at + n_out:][:13]
    if n_cut:
        cut_ref, (cut_scr, cut_sem) = refs[at - 1], refs[-2:]
    T = RUN
    c = (HD ** -0.5) * LOG2E
    n_blocks = tab_ref[base]
    carried = base + 1
    row0 = carried + n_tiles
    null = len(kv_src)

    q_copies = [pltpu.make_async_copy(qs[a].at[i], q_scr.at[t], q_sem.at[t]) for t, (a, i) in enumerate(q_src)]
    kv_copies = [pltpu.make_async_copy(kvs[a].at[i], kv_scr.at[r], kv_sem.at[r]) for r, (a, i) in enumerate(kv_src)]

    def load_state(t):
        if st_src[t] is not None:
            @pl.when(tab_ref[carried + t] != 0)
            def _():
                pltpu.make_async_copy(sts[0].at[st_src[t]], st_scr.at[t], st_sem.at[t]).start()

    q_copies[0].start()
    for cp in kv_copies[:4]:
        cp.start()
    load_state(0)
    for cp in kv_copies[4:]:
        cp.start()
    for t in range(1, n_tiles):
        q_copies[t].start()
        load_state(t)
    kv_scr[null, 1] = jnp.zeros((RUN, RUN), BF)
    if n_cut:
        cut_in = pltpu.make_async_copy(cut_ref.at[pl.ds(lax.axis_index('cp') * cut_scr.shape[0], cut_scr.shape[0]), :], cut_scr,
                                       cut_sem)
        part = cut_scr.shape[0] // n_cut
        cut_out = [pltpu.make_async_copy(cut_scr.at[pl.ds(k * part, part), :], outs[1 + k], cut_sem) for k in range(n_cut)]
        cut_in.start()

    def block(i):
        g = lax.div(i, n_blocks)
        return row0 + BLK * (i - g * n_blocks), g

    def arrived(have, need):
        def one(r, carry):
            pltpu.make_async_copy(kv_scr.at[r], kv_scr.at[r], kv_sem.at[r]).wait()
            return carry

        lax.fori_loop(have, need, one, 0)
        return jnp.maximum(have, need)

    def put(s, h, k):
        s_scr[h, pl.ds(k * RUN, RUN), :] = s
        mb_scr[h, k] = jnp.max(s.reshape(RUN // 8, 8, T), axis=0)

    def stage_a(row, g, h):
        col = pl.multiple_of(g * HD, HD)
        qt = q_scr[tab_ref[row], pl.ds(pl.multiple_of((g * G + h) * HD, HD), HD), :]
        for k in range(4):
            put(lax.dot_general(kv_scr[tab_ref[row + 3 + k], 0, :, pl.ds(col, HD)], qt, DN, preferred_element_type=F32), h, k)

    def stage_b(row, g, h):
        col = pl.multiple_of(g * HD, HD)
        m_prev = m_scr[h]
        mb = jnp.maximum(jnp.maximum(mb_scr[h, 0], mb_scr[h, 1]), jnp.maximum(mb_scr[h, 2], mb_scr[h, 3]))
        for r in (4, 2, 1):
            mb = jnp.maximum(mb, pltpu.roll(mb, r, 0))
        m_new = jnp.maximum(m_prev, mb)
        m_scr[h] = m_new
        m_c = m_new * c
        alpha = jnp.exp2(m_prev * c - m_c)
        l, pv = l_scr[h] * alpha, None
        for k in range(4):
            run = tab_ref[row + 7 + k]
            p = jnp.exp2(s_scr[h, k * RUN:(k + 1) * RUN].reshape(RUN // 8, 8, T) * c - m_c[None])
            l = l + jnp.sum(p, axis=0) * jnp.where(run < 0, 0.0, 1.0)
            d = lax.dot_general(kv_scr[jnp.where(run < 0, null, run), 1, pl.ds(col, HD), :], p.reshape(RUN, T).astype(BF), DN,
                                preferred_element_type=F32)
            pv = d if pv is None else pv + d
        l_scr[h] = l
        acc_scr[h] = (acc_scr[h].reshape(HD // 8, 8, T) * alpha[None]).reshape(HD, T) + pv

    def mask_runs(flags):
        seen = lax.broadcasted_iota(jnp.int32, (RUN, T), 0) <= lax.broadcasted_iota(jnp.int32, (RUN, T), 1)

        def one(k, carry):
            @pl.when((lax.shift_right_logical(flags, k) & 1) != 0)
            def _():
                rows = pl.multiple_of(k * RUN, RUN)
                for h in range(G):
                    put(jnp.where(seen, s_scr[h, pl.ds(rows, RUN), :], NEG), h, k)

            return carry

        lax.fori_loop(0, 4, one, 0)

    def finish(tile, g, get):
        for h in range(G):
            acc, l = get(h)
            o_scr[tile, :, pl.ds(pl.multiple_of((g * G + h) * HD, HD), HD)] = (acc / jnp.sum(l, axis=0, keepdims=True)).T.astype(BF)

        @pl.when(g == n_heads - 1)
        def _():
            for k in range(n_tiles):
                @pl.when(tile == k)
                def _():
                    pltpu.make_async_copy(o_scr.at[k], outs[k].at[slot], o_sem.at[k]).start()

    if final and n_st:
        def idle(i, carry):
            tile, g = lax.div(i, n_heads), lax.rem(i, n_heads)

            @pl.when(tab_ref[carried + tile] == 2)
            def _():
                @pl.when(g == 0)
                def _():
                    pltpu.make_async_copy(q_scr.at[tile], q_scr.at[tile], q_sem.at[tile]).wait()
                    pltpu.make_async_copy(st_scr.at[tile], st_scr.at[tile], st_sem.at[tile]).wait()

                finish(tile, g, lambda h: (st_scr[tile, g, h, :HD, :], st_scr[tile, g, h, HD + 8:, :]))

            return carry

        lax.fori_loop(0, n_tiles * n_heads, idle, 0)

    def query(row):
        t = tab_ref[row]
        pltpu.make_async_copy(q_scr.at[t], q_scr.at[t], q_sem.at[t]).wait()

    row, g = block(0)
    query(row)
    have = arrived(0, tab_ref[row + 2])
    for h in range(G):
        stage_a(row, g, h)

    def body(i, have):
        row, g = block(i)
        nrow, ng = block(jnp.minimum(i + 1, n_heads * n_blocks - 1))
        have = arrived(have, tab_ref[nrow + 2])
        flags = tab_ref[row + 1]
        tile = tab_ref[row]

        @pl.when((i + 1 < n_blocks) & ((tab_ref[nrow + 1] & FIRST) != 0))
        def _():
            query(nrow)

        @pl.when((flags & (FIRST | CARRY)) == FIRST)
        def _():
            acc_scr[:] = jnp.zeros_like(acc_scr)
            l_scr[:] = jnp.zeros_like(l_scr)
            m_scr[:] = jnp.full_like(m_scr, NEG)

        if n_st:
            @pl.when((flags & (FIRST | CARRY)) == (FIRST | CARRY))
            def _():
                @pl.when(g == 0)
                def _():
                    pltpu.make_async_copy(st_scr.at[tile], st_scr.at[tile], st_sem.at[tile]).wait()

                for h in range(G):
                    acc_scr[h] = st_scr[tile, g, h, :HD, :]
                    m_scr[h] = st_scr[tile, g, h, HD:HD + 8, :]
                    l_scr[h] = st_scr[tile, g, h, HD + 8:, :]

        if n_cut:
            @pl.when(i == n_blocks)
            def _():
                cut_in.wait()
                for cp in cut_out:
                    cp.start()

        @pl.when((flags & 15) != 0)
        def _():
            mask_runs(flags)

        for h in range(G):
            stage_b(row, g, h)
            stage_a(nrow, ng, h)

        @pl.when((flags & LAST) != 0)
        def _():
            if final:
                finish(tile, g, lambda h: (acc_scr[h], l_scr[h]))
            else:
                for h in range(G):
                    st_scr[tile, g, h, :HD, :] = acc_scr[h]
                    st_scr[tile, g, h, HD:HD + 8, :] = m_scr[h]
                    st_scr[tile, g, h, HD + 8:, :] = l_scr[h]

                @pl.when(g == n_heads - 1)
                def _():
                    pltpu.make_async_copy(st_scr.at[tile], outs[0].at[tile], o_sem.at[tile]).start()

        return have

    have = lax.fori_loop(0, n_heads * n_blocks, body, have)
    arrived(have, len(kv_src))
    if final:
        for k in range(n_tiles):
            pltpu.make_async_copy(o_scr.at[k], outs[k].at[slot], o_sem.at[k]).wait()
    else:
        def wait_out(i, carry):
            row = row0 + BLK * i

            @pl.when((tab_ref[row + 1] & LAST) != 0)
            def _():
                t = tab_ref[row]
                pltpu.make_async_copy(st_scr.at[t], st_scr.at[t], o_sem.at[t]).wait()

            return carry

        lax.fori_loop(0, n_blocks, wait_out, 0)
        for cp in cut_out:
            cp.wait()


def flash(tab, qs, q_src, kvs, *, base, work, st=None, st_src=None, old=None, cut=None, n_cut=0, slots=1, after=()):
    nq = qs[0].shape[1]
    n_heads = 2
    G = nq // HD // n_heads
    n_tiles = len(q_src)
    final = cut is None
    kv_src = [(a, i) for a, kv in enumerate(kvs) for i in range(kv.shape[0])]
    n_runs = len(kv_src)
    sts = () if st is None else (st,)
    old = old or ()
    more = (*old, *(() if final else (cut,)))
    n_in = 1 + len(qs) + len(kvs) + len(sts) + len(more)
    state = (n_heads, G, ST, RUN)
    has_st = not final or sts
    if final:
        out_shape = [jax.ShapeDtypeStruct((slots, RUN, nq), BF)] * n_tiles + [jax.ShapeDtypeStruct((8, HD), F32)]
        scratch = []
    else:
        half = cut.shape[0] // 2
        out_shape = [jax.ShapeDtypeStruct((n_tiles, *state), F32)]
        out_shape += [jax.ShapeDtypeStruct((half // n_cut, cut.shape[1]), BF)] * n_cut
        scratch = [pltpu.VMEM((half, cut.shape[1]), BF), pltpu.SemaphoreType.DMA]
    return pl.pallas_call(
        ordered(functools.partial(flash_kernel, q_src=q_src, kv_src=kv_src, n_q=len(qs), n_kv=len(kvs),
                                  st_src=st_src or [None] * n_tiles, n_st=len(sts), n_old=len(more), n_cut=n_cut,
                                  slot=slots - 1 if old else 0, base=base, G=G, n_tiles=n_tiles, n_heads=n_heads, final=final),
                n_in, after),
        grid_spec=pltpu.PrefetchScalarGridSpec(
            num_scalar_prefetch=1, grid=(),
            in_specs=[ANY] * (n_in - 1 + len(after)),
            out_specs=[ANY] * len(out_shape),
            scratch_shapes=[pltpu.VMEM((n_tiles, nq, RUN), BF),
                            pltpu.VMEM((n_runs + 1, 2, RUN, RUN), BF),
                            pltpu.VMEM((n_tiles if final else 1, RUN, nq), BF),
                            pltpu.VMEM((n_tiles if has_st else 1, *state), F32),
                            pltpu.VMEM((G, 4 * RUN, RUN), F32),
                            pltpu.VMEM((G, 4, 8, RUN), F32),
                            pltpu.VMEM((G, HD, RUN), F32),
                            pltpu.VMEM((G, 8, RUN), F32),
                            pltpu.VMEM((G, 8, RUN), F32),
                            pltpu.SemaphoreType.DMA((n_tiles,)),
                            pltpu.SemaphoreType.DMA((n_runs,)),
                            pltpu.SemaphoreType.DMA((n_tiles,)),
                            pltpu.SemaphoreType.DMA((n_tiles,)), *scratch]),
        out_shape=out_shape,
        input_output_aliases={n_in - len(old) + k: k for k in range(len(old))},
        name="flash" if final else "flash_part", compiler_params=PARAMS,
        cost_estimate=cost(8 * work * RUN * RUN * nq, n_runs * RUN * nq),
    )(tab, *qs, *kvs, *sts, *more, *after)


def out_kernel(*refs, blocks, n_w, n_run, at, n_shared):
    n_o, n_out = 4, 2 * n_run
    o_refs, w_refs, x_ref, g_ref = refs[:n_o], refs[n_o:n_o + n_w], refs[n_o + n_w], refs[n_o + n_w + 1]
    outs = refs[n_o + n_w + 2:n_o + n_w + 2 + n_out]
    o_scr, w_scr, x_scr, acc_scr, o_sem, w_sem, x_sem, out_sem, sent_sem = refs[n_o + n_w + 2 + n_out:]
    width = o_refs[0].shape[-1]
    half = width // 2
    n_local = len(blocks)
    landing = w_scr.shape[0] - n_shared
    n_slots = landing - n_shared
    mate = other_core()
    barrier = pltpu.get_barrier_semaphore()
    pl.semaphore_signal(barrier, inc=1, device_id=mate, device_id_type=pl.DeviceIdType.MESH)

    def place(i):
        return i if i < n_shared else n_shared + (i - n_shared) % n_slots

    def fetch(k):
        for i, pieces in enumerate(blocks):
            @pl.when(k == i)
            def _():
                to = 0
                for a, r0, n in pieces:
                    pltpu.make_async_copy(w_refs[a].at[pl.ds(r0, n), :], w_scr.at[place(i), pl.ds(to, n), :],
                                          w_sem.at[place(i)]).start()
                    to += n

    mine = lax.axis_index('cp')
    loads = [[] for _ in range(n_local + n_shared)]
    for i in range(n_run):
        rows = pl.ds(i * RUN, RUN)
        for k, at_block in enumerate((n_shared, 2 * n_shared, 0, n_local)):
            src = o_refs[k].at[i]
            for p, part in enumerate((mine, 1 - mine) if at_block in (0, n_local) else PAIR):
                loads[at_block + p].append((src.at[:, pl.ds(pl.multiple_of(part * half, half), half)],
                                            o_scr.at[rows, pl.ds((at_block + p) * half, half)]))
    copies = [[pltpu.make_async_copy(src, dst, o_sem.at[k, i]) for i, (src, dst) in enumerate(ls)] for k, ls in enumerate(loads)]
    x_copy = pltpu.make_async_copy(x_ref.at[pl.ds(at * n_run * RUN, n_run * RUN), :], x_scr, x_sem)
    for cp in copies[0]:
        cp.start()
    for i in range(n_slots):
        fetch(jnp.int32(i))
    pl.semaphore_wait(barrier, 1)
    shared = [pltpu.make_async_remote_copy(
        src_ref=w_scr.at[b], dst_ref=w_scr.at[landing + b], send_sem=sent_sem.at[b], recv_sem=w_sem.at[landing + b],
        device_id=mate, device_id_type=pl.DeviceIdType.MESH) for b in range(n_shared)]
    for ls in copies[1:]:
        for cp in ls:
            cp.start()
    x_copy.start()
    acc_scr[:] = jnp.zeros_like(acc_scr)

    def one(k, carry):
        @pl.when(k > 0)
        def _():
            fetch(k + n_slots - 1)

        for i, ls in enumerate(copies):
            @pl.when(k == i)
            def _():
                for cp in ls:
                    cp.wait()
        turn = jnp.where(k < n_shared, k, n_shared + lax.rem(k - n_shared + n_slots, n_slots))
        slot = jnp.where(k < n_local, turn, k - n_local + landing)
        pltpu.make_async_copy(w_scr.at[slot], w_scr.at[slot], w_sem.at[slot]).wait()
        for b, cp in enumerate(shared):
            @pl.when(k == b)
            def _():
                cp.start()
        acc_scr[:] += jnp.dot(o_scr[:, pl.ds(pl.multiple_of(k * half, half), half)], w_scr[slot], preferred_element_type=F32)
        return carry

    lax.fori_loop(0, len(loads), one, 0)
    x_copy.wait()

    strip = 32

    def one_strip(r, carry):
        rows = pl.ds(pl.multiple_of(r * strip, strip), strip)
        y = (x_scr[rows, :].astype(F32) + acc_scr[rows, :].astype(BF).astype(F32)).astype(BF)
        x_scr[rows, :] = y
        o_scr[rows, :] = norm_rows(y, g_ref[:])
        return carry

    stores, per = [], RUN // strip
    for i in range(n_run):
        lax.fori_loop(i * per, (i + 1) * per, one_strip, 0)
        for k, scr in enumerate((x_scr, o_scr)):
            stores.append(pltpu.make_async_copy(scr.at[pl.ds(i * RUN, RUN), :], outs[2 * i + k], out_sem.at[2 * i + k]))
            stores[-1].start()
    for cp in stores:
        cp.wait()
    for cp in shared:
        cp.wait_send()


def out_proj(os, ws, blocks, n_shared, x_rows, gain, at, call, after=()):
    dim = x_rows.shape[1]
    n_run, _, width = os[0].shape
    rows = n_run * RUN
    n_w = 3 + 2 * n_shared
    return pl.pallas_call(
        ordered(functools.partial(out_kernel, blocks=blocks, n_w=len(ws), n_run=n_run, at=at, n_shared=n_shared),
                len(os) + len(ws) + 2, after),
        grid=(1,),
        in_specs=[ANY] * (len(os) + len(ws) + 1) + [pl.BlockSpec((1, dim), lambda i: (0, 0))] + [ANY] * len(after),
        out_specs=[ANY] * (2 * n_run),
        out_shape=[jax.ShapeDtypeStruct((RUN, dim), BF)] * (2 * n_run),
        scratch_shapes=[pltpu.VMEM((rows, 4 * width), BF), pltpu.VMEM((n_w, width // 2, dim), BF), pltpu.VMEM((rows, dim), BF),
                        pltpu.VMEM((rows, dim), F32), pltpu.SemaphoreType.DMA((len(blocks) + n_shared, 2 * n_run)),
                        pltpu.SemaphoreType.DMA((n_w,)), pltpu.SemaphoreType.DMA, pltpu.SemaphoreType.DMA((2 * n_run,)),
                        pltpu.SemaphoreType.DMA((n_shared,))],
        name="outp",
        compiler_params=pltpu.CompilerParams(vmem_limit_bytes=VMEM, collective_id=call, has_side_effects=True),
        cost_estimate=cost(8 * rows * width * dim, 8 * width * dim),
    )(*os, *ws, x_rows, gain, *after)


def mlp_kernel(*refs, n_in, first, rb, tn, td, nk, nd, cross):
    b_refs = refs[:n_in]
    wg_ref, wu_ref, wd_ref, *outs = refs[n_in:n_in + (4 if cross else 5)]
    (b_scr, u_scr, w_scr, d_scr, keep_scr, out_scr, in_scr, b_sem, w_sem, d_sem, out_sem, in_sem,
     rows_sem, *more) = refs[n_in + (4 if cross else 5):]
    i = pl.program_id(0)
    mate = other_core()
    peers = [mate]
    if cross:
        own_scr, far_scr, back_scr, far_sem, back_sem = more
        half_tp = lax.axis_size('tp') // 2
        peers.append({'tp': lax.rem(lax.axis_index('tp') + half_tp, 2 * half_tp)})
    barrier = pltpu.get_barrier_semaphore()

    def fetch(j):
        @pl.when(j < nk)
        def _():
            slot, cols = lax.rem(j, 2), pl.ds(pl.multiple_of(j * tn, tn), tn)
            for k, w in enumerate((wg_ref, wu_ref)):
                pltpu.make_async_copy(w.at[:, cols], w_scr.at[slot, k], w_sem.at[slot]).start()

        @pl.when((j >= nk) & (j < nk + nd))
        def _():
            n, slot = j - nk, lax.rem(j - nk, 2)
            pltpu.make_async_copy(wd_ref.at[:, pl.ds(pl.multiple_of(n * td, td), td)], d_scr.at[slot], d_sem.at[slot]).start()

    def gated(rows, cols, slot):
        b = b_scr[rows, :]
        gate = jnp.dot(b, w_scr[slot, 0], preferred_element_type=F32)
        up = jnp.dot(b, w_scr[slot, 1], preferred_element_type=F32)
        u_scr[rows, cols] = (jax.nn.silu(gate) * up).astype(BF)

    def to_mate(n):
        return pltpu.make_async_remote_copy(src_ref=out_scr.at[n], dst_ref=in_scr.at[n], send_sem=out_sem.at[n],
                                            recv_sem=in_sem.at[n], device_id=mate, device_id_type=pl.DeviceIdType.MESH)

    def to_far(n):
        return pltpu.make_async_remote_copy(src_ref=far_scr.at[n], dst_ref=back_scr.at[n], send_sem=far_sem.at[n],
                                            recv_sem=back_sem.at[n], device_id=peers[-1], device_id_type=pl.DeviceIdType.MESH)

    def rows_to_mate(n):
        return pltpu.make_async_remote_copy(
            src_ref=b_refs[n].at[pl.ds(first, rb), :], dst_ref=b_scr.at[pl.ds((n_in + n) * rb, rb), :],
            send_sem=rows_sem.at[n], recv_sem=b_sem.at[n_in + n], device_id=mate, device_id_type=pl.DeviceIdType.MESH)

    @pl.when(i == 0)
    def _():
        copies = [pltpu.make_async_copy(r.at[pl.ds(first, rb), :], b_scr.at[pl.ds(k * rb, rb), :], b_sem.at[k])
                  for k, r in enumerate(b_refs)]
        for peer in peers:
            pl.semaphore_signal(barrier, inc=1, device_id=peer, device_id_type=pl.DeviceIdType.MESH)
        copies[0].start()
        fetch(i)
        for cp in copies[1:]:
            cp.start()
        pl.semaphore_wait(barrier, len(peers))
        for n in range(n_in):
            rows_to_mate(n).start()

    fetch(i + 1)

    @pl.when(i < nk)
    def _():
        slot = lax.rem(i, 2)
        pltpu.make_async_copy(w_scr.at[slot], w_scr.at[slot], w_sem.at[slot]).wait()

    @pl.when(i == 0)
    def _():
        def one(k, carry):
            rows = pl.ds(pl.multiple_of(k * rb, rb), rb)
            pltpu.make_async_copy(b_scr.at[rows, :], b_scr.at[rows, :], b_sem.at[k]).wait()
            gated(rows, pl.ds(0, tn), 0)
            return carry

        lax.fori_loop(0, 2 * n_in, one, 0)

    @pl.when((i > 0) & (i < nk))
    def _():
        gated(slice(None), pl.ds(pl.multiple_of(i * tn, tn), tn), lax.rem(i, 2))

    n = i - nk

    @pl.when((n > 0) & (n <= nd))
    def _():
        to_mate(n - 1).start()

    if cross:
        @pl.when((n > 1) & (n <= nd + 1))
        def _():
            to_far(n - 2).start()

    @pl.when((n >= 0) & (n < nd))
    def _():
        slot = lax.rem(n, 2)
        pltpu.make_async_copy(d_scr.at[slot], d_scr.at[slot], d_sem.at[slot]).wait()
        d = jnp.dot(u_scr[:], d_scr[slot], preferred_element_type=F32).astype(BF)
        half = d.shape[0] // 2
        keep_scr[slot] = d[:half]
        out_scr[n] = d[half:]

    @pl.when((n > 0) & (n <= nd))
    def _():
        m = n - 1
        to_mate(m).wait_recv()
        total = (keep_scr[lax.rem(m, 2)].astype(F32) + in_scr[m].astype(F32)).astype(BF)
        size = total.shape[0] // 2
        if cross:
            own_scr[m] = total[:size]
            far_scr[m] = total[size:]
        else:
            outs[0][:] = total[:size]
            outs[1][:] = total[size:]

    if cross:
        @pl.when(n > nd)
        def _():
            m = n - nd - 1
            to_far(m).wait_recv()
            outs[0][:] = (own_scr[m].astype(F32) + back_scr[m].astype(F32)).astype(BF)

    @pl.when(i == pl.num_programs(0) - 1)
    def _():
        def sent(k, carry):
            to_mate(k).wait_send()
            if cross:
                to_far(k).wait_send()
            return carry

        lax.fori_loop(0, nd, sent, 0)
        for k in range(n_in):
            rows_to_mate(k).wait_send()


def mlp(bs, first, rb, wg, wu, wd, call, cross=False, after=()):
    dim = bs[0].shape[1]
    rows = 2 * rb * len(bs)
    ffn = wg.shape[1]
    td = 512
    tn = td if rows <= td else td // 2
    nk, nd = ffn // tn, dim // td
    half = rows // 2
    lag = nk + 1 + nd * cross
    n_out = 1 if cross else 2
    tiles = pltpu.VMEM((nd, half, td), BF)
    sem = pltpu.SemaphoreType.DMA
    return pl.pallas_call(
        ordered(functools.partial(mlp_kernel, n_in=len(bs), first=first, rb=rb, tn=tn, td=td, nk=nk, nd=nd, cross=cross),
                len(bs) + 3, after),
        grid=(nd + lag,),
        in_specs=[ANY] * (len(bs) + 3 + len(after)),
        out_specs=[pl.BlockSpec((rb, td), lambda i: (0, jnp.clip(i - lag, 0, nd - 1)))] * n_out,
        out_shape=[jax.ShapeDtypeStruct((rb, dim), BF)] * n_out,
        scratch_shapes=[pltpu.VMEM((rows, dim), BF), pltpu.VMEM((rows, ffn), BF), pltpu.VMEM((2, 2, dim, tn), BF),
                        pltpu.VMEM((2, ffn, td), BF), pltpu.VMEM((2, half, td), BF), tiles, tiles]
        + [sem((n,)) for n in (2 * len(bs), 2, 2, nd, nd, len(bs))]
        + ([pltpu.VMEM((nd, rb, td), BF)] * 3 + [sem((nd,))] * 2 if cross else []),
        name="mlp",
        compiler_params=pltpu.CompilerParams(vmem_limit_bytes=VMEM, collective_id=call, has_side_effects=True),
        cost_estimate=cost(6 * rows * dim * ffn, 6 * dim * ffn),
    )(*bs, wg, wu, wd, *after)


def sum_kernel(*refs, n):
    *parts, y_ref, z_ref = refs[-2 - n:]
    total = sum(p[:].astype(F32) for p in parts).astype(BF)
    z_ref[:] = (y_ref[:].astype(F32) + total.astype(F32)).astype(BF)


def sum_rows(z, parts, y, y_first, first, total, after=(), tile=64):
    rows, dim = parts[0].shape
    at = lambda r0: pl.BlockSpec((tile, dim), lambda i: (r0 // tile + i, 0))
    prev = () if z is None else (z,)
    n = len(parts)
    return pl.pallas_call(
        ordered(functools.partial(sum_kernel, n=n), len(prev) + n + 1, after), grid=(rows // tile,),
        in_specs=[ANY] * len(prev) + [at(0)] * n + [at(y_first)] + [ANY] * len(after),
        out_specs=at(first),
        out_shape=jax.ShapeDtypeStruct((total, dim), BF),
        input_output_aliases={0: 0} if prev else {},
        name="zsum", compiler_params=PARAMS,
        cost_estimate=cost(rows * dim, rows * dim),
    )(*prev, *parts, y, *after)


def run_positions(xi, ci, y, cps, piece):
    def start(x, c):
        return (y if x == 0 else 2 * cps - 1 - y) * piece + c * (piece // 2)

    per = piece // 2 // RUN
    out = [start(xi, ci) + RUN * j for j in range(per)] + [start(xi, 1 - ci) + RUN * j for j in range(per)]
    for j in range(per):
        out += [start(1 - xi, ci) + RUN * j, start(1 - xi, 1 - ci) + RUN * j]
    return out


def block_list(tile, ids, diag):
    own = [] if diag is None else [diag]
    n_tail = (len(ids) + len(own)) % 4 or 4
    n_tail -= len(own)
    head, tail = ids[:len(ids) - n_tail], own + ids[len(ids) - n_tail:]
    blocks = [[0, head[i:i + 4], head[i:i + 4]] for i in range(0, len(head), 4)]
    fill = 4 - len(tail)
    keys = tail + [ids[-1] if ids else diag] * fill
    blocks.append([sum(1 << k for k, r in enumerate(keys) if r == diag), keys, tail + [-1] * fill])
    blocks[-1][0] |= LAST
    blocks[0][0] |= FIRST
    return [[tile, flags, 0] + keys + values for flags, keys, values in blocks]


def call_table(tiles, pairs, carry, idle):
    rows, most = [], 0
    carry = [c if pairs[t][0] or pairs[t][1] else idle for t, c in enumerate(carry)]
    for t, tile in enumerate(tiles):
        ids, own = pairs[t]
        if ids or own:
            mine = block_list(t, ids, tile if own else None)
            mine[0][1] |= CARRY if carry[t] else 0
            rows += mine
    for row in rows:
        most = max(most, max(row[3:7]) + 1)
        row[2] = most
    return [len(rows)] + carry + [v for row in rows for v in row], len(rows)


def work_tables(cps, piece):
    per = piece // 2 // RUN
    early, more = 2 * per + 2, 2 * per + 4
    stage = lambda r: 0 if r < early else 1
    soon_pair = lambda r, t: r < early and t < early or r < more and t in (0, 1, per, per + 1)
    calls = [(0, list(range(early)))]
    calls += [(1, [j, per + j, 2 * per + 2 * j, 2 * per + 2 * j + 1]) for j in range(per)]
    tabs, all_runs, sizes = [], [], []
    for y in range(cps):
        for xi in range(2):
            for ci in range(2):
                mine = run_positions(xi, ci, y, cps, piece)
                pos = mine + run_positions(xi, ci, 1 - y, cps, piece)
                all_runs.append(mine)
                tabs.append([])
                sizes.append([])
                for now, tiles in calls:
                    pairs, carry = [], []
                    for t in tiles:
                        seen = [r for r in range(len(pos)) if pos[r] < pos[t]]
                        when = {r: 0 if soon_pair(r, t) else 1 for r in seen}
                        late = list(when.values()).count(1) + stage(t)
                        soon = len(seen) + 1 - late
                        if late and soon % 4 <= -late % 4:
                            for r in [r for r in seen if not when[r]][:soon % 4]:
                                when[r] = 1
                        pairs.append(([r for r in seen if when[r] == now], stage(t) == now))
                        carry.append(int(stage(t) < now))
                    tab, n = call_table(tiles, pairs, carry, 2 if now == 1 else 0)
                    tabs[-1].append(tab)
                    sizes[-1].append(n)
    widths = [max(len(t[k]) for t in tabs) for k in range(len(calls))]
    flat = [[v for k, t in enumerate(tab) for v in t + [0] * (widths[k] - len(t))] for tab in tabs]
    bases = [sum(widths[:k]) for k in range(len(calls))]
    return np.array(flat, np.int32), np.array(all_runs, np.int32), bases, np.array(sizes).max(0) * 4


def solution(mesh):
    cps = mesh.shape['cp']
    row_spec = P('dp', ('cp', 'tp'), None)
    head_cols = P(None, 'tp', None)
    n_tp = mesh.shape['tp']

    over_core, over_x, over_both = (('tp', [(t, t ^ k) for t in range(n_tp)]) for k in (1, 2, 3))
    over_y = ('cp', [(i, i ^ 1) for i in range(cps)])

    def layer(x, g_attn, w_q, w_k, w_v, w_o, g_mlp, w_gate, w_up, w_down):
        x_rows = x[0]
        dim = x_rows.shape[1]
        n_run = x_rows.shape[0] // RUN
        piece = 2 * x_rows.shape[0]
        t_id, y_id = lax.axis_index('tp'), lax.axis_index('cp')
        np_tab, np_runs, bases, work = work_tables(cps, piece)
        dev = y_id * n_tp + t_id
        tab = lax.dynamic_index_in_dim(jnp.asarray(np_tab), dev, 0, keepdims=False)
        run_pos = lax.dynamic_index_in_dim(jnp.asarray(np_runs), dev, 0, keepdims=False)

        def tied(v, *others):
            return lax.optimization_barrier((v, *others))[0]

        def send(axis_pairs, v):
            return lax.ppermute(v, *axis_pairs)

        ga, gm = g_attn.reshape(1, dim), g_mlp.reshape(1, dim)
        own = list(norm_runs(x_rows, ga, [0]))
        own += norm_runs(x_rows, ga, list(range(1, n_run)), after=own)
        far = [send(over_x, own[j]) for j in range(n_run)]
        mate = [send(over_core, own[j]) for j in range(n_run)]

        w_all = jnp.concatenate([tied(w, own[-1]).reshape(dim, -1) for w in (w_q, w_k, w_v)], axis=1)
        row_pos = run_pos[:, None] + jnp.arange(RUN, dtype=jnp.int32)[None, :]
        tables = rope_tables(tied(row_pos[:2 * n_run], own[-1]))

        q_here, kv_here = qkv(own + mate, w_all, (tables, 0))
        kvs, q_far = [kv_here], []
        far_tables = rope_tables(tied(row_pos[2 * n_run:], kv_here))

        def far_qkv(j, after):
            here = tied(far[j], after)
            rows = [here, send(over_core, here)], w_all, (far_tables, 2 * j)
            if j + 1 < n_run:
                q, kv = qkv(*rows, after=(after,))
            else:
                kv, = qkv(*rows, False, after=(after,))
                q, = qkv(*rows, True, False, after=(kv, gm))
            q_far.append(q)
            kvs.append(kv)
            return kv

        far_qkv(1, far_qkv(0, kv_here))

        wo = w_o.reshape(-1, dim)
        half = wo.shape[0] // 2
        n_piece = 2
        rows = half // n_piece
        wo_c = send(over_core, tied(wo, kvs[-1]))

        tiles = [(0, i) for i in range(2 * n_run)] + [(1, i) for i in PAIR]
        st, *wo_x = flash(tab, [q_here, q_far[0]], tiles, kvs, base=bases[0], work=int(work[0]), cut=wo,
                         n_cut=n_piece)
        wo_x = [send(over_x, w) for w in wo_x]
        far_qkv(3, far_qkv(2, st))
        kvs = kvs + [send(over_y, kv) for kv in kvs]

        os, outs, prev = [], [], q_far[-1]
        wo_a, wo_b = [], []

        def forward_w(p):
            wo_a.append(tied(wo_x[p], prev))
            wo_b.append(send(over_y, wo_a[p]))

        def attend(j):
            held = 2 * n_run + 2 * j
            carried = [j, n_run + j] + ([held, held + 1] if j == 0 else [None, None])
            pair = j % 2
            *o, done = flash(
                tab, [q_here, q_far[j]], [(0, j), (0, n_run + j), (1, 0), (1, 1)], kvs,
                base=bases[1 + j], work=int(work[1 + j]), st=st, st_src=carried, old=os.pop() if pair else None, slots=2,
                after=(prev,))
            if pair:
                o = [o[0], send(over_core, o[1]), send(over_x, o[2]), send(over_both, o[3])]
            os.append(o)
            return done

        def project(i):
            ws = [wo, wo_c, *wo_a, *wo_b]
            blocks = [[(2 + b * n_piece + p, 0, rows) for p in range(n_piece)] for b in PAIR]
            blocks += [[(a, r, half)] for a in PAIR for r in (0, half)]
            got = out_proj(os[i], ws, blocks, 2, x_rows, gm, i, n_run + 1 + i, after=(prev,))
            for y, b in zip(got[::2], got[1::2]):
                outs.append((y, b, send(over_x, b)))
            return got[0]

        last = n_run - 1
        for j in range(last):
            prev = attend(j)
            if j < n_piece:
                forward_w(j)
        prev = project(0)
        prev = attend(last)

        z, sums = None, []

        chunks = [(j, 0, RUN) for j in range(last)] + [(last, 0, RUN // 2), (last, RUN // 2, RUN // 2)]

        def finish(c):
            j, first, _ = chunks[c]
            return sum_rows(z, sums[c], outs[j][0], first, j * RUN + first, n_run * RUN,
                        after=() if prev is z else (prev,))

        for c, (j, first, size) in enumerate(chunks):
            prev, *s_far = mlp(outs[j][1:], first, size, w_gate, w_up, w_down, c, c == n_run, after=(prev,))
            sums.append([prev] + [send(over_x, v) for v in s_far])
            if c == 0:
                prev = project(1)
            elif c < n_run:
                prev = z = finish(c - 1)
        for c in (last, n_run):
            prev = z = finish(c)
        return z[None]

    return jax.shard_map(layer, mesh=mesh,
                         in_specs=(row_spec, P(), head_cols, head_cols, head_cols, P('tp', None, None),
                                   P(), P(None, 'tp'), P(None, 'tp'), P('tp', None)),
                         out_specs=row_spec, check_vma=False)
```

```python
import functools
import math
import jax
import jax.numpy as jnp
import numpy as np
from jax import lax
from jax.experimental import pallas as pl
from jax.experimental.pallas import tpu as pltpu
from jax.sharding import PartitionSpec as P

NORM_EPS = 1e-5
ROPE_THETA = 500000.0
HD = 128
RUN = 256
NEG = -1e30
LOG2E = math.log2(math.e)
DN = (((1,), (0,)), ((), ()))
BF = jnp.bfloat16
F32 = jnp.float32
ANY = pl.BlockSpec(memory_space=pltpu.HBM)


VMEM = 67043328
PAIR = (0, 1)
PARAMS = pltpu.CompilerParams(vmem_limit_bytes=VMEM)


def rope_tables(positions):
    half = HD // 2
    inv_freq = ROPE_THETA ** (-2.0 * jnp.arange(half, dtype=F32) / HD)
    angles = inv_freq[:, None] * positions.astype(F32)[..., None, :]
    return jnp.cos(angles), jnp.sin(angles)


def norm_rows(rows, gain):
    f = rows.astype(F32)
    mean_sq = jnp.mean(f * f, axis=-1, keepdims=True)
    return (f * lax.rsqrt(mean_sq + NORM_EPS) * gain.astype(F32)).astype(BF)


def other_core():
    me = lax.axis_index('tp')
    return {'tp': me + 1 - 2 * lax.rem(me, 2)}


def cost(flops, moved):
    return pl.CostEstimate(flops=flops, transcendentals=0, bytes_accessed=moved)


def ordered(kernel, n_in, after):
    n = len(after)
    return lambda *refs: kernel(*refs[:n_in], *refs[n_in + n:])


def norm_kernel(x_ref, g_ref, *refs, per):
    for k, o_ref in enumerate(refs):
        @pl.when(lax.div(pl.program_id(0), per) == k)
        def _():
            o_ref[:] = norm_rows(x_ref[:], g_ref[:])


def norm_runs(x_rows, gain, runs, after=(), tile=128):
    dim = x_rows.shape[1]
    per = RUN // tile
    n = len(runs)
    return pl.pallas_call(
        ordered(functools.partial(norm_kernel, per=per), 2, after), grid=(n * per,),
        in_specs=[pl.BlockSpec((tile, dim), lambda i: (runs[0] * per + i, 0)), pl.BlockSpec((1, dim), lambda i: (0, 0))]
        + [ANY] * len(after),
        out_specs=[pl.BlockSpec((tile, dim), lambda i, k=k: (jnp.clip(i - k * per, 0, per - 1), 0)) for k in range(n)],
        out_shape=[jax.ShapeDtypeStruct((RUN, dim), BF)] * n,
        name="norm", compiler_params=PARAMS,
        cost_estimate=cost(n * RUN * dim, n * RUN * dim),
    )(x_rows, gain, *after)


def qkv_kernel(*refs, n_in, n_q, group, first, with_q, with_kv):
    a_refs = refs[:n_in]
    w_ref, cos_ref, sin_ref, *outs, a_scr, sem = refs[n_in:]
    q_ref, kv_ref = outs[0], outs[-1]
    n = pl.program_id(0) + first
    heads = w_ref.shape[1] // HD

    @pl.when(n == first)
    def _():
        for k, r in enumerate(a_refs):
            pltpu.make_async_copy(r, a_scr.at[pl.ds(k * RUN, RUN), :], sem.at[k]).start()

    def rope(f, i):
        f = f.astype(BF).astype(F32)
        lo, hi, cos, sin = f[:HD // 2], f[HD // 2:], cos_ref[i], sin_ref[i]
        return jnp.concatenate([lo * cos - hi * sin, hi * cos + lo * sin], axis=0)

    def one(k, carry):
        @pl.when(n == first)
        def _():
            for i in range(group):
                rows = pl.ds(pl.multiple_of((k * group + i) * RUN, RUN), RUN)
                pltpu.make_async_copy(a_scr.at[rows, :], a_scr.at[rows, :], sem.at[k * group + i]).wait()

        runs = [k * group + i for i in range(group)]

        def products():
            return [jnp.dot(a_scr[pl.ds(pl.multiple_of(run * RUN, RUN), RUN), :], w_ref[:], preferred_element_type=F32)
                    for run in runs]

        if with_q:
            @pl.when(n < n_q)
            def _():
                for run, r in zip(runs, products()):
                    for h in range(heads):
                        cols = slice(h * HD, (h + 1) * HD)
                        q_ref[run, cols, :] = rope(r[:, cols].T, run).astype(BF)

        if with_kv:
            @pl.when(n == n_q)
            def _():
                for run, r in zip(runs, products()):
                    for h in range(heads // 2):
                        cols, past = slice(h * HD, (h + 1) * HD), heads // 2 * HD
                        kv_ref[run, 0, :, cols] = rope(r[:, cols].T, run).T.astype(BF)
                        kv_ref[run, 1, cols, :] = r[:, past + h * HD:past + (h + 1) * HD].T.astype(BF)
        return carry

    lax.fori_loop(0, n_in // group, one, 0)


def qkv(rows, w_all, tables, with_q=True, with_kv=True, after=()):
    n_in = len(rows)
    dim = w_all.shape[0]
    tn = 512
    n_q = w_all.shape[1] // tn - 1
    (cos, sin), first_run = tables
    group = 2
    at = first_run // n_in
    start = 0 if with_q else n_q
    kv_shape = (n_in, 2, RUN, RUN)
    tab = pl.BlockSpec((n_in, HD // 2, RUN), lambda n: (at, 0, 0))
    return pl.pallas_call(
        ordered(functools.partial(qkv_kernel, n_in=n_in, n_q=n_q, group=group, first=start, with_q=with_q, with_kv=with_kv),
                n_in + 3, after),
        grid=(n_q * with_q + with_kv,),
        in_specs=[ANY] * n_in + [pl.BlockSpec((dim, tn), lambda n: (0, n + start)), tab, tab] + [ANY] * len(after),
        out_specs=[pl.BlockSpec((n_in, tn, RUN), lambda n: (0, jnp.minimum(n, n_q - 1), 0))] * with_q
        + [pl.BlockSpec(kv_shape, lambda n: (0,) * len(kv_shape))] * with_kv,
        out_shape=[jax.ShapeDtypeStruct((n_in, n_q * tn, RUN), BF)] * with_q + [jax.ShapeDtypeStruct(kv_shape, BF)] * with_kv,
        scratch_shapes=[pltpu.VMEM((n_in * RUN, dim), BF), pltpu.SemaphoreType.DMA((n_in,))],
        name="qkv", compiler_params=PARAMS,
        cost_estimate=cost(2 * n_in * RUN * w_all.size, 2 * w_all.size),
    )(*rows, w_all, cos, sin, *after)


BLK = 11
LAST, FIRST, CARRY = 16, 32, 64
ST = HD + 16


def flash_kernel(tab_ref, *refs, q_src, kv_src, n_q, n_kv, st_src, n_st, n_old, n_cut, slot, base, G, n_tiles, n_heads, final):
    qs, kvs, sts = refs[:n_q], refs[n_q:n_q + n_kv], refs[n_q + n_kv:n_q + n_kv + n_st]
    n_out = n_tiles + 1 if final else 1 + n_cut
    at = n_q + n_kv + n_st + n_old
    outs = refs[at:at + n_out]
    q_scr, kv_scr, o_scr, st_scr, s_scr, mb_scr, acc_scr, m_scr, l_scr, q_sem, kv_sem, o_sem, st_sem = refs[at + n_out:][:13]
    if n_cut:
        cut_ref, (cut_scr, cut_sem) = refs[at - 1], refs[-2:]
    T = RUN
    c = (HD ** -0.5) * LOG2E
    n_blocks = tab_ref[base]
    carried = base + 1
    row0 = carried + n_tiles
    null = len(kv_src)

    q_copies = [pltpu.make_async_copy(qs[a].at[i], q_scr.at[t], q_sem.at[t]) for t, (a, i) in enumerate(q_src)]
    kv_copies = [pltpu.make_async_copy(kvs[a].at[i], kv_scr.at[r], kv_sem.at[r]) for r, (a, i) in enumerate(kv_src)]

    def load_state(t):
        if st_src[t] is not None:
            @pl.when(tab_ref[carried + t] != 0)
            def _():
                pltpu.make_async_copy(sts[0].at[st_src[t]], st_scr.at[t], st_sem.at[t]).start()

    q_copies[0].start()
    for cp in kv_copies[:4]:
        cp.start()
    load_state(0)
    for cp in kv_copies[4:]:
        cp.start()
    for t in range(1, n_tiles):
        q_copies[t].start()
        load_state(t)
    kv_scr[null, 1] = jnp.zeros((RUN, RUN), BF)
    if n_cut:
        cut_in = pltpu.make_async_copy(cut_ref.at[pl.ds(lax.axis_index('cp') * cut_scr.shape[0], cut_scr.shape[0]), :], cut_scr,
                                       cut_sem)
        part = cut_scr.shape[0] // n_cut
        cut_out = [pltpu.make_async_copy(cut_scr.at[pl.ds(k * part, part), :], outs[1 + k], cut_sem) for k in range(n_cut)]
        cut_in.start()

    def block(i):
        g = lax.div(i, n_blocks)
        return row0 + BLK * (i - g * n_blocks), g

    def arrived(have, need):
        def one(r, carry):
            pltpu.make_async_copy(kv_scr.at[r], kv_scr.at[r], kv_sem.at[r]).wait()
            return carry

        lax.fori_loop(have, need, one, 0)
        return jnp.maximum(have, need)

    def put(s, h, k):
        s_scr[h, pl.ds(k * RUN, RUN), :] = s
        mb_scr[h, k] = jnp.max(s.reshape(RUN // 8, 8, T), axis=0)

    def stage_a(row, g, h):
        col = pl.multiple_of(g * HD, HD)
        qt = q_scr[tab_ref[row], pl.ds(pl.multiple_of((g * G + h) * HD, HD), HD), :]
        for k in range(4):
            put(lax.dot_general(kv_scr[tab_ref[row + 3 + k], 0, :, pl.ds(col, HD)], qt, DN, preferred_element_type=F32), h, k)

    def stage_b(row, g, h):
        col = pl.multiple_of(g * HD, HD)
        m_prev = m_scr[h]
        mb = jnp.maximum(jnp.maximum(mb_scr[h, 0], mb_scr[h, 1]), jnp.maximum(mb_scr[h, 2], mb_scr[h, 3]))
        for r in (4, 2, 1):
            mb = jnp.maximum(mb, pltpu.roll(mb, r, 0))
        m_new = jnp.maximum(m_prev, mb)
        m_scr[h] = m_new
        m_c = m_new * c
        alpha = jnp.exp2(m_prev * c - m_c)
        l, pv = l_scr[h] * alpha, None
        for k in range(4):
            run = tab_ref[row + 7 + k]
            p = jnp.exp2(s_scr[h, k * RUN:(k + 1) * RUN].reshape(RUN // 8, 8, T) * c - m_c[None])
            l = l + jnp.sum(p, axis=0) * jnp.where(run < 0, 0.0, 1.0)
            d = lax.dot_general(kv_scr[jnp.where(run < 0, null, run), 1, pl.ds(col, HD), :], p.reshape(RUN, T).astype(BF), DN,
                                preferred_element_type=F32)
            pv = d if pv is None else pv + d
        l_scr[h] = l
        acc_scr[h] = (acc_scr[h].reshape(HD // 8, 8, T) * alpha[None]).reshape(HD, T) + pv

    def mask_runs(flags):
        seen = lax.broadcasted_iota(jnp.int32, (RUN, T), 0) <= lax.broadcasted_iota(jnp.int32, (RUN, T), 1)

        def one(k, carry):
            @pl.when((lax.shift_right_logical(flags, k) & 1) != 0)
            def _():
                rows = pl.multiple_of(k * RUN, RUN)
                for h in range(G):
                    put(jnp.where(seen, s_scr[h, pl.ds(rows, RUN), :], NEG), h, k)

            return carry

        lax.fori_loop(0, 4, one, 0)

    def finish(tile, g, get):
        for h in range(G):
            acc, l = get(h)
            o_scr[tile, :, pl.ds(pl.multiple_of((g * G + h) * HD, HD), HD)] = (acc / jnp.sum(l, axis=0, keepdims=True)).T.astype(BF)

        @pl.when(g == n_heads - 1)
        def _():
            for k in range(n_tiles):
                @pl.when(tile == k)
                def _():
                    pltpu.make_async_copy(o_scr.at[k], outs[k].at[slot], o_sem.at[k]).start()

    if final and n_st:
        def idle(i, carry):
            tile, g = lax.div(i, n_heads), lax.rem(i, n_heads)

            @pl.when(tab_ref[carried + tile] == 2)
            def _():
                @pl.when(g == 0)
                def _():
                    pltpu.make_async_copy(q_scr.at[tile], q_scr.at[tile], q_sem.at[tile]).wait()
                    pltpu.make_async_copy(st_scr.at[tile], st_scr.at[tile], st_sem.at[tile]).wait()

                finish(tile, g, lambda h: (st_scr[tile, g, h, :HD, :], st_scr[tile, g, h, HD + 8:, :]))

            return carry

        lax.fori_loop(0, n_tiles * n_heads, idle, 0)

    def query(row):
        t = tab_ref[row]
        pltpu.make_async_copy(q_scr.at[t], q_scr.at[t], q_sem.at[t]).wait()

    row, g = block(0)
    query(row)
    have = arrived(0, tab_ref[row + 2])
    for h in range(G):
        stage_a(row, g, h)

    def body(i, have):
        row, g = block(i)
        nrow, ng = block(jnp.minimum(i + 1, n_heads * n_blocks - 1))
        have = arrived(have, tab_ref[nrow + 2])
        flags = tab_ref[row + 1]
        tile = tab_ref[row]

        @pl.when((i + 1 < n_blocks) & ((tab_ref[nrow + 1] & FIRST) != 0))
        def _():
            query(nrow)

        @pl.when((flags & (FIRST | CARRY)) == FIRST)
        def _():
            acc_scr[:] = jnp.zeros_like(acc_scr)
            l_scr[:] = jnp.zeros_like(l_scr)
            m_scr[:] = jnp.full_like(m_scr, NEG)

        if n_st:
            @pl.when((flags & (FIRST | CARRY)) == (FIRST | CARRY))
            def _():
                @pl.when(g == 0)
                def _():
                    pltpu.make_async_copy(st_scr.at[tile], st_scr.at[tile], st_sem.at[tile]).wait()

                for h in range(G):
                    acc_scr[h] = st_scr[tile, g, h, :HD, :]
                    m_scr[h] = st_scr[tile, g, h, HD:HD + 8, :]
                    l_scr[h] = st_scr[tile, g, h, HD + 8:, :]

        if n_cut:
            @pl.when(i == n_blocks)
            def _():
                cut_in.wait()
                for cp in cut_out:
                    cp.start()

        @pl.when((flags & 15) != 0)
        def _():
            mask_runs(flags)

        for h in range(G):
            stage_b(row, g, h)
            stage_a(nrow, ng, h)

        @pl.when((flags & LAST) != 0)
        def _():
            if final:
                finish(tile, g, lambda h: (acc_scr[h], l_scr[h]))
            else:
                for h in range(G):
                    st_scr[tile, g, h, :HD, :] = acc_scr[h]
                    st_scr[tile, g, h, HD:HD + 8, :] = m_scr[h]
                    st_scr[tile, g, h, HD + 8:, :] = l_scr[h]

                @pl.when(g == n_heads - 1)
                def _():
                    pltpu.make_async_copy(st_scr.at[tile], outs[0].at[tile], o_sem.at[tile]).start()

        return have

    have = lax.fori_loop(0, n_heads * n_blocks, body, have)
    arrived(have, len(kv_src))
    if final:
        for k in range(n_tiles):
            pltpu.make_async_copy(o_scr.at[k], outs[k].at[slot], o_sem.at[k]).wait()
    else:
        def wait_out(i, carry):
            row = row0 + BLK * i

            @pl.when((tab_ref[row + 1] & LAST) != 0)
            def _():
                t = tab_ref[row]
                pltpu.make_async_copy(st_scr.at[t], st_scr.at[t], o_sem.at[t]).wait()

            return carry

        lax.fori_loop(0, n_blocks, wait_out, 0)
        for cp in cut_out:
            cp.wait()


def flash(tab, qs, q_src, kvs, *, base, work, st=None, st_src=None, old=None, cut=None, n_cut=0, slots=1, after=()):
    nq = qs[0].shape[1]
    n_heads = 2
    G = nq // HD // n_heads
    n_tiles = len(q_src)
    final = cut is None
    kv_src = [(a, i) for a, kv in enumerate(kvs) for i in range(kv.shape[0])]
    n_runs = len(kv_src)
    sts = () if st is None else (st,)
    old = old or ()
    more = (*old, *(() if final else (cut,)))
    n_in = 1 + len(qs) + len(kvs) + len(sts) + len(more)
    state = (n_heads, G, ST, RUN)
    has_st = not final or sts
    if final:
        out_shape = [jax.ShapeDtypeStruct((slots, RUN, nq), BF)] * n_tiles + [jax.ShapeDtypeStruct((8, HD), F32)]
        scratch = []
    else:
        half = cut.shape[0] // 2
        out_shape = [jax.ShapeDtypeStruct((n_tiles, *state), F32)]
        out_shape += [jax.ShapeDtypeStruct((half // n_cut, cut.shape[1]), BF)] * n_cut
        scratch = [pltpu.VMEM((half, cut.shape[1]), BF), pltpu.SemaphoreType.DMA]
    return pl.pallas_call(
        ordered(functools.partial(flash_kernel, q_src=q_src, kv_src=kv_src, n_q=len(qs), n_kv=len(kvs),
                                  st_src=st_src or [None] * n_tiles, n_st=len(sts), n_old=len(more), n_cut=n_cut,
                                  slot=slots - 1 if old else 0, base=base, G=G, n_tiles=n_tiles, n_heads=n_heads, final=final),
                n_in, after),
        grid_spec=pltpu.PrefetchScalarGridSpec(
            num_scalar_prefetch=1, grid=(),
            in_specs=[ANY] * (n_in - 1 + len(after)),
            out_specs=[ANY] * len(out_shape),
            scratch_shapes=[pltpu.VMEM((n_tiles, nq, RUN), BF),
                            pltpu.VMEM((n_runs + 1, 2, RUN, RUN), BF),
                            pltpu.VMEM((n_tiles if final else 1, RUN, nq), BF),
                            pltpu.VMEM((n_tiles if has_st else 1, *state), F32),
                            pltpu.VMEM((G, 4 * RUN, RUN), F32),
                            pltpu.VMEM((G, 4, 8, RUN), F32),
                            pltpu.VMEM((G, HD, RUN), F32),
                            pltpu.VMEM((G, 8, RUN), F32),
                            pltpu.VMEM((G, 8, RUN), F32),
                            pltpu.SemaphoreType.DMA((n_tiles,)),
                            pltpu.SemaphoreType.DMA((n_runs,)),
                            pltpu.SemaphoreType.DMA((n_tiles,)),
                            pltpu.SemaphoreType.DMA((n_tiles,)), *scratch]),
        out_shape=out_shape,
        input_output_aliases={n_in - len(old) + k: k for k in range(len(old))},
        name="flash" if final else "flash_part",
        compiler_params=pltpu.CompilerParams(
            vmem_limit_bytes=VMEM),
        cost_estimate=cost(8 * work * RUN * RUN * nq, n_runs * RUN * nq),
    )(tab, *qs, *kvs, *sts, *more, *after)


def out_kernel(*refs, blocks, n_w, n_run, at, n_shared):
    n_o, n_out = 4, 2 * n_run
    o_refs, w_refs, x_ref, g_ref = refs[:n_o], refs[n_o:n_o + n_w], refs[n_o + n_w], refs[n_o + n_w + 1]
    outs = refs[n_o + n_w + 2:n_o + n_w + 2 + n_out]
    o_scr, w_scr, x_scr, acc_scr, o_sem, w_sem, x_sem, out_sem, sent_sem = refs[n_o + n_w + 2 + n_out:]
    width = o_refs[0].shape[-1]
    half = width // 2
    n_slots = w_scr.shape[0] - n_shared
    n_local = len(blocks)
    mate = other_core()
    barrier = pltpu.get_barrier_semaphore()
    pl.semaphore_signal(barrier, inc=1, device_id=mate, device_id_type=pl.DeviceIdType.MESH)

    def fetch(k):
        for i, pieces in enumerate(blocks):
            @pl.when(k == i)
            def _():
                to = 0
                for a, r0, n in pieces:
                    pltpu.make_async_copy(w_refs[a].at[pl.ds(r0, n), :], w_scr.at[i % n_slots, pl.ds(to, n), :],
                                          w_sem.at[i % n_slots]).start()
                    to += n

    mine = lax.axis_index('cp')
    loads = [[] for _ in range(n_local + n_shared)]
    for i in range(n_run):
        rows = pl.ds(i * RUN, RUN)
        for k in range(4):
            src = o_refs[k].at[i]
            if k < 2:
                loads[2 * k].append((src, o_scr.at[rows, pl.ds(k * width, width)]))
            else:
                for p, part in enumerate((mine, 1 - mine)):
                    loads[2 * k + p].append((src.at[:, pl.ds(pl.multiple_of(part * half, half), half)],
                                             o_scr.at[rows, pl.ds(k * width + p * half, half)]))
    copies = [[pltpu.make_async_copy(src, dst, o_sem.at[k, i]) for i, (src, dst) in enumerate(ls)] for k, ls in enumerate(loads)]
    x_copy = pltpu.make_async_copy(x_ref.at[pl.ds(at * n_run * RUN, n_run * RUN), :], x_scr, x_sem)
    for cp in copies[0]:
        cp.start()
    for i in range(n_slots - 1):
        fetch(jnp.int32(i))
    shared = []
    pl.semaphore_wait(barrier, 1)
    for b in range(n_shared):
        to = 0
        for a, r0, n in blocks[b - n_shared]:
            shared.append(pltpu.make_async_remote_copy(
                src_ref=w_refs[a].at[pl.ds(r0, n), :], dst_ref=w_scr.at[n_slots + b, pl.ds(to, n), :],
                send_sem=sent_sem.at[len(shared)], recv_sem=w_sem.at[n_slots + b], device_id=mate,
                device_id_type=pl.DeviceIdType.MESH))
            shared[-1].start()
            to += n
    for ls in copies[1:]:
        for cp in ls:
            cp.start()
    x_copy.start()
    acc_scr[:] = jnp.zeros_like(acc_scr)

    def one(k, carry):
        fetch(k + n_slots - 1)
        for i, ls in enumerate(copies):
            if ls:
                @pl.when(k == i)
                def _():
                    for cp in ls:
                        cp.wait()
        slot = jnp.where(k < n_local, lax.rem(k, n_slots), k - n_local + n_slots)
        pltpu.make_async_copy(w_scr.at[slot], w_scr.at[slot], w_sem.at[slot]).wait()
        acc_scr[:] += jnp.dot(o_scr[:, pl.ds(pl.multiple_of(k * half, half), half)], w_scr[slot], preferred_element_type=F32)
        return carry

    lax.fori_loop(0, len(loads), one, 0)
    x_copy.wait()

    strip = 64

    def one_strip(r, carry):
        rows = pl.ds(pl.multiple_of(r * strip, strip), strip)
        y = (x_scr[rows, :].astype(F32) + acc_scr[rows, :].astype(BF).astype(F32)).astype(BF)
        x_scr[rows, :] = y
        o_scr[rows, :] = norm_rows(y, g_ref[:])
        return carry

    stores, part = [], RUN // 2
    for i in range(n_run):
        for h in PAIR:
            r0 = i * RUN + h * part
            lax.fori_loop(r0 // strip, (r0 + part) // strip, one_strip, 0)
            for k, scr in enumerate((x_scr, o_scr)):
                stores.append(pltpu.make_async_copy(scr.at[pl.ds(r0, part), :], outs[2 * i + k].at[pl.ds(h * part, part), :],
                                                    out_sem.at[len(stores)]))
                stores[-1].start()
    for cp in stores:
        cp.wait()
    for cp in shared:
        cp.wait_send()


def out_proj(os, ws, blocks, n_shared, x_rows, gain, at, call, after=()):
    dim = x_rows.shape[1]
    n_run, _, width = os[0].shape
    rows = n_run * RUN
    return pl.pallas_call(
        ordered(functools.partial(out_kernel, blocks=blocks, n_w=len(ws), n_run=n_run, at=at, n_shared=n_shared),
                len(os) + len(ws) + 2, after),
        grid=(1,),
        in_specs=[ANY] * (len(os) + len(ws) + 1) + [pl.BlockSpec((1, dim), lambda i: (0, 0))] + [ANY] * len(after),
        out_specs=[ANY] * (2 * n_run),
        out_shape=[jax.ShapeDtypeStruct((RUN, dim), BF)] * (2 * n_run),
        scratch_shapes=[pltpu.VMEM((rows, 4 * width), BF), pltpu.VMEM((3 + n_shared, width // 2, dim), BF), pltpu.VMEM((rows, dim), BF),
                        pltpu.VMEM((rows, dim), F32), pltpu.SemaphoreType.DMA((len(blocks) + n_shared, 2 * n_run)),
                        pltpu.SemaphoreType.DMA((3 + n_shared,)), pltpu.SemaphoreType.DMA, pltpu.SemaphoreType.DMA((4 * n_run,)),
                        pltpu.SemaphoreType.DMA((len(ws),))],
        name="outp",
        compiler_params=pltpu.CompilerParams(vmem_limit_bytes=VMEM, collective_id=call, has_side_effects=True),
        cost_estimate=cost(8 * rows * width * dim, 8 * width * dim),
    )(*os, *ws, x_rows, gain, *after)


def mlp_kernel(*refs, n_in, first, rb, tn, td, nk, nd, cross):
    b_refs = refs[:n_in]
    wg_ref, wu_ref, wd_ref, *outs = refs[n_in:n_in + (4 if cross else 5)]
    (b_scr, u_scr, w_scr, d_scr, keep_scr, out_scr, in_scr, b_sem, w_sem, d_sem, out_sem, in_sem,
     rows_sem, *more) = refs[n_in + (4 if cross else 5):]
    i = pl.program_id(0)
    mate = other_core()
    peers = [mate]
    if cross:
        own_scr, far_scr, back_scr, far_sem, back_sem = more
        half_tp = lax.axis_size('tp') // 2
        peers.append({'tp': lax.rem(lax.axis_index('tp') + half_tp, 2 * half_tp)})
    barrier = pltpu.get_barrier_semaphore()

    def fetch(j):
        @pl.when(j < nk)
        def _():
            slot, cols = lax.rem(j, 2), pl.ds(pl.multiple_of(j * tn, tn), tn)
            for k, w in enumerate((wg_ref, wu_ref)):
                pltpu.make_async_copy(w.at[:, cols], w_scr.at[slot, k], w_sem.at[slot]).start()

        @pl.when((j >= nk) & (j < nk + nd))
        def _():
            n, slot = j - nk, lax.rem(j - nk, 2)
            pltpu.make_async_copy(wd_ref.at[:, pl.ds(pl.multiple_of(n * td, td), td)], d_scr.at[slot], d_sem.at[slot]).start()

    def gated(rows, cols, slot):
        b = b_scr[rows, :]
        gate = jnp.dot(b, w_scr[slot, 0], preferred_element_type=F32)
        up = jnp.dot(b, w_scr[slot, 1], preferred_element_type=F32)
        u_scr[rows, cols] = (jax.nn.silu(gate) * up).astype(BF)

    def to_mate(n):
        return pltpu.make_async_remote_copy(src_ref=out_scr.at[n], dst_ref=in_scr.at[n], send_sem=out_sem.at[n],
                                            recv_sem=in_sem.at[n], device_id=mate, device_id_type=pl.DeviceIdType.MESH)

    def to_far(n):
        return pltpu.make_async_remote_copy(src_ref=far_scr.at[n], dst_ref=back_scr.at[n], send_sem=far_sem.at[n],
                                            recv_sem=back_sem.at[n], device_id=peers[-1], device_id_type=pl.DeviceIdType.MESH)

    def rows_to_mate(n):
        return pltpu.make_async_remote_copy(
            src_ref=b_refs[n].at[pl.ds(first, rb), :], dst_ref=b_scr.at[pl.ds((n_in + n) * rb, rb), :],
            send_sem=rows_sem.at[n], recv_sem=b_sem.at[n_in + n], device_id=mate, device_id_type=pl.DeviceIdType.MESH)

    @pl.when(i == 0)
    def _():
        copies = [pltpu.make_async_copy(r.at[pl.ds(first, rb), :], b_scr.at[pl.ds(k * rb, rb), :], b_sem.at[k])
                  for k, r in enumerate(b_refs)]
        for peer in peers:
            pl.semaphore_signal(barrier, inc=1, device_id=peer, device_id_type=pl.DeviceIdType.MESH)
        copies[0].start()
        fetch(i)
        for cp in copies[1:]:
            cp.start()
        pl.semaphore_wait(barrier, len(peers))
        for n in range(n_in):
            rows_to_mate(n).start()

    fetch(i + 1)

    @pl.when(i < nk)
    def _():
        slot = lax.rem(i, 2)
        pltpu.make_async_copy(w_scr.at[slot], w_scr.at[slot], w_sem.at[slot]).wait()

    @pl.when(i == 0)
    def _():
        def one(k, carry):
            rows = pl.ds(pl.multiple_of(k * rb, rb), rb)
            pltpu.make_async_copy(b_scr.at[rows, :], b_scr.at[rows, :], b_sem.at[k]).wait()
            gated(rows, pl.ds(0, tn), 0)
            return carry

        lax.fori_loop(0, 2 * n_in, one, 0)

    @pl.when((i > 0) & (i < nk))
    def _():
        gated(slice(None), pl.ds(pl.multiple_of(i * tn, tn), tn), lax.rem(i, 2))

    n = i - nk

    @pl.when((n > 0) & (n <= nd))
    def _():
        to_mate(n - 1).start()

    if cross:
        @pl.when((n > 1) & (n <= nd + 1))
        def _():
            to_far(n - 2).start()

    @pl.when((n >= 0) & (n < nd))
    def _():
        slot = lax.rem(n, 2)
        pltpu.make_async_copy(d_scr.at[slot], d_scr.at[slot], d_sem.at[slot]).wait()
        d = jnp.dot(u_scr[:], d_scr[slot], preferred_element_type=F32).astype(BF)
        half = d.shape[0] // 2
        keep_scr[slot] = d[:half]
        out_scr[n] = d[half:]

    @pl.when((n > 0) & (n <= nd))
    def _():
        m = n - 1
        to_mate(m).wait_recv()
        total = (keep_scr[lax.rem(m, 2)].astype(F32) + in_scr[m].astype(F32)).astype(BF)
        size = total.shape[0] // 2
        if cross:
            own_scr[m] = total[:size]
            far_scr[m] = total[size:]
        else:
            outs[0][:] = total[:size]
            outs[1][:] = total[size:]

    if cross:
        @pl.when(n > nd)
        def _():
            m = n - nd - 1
            to_far(m).wait_recv()
            outs[0][:] = (own_scr[m].astype(F32) + back_scr[m].astype(F32)).astype(BF)

    @pl.when(i == pl.num_programs(0) - 1)
    def _():
        def sent(k, carry):
            to_mate(k).wait_send()
            if cross:
                to_far(k).wait_send()
            return carry

        lax.fori_loop(0, nd, sent, 0)
        for k in range(n_in):
            rows_to_mate(k).wait_send()


def mlp(bs, first, rb, wg, wu, wd, call, cross=False, after=()):
    dim = bs[0].shape[1]
    rows = 2 * rb * len(bs)
    ffn = wg.shape[1]
    td = 512
    tn = td if rows <= td else td // 2
    nk, nd = ffn // tn, dim // td
    half = rows // 2
    lag = nk + 1 + nd * cross
    n_out = 1 if cross else 2
    tiles = pltpu.VMEM((nd, half, td), BF)
    sem = pltpu.SemaphoreType.DMA
    return pl.pallas_call(
        ordered(functools.partial(mlp_kernel, n_in=len(bs), first=first, rb=rb, tn=tn, td=td, nk=nk, nd=nd, cross=cross),
                len(bs) + 3, after),
        grid=(nd + lag,),
        in_specs=[ANY] * (len(bs) + 3 + len(after)),
        out_specs=[pl.BlockSpec((rb, td), lambda i: (0, jnp.clip(i - lag, 0, nd - 1)))] * n_out,
        out_shape=[jax.ShapeDtypeStruct((rb, dim), BF)] * n_out,
        scratch_shapes=[pltpu.VMEM((rows, dim), BF), pltpu.VMEM((rows, ffn), BF), pltpu.VMEM((2, 2, dim, tn), BF),
                        pltpu.VMEM((2, ffn, td), BF), pltpu.VMEM((2, half, td), BF), tiles, tiles]
        + [sem((n,)) for n in (2 * len(bs), 2, 2, nd, nd, len(bs))]
        + ([pltpu.VMEM((nd, rb, td), BF)] * 3 + [sem((nd,))] * 2 if cross else []),
        name="mlp",
        compiler_params=pltpu.CompilerParams(vmem_limit_bytes=VMEM, collective_id=call, has_side_effects=True),
        cost_estimate=cost(6 * rows * dim * ffn, 6 * dim * ffn),
    )(*bs, wg, wu, wd, *after)


def sum_kernel(*refs, n):
    *parts, y_ref, z_ref = refs[-2 - n:]
    total = sum(p[:].astype(F32) for p in parts).astype(BF)
    z_ref[:] = (y_ref[:].astype(F32) + total.astype(F32)).astype(BF)


def sum_rows(z, parts, y, y_first, first, total, after=(), tile=64):
    rows, dim = parts[0].shape
    at = lambda r0: pl.BlockSpec((tile, dim), lambda i: (r0 // tile + i, 0))
    prev = () if z is None else (z,)
    n = len(parts)
    return pl.pallas_call(
        ordered(functools.partial(sum_kernel, n=n), len(prev) + n + 1, after), grid=(rows // tile,),
        in_specs=[ANY] * len(prev) + [at(0)] * n + [at(y_first)] + [ANY] * len(after),
        out_specs=at(first),
        out_shape=jax.ShapeDtypeStruct((total, dim), BF),
        input_output_aliases={0: 0} if prev else {},
        name="zsum", compiler_params=PARAMS,
        cost_estimate=cost(rows * dim, rows * dim),
    )(*prev, *parts, y, *after)


def run_positions(xi, ci, y, cps, piece):
    def start(x, c):
        return (y if x == 0 else 2 * cps - 1 - y) * piece + c * (piece // 2)

    per = piece // 2 // RUN
    out = [start(xi, ci) + RUN * j for j in range(per)] + [start(xi, 1 - ci) + RUN * j for j in range(per)]
    for j in range(per):
        out += [start(1 - xi, ci) + RUN * j, start(1 - xi, 1 - ci) + RUN * j]
    return out


def block_list(tile, ids, diag):
    own = [] if diag is None else [diag]
    n_tail = (len(ids) + len(own)) % 4 or 4
    n_tail -= len(own)
    head, tail = ids[:len(ids) - n_tail], own + ids[len(ids) - n_tail:]
    blocks = [[0, head[i:i + 4], head[i:i + 4]] for i in range(0, len(head), 4)]
    fill = 4 - len(tail)
    keys = tail + [ids[-1] if ids else diag] * fill
    blocks.append([sum(1 << k for k, r in enumerate(keys) if r == diag), keys, tail + [-1] * fill])
    blocks[-1][0] |= LAST
    blocks[0][0] |= FIRST
    return [[tile, flags, 0] + keys + values for flags, keys, values in blocks]


def call_table(tiles, pairs, carry, idle):
    rows, most = [], 0
    carry = [c if pairs[t][0] or pairs[t][1] else idle for t, c in enumerate(carry)]
    for t, tile in enumerate(tiles):
        ids, own = pairs[t]
        if ids or own:
            mine = block_list(t, ids, tile if own else None)
            mine[0][1] |= CARRY if carry[t] else 0
            rows += mine
    for row in rows:
        most = max(most, max(row[3:7]) + 1)
        row[2] = most
    return [len(rows)] + carry + [v for row in rows for v in row], len(rows)


def work_tables(cps, piece):
    per = piece // 2 // RUN
    early, more = 2 * per + 2, 2 * per + 4
    stage = lambda r: 0 if r < early else 1
    soon_pair = lambda r, t: r < early and t < early or r < more and t in (0, 1, per, per + 1)
    calls = [(0, list(range(early)))]
    calls += [(1, [j, per + j, 2 * per + 2 * j, 2 * per + 2 * j + 1]) for j in range(per)]
    tabs, all_runs, sizes = [], [], []
    for y in range(cps):
        for xi in range(2):
            for ci in range(2):
                mine = run_positions(xi, ci, y, cps, piece)
                pos = mine + run_positions(xi, ci, 1 - y, cps, piece)
                all_runs.append(mine)
                tabs.append([])
                sizes.append([])
                for now, tiles in calls:
                    pairs, carry = [], []
                    for t in tiles:
                        seen = [r for r in range(len(pos)) if pos[r] < pos[t]]
                        when = {r: 0 if soon_pair(r, t) else 1 for r in seen}
                        late = list(when.values()).count(1) + stage(t)
                        soon = len(seen) + 1 - late
                        if late and soon % 4 <= -late % 4:
                            for r in [r for r in seen if not when[r]][:soon % 4]:
                                when[r] = 1
                        pairs.append(([r for r in seen if when[r] == now], stage(t) == now))
                        carry.append(int(stage(t) < now))
                    tab, n = call_table(tiles, pairs, carry, 2 if now == 1 else 0)
                    tabs[-1].append(tab)
                    sizes[-1].append(n)
    widths = [max(len(t[k]) for t in tabs) for k in range(len(calls))]
    flat = [[v for k, t in enumerate(tab) for v in t + [0] * (widths[k] - len(t))] for tab in tabs]
    bases = [sum(widths[:k]) for k in range(len(calls))]
    return np.array(flat, np.int32), np.array(all_runs, np.int32), bases, np.array(sizes).max(0) * 4


def solution(mesh):
    cps = mesh.shape['cp']
    row_spec = P('dp', ('cp', 'tp'), None)
    head_cols = P(None, 'tp', None)
    n_tp = mesh.shape['tp']

    over_core, over_x, over_both = (('tp', [(t, t ^ k) for t in range(n_tp)]) for k in (1, 2, 3))
    over_y = ('cp', [(i, i ^ 1) for i in range(cps)])

    def layer(x, g_attn, w_q, w_k, w_v, w_o, g_mlp, w_gate, w_up, w_down):
        x_rows = x[0]
        dim = x_rows.shape[1]
        n_run = x_rows.shape[0] // RUN
        piece = 2 * x_rows.shape[0]
        t_id, y_id = lax.axis_index('tp'), lax.axis_index('cp')
        np_tab, np_runs, bases, work = work_tables(cps, piece)
        dev = y_id * n_tp + t_id
        tab = lax.dynamic_index_in_dim(jnp.asarray(np_tab), dev, 0, keepdims=False)
        run_pos = lax.dynamic_index_in_dim(jnp.asarray(np_runs), dev, 0, keepdims=False)

        def tied(v, *others):
            return lax.optimization_barrier((v, *others))[0]

        def send(axis_pairs, v):
            return lax.ppermute(v, *axis_pairs)

        ga, gm = g_attn.reshape(1, dim), g_mlp.reshape(1, dim)
        own = list(norm_runs(x_rows, ga, [0]))
        own += norm_runs(x_rows, ga, list(range(1, n_run)), after=own)
        far = [send(over_x, own[j]) for j in range(n_run)]
        mate = [send(over_core, own[j]) for j in range(n_run)]

        w_all = jnp.concatenate([tied(w, own[-1]).reshape(dim, -1) for w in (w_q, w_k, w_v)], axis=1)
        row_pos = run_pos[:, None] + jnp.arange(RUN, dtype=jnp.int32)[None, :]
        tables = rope_tables(tied(row_pos[:2 * n_run], own[-1]))

        q_here, kv_here = qkv(own + mate, w_all, (tables, 0))
        kvs, q_far = [kv_here], []
        far_tables = rope_tables(tied(row_pos[2 * n_run:], kv_here))

        def far_qkv(j, after):
            here = tied(far[j], after)
            rows = [here, send(over_core, here)], w_all, (far_tables, 2 * j)
            if j + 1 < n_run:
                q, kv = qkv(*rows, after=(after,))
            else:
                kv, = qkv(*rows, False, after=(after,))
                q, = qkv(*rows, True, False, after=(kv, gm))
            q_far.append(q)
            kvs.append(kv)
            return kv

        far_qkv(1, far_qkv(0, kv_here))

        wo = w_o.reshape(-1, dim)
        half = wo.shape[0] // 2
        n_piece = 2
        rows = half // n_piece
        wo_c = send(over_core, tied(wo, kvs[-1]))

        tiles = [(0, i) for i in range(2 * n_run)] + [(1, i) for i in PAIR]
        st, *wo_x = flash(tab, [q_here, q_far[0]], tiles, kvs, base=bases[0], work=int(work[0]), cut=wo,
                         n_cut=n_piece)
        wo_x = [send(over_x, w) for w in wo_x]
        far_qkv(3, far_qkv(2, st))
        kvs = kvs + [send(over_y, kv) for kv in kvs]

        os, outs, prev = [], [], q_far[-1]
        wo_a, wo_b = [], []

        def forward_w(p):
            wo_a.append(tied(wo_x[p], prev))
            wo_b.append(send(over_y, wo_a[p]))

        def attend(j):
            held = 2 * n_run + 2 * j
            carried = [j, n_run + j] + ([held, held + 1] if j == 0 else [None, None])
            pair = j % 2
            *o, done = flash(
                tab, [q_here, q_far[j]], [(0, j), (0, n_run + j), (1, 0), (1, 1)], kvs,
                base=bases[1 + j], work=int(work[1 + j]), st=st, st_src=carried, old=os.pop() if pair else None, slots=2,
                after=(prev,))
            if pair:
                o = [o[0], send(over_core, o[1]), send(over_x, o[2]), send(over_both, o[3])]
            os.append(o)
            return done

        def project(i):
            ws = [wo, wo_c, *wo_a, *wo_b]
            blocks = [[(a, r, half)] for a in PAIR for r in (0, half)]
            blocks += [[(2 + b * n_piece + p, 0, rows) for p in range(n_piece)] for b in PAIR]
            got = out_proj(os[i], ws, blocks, 2, x_rows, gm, i, n_run + 1 + i, after=(prev,))
            for y, b in zip(got[::2], got[1::2]):
                outs.append((y, b, send(over_x, b)))
            return got[0]

        last = n_run - 1
        for j in range(last):
            prev = attend(j)
            if j < n_piece:
                forward_w(j)
        prev = project(0)
        prev = attend(last)

        z, sums = None, []

        chunks = [(j, 0, RUN) for j in range(last)] + [(last, 0, RUN // 2), (last, RUN // 2, RUN // 2)]

        def finish(c):
            j, first, _ = chunks[c]
            return sum_rows(z, sums[c], outs[j][0], first, j * RUN + first, n_run * RUN,
                        after=() if prev is z else (prev,))

        for c, (j, first, size) in enumerate(chunks):
            prev, *s_far = mlp(outs[j][1:], first, size, w_gate, w_up, w_down, c, c == n_run, after=(prev,))
            sums.append([prev] + [send(over_x, v) for v in s_far])
            if c == 0:
                prev = project(1)
            elif c < n_run:
                prev = z = finish(c - 1)
        for c in (last, n_run):
            prev = z = finish(c)
        return z[None]

    return jax.shard_map(layer, mesh=mesh,
                         in_specs=(row_spec, P(), head_cols, head_cols, head_cols, P('tp', None, None),
                                   P(), P(None, 'tp'), P(None, 'tp'), P('tp', None)),
                         out_specs=row_spec, check_vma=False)
```
